256 devices in a mesh: ep: 256 (over z, y, x, core).
Axes of the slice: x: 4, y: 4, z: 8, core: 2. Of those that a mesh axis runs over, the one named last changes fastest.
Arguments:
- tokens: bfloat16 [8192, 256], P('ep')
- grad_out: bfloat16 [8192, 256], P('ep')
- expert_ids: int32 [8192, 2], P('ep')
- w_gate: bfloat16 [256, 256], replicated
- w_in: bfloat16 [256, 256, 1024], P('ep')
- w_out: bfloat16 [256, 1024, 256], P('ep')
Outputs:
- output 1: bfloat16 [8192, 256], P('ep')
- output 2: bfloat16 [8192, 256], P('ep')
- output 3: float32 [256, 256, 1024], P('ep')
- output 4: float32 [256, 1024, 256], P('ep')
- output 5: float32 [256, 256], replicated
All inputs are finite; a program needn't handle non-finite values.
Results may differ from the reference program's by a relative error of at most 0.00483969.
Values are sent between devices in bfloat16 or wider.
A program may use at most 768 MiB of HBM per device.

```python
import jax
import jax.numpy as jnp
from jax import lax

EXPERTS = 256
TOKENS_DEV = 32
D_MODEL = 256
D_HIDDEN = 1024
HOT_EXPERTS = 3

CAP_ROWS = TOKENS_DEV // 4
ALL_TOKENS = EXPERTS * TOKENS_DEV
CAP_ALL = EXPERTS * CAP_ROWS


def draw_routes(route_key):
    k_perm, k_shift, k_order, k_swap = jax.random.split(route_key, 4)
    n_cold = EXPERTS - HOT_EXPERTS
    cold_choices = 2 * TOKENS_DEV - HOT_EXPERTS * CAP_ROWS
    slot_pos = jnp.arange(2 * TOKENS_DEV)
    hot_rank = jnp.minimum(slot_pos // CAP_ROWS, HOT_EXPERTS - 1)
    cold_block = (jnp.maximum(slot_pos - HOT_EXPERTS * CAP_ROWS, 0) * n_cold) // cold_choices
    shifts = jax.random.randint(k_shift, (EXPERTS, 1), 0, n_cold)
    cold_rank = HOT_EXPERTS + (cold_block[None, :] + shifts) % n_cold
    rank_ids = jnp.where(slot_pos[None, :] < HOT_EXPERTS * CAP_ROWS, hot_rank[None, :], cold_rank)
    expert_perm = jax.random.permutation(k_perm, EXPERTS)
    choice_ids = expert_perm[rank_ids]
    pair_ids = jnp.stack([choice_ids[:, :TOKENS_DEV], choice_ids[:, TOKENS_DEV:]], axis=-1)
    token_perm = jax.random.permutation(k_order, jnp.tile(jnp.arange(TOKENS_DEV), (EXPERTS, 1)), axis=1, independent=True)
    pair_ids = jnp.take_along_axis(pair_ids, token_perm[:, :, None], axis=1)
    swap_bit = jax.random.randint(k_swap, (EXPERTS, TOKENS_DEV, 1), 0, 2)
    pair_ids = jnp.where(swap_bit == 1, pair_ids[:, :, ::-1], pair_ids)
    return pair_ids.reshape(ALL_TOKENS, 2).astype(jnp.int32)


def setup_inputs(seed: int = 0) -> dict:
    rng_key = jax.random.key(seed)
    k_tok, k_grad, k_route, k_gate, k_in, k_out = jax.random.split(rng_key, 6)
    tokens = jax.random.normal(k_tok, (ALL_TOKENS, D_MODEL), jnp.float32).astype(jnp.bfloat16)
    grad_out = jax.random.normal(k_grad, (ALL_TOKENS, D_MODEL), jnp.float32).astype(jnp.bfloat16)
    expert_ids = draw_routes(k_route)
    w_gate = (jax.random.normal(k_gate, (D_MODEL, EXPERTS), jnp.float32) * D_MODEL ** -0.5).astype(jnp.bfloat16)
    w_in = (jax.random.normal(k_in, (EXPERTS, D_MODEL, D_HIDDEN), jnp.float32) * D_MODEL ** -0.5).astype(jnp.bfloat16)
    w_out = (jax.random.normal(k_out, (EXPERTS, D_HIDDEN, D_MODEL), jnp.float32) * D_HIDDEN ** -0.5).astype(jnp.bfloat16)
    return {'tokens': tokens, 'grad_out': grad_out, 'expert_ids': expert_ids, 'w_gate': w_gate, 'w_in': w_in, 'w_out': w_out}


def reference(tokens, grad_out, expert_ids, w_gate, w_in, w_out):
    n_choice = 2 * ALL_TOKENS
    logits = jnp.dot(tokens, w_gate, preferred_element_type=jnp.float32)
    prob_all = jax.nn.softmax(logits, axis=-1)
    picked = jnp.take_along_axis(prob_all, expert_ids, axis=1)
    gate_val = picked / jnp.sum(picked, axis=1, keepdims=True)
    flat_ids = expert_ids.reshape(-1)
    sort_order = jnp.argsort(flat_ids, stable=True)
    counts = jnp.bincount(flat_ids, length=EXPERTS)
    starts = jnp.cumsum(counts) - counts
    pad_rows = jnp.zeros((CAP_ALL, D_MODEL), jnp.bfloat16)
    x_sorted = jnp.concatenate([tokens[sort_order // 2], pad_rows], axis=0)
    dy_flat = (gate_val[:, :, None] * grad_out[:, None, :].astype(jnp.float32)).astype(jnp.bfloat16).reshape(n_choice, D_MODEL)
    dy_sorted = jnp.concatenate([dy_flat[sort_order], pad_rows], axis=0)
    row_iota = jnp.arange(CAP_ALL)[:, None]

    def expert_step(scan_carry, per_expert):
        y_acc, dx_acc = scan_carry
        w_one, w_two, start_row, row_count = per_expert
        keep_row = row_iota < row_count
        x_rows = jnp.where(keep_row, lax.dynamic_slice_in_dim(x_sorted, start_row, CAP_ALL), 0)
        dy_rows = jnp.where(keep_row, lax.dynamic_slice_in_dim(dy_sorted, start_row, CAP_ALL), 0)
        a_pre = jnp.dot(x_rows, w_one, preferred_element_type=jnp.float32)
        hidden, gelu_vjp = jax.vjp(jax.nn.gelu, a_pre)
        hid_b = hidden.astype(jnp.bfloat16)
        y_rows = jnp.dot(hid_b, w_two, preferred_element_type=jnp.float32).astype(jnp.bfloat16)
        g_two = jnp.dot(hid_b.T, dy_rows, preferred_element_type=jnp.float32)
        d_hid = jnp.dot(dy_rows, w_two.T, preferred_element_type=jnp.float32)
        d_pre = gelu_vjp(d_hid)[0].astype(jnp.bfloat16)
        g_one = jnp.dot(x_rows.T, d_pre, preferred_element_type=jnp.float32)
        dx_rows = jnp.dot(d_pre, w_one.T, preferred_element_type=jnp.float32).astype(jnp.bfloat16)
        y_acc = lax.dynamic_update_slice_in_dim(y_acc, lax.dynamic_slice_in_dim(y_acc, start_row, CAP_ALL) + y_rows.astype(jnp.float32), start_row, axis=0)
        dx_acc = lax.dynamic_update_slice_in_dim(dx_acc, lax.dynamic_slice_in_dim(dx_acc, start_row, CAP_ALL) + dx_rows.astype(jnp.float32), start_row, axis=0)
        return (y_acc, dx_acc), (g_one, g_two)

    acc_init = jnp.zeros((n_choice + CAP_ALL, D_MODEL), jnp.float32)
    acc_done, grads = lax.scan(expert_step, (acc_init, acc_init), (w_in, w_out, starts, counts))
    g_in, g_out = grads
    y_sorted = acc_done[0][:n_choice]
    dx_sorted = acc_done[1][:n_choice]
    y_pair = jnp.zeros_like(y_sorted).at[sort_order].set(y_sorted).reshape(ALL_TOKENS, 2, D_MODEL)
    dx_pair = jnp.zeros_like(dx_sorted).at[sort_order].set(dx_sorted).reshape(ALL_TOKENS, 2, D_MODEL)
    y_out = jnp.sum(gate_val[:, :, None] * y_pair, axis=1).astype(jnp.bfloat16)
    d_gate = jnp.sum(grad_out.astype(jnp.float32)[:, None, :] * y_pair, axis=-1)
    d_sel = gate_val * (d_gate - jnp.sum(gate_val * d_gate, axis=1, keepdims=True))
    choice_hot = expert_ids[:, :, None] == jnp.arange(EXPERTS)[None, None, :]
    d_logits = jnp.sum(jnp.where(choice_hot, d_sel[:, :, None], 0.0), axis=1).astype(jnp.bfloat16)
    grad_x = (jnp.sum(dx_pair, axis=1) + jnp.dot(d_logits, w_gate.T, preferred_element_type=jnp.float32)).astype(jnp.bfloat16)
    grad_w_gate = jnp.dot(tokens.T, d_logits, preferred_element_type=jnp.float32)
    return y_out, grad_x, g_in, g_out, grad_w_gate
```

```python
import jax
import jax.numpy as jnp
from jax import lax
from jax.sharding import PartitionSpec as P


def route_slots(expert_ids, n_exp):
    flat_ids = expert_ids.reshape(-1)
    one_hot = (flat_ids[:, None] == jnp.arange(n_exp)[None, :]).astype(jnp.int32)
    rank_in = jnp.sum((jnp.cumsum(one_hot, axis=0) - one_hot) * one_hot, axis=1)
    return flat_ids, one_hot, rank_in


def slot_owner(dest_slot, n_slots):
    n_choice = dest_slot.shape[0]
    return jnp.full((n_slots,), n_choice, jnp.int32).at[dest_slot].set(jnp.arange(n_choice, dtype=jnp.int32), mode='drop')


def local_block(tokens, grad_out, expert_ids, w_gate, w_in, w_out):
    n_exp = w_gate.shape[1]
    tok_dev, d_model = tokens.shape
    cap_rows = tok_dev // 4
    n_choice = 2 * tok_dev
    n_slots = n_exp * cap_rows
    w_one = w_in[0]
    w_two = w_out[0]
    flat_ids, one_hot, rank_in = route_slots(expert_ids, n_exp)
    dest_slot = flat_ids * cap_rows + rank_in
    src_choice = slot_owner(dest_slot, n_slots)
    zero_row = jnp.zeros((1, d_model), jnp.bfloat16)
    x_table = jnp.concatenate([tokens, zero_row], axis=0)
    send_x = jnp.take(x_table, jnp.where(src_choice < n_choice, src_choice // 2, tok_dev), axis=0)
    recv_x = lax.all_to_all(send_x.reshape(n_exp, cap_rows, d_model), 'ep', 0, 0, tiled=True).reshape(n_slots, d_model)
    a_pre = jnp.dot(recv_x, w_one, preferred_element_type=jnp.float32)
    hidden, gelu_vjp = jax.vjp(jax.nn.gelu, a_pre)
    hid_b = hidden.astype(jnp.bfloat16)
    y_rows = jnp.dot(hid_b, w_two, preferred_element_type=jnp.float32).astype(jnp.bfloat16)
    y_back = lax.all_to_all(y_rows.reshape(n_exp, cap_rows, d_model), 'ep', 0, 0, tiled=True).reshape(n_slots, d_model)
    y_pair = jnp.take(y_back, dest_slot, axis=0).reshape(tok_dev, 2, d_model)
    logits = jnp.dot(tokens, w_gate, preferred_element_type=jnp.float32)
    choice_hot = one_hot.reshape(tok_dev, 2, n_exp) > 0
    sel_logit = jnp.sum(jnp.where(choice_hot, logits[:, None, :], 0.0), axis=-1)
    gate_val = jax.nn.softmax(sel_logit, axis=1)
    y_out = jnp.sum(gate_val[:, :, None] * y_pair.astype(jnp.float32), axis=1).astype(jnp.bfloat16)
    d_gate = jnp.einsum('tm,tkm->tk', grad_out, y_pair, preferred_element_type=jnp.float32)
    dy_flat = (gate_val[:, :, None] * grad_out[:, None, :].astype(jnp.float32)).astype(jnp.bfloat16).reshape(n_choice, d_model)
    send_dy = jnp.take(jnp.concatenate([dy_flat, zero_row], axis=0), src_choice, axis=0)
    recv_dy = lax.all_to_all(send_dy.reshape(n_exp, cap_rows, d_model), 'ep', 0, 0, tiled=True).reshape(n_slots, d_model)
    g_w_out = jnp.einsum('rh,rm->hm', hid_b, recv_dy, preferred_element_type=jnp.float32)
    d_hid = jnp.einsum('rm,hm->rh', recv_dy, w_two, preferred_element_type=jnp.float32)
    d_pre = gelu_vjp(d_hid)[0].astype(jnp.bfloat16)
    g_w_in = jnp.einsum('rm,rh->mh', recv_x, d_pre, preferred_element_type=jnp.float32)
    dx_rows = jnp.einsum('rh,mh->rm', d_pre, w_one, preferred_element_type=jnp.float32).astype(jnp.bfloat16)
    dx_back = lax.all_to_all(dx_rows.reshape(n_exp, cap_rows, d_model), 'ep', 0, 0, tiled=True).reshape(n_slots, d_model)
    dx_pair = jnp.take(dx_back, dest_slot, axis=0).reshape(tok_dev, 2, d_model)
    d_sel = gate_val * (d_gate - jnp.sum(gate_val * d_gate, axis=1, keepdims=True))
    d_logits = jnp.sum(jnp.where(choice_hot, d_sel[:, :, None], 0.0), axis=1).astype(jnp.bfloat16)
    grad_x = (jnp.sum(dx_pair.astype(jnp.float32), axis=1) + jnp.einsum('te,me->tm', d_logits, w_gate, preferred_element_type=jnp.float32)).astype(jnp.bfloat16)
    d_slots = jnp.take(jnp.concatenate([d_sel.reshape(-1).astype(jnp.bfloat16), jnp.zeros((1,), jnp.bfloat16)]), src_choice, axis=0)
    recv_d = lax.all_to_all(d_slots.reshape(n_exp, cap_rows), 'ep', 0, 0, tiled=True).reshape(1, n_slots)
    gate_col = jnp.dot(recv_d, recv_x, preferred_element_type=jnp.float32)
    grad_w_gate = lax.all_gather(gate_col, 'ep', axis=0, tiled=True).T
    return y_out, grad_x, g_w_in[None], g_w_out[None], grad_w_gate


def solution(mesh):
    return jax.shard_map(local_block, mesh=mesh, in_specs=(P('ep'), P('ep'), P('ep'), P(), P('ep'), P('ep')), out_specs=(P('ep'), P('ep'), P('ep'), P('ep'), P()), check_vma=False)
```

```python
import functools

import jax
import jax.numpy as jnp
from jax import lax
from jax.experimental import pallas as pl
from jax.experimental.pallas import tpu as pltpu
from jax.sharding import PartitionSpec as P

MESH = pl.DeviceIdType.MESH
F32 = jnp.float32
BF16 = jnp.bfloat16
CAP = 8


def coords(dims):
    nz, ny, nx, nc = dims
    me = lax.axis_index('ep')
    c = lax.rem(me, nc)
    x = lax.rem(me // nc, nx)
    y = lax.rem(me // (nc * nx), ny)
    z = me // (nc * nx * ny)

    def dev(z, y, x, c):
        return (((z * ny + y) * nx + x) * nc + c,)

    return z, y, x, c, dev


def meet(peers):
    barrier = pltpu.get_barrier_semaphore()
    for peer in peers:
        pl.semaphore_signal(barrier, inc=1, device_id=peer, device_id_type=MESH)
    pl.semaphore_wait(barrier, len(peers))


def gather_kernel(dims, kinds, *refs):
    nz, ny, nx, nc = dims
    n = len(kinds)
    ins, held, load_sem = refs[:n], refs[n:2 * n], refs[2 * n]
    send, recv = refs[2 * n + 1:3 * n + 1], refs[3 * n + 1:4 * n + 1]
    z, y, x, c, dev = coords(dims)
    loads = [pltpu.make_async_copy(ins[a], held[a].at[z, y, x, c], load_sem.at[a]) for a in range(n)]
    for ld in loads:
        ld.start()
    peers = [dev(lax.rem(z + d, nz), y, x, c) for d in range(1, nz)]
    for d in ((1, 3, 2) if 'small' in kinds else (1, 3)):
        peers.append(dev(z, lax.rem(y + d, ny), x, c))
        peers.append(dev(z, y, lax.rem(x + d, nx), c))
    peers.append(dev(z, y, x, 1 - c))
    meet(peers)

    count = [0] * n

    def copy(a, src, to):
        k = count[a]
        count[a] += 1
        return pltpu.make_async_remote_copy(src_ref=src, dst_ref=src, send_sem=send[a].at[k], recv_sem=recv[a].at[k],
                                            device_id=to, device_id_type=MESH)

    sent = []

    def go(cp):
        cp.start()
        sent.append(cp)
        return cp

    zcopies = []
    for a in range(n):
        loads[a].wait()
        zcopies.append([go(copy(a, held[a].at[z, y, x, c], dev(lax.rem(z + d, nz), y, x, c))) for d in range(1, nz)])

    low, high, full = pl.ds(0, nz // 2), pl.ds(nz // 2, nz // 2), slice(None)

    def plans(a):
        yx = kinds[a] == 'yx'
        p0, q0 = (y, x) if yx else (x, y)
        npp, nq = (ny, nx) if yx else (nx, ny)

        def at(zs, p, q):
            return held[a].at[zs, p, q, c] if yx else held[a].at[zs, q, p, c]

        def to(p, q):
            return dev(z, p, q, c) if yx else dev(z, q, p, c)

        def shift(v, d, m):
            return lax.rem(v + d, m)

        cross = []

        def over(p, q):
            cross.append(go(copy(a, at(full, p, q), dev(z, y, x, 1 - c))))

        for cp in zcopies[a]:
            yield
            cp.wait_recv()
        pm, pp, po = shift(p0, npp - 1, npp), shift(p0, 1, npp), shift(p0, 2, npp)
        qm, qp, qo = shift(q0, nq - 1, nq), shift(q0, 1, nq), shift(q0, 2, nq)
        p_up = go(copy(a, at(full, p0, q0), to(pp, q0)))
        p_dn = go(copy(a, at(full, p0, q0), to(pm, q0)))
        qs = []

        def spread(p):
            qs.append((p, go(copy(a, at(full, p, q0), to(p0, qp))), go(copy(a, at(full, p, q0), to(p0, qm)))))
            over(p, q0)

        spread(p0)
        yield
        p_up.wait_recv()
        f_up = go(copy(a, at(low, pm, q0), to(pp, q0)))
        yield
        p_dn.wait_recv()
        f_dn = go(copy(a, at(high, pp, q0), to(pm, q0)))
        spread(pm)
        spread(pp)
        relays = []

        def relay(i):
            p, up, dn = qs[i]
            up.wait_recv()
            r_up = go(copy(a, at(low, p, qm), to(p0, qp)))
            over(p, qm)
            dn.wait_recv()
            r_dn = go(copy(a, at(high, p, qp), to(p0, qm)))
            over(p, qp)
            relays.append((p, r_up, r_dn))

        yield
        relay(0)
        yield
        f_up.wait_recv()
        f_dn.wait_recv()
        spread(po)
        for i in (1, 2, 3):
            yield
            relay(i)
            p, r_up, r_dn = relays[i - 1]
            r_up.wait_recv()
            r_dn.wait_recv()
            over(p, qo)
        yield
        p, r_up, r_dn = relays[3]
        r_up.wait_recv()
        r_dn.wait_recv()
        over(p, qo)
        for cp in cross:
            yield
            cp.wait_recv()

    def small(a):
        h = held[a]
        for cp in zcopies[a]:
            yield
            cp.wait_recv()
        ys = [go(copy(a, h.at[:, y, x, c], dev(z, lax.rem(y + d, ny), x, c))) for d in range(1, ny)]
        for cp in ys:
            yield
            cp.wait_recv()
        xs = [go(copy(a, h.at[:, :, x, c], dev(z, y, lax.rem(x + d, nx), c))) for d in range(1, nx)]
        for cp in xs:
            yield
            cp.wait_recv()
        cs = go(copy(a, h.at[:, :, :, c], dev(z, y, x, 1 - c)))
        yield
        cs.wait_recv()

    live = [small(a) if kinds[a] == 'small' else plans(a) for a in range(n)]
    while live:
        for g in list(live):
            try:
                next(g)
            except StopIteration:
                live.remove(g)
    for cp in sent:
        cp.wait_send()


def n_copies(dims, kind):
    nz, ny, nx, _ = dims
    return nz - 1 + (ny - 1 + nx - 1 + 1 if kind == 'small' else 4 + 16 + 16)


def all_gather(dims, arrays, kinds, cid):
    n = len(arrays)
    outs = [jax.ShapeDtypeStruct(dims + a.shape, a.dtype) for a in arrays]
    any_ = pl.BlockSpec(memory_space=pl.ANY)
    sems = [pltpu.SemaphoreType.DMA((n_copies(dims, k),)) for k in kinds]
    return pl.pallas_call(
        functools.partial(gather_kernel, dims, kinds),
        out_shape=outs,
        in_specs=[any_] * n,
        out_specs=[any_] * n,
        scratch_shapes=[pltpu.SemaphoreType.DMA((n,))] + sems + sems,
        compiler_params=pltpu.CompilerParams(collective_id=cid, has_side_effects=True, vmem_limit_bytes=2 ** 20),
        name=f'gather_{cid}',
    )(*arrays)


def quads(m):
    return jnp.sum(m.reshape(m.shape[0] // 4, 4, 8, 128), axis=1)


def gelu_parts(a):
    k = 0.7978845608028654
    sq = a * a
    t = jnp.tanh(a * (k + (k * 0.044715) * sq))
    half = 0.5 + 0.5 * t
    slope = half + (0.5 * a) * (1.0 - t * t) * (k + (3 * k * 0.044715) * sq)
    return a * half, slope


def dot(a, b, ca, cb):
    return lax.dot_general(a, b, (((ca,), (cb,)), ((), ())), preferred_element_type=F32)


def expert_kernel(x_ref, d_ref, m_ref, w1_ref, w2_ref, y_ref, dx_ref, g1_ref, g2_ref):
    me = lax.axis_index('ep').astype(F32)
    meta = quads(m_ref[...])
    n_pair = meta.shape[0] // 2

    def rows(k):
        return jnp.concatenate([jnp.concatenate([meta[2 * p, k:k + 1], meta[2 * p + 1, k:k + 1]], axis=1) for p in range(n_pair)], axis=0)

    i0, i1, g0, g1 = (rows(k) for k in range(4))
    hit0, hit1 = i0 == me, i1 == me
    hit = (hit0 | hit1).astype(F32)
    gate = jnp.where(hit0, g0, 0.0) + jnp.where(hit1, g1, 0.0)
    before = lax.broadcasted_iota(jnp.int32, (256, 256), 0)
    after = lax.broadcasted_iota(jnp.int32, (256, 256), 1)
    tri = ((before < after) & (before // 32 == after // 32)).astype(F32).astype(BF16)
    rank = dot(hit.astype(BF16), tri, 1, 0)
    src = (lax.broadcasted_iota(jnp.int32, (n_pair, 256), 1) // 32).astype(F32)
    key = jnp.where(hit > 0.0, src * CAP + rank, -1.0)
    slot = lax.broadcasted_iota(jnp.int32, (8 * CAP, 256), 0).astype(F32)
    xs, dys = [], []
    for p in range(n_pair):
        sel = (slot == key[p:p + 1]).astype(F32)
        g = jnp.sum(sel * gate[p:p + 1], axis=1, keepdims=True)
        sel = sel.astype(BF16)
        xs.append(dot(sel, x_ref[256 * p:256 * (p + 1)], 1, 0).astype(BF16))
        dys.append((g * dot(sel, d_ref[256 * p:256 * (p + 1)], 1, 0)).astype(BF16))
    xs, dys = jnp.concatenate(xs, axis=0), jnp.concatenate(dys, axis=0)
    h, slope = gelu_parts(dot(xs, w1_ref[...], 1, 0))
    h = h.astype(BF16)
    y_ref[...] = dot(h, w2_ref[...], 1, 0).astype(BF16)
    da = (dot(dys, w2_ref[...], 1, 1) * slope).astype(BF16)
    dx_ref[...] = dot(da, w1_ref[...], 1, 1).astype(BF16)
    gw2 = dot(h, dys, 0, 0)
    gw1 = dot(xs, da, 0, 0)

    @pl.when(pl.program_id(0) == 0)
    def _():
        g1_ref[...] = gw1
        g2_ref[...] = gw2

    @pl.when(pl.program_id(0) > 0)
    def _():
        g1_ref[...] += gw1
        g2_ref[...] += gw2


def expert_block(x_all, d_all, m_all, w1, w2):
    steps = 4
    n_src = m_all.shape[0]
    tok, slots = x_all.shape[0] // steps, n_src * CAP // steps
    d_model, d_hidden = w1.shape
    whole = lambda shape: pl.BlockSpec(shape, lambda i: (0, 0))
    part = lambda r: pl.BlockSpec((r, d_model), lambda i: (i, 0))
    return pl.pallas_call(
        expert_kernel,
        grid=(steps,),
        out_shape=[jax.ShapeDtypeStruct((n_src * CAP, d_model), BF16)] * 2
        + [jax.ShapeDtypeStruct((d_model, d_hidden), F32), jax.ShapeDtypeStruct((d_hidden, d_model), F32)],
        in_specs=[part(tok), part(tok), pl.BlockSpec((n_src // steps, 8, 128), lambda i: (i, 0, 0)), whole(w1.shape), whole(w2.shape)],
        out_specs=[part(slots), part(slots), whole((d_model, d_hidden)), whole((d_hidden, d_model))],
        compiler_params=pltpu.CompilerParams(dimension_semantics=('arbitrary',), vmem_limit_bytes=32 * 2 ** 20),
        name='expert',
    )(x_all, d_all, m_all, w1, w2)


def gate_kernel(x_ref, m_ref, d_ref, o_ref, acc):
    meta, grad = quads(m_ref[...]), quads(d_ref[...])
    expert = lax.broadcasted_iota(jnp.int32, (acc.shape[0], 256), 0).astype(F32)

    @pl.when(pl.program_id(0) == 0)
    def _():
        acc[...] = jnp.zeros_like(acc)

    total = acc[...]
    for p in range(meta.shape[0] // 2):
        def row(v, k):
            return jnp.concatenate([v[2 * p, k:k + 1], v[2 * p + 1, k:k + 1]], axis=1)

        spread = jnp.where(expert == row(meta, 0), row(grad, 0), jnp.where(expert == row(meta, 1), row(grad, 1), 0.0))
        total += dot(spread.astype(BF16), x_ref[256 * p:256 * (p + 1)], 1, 0)
    acc[...] = total

    @pl.when(pl.program_id(0) == pl.num_programs(0) - 1)
    def _():
        o_ref[...] = total.T


def gate_grad(x_all, m_all, d_all):
    steps = 8
    n_src = m_all.shape[0]
    d_model = x_all.shape[1]
    meta = pl.BlockSpec((n_src // steps, 8, 128), lambda i: (i, 0, 0))
    return pl.pallas_call(
        gate_kernel,
        grid=(steps,),
        out_shape=jax.ShapeDtypeStruct((d_model, n_src), F32),
        in_specs=[pl.BlockSpec((x_all.shape[0] // steps, d_model), lambda i: (i, 0)), meta, meta],
        out_specs=pl.BlockSpec((d_model, n_src), lambda i: (0, 0)),
        scratch_shapes=[pltpu.VMEM((n_src, d_model), F32)],
        compiler_params=pltpu.CompilerParams(dimension_semantics=('arbitrary',), vmem_limit_bytes=8 * 2 ** 20),
        name='gate_grad',
    )(x_all, m_all, d_all)


def lane_place(rows):
    k, t = rows.shape
    here = lax.broadcasted_iota(jnp.int32, (k, 4 * t), 1) // t == lax.rem(lax.axis_index('ep'), 4)
    return jnp.pad(jnp.where(here, jnp.tile(rows, (1, 4)), 0.0), ((0, 8 - k), (0, 0)))


def local_block(dims, tokens, grad_out, expert_ids, w_gate, w_in, w_out):
    n_exp = w_gate.shape[1]
    tok_dev, d_model = tokens.shape
    n_choice = 2 * tok_dev
    n_slots = n_exp * CAP
    choice_hot = expert_ids[:, :, None] == jnp.arange(n_exp)[None, None, :]
    logits = jnp.dot(tokens, w_gate, preferred_element_type=F32)
    sel_logit = jnp.sum(jnp.where(choice_hot, logits[:, None, :], 0.0), axis=-1)
    gate_val = jax.nn.softmax(sel_logit, axis=1)
    meta = lane_place(jnp.concatenate([expert_ids.astype(F32), gate_val], axis=1).T)
    x_all, d_all, m_all = all_gather(dims, [tokens, grad_out, meta], ('yx', 'xy', 'small'), 0)
    x_all, d_all = x_all.reshape(-1, d_model), d_all.reshape(-1, d_model)
    m_all = m_all.reshape(n_exp, 8, 128)
    y_rows, dx_rows, g_w_in, g_w_out = expert_block(x_all, d_all, m_all, w_in[0], w_out[0])

    one_hot = choice_hot.any(axis=1).astype(jnp.int32)
    earlier = jnp.cumsum(one_hot, axis=0) - one_hot
    dest_slot = expert_ids * CAP + jnp.sum(jnp.where(choice_hot, earlier[:, None, :], 0), axis=-1)
    y_back = lax.all_to_all(y_rows.reshape(n_exp, CAP, d_model), 'ep', 0, 0, tiled=True).reshape(n_slots, d_model)
    y_pair = jnp.take(y_back, dest_slot.reshape(-1), axis=0).reshape(tok_dev, 2, d_model)
    y_out = jnp.sum(gate_val[:, :, None] * y_pair.astype(F32), axis=1).astype(BF16)
    d_gate = jnp.einsum('tm,tkm->tk', grad_out, y_pair, preferred_element_type=F32)
    d_sel = gate_val * (d_gate - jnp.sum(gate_val * d_gate, axis=1, keepdims=True))
    d_bf = d_sel.astype(BF16)
    g_all, = all_gather(dims, [lane_place(d_bf.astype(F32).T)], ('small',), 1)
    grad_w_gate = gate_grad(x_all, m_all, g_all.reshape(n_exp, 8, 128))
    dx_back = lax.all_to_all(dx_rows.reshape(n_exp, CAP, d_model), 'ep', 0, 0, tiled=True).reshape(n_slots, d_model)
    dx_pair = jnp.take(dx_back, dest_slot.reshape(-1), axis=0).reshape(tok_dev, 2, d_model)
    d_logits = jnp.sum(jnp.where(choice_hot, d_sel[:, :, None], 0.0), axis=1).astype(BF16)
    grad_x = (jnp.sum(dx_pair.astype(F32), axis=1) + jnp.einsum('te,me->tm', d_logits, w_gate, preferred_element_type=F32)).astype(BF16)
    return y_out, grad_x, g_w_in[None], g_w_out[None], grad_w_gate


def solution(mesh):
    dims = (8, 4, 4, 2)
    return jax.shard_map(functools.partial(local_block, dims), mesh=mesh, in_specs=(P('ep'), P('ep'), P('ep'), P(), P('ep'), P('ep')), out_specs=(P('ep'), P('ep'), P('ep'), P('ep'), P()), check_vma=False)
```

```python
import functools

import jax
import jax.numpy as jnp
from jax import lax
from jax.experimental import pallas as pl
from jax.experimental.pallas import tpu as pltpu
from jax.sharding import PartitionSpec as P

MESH = pl.DeviceIdType.MESH
F32 = jnp.float32
BF16 = jnp.bfloat16
CAP = 8


def coords(dims):
    nz, ny, nx, nc = dims
    me = lax.axis_index('ep')
    c = lax.rem(me, nc)
    x = lax.rem(me // nc, nx)
    y = lax.rem(me // (nc * nx), ny)
    z = me // (nc * nx * ny)

    def dev(z, y, x, c):
        return (((z * ny + y) * nx + x) * nc + c,)

    return z, y, x, c, dev


def meet(peers):
    barrier = pltpu.get_barrier_semaphore()
    for peer in peers:
        pl.semaphore_signal(barrier, inc=1, device_id=peer, device_id_type=MESH)
    pl.semaphore_wait(barrier, len(peers))


def dot(a, b, ca, cb):
    return lax.dot_general(a, b, (((ca,), (cb,)), ((), ())), preferred_element_type=F32)


def iota(shape, axis):
    return lax.broadcasted_iota(jnp.int32, shape, axis)


def as_row(col):
    n = col.shape[0]
    return jnp.sum(jnp.where(iota((n, n), 0) == iota((n, n), 1), col, 0.0), axis=0, keepdims=True)


def gates(tok, ids, w_gate):
    logits = dot(tok, w_gate, 1, 0)
    expert = iota(logits.shape, 1)
    l0, l1 = (jnp.sum(jnp.where(expert == ids[:, k:k + 1], logits, 0.0), axis=1, keepdims=True) for k in range(2))
    top = jnp.maximum(l0, l1)
    p0, p1 = jnp.exp(l0 - top), jnp.exp(l1 - top)
    total = p0 + p1
    return ids[:, 0:1].astype(F32), ids[:, 1:2].astype(F32), p0 / total, p1 / total


def choice_row(tok, ids, w_gate):
    i0, i1, g0, g1 = gates(tok, ids, w_gate)
    r0, r1 = as_row(i0), as_row(i1)

    def code(i):
        n = jnp.sum((i == r0).astype(F32) + (i == r1).astype(F32), axis=1, keepdims=True)
        return as_row(jnp.where(n > 1.5, i + 256.0, i))

    return jnp.concatenate([code(i0), code(i1), as_row(g0), as_row(g1)], axis=1)


def gather_kernel(dims, kinds, first, *refs):
    nz, ny, nx, nc = dims
    n = len(kinds)
    ins, refs = list(refs[:n]), refs[n:]
    if first:
        (tok_ref, gate_ref), refs = refs[:2], refs[2:]
    held, load_sem, refs = refs[:n], refs[n], refs[n + 1:]
    send, recv, refs = refs[:n], refs[n:2 * n], refs[2 * n:]
    if first:
        ids_ref, ins[-1] = ins[-1], refs[0]
    z, y, x, c, dev = coords(dims)
    loads = [pltpu.make_async_copy(ins[a], held[a].at[z, y, x, c], load_sem.at[a]) for a in range(n)]
    for ld in loads[:-1] if first else loads:
        ld.start()
    peers = [dev(lax.rem(z + d, nz), y, x, c) for d in range(1, nz)]
    for d in ((1, 3, 2) if 'small' in kinds else (1, 3)):
        peers.append(dev(z, lax.rem(y + d, ny), x, c))
        peers.append(dev(z, y, lax.rem(x + d, nx), c))
    peers.append(dev(z, y, x, 1 - c))
    meet(peers)

    count = [0] * n

    def copy(a, src, to):
        k = count[a]
        count[a] += 1
        return pltpu.make_async_remote_copy(src_ref=src, dst_ref=src, send_sem=send[a].at[k], recv_sem=recv[a].at[k],
                                            device_id=to, device_id_type=MESH)

    sent = []

    def go(cp):
        cp.start()
        sent.append(cp)
        return cp

    zcopies = []
    for a in range(n):
        if first and a == n - 1:
            ins[a][...] = choice_row(tok_ref[...], ids_ref[...], gate_ref[...])
            loads[a].start()
        loads[a].wait()
        zcopies.append([go(copy(a, held[a].at[z, y, x, c], dev(lax.rem(z + d, nz), y, x, c))) for d in range(1, nz)])

    low, high, full = pl.ds(0, nz // 2), pl.ds(nz // 2, nz // 2), slice(None)

    def plans(a):
        yx = kinds[a] == 'yx'
        p0, q0 = (y, x) if yx else (x, y)
        npp, nq = (ny, nx) if yx else (nx, ny)

        def at(zs, p, q):
            return held[a].at[zs, p, q, c] if yx else held[a].at[zs, q, p, c]

        def to(p, q):
            return dev(z, p, q, c) if yx else dev(z, q, p, c)

        def shift(v, d, m):
            return lax.rem(v + d, m)

        cross = []

        def over(p, q):
            cross.append(go(copy(a, at(full, p, q), dev(z, y, x, 1 - c))))

        for cp in zcopies[a]:
            yield
            cp.wait_recv()
        pm, pp, po = shift(p0, npp - 1, npp), shift(p0, 1, npp), shift(p0, 2, npp)
        qm, qp, qo = shift(q0, nq - 1, nq), shift(q0, 1, nq), shift(q0, 2, nq)
        p_up = go(copy(a, at(full, p0, q0), to(pp, q0)))
        p_dn = go(copy(a, at(full, p0, q0), to(pm, q0)))
        qs = []

        def spread(p):
            qs.append((p, go(copy(a, at(full, p, q0), to(p0, qp))), go(copy(a, at(full, p, q0), to(p0, qm)))))
            over(p, q0)

        spread(p0)
        yield
        p_up.wait_recv()
        f_up = go(copy(a, at(low, pm, q0), to(pp, q0)))
        yield
        p_dn.wait_recv()
        f_dn = go(copy(a, at(high, pp, q0), to(pm, q0)))
        spread(pm)
        spread(pp)
        relays = []

        def relay(i):
            p, up, dn = qs[i]
            up.wait_recv()
            r_up = go(copy(a, at(low, p, qm), to(p0, qp)))
            over(p, qm)
            dn.wait_recv()
            r_dn = go(copy(a, at(high, p, qp), to(p0, qm)))
            over(p, qp)
            relays.append((p, r_up, r_dn))

        yield
        relay(0)
        yield
        f_up.wait_recv()
        f_dn.wait_recv()
        spread(po)
        for i in (1, 2, 3):
            yield
            relay(i)
            p, r_up, r_dn = relays[i - 1]
            r_up.wait_recv()
            r_dn.wait_recv()
            over(p, qo)
        yield
        p, r_up, r_dn = relays[3]
        r_up.wait_recv()
        r_dn.wait_recv()
        over(p, qo)
        for cp in cross:
            yield
            cp.wait_recv()

    def small(a):
        h = held[a]
        for cp in zcopies[a]:
            yield
            cp.wait_recv()
        ys = [go(copy(a, h.at[:, y, x, c], dev(z, lax.rem(y + d, ny), x, c))) for d in range(1, ny)]
        for cp in ys:
            yield
            cp.wait_recv()
        xs = [go(copy(a, h.at[:, :, x, c], dev(z, y, lax.rem(x + d, nx), c))) for d in range(1, nx)]
        for cp in xs:
            yield
            cp.wait_recv()
        cs = go(copy(a, h.at[:, :, :, c], dev(z, y, x, 1 - c)))
        yield
        cs.wait_recv()

    live = [small(a) if kinds[a] == 'small' else plans(a) for a in range(n)]
    while live:
        for g in list(live):
            try:
                next(g)
            except StopIteration:
                live.remove(g)
    for cp in sent:
        cp.wait_send()


def n_copies(dims, kind):
    nz, ny, nx, _ = dims
    return nz - 1 + (ny - 1 + nx - 1 + 1 if kind == 'small' else 4 + 16 + 16)


def all_gather(dims, arrays, kinds, cid, first=()):
    n = len(arrays)
    blocks = [(a.shape, a.dtype) for a in arrays]
    if first:
        blocks[-1] = ((1, 128), F32)
    outs = [jax.ShapeDtypeStruct(dims + s, t) for s, t in blocks]
    hbm, vmem = pl.BlockSpec(memory_space=pltpu.HBM), pl.BlockSpec(memory_space=pltpu.VMEM)
    sems = [pltpu.SemaphoreType.DMA((n_copies(dims, k),)) for k in kinds]
    return pl.pallas_call(
        functools.partial(gather_kernel, dims, kinds, bool(first)),
        out_shape=outs,
        in_specs=[hbm] * (n - 1) + [vmem if first else pl.BlockSpec(memory_space=pl.ANY)] + [vmem] * len(first),
        out_specs=[pl.BlockSpec(memory_space=pl.ANY)] * n,
        scratch_shapes=[pltpu.SemaphoreType.DMA((n,))] + sems + sems + ([pltpu.VMEM((1, 128), F32)] if first else []),
        compiler_params=pltpu.CompilerParams(collective_id=cid, has_side_effects=True, vmem_limit_bytes=2 ** 20),
        name=f'gather_{cid}',
    )(*arrays, *first)


def gelu_parts(a):
    k = 0.7978845608028654
    sq = a * a
    t = jnp.tanh(a * (k + (k * 0.044715) * sq))
    half = 0.5 + 0.5 * t
    slope = half + (0.5 * a) * (1.0 - t * t) * (k + (3 * k * 0.044715) * sq)
    return a * half, slope


def token_lanes(ref, k, start, n):
    lane = iota((n, 128), 1) // 32
    out = jnp.zeros((n, 128), F32)
    for j in range(4):
        r = ref[pl.ds(start + j, n, stride=4), :]
        out = jnp.where(lane == j, r if j == k else pltpu.roll(r, 32 * (j - k) % 128, 1), out)
    return out


def pair_rows(v):
    return jnp.concatenate([jnp.concatenate([v[2 * i:2 * i + 1], v[2 * i + 1:2 * i + 2]], axis=1) for i in range(v.shape[0] // 2)], axis=0)


def plain_id(code):
    return jnp.where(code >= 256.0, code - 256.0, code)


def expert_kernel(dims, x_ref, d_ref, m_ref, all_ref, w1_ref, w2_ref, y_ref, dx_ref, g1_ref, g2_ref, hot_ref):
    _, ny, nx, nc = dims
    me = lax.axis_index('ep').astype(F32)
    n_quad = m_ref.shape[0] // 4
    c0, c1, g0, g1 = (pair_rows(token_lanes(m_ref, k, 0, n_quad)) for k in range(4))
    n_pair = n_quad // 2
    hit0, hit1 = plain_id(c0) == me, plain_id(c1) == me
    hit = (hit0 | hit1).astype(F32)
    gate = jnp.where(hit0, g0, 0.0) + jnp.where(hit1, g1, 0.0)
    before, after = iota((256, 256), 0), iota((256, 256), 1)
    tri = ((before < after) & (before // 32 == after // 32)).astype(F32).astype(BF16)
    rank = dot(hit.astype(BF16), tri, 1, 0)
    src = (iota((n_pair, 256), 1) // 32).astype(F32)
    key = jnp.where(hit > 0.0, src * CAP + rank, -1.0)
    slot = iota((8 * CAP, 256), 0).astype(F32)
    xs, dys = [], []
    for p in range(n_pair):
        sel = (slot == key[p:p + 1]).astype(F32)
        g = jnp.sum(sel * gate[p:p + 1], axis=1, keepdims=True)
        sel = sel.astype(BF16)
        xs.append(dot(sel, x_ref[256 * p:256 * (p + 1)], 1, 0))
        dys.append(g * dot(sel, d_ref[256 * p:256 * (p + 1)], 1, 0))
    places = [(c, x, y, z) for c in range(nc) for x in range(nx) for y in range(ny) for z in range(n_pair // ny)]

    def by_place(parts):
        return jnp.concatenate([parts[z * ny + y][8 * (x * nc + c):8 * (x * nc + c + 1)] for c, x, y, z in places], axis=0).astype(BF16)

    xs, dys = by_place(xs), by_place(dys)
    h, slope = gelu_parts(dot(xs, w1_ref[...], 1, 0))
    h = h.astype(BF16)
    y = dot(h, w2_ref[...], 1, 0)
    da = (dot(dys, w2_ref[...], 1, 1) * slope).astype(BF16)
    dx = dot(da, w1_ref[...], 1, 1)
    for i, place in enumerate(places):
        y_ref[place] = y[8 * i:8 * (i + 1)].astype(BF16)
        dx_ref[place] = dx[8 * i:8 * (i + 1)].astype(BF16)
    gw2 = dot(h, dys, 0, 0)
    gw1 = dot(xs, da, 0, 0)

    @pl.when(pl.program_id(0) == 0)
    def _():
        g1_ref[...] = gw1
        g2_ref[...] = gw2
        code = all_ref[...]
        ids = jnp.where((iota(code.shape, 1) < 64) & (code >= 256.0), code - 256.0, 999.0)
        found = []
        for _ in range(3):
            best = jnp.min(jnp.min(ids, axis=0, keepdims=True), axis=1, keepdims=True)
            ids = jnp.where(ids == best, 999.0, ids)
            found.append(jnp.broadcast_to(best, (1, 128)))
        hot_ref[...] = jnp.concatenate(found + [jnp.full((5, 128), 999.0, F32)], axis=0)

    @pl.when(pl.program_id(0) > 0)
    def _():
        g1_ref[...] += gw1
        g2_ref[...] += gw2


def expert_block(dims, x_all, d_all, m_all, w1, w2):
    steps = 4
    nz, ny, nx, nc = dims
    n_src = m_all.shape[0]
    if nz < 8:
        steps = nz // 2
    tok = x_all.shape[0] // steps
    d_model, d_hidden = w1.shape
    whole = lambda shape: pl.BlockSpec(shape, lambda i: (0, 0))
    part = lambda r: pl.BlockSpec((r, d_model), lambda i: (i, 0))
    back = (nc, nx, ny, nz // steps, CAP, d_model)
    back_spec = pl.BlockSpec(back, lambda i: (0, 0, 0, i, 0, 0))
    return pl.pallas_call(
        functools.partial(expert_kernel, dims),
        grid=(steps,),
        out_shape=[jax.ShapeDtypeStruct((nc, nx, ny, nz, CAP, d_model), BF16)] * 2
        + [jax.ShapeDtypeStruct((d_model, d_hidden), F32), jax.ShapeDtypeStruct((d_hidden, d_model), F32), jax.ShapeDtypeStruct((8, 128), F32)],
        in_specs=[part(tok), part(tok), pl.BlockSpec((n_src // steps, 128), lambda i: (i, 0)), whole(m_all.shape), whole(w1.shape), whole(w2.shape)],
        out_specs=[back_spec, back_spec, whole((d_model, d_hidden)), whole((d_hidden, d_model)), whole((8, 128))],
        compiler_params=pltpu.CompilerParams(dimension_semantics=('arbitrary',), vmem_limit_bytes=32 * 2 ** 20),
        name='expert',
    )(x_all, d_all, m_all, m_all, w1, w2)


def return_kernel(dims, hot_ref, *refs):
    nz, ny, nx, nc = dims
    z, y, x, c, dev = coords(dims)
    peers = [dev(z, y, x, 1 - c)]
    for d in (1, 3):
        peers.append(dev(z, lax.rem(y + d, ny), x, c))
        peers.append(dev(z, y, lax.rem(x + d, nx), c))
    peers += [dev(lax.rem(z + d, nz), y, x, c) for d in range(1, nz)]
    meet(peers)
    sent = []

    def plan(i):
        h, hot_land, cold_land = refs[i], refs[2 + 2 * i], refs[3 + 2 * i]
        other, near, via, out2, via2, in2, out3 = refs[6 + 7 * i:13 + 7 * i]
        send, recv, keep = refs[20 + 3 * i:23 + 3 * i]
        x_first = i == 0
        a, b = (x, y) if x_first else (y, x)
        count = [0]

        def go(src, dst, to):
            k = count[0]
            count[0] += 1
            cp = pltpu.make_async_remote_copy(src_ref=src, dst_ref=dst, send_sem=send.at[k], recv_sem=recv.at[k], device_id=to, device_id_type=MESH)
            cp.start()
            sent.append(cp)
            return cp

        def to(a, b):
            return dev(z, b, a, c) if x_first else dev(z, a, b, c)

        def index(lead, a, bs):
            return lead + ((a, bs) if x_first else (bs, a))

        def step(v, d):
            return lax.rem(v + d, 4)

        up, dn, far = step(a, 1), step(a, 3), step(a, 2)
        lo, hi, full = pl.ds(0, 2), pl.ds(2, 2), slice(None)
        cross = go(h.at[1 - c], other, dev(z, y, x, 1 - c))

        def spread(ref, lead, e):
            return [go(ref.at[index(lead, far, lo)], via.at[0, e], to(up, b)), go(ref.at[index(lead, far, hi)], via.at[1, e], to(dn, b)),
                    go(ref.at[index(lead, up, full)], near.at[a, e], to(up, b)), go(ref.at[index(lead, dn, full)], near.at[a, e], to(dn, b))]

        def relay(cps, e):
            cps[0].wait_recv()
            r_up = go(via.at[0, e], near.at[dn, e, lo], to(up, b))
            cps[1].wait_recv()
            r_dn = go(via.at[1, e], near.at[up, e, hi], to(dn, b))
            return [cps[2], cps[3], r_up, r_dn]

        own = spread(h, (c,), c)
        yield
        cross.wait_recv()
        his = spread(other, (), 1 - c)
        yield
        waits = relay(own, c)
        yield
        waits += relay(his, 1 - c)
        for cp in waits:
            yield
            cp.wait_recv()

        def expert(s, e):
            return ((z * ny + y) * nx + s) * nc + e if x_first else ((z * ny + s) * nx + x) * nc + e

        places = [(step(a, d), e) for d in range(4) for e in (c, 1 - c)]
        is_hot = [[(hot_ref[j:j + 1, :] == expert(s, e).astype(F32)).astype(F32) for s, e in places] for j in range(3)]

        def wide(v):
            v = jnp.broadcast_to(v, (8, 128))
            return jnp.concatenate([v, v], axis=1)

        weight = [[wide(v).astype(BF16) for v in row] for row in is_hot]
        line = iota((8, 256), 0)
        mine = [(wide(is_hot[0][k] + is_hot[1][k] + is_hot[2][k]) < 0.5) & (line == s * nc + e) for k, (s, e) in enumerate(places)]

        def squeeze(bb, carry):
            parts = [h[index((c,), a, bb)], other[index((), a, bb)]] + [near[s, e, bb] for s, e in places[2:]]
            for j in range(3):
                out2[bb, j] = sum(parts[k] * weight[j][k] for k in range(8))
            singles = jnp.zeros((nz, 8, 256), F32)
            for k in range(8):
                singles = jnp.where(mine[k], jnp.sum(parts[k].astype(F32), axis=1, keepdims=True), singles)
            out2[bb, 3] = singles.astype(BF16)
            return carry

        lax.fori_loop(0, 4, squeeze, 0)
        in2[b] = out2[b]
        yield
        up, dn, far = step(b, 1), step(b, 3), step(b, 2)
        lo, hi = pl.ds(0, nz // 2), pl.ds(nz // 2, nz // 2)
        f_up, f_dn = go(out2.at[far, :, lo], via2.at[0], to(a, up)), go(out2.at[far, :, hi], via2.at[1], to(a, dn))
        n_up, n_dn = go(out2.at[up], in2.at[b], to(a, up)), go(out2.at[dn], in2.at[b], to(a, dn))
        yield
        f_up.wait_recv()
        r_up = go(via2.at[0], in2.at[dn, :, lo], to(a, up))
        f_dn.wait_recv()
        r_dn = go(via2.at[1], in2.at[up, :, hi], to(a, dn))
        for cp in (n_up, n_dn, r_up, r_dn):
            yield
            cp.wait_recv()
        for j in range(3):
            out3[:, j] = (in2[0, j] + in2[1, j]) + (in2[2, j] + in2[3, j])
        last = []
        for d in range(1, nz):
            zz = lax.rem(z + d, nz)
            last.append(go(in2.at[:, 3, zz], cold_land.at[z], dev(zz, y, x, c)))
        for d in range(1, nz):
            zz = lax.rem(z + d, nz)
            last.append(go(out3.at[zz], hot_land.at[z], dev(zz, y, x, c)))
        stay = [pltpu.make_async_copy(in2.at[:, 3, z], cold_land.at[z], keep.at[0]), pltpu.make_async_copy(out3.at[z], hot_land.at[z], keep.at[1])]
        for cp in stay:
            cp.start()
        for cp in last:
            yield
            cp.wait_recv()
        for cp in stay:
            cp.wait()

    live = [plan(0), plan(1)]
    while live:
        for g in list(live):
            try:
                next(g)
            except StopIteration:
                live.remove(g)
    for cp in sent:
        cp.wait_send()


def return_rows(dims, hot, y_rows, dx_rows):
    nz = dims[0]
    tile = y_rows.shape[-2:]
    n_cp = 1 + 12 + 6 + 2 * (nz - 1)
    vmem, any_ = pl.BlockSpec(memory_space=pltpu.VMEM), pl.BlockSpec(memory_space=pl.ANY)
    work = [(4, 4, nz), (4, 2, 4, nz), (2, 2, 2, nz), (4, 4, nz), (2, 4, nz // 2), (4, 4, nz), (nz, 3)]
    sems = [pltpu.SemaphoreType.DMA((n_cp,)), pltpu.SemaphoreType.DMA((n_cp,)), pltpu.SemaphoreType.DMA((2,))]
    return pl.pallas_call(
        functools.partial(return_kernel, dims),
        out_shape=[jax.ShapeDtypeStruct((nz, 3) + tile, BF16), jax.ShapeDtypeStruct((nz, 4) + tile, BF16)] * 2,
        in_specs=[vmem] * 3,
        out_specs=[any_] * 4,
        scratch_shapes=[pltpu.VMEM(w + tile, BF16) for w in work] * 2 + sems * 2,
        compiler_params=pltpu.CompilerParams(collective_id=1, has_side_effects=True, vmem_limit_bytes=24 * 2 ** 20),
        name='return_rows',
    )(hot, y_rows, dx_rows)


def combine_kernel(dims, tok_ref, dout_ref, ids_ref, gate_ref, hot_ref, hy_ref, cy_ref, hdx_ref, cdx_ref, out_ref, gx_ref, d_ref):
    nz, ny, nx, nc = dims
    ids = ids_ref[...]
    i0, i1, g0, g1 = gates(tok_ref[...], ids, gate_ref[...])
    r0, r1 = as_row(i0), as_row(i1)
    n_tok = ids.shape[0]
    earlier = iota((n_tok, n_tok), 1) < iota((n_tok, n_tok), 0)
    hot = [hot_ref[j:j + 1, 0:1] for j in range(3)]
    n_cold = cy_ref.shape[0]

    def table(ref):
        v = jnp.sum(ref[...].astype(F32), axis=0)
        return jnp.concatenate([v, jnp.zeros((8, v.shape[1]), F32)], axis=0).astype(BF16)

    hot_y, hot_dx = table(hy_ref), table(hdx_ref)

    def pick(k):
        i = (i0, i1)[k]
        e = ids[:, k:k + 1]
        rank = jnp.sum(jnp.where(earlier & ((i == r0) | (i == r1)), 1.0, 0.0), axis=1, keepdims=True)
        place = jnp.full((n_tok, 1), -1.0, F32)
        for j in range(3):
            place = jnp.where(i == hot[j], CAP * j + rank, place)
        sel_hot = (iota((n_tok, 32), 1).astype(F32) == place).astype(F32).astype(BF16)
        cold = place < 0.0
        core, xx, yy, zz = e % nc, (e // nc) % nx, (e // (nc * nx)) % ny, e // (nc * nx * ny)
        lane = iota((n_tok, n_cold), 1)
        in_y = ((lane == e) & cold).astype(F32).astype(BF16)
        in_dx = ((lane == ((zz * nx + xx) * ny + yy) * nc + core) & cold).astype(F32).astype(BF16)
        return (dot(sel_hot, hot_y, 1, 0) + dot(in_y, cy_ref[...], 1, 0), dot(sel_hot, hot_dx, 1, 0) + dot(in_dx, cdx_ref[...], 1, 0))

    (y0, dx0), (y1, dx1) = pick(0), pick(1)
    out_ref[...] = (g0 * y0 + g1 * y1).astype(BF16)
    dout = dout_ref[...].astype(F32)
    dg0, dg1 = (jnp.sum(dout * v, axis=1, keepdims=True) for v in (y0, y1))
    mean = g0 * dg0 + g1 * dg1
    d0, d1 = ((g * (dg - mean)).astype(BF16).astype(F32) for g, dg in ((g0, dg0), (g1, dg1)))
    expert = iota((n_tok, gate_ref.shape[1]), 1)
    spread = jnp.where(expert == ids[:, 0:1], d0, jnp.where(expert == ids[:, 1:2], d1, 0.0)).astype(BF16)
    gx_ref[...] = (dx0 + dx1 + dot(spread, gate_ref[...], 1, 1)).astype(BF16)
    d_ref[...] = jnp.concatenate([as_row(d0), as_row(d1), jnp.zeros((1, 2 * n_tok), F32)], axis=1)


def combine(dims, tokens, grad_out, ids, w_gate, hot, back):
    nz = dims[0]
    d_model = tokens.shape[1]
    back = [v.reshape((nz, 24, d_model) if k % 2 == 0 else (nz * 32, d_model)) for k, v in enumerate(back)]
    return pl.pallas_call(
        functools.partial(combine_kernel, dims),
        out_shape=[jax.ShapeDtypeStruct(tokens.shape, BF16)] * 2 + [jax.ShapeDtypeStruct((1, 128), F32)],
        compiler_params=pltpu.CompilerParams(vmem_limit_bytes=16 * 2 ** 20),
        name='combine',
    )(tokens, grad_out, ids, w_gate, hot, *back)


def gate_kernel(x_ref, m_ref, d_ref, o_ref, acc):
    n_quad = m_ref.shape[0] // 4
    i0, i1 = (plain_id(pair_rows(token_lanes(m_ref, k, 0, n_quad))) for k in range(2))
    d0, d1 = (pair_rows(token_lanes(d_ref, k, 0, n_quad)) for k in range(2))
    expert = iota((acc.shape[0], 256), 0).astype(F32)

    @pl.when(pl.program_id(0) == 0)
    def _():
        acc[...] = jnp.zeros_like(acc)

    total = acc[...]
    for p in range(n_quad // 2):
        q = slice(p, p + 1)
        spread = jnp.where(expert == i0[q], d0[q], jnp.where(expert == i1[q], d1[q], 0.0))
        total += dot(spread.astype(BF16), x_ref[256 * p:256 * (p + 1)], 1, 0)
    acc[...] = total

    @pl.when(pl.program_id(0) == pl.num_programs(0) - 1)
    def _():
        o_ref[...] = total.T


def gate_grad(x_all, m_all, d_all):
    n_src = m_all.shape[0]
    steps = 8 if n_src == 256 else 2
    d_model = x_all.shape[1]
    meta = pl.BlockSpec((n_src // steps, 128), lambda i: (i, 0))
    return pl.pallas_call(
        gate_kernel,
        grid=(steps,),
        out_shape=jax.ShapeDtypeStruct((d_model, n_src), F32),
        in_specs=[pl.BlockSpec((x_all.shape[0] // steps, d_model), lambda i: (i, 0)), meta, meta],
        out_specs=pl.BlockSpec((d_model, n_src), lambda i: (0, 0)),
        scratch_shapes=[pltpu.VMEM((n_src, d_model), F32)],
        compiler_params=pltpu.CompilerParams(dimension_semantics=('arbitrary',), vmem_limit_bytes=8 * 2 ** 20),
        name='gate_grad',
    )(x_all, m_all, d_all)


def local_block(dims, tokens, grad_out, expert_ids, w_gate, w_in, w_out):
    n_exp = w_gate.shape[1]
    d_model = tokens.shape[1]
    x_all, d_all, m_all = all_gather(dims, [tokens, grad_out, expert_ids], ('yx', 'xy', 'small'), 0, (tokens, w_gate))
    x_all, d_all, m_all = x_all.reshape(-1, d_model), d_all.reshape(-1, d_model), m_all.reshape(n_exp, 128)
    y_rows, dx_rows, g_w_in, g_w_out, hot = expert_block(dims, x_all, d_all, m_all, w_in[0], w_out[0])
    back = return_rows(dims, hot, y_rows, dx_rows)
    y_out, grad_x, d_row = combine(dims, tokens, grad_out, expert_ids, w_gate, hot, back)
    g_all, = all_gather(dims, [d_row], ('small',), 2)
    grad_w_gate = gate_grad(x_all, m_all, g_all.reshape(n_exp, 128))
    return y_out, grad_x, g_w_in[None], g_w_out[None], grad_w_gate


def solution(mesh):
    dims = (8, 4, 4, 2)
    return jax.shard_map(functools.partial(local_block, dims), mesh=mesh, in_specs=(P('ep'), P('ep'), P('ep'), P(), P('ep'), P('ep')), out_specs=(P('ep'), P('ep'), P('ep'), P('ep'), P()), check_vma=False)
```

```python
import functools
import itertools

import jax
import jax.numpy as jnp
from jax import lax
from jax.experimental import pallas as pl
from jax.experimental.pallas import tpu as pltpu
from jax.sharding import PartitionSpec as P

MESH = pl.DeviceIdType.MESH
F32 = jnp.float32
BF16 = jnp.bfloat16
CAP = 8


def coords(dims):
    nz, ny, nx, nc = dims
    me = lax.axis_index('ep')
    c = lax.rem(me, nc)
    x = lax.rem(me // nc, nx)
    y = lax.rem(me // (nc * nx), ny)
    z = me // (nc * nx * ny)

    def dev(z, y, x, c):
        return (((z * ny + y) * nx + x) * nc + c,)

    return z, y, x, c, dev


def meet(peers):
    barrier = pltpu.get_barrier_semaphore()
    for peer in peers:
        pl.semaphore_signal(barrier, inc=1, device_id=peer, device_id_type=MESH)
    pl.semaphore_wait(barrier, len(peers))


def dot(a, b, ca, cb):
    return lax.dot_general(a, b, (((ca,), (cb,)), ((), ())), preferred_element_type=F32)


def iota(shape, axis):
    return lax.broadcasted_iota(jnp.int32, shape, axis)


def as_row(col):
    n = col.shape[0]
    return jnp.sum(jnp.where(iota((n, n), 0) == iota((n, n), 1), col, 0.0), axis=0, keepdims=True)


def as_col(row):
    n = row.shape[1]
    return jnp.sum(jnp.where(iota((n, n), 0) == iota((n, n), 1), row, 0.0), axis=1, keepdims=True)


def gates(tok, i0, i1, w_gate):
    logits = dot(tok, w_gate, 1, 0)
    expert = iota(logits.shape, 1).astype(F32)
    l0, l1 = (jnp.sum(jnp.where(expert == i, logits, 0.0), axis=1, keepdims=True) for i in (i0, i1))
    top = jnp.maximum(l0, l1)
    p0, p1 = jnp.exp(l0 - top), jnp.exp(l1 - top)
    total = p0 + p1
    return p0 / total, p1 / total


def choice_row(tok, ids, w_gate):
    r0, r1 = ids[0:1].astype(F32), ids[1:2].astype(F32)
    i0, i1 = as_col(r0), as_col(r1)
    g0, g1 = gates(tok, i0, i1, w_gate)

    def code(i):
        n = jnp.sum((i == r0).astype(F32) + (i == r1).astype(F32), axis=1, keepdims=True)
        return as_row(jnp.where(n > 1.5, i + 256.0, i))

    return jnp.concatenate([code(i0), code(i1), as_row(g0), as_row(g1)], axis=1)


def gelu_parts(a):
    k = 0.7978845608028654
    sq = a * a
    t = jnp.tanh(a * (k + (k * 0.044715) * sq))
    half = 0.5 + 0.5 * t
    slope = half + (0.5 * a) * (1.0 - t * t) * (k + (3 * k * 0.044715) * sq)
    return a * half, slope


def token_lanes(ref, k, start, n):
    lane = iota((n, 128), 1) // 32
    out = jnp.zeros((n, 128), F32)
    for j in range(4):
        r = ref[pl.ds(start + j, n, stride=4), :]
        out = jnp.where(lane == j, r if j == k else pltpu.roll(r, 32 * (j - k) % 128, 1), out)
    return out


def pair_rows(v):
    return jnp.concatenate([jnp.concatenate([v[2 * i:2 * i + 1], v[2 * i + 1:2 * i + 2]], axis=1) for i in range(v.shape[0] // 2)], axis=0)


def plain_id(code):
    return jnp.where(code >= 256.0, code - 256.0, code)


class Links:
    def __init__(self, send, recv, sent):
        self.send, self.recv, self.sent, self.k = send, recv, sent, 0

    def go(self, src, dst, to):
        cp = pltpu.make_async_remote_copy(src_ref=src, dst_ref=dst, send_sem=self.send.at[self.k], recv_sem=self.recv.at[self.k], device_id=to, device_id_type=MESH)
        self.k += 1
        cp.start()
        self.sent.append(cp)
        return cp


def take_turns(plans):
    live = list(plans)
    while live:
        for g in list(live):
            if next(g, 'end') == 'end':
                live.remove(g)


def block_kernel(dims, sizes, *refs):
    nz, ny, nx, nc = dims
    refs = iter(refs)
    refs = [list(itertools.islice(refs, n)) for n in sizes]
    (tok_hbm, dout_hbm, ids_hbm, wg_hbm, w1_hbm, w2_hbm), outs, held, kept, rows, works, (load_sem, keep_sem, save_sem), sems = refs
    out_ref, gx_ref, x_all, m_all, d_land, g1_ref, g2_ref = held
    tok, dout, ids, wg, w1, w2, row, m_land, g_all, xs_ref, dys_ref, h_ref, da_ref, hot_ref, d_row = kept
    z, y, x, c, dev = coords(dims)
    sent, saves = [], []

    def save(k, part=None):
        src, dst = (held[k], outs[k]) if part is None else (held[k].at[part], outs[k].at[part])
        cp = pltpu.make_async_copy(src, dst, save_sem.at[len(saves)])
        cp.start()
        saves.append(cp)

    links = [Links(send, recv, sent) for send, recv in zip(sems[::2], sems[1::2])]

    loads = [pltpu.make_async_copy(s, d, load_sem.at[k]) for k, (s, d) in enumerate(
        [(tok_hbm, x_all.at[z, y, x, c]), (dout_hbm, g_all.at[z, y, x, c]), (tok_hbm, tok), (ids_hbm, ids), (wg_hbm, wg), (dout_hbm, dout), (w1_hbm, w1), (w2_hbm, w2)])]
    for ld in loads:
        ld.start()
    peers = [dev(lax.rem(z + d, nz), y, x, c) for d in range(1, nz)]
    for d in (1, 2, 3):
        peers.append(dev(z, lax.rem(y + d, ny), x, c))
        peers.append(dev(z, y, lax.rem(x + d, nx), c))
    peers.append(dev(z, y, x, 1 - c))
    meet(peers)

    full = slice(None)

    def along_z(link, ref):
        return [link.go(ref.at[z, y, x, c], ref.at[z, y, x, c], dev(lax.rem(z + d, nz), y, x, c)) for d in range(1, nz)]

    def gather(i, held, zcopies):
        link = links[i]
        yx = i == 0
        p0, q0 = (y, x) if yx else (x, y)
        low, high = pl.ds(0, nz // 2), pl.ds(nz // 2, nz // 2)

        def at(zs, p, q):
            return held.at[zs, p, q, c] if yx else held.at[zs, q, p, c]

        def to(p, q):
            return dev(z, p, q, c) if yx else dev(z, q, p, c)

        def go(ref, to):
            return link.go(ref, ref, to)

        def step(v, d):
            return lax.rem(v + d, 4)

        cross = []

        def over(p, q):
            cross.append(go(at(full, p, q), dev(z, y, x, 1 - c)))

        for cp in zcopies:
            yield
            cp.wait_recv()
        pm, pp, po = step(p0, 3), step(p0, 1), step(p0, 2)
        qm, qp, qo = step(q0, 3), step(q0, 1), step(q0, 2)
        p_up = go(at(full, p0, q0), to(pp, q0))
        p_dn = go(at(full, p0, q0), to(pm, q0))
        qs, relays = [], []

        def spread(p):
            qs.append((p, go(at(full, p, q0), to(p0, qp)), go(at(full, p, q0), to(p0, qm))))
            over(p, q0)

        def relay(i):
            p, up, dn = qs[i]
            up.wait_recv()
            r_up = go(at(low, p, qm), to(p0, qp))
            over(p, qm)
            dn.wait_recv()
            r_dn = go(at(high, p, qp), to(p0, qm))
            over(p, qp)
            relays.append((p, r_up, r_dn))

        spread(p0)
        yield
        p_up.wait_recv()
        f_up = go(at(low, pm, q0), to(pp, q0))
        yield
        p_dn.wait_recv()
        f_dn = go(at(high, pp, q0), to(pm, q0))
        spread(pm)
        spread(pp)
        yield
        relay(0)
        yield
        f_up.wait_recv()
        f_dn.wait_recv()
        spread(po)
        for i in range(1, 5):
            yield
            if i < 4:
                relay(i)
            p, r_up, r_dn = relays[i - 1]
            r_up.wait_recv()
            r_dn.wait_recv()
            over(p, qo)
        for cp in cross:
            yield
            cp.wait_recv()

    def gather_rows(link, held, order):
        have = [z, y, x, c]
        for axis in order:
            size = (nz, ny, nx, nc)[axis]
            part = held.at[tuple(have)]
            copies = []
            for d in range(1, size):
                there = [z, y, x, c]
                there[axis] = lax.rem(there[axis] + d, size)
                copies.append(link.go(part, part, dev(*there)))
            have[axis] = full
            for cp in copies:
                yield
                cp.wait_recv()

    loads[0].wait()
    z_tok = along_z(links[0], x_all)
    loads[1].wait()
    z_dout = along_z(links[1], g_all)
    for ld in loads[2:5]:
        ld.wait()
    row[...] = choice_row(tok[...], ids[...], wg[...])
    place = pltpu.make_async_copy(row, m_land.at[z, y, x, c], keep_sem.at[0])
    place.start()
    place.wait()
    take_turns([gather(0, x_all, z_tok), gather(1, g_all, z_dout), gather_rows(links[2], m_land, (0, 1, 2, 3))])

    def flatten(zz, carry):
        for k in range(ny * nx * nc):
            m_all[pl.ds(zz * (ny * nx * nc) + k, 1), :] = m_land[zz, k // (nx * nc), k // nc % nx, k % nc]
        return carry

    lax.fori_loop(0, nz, flatten, 0)
    for ld in loads[5:]:
        ld.wait()
    save(2)
    save(3)

    me = lax.axis_index('ep').astype(F32)
    code = m_all[...]
    left = jnp.where((iota(code.shape, 1) < 64) & (code >= 256.0), code - 256.0, 999.0)
    found = []
    for _ in range(3):
        best = jnp.min(jnp.min(left, axis=0, keepdims=True), axis=1, keepdims=True)
        left = jnp.where(left == best, 999.0, left)
        found.append(jnp.broadcast_to(best, (1, 128)))
    hot_ref[...] = jnp.concatenate(found + [jnp.full((5, 128), 999.0, F32)], axis=0)
    steps = 4 if nz == 8 else 1
    per = nz // steps
    n_quad = per * ny * nx * nc // 4
    n_pair = n_quad // 2
    n_slot = n_pair * 8 * CAP

    def run_expert(i, carry):
        c0, c1, g0, g1 = (pair_rows(token_lanes(m_all, k, pl.multiple_of(4 * n_quad * i, 4 * n_quad), n_quad)) for k in range(4))
        hit0, hit1 = plain_id(c0) == me, plain_id(c1) == me
        hit = (hit0 | hit1).astype(F32)
        gate = jnp.where(hit0, g0, 0.0) + jnp.where(hit1, g1, 0.0)
        before, after = iota((256, 256), 0), iota((256, 256), 1)
        tri = ((before < after) & (before // 32 == after // 32)).astype(F32).astype(BF16)
        rank = dot(hit.astype(BF16), tri, 1, 0)
        src = (iota((n_pair, 256), 1) // 32).astype(F32)
        key = jnp.where(hit > 0.0, src * CAP + rank, -1.0)
        slot = iota((8 * CAP, 256), 0).astype(F32)
        xs, dys = [], []
        for p in range(n_pair):
            sel = (slot == key[p:p + 1]).astype(F32)
            g = jnp.sum(sel * gate[p:p + 1], axis=1, keepdims=True)
            sel = sel.astype(BF16)
            xs.append(dot(sel, x_all[i * per + p // ny, p % ny].reshape(256, 256), 1, 0))
            dys.append(g * dot(sel, g_all[i * per + p // ny, p % ny].reshape(256, 256), 1, 0))
        places = [(cc, xx, yy, zz) for cc in range(nc) for xx in range(nx) for yy in range(ny) for zz in range(per)]

        def by_place(parts):
            return jnp.concatenate([parts[zz * ny + yy][8 * (xx * nc + cc):8 * (xx * nc + cc + 1)] for cc, xx, yy, zz in places], axis=0).astype(BF16)

        xs, dys = by_place(xs), by_place(dys)
        h, slope = gelu_parts(dot(xs, w1[...], 1, 0))
        h = h.astype(BF16)
        here = pl.ds(pl.multiple_of(i * n_slot, n_slot), n_slot)
        xs_ref[here], dys_ref[here], h_ref[here] = xs, dys, h
        yv = dot(h, w2[...], 1, 0)
        da = (dot(dys, w2[...], 1, 1) * slope).astype(BF16)
        da_ref[here] = da
        dxv = dot(da, w1[...], 1, 1)
        for k, (cc, xx, yy, zz) in enumerate(places):
            for half in range(2):
                lanes = slice(128 * half, 128 * (half + 1))
                rows[half][cc, xx, yy, i * per + zz] = yv[8 * k:8 * (k + 1), lanes].astype(BF16)
                rows[2 + half][cc, xx, yy, i * per + zz] = dxv[8 * k:8 * (k + 1), lanes].astype(BF16)
        return carry

    lax.fori_loop(0, steps, run_expert, 0)

    def back(i):
        h = rows[i]
        other, near, via, out2, via2, in2, out3, hot_land, cold_land = works[9 * i:9 * i + 9]
        go = links[3 + i].go
        x_first = i % 2 == 0
        a, b = (x, y) if x_first else (y, x)

        def to(a, b):
            return dev(z, b, a, c) if x_first else dev(z, a, b, c)

        def index(lead, a, bs):
            return lead + ((a, bs) if x_first else (bs, a))

        def step(v, d):
            return lax.rem(v + d, 4)

        up, dn, far = step(a, 1), step(a, 3), step(a, 2)
        lo, hi = pl.ds(0, 2), pl.ds(2, 2)
        cross = go(h.at[1 - c], other, dev(z, y, x, 1 - c))

        def spread(ref, lead, e):
            return [go(ref.at[index(lead, far, lo)], via.at[0, e], to(up, b)), go(ref.at[index(lead, far, hi)], via.at[1, e], to(dn, b)),
                    go(ref.at[index(lead, up, full)], near.at[a, e], to(up, b)), go(ref.at[index(lead, dn, full)], near.at[a, e], to(dn, b))]

        def relay(cps, e):
            cps[0].wait_recv()
            r_up = go(via.at[0, e], near.at[dn, e, lo], to(up, b))
            cps[1].wait_recv()
            r_dn = go(via.at[1, e], near.at[up, e, hi], to(dn, b))
            return [cps[2], cps[3], r_up, r_dn]

        own = spread(h, (c,), c)
        yield
        cross.wait_recv()
        his = spread(other, (), 1 - c)
        yield
        waits = relay(own, c)
        yield
        waits += relay(his, 1 - c)
        yield
        for cp in waits:
            cp.wait_recv()

        def expert(s, e):
            return ((z * ny + y) * nx + s) * nc + e if x_first else ((z * ny + s) * nx + x) * nc + e

        places = [(step(a, d), e) for d in range(4) for e in (c, 1 - c)]
        is_hot = [[(hot_ref[j:j + 1, :] == expert(s, e).astype(F32)).astype(F32) for s, e in places] for j in range(3)]
        wide = lambda v: jnp.broadcast_to(v, (8, 128))
        weight = [[wide(v).astype(BF16) for v in r] for r in is_hot]
        line = iota((8, 128), 0)
        mine = [(wide(is_hot[0][k] + is_hot[1][k] + is_hot[2][k]) < 0.5) & (line == s * nc + e) for k, (s, e) in enumerate(places)]

        def squeeze(bb, carry):
            parts = [h[index((c,), a, bb)], other[index((), a, bb)]] + [near[s, e, bb] for s, e in places[2:]]
            for j in range(3):
                out2[bb, j] = sum(parts[k] * weight[j][k] for k in range(8))
            singles = jnp.zeros((nz, 8, 128), F32)
            for k in range(8):
                singles = jnp.where(mine[k], jnp.sum(parts[k].astype(F32), axis=1, keepdims=True), singles)
            out2[bb, 3] = singles.astype(BF16)
            return carry

        lax.fori_loop(0, 4, squeeze, 0)
        up, dn, far = step(b, 1), step(b, 3), step(b, 2)
        lo, hi = pl.ds(0, nz // 2), pl.ds(nz // 2, nz // 2)
        f_up, f_dn = go(out2.at[far, :, lo], via2.at[0], to(a, up)), go(out2.at[far, :, hi], via2.at[1], to(a, dn))
        n_up, n_dn = go(out2.at[up], in2.at[b], to(a, up)), go(out2.at[dn], in2.at[b], to(a, dn))
        in2[b] = out2[b]
        yield
        f_up.wait_recv()
        r_up = go(via2.at[0], in2.at[dn, :, lo], to(a, up))
        f_dn.wait_recv()
        r_dn = go(via2.at[1], in2.at[up, :, hi], to(a, dn))
        yield
        for cp in (n_up, n_dn, r_up, r_dn):
            cp.wait_recv()
        for j in range(3):
            out3[:, j] = (in2[0, j] + in2[1, j]) + (in2[2, j] + in2[3, j])
        last = []
        for d in range(1, nz):
            zz = lax.rem(z + d, nz)
            last.append(go(in2.at[:, 3, zz], cold_land.at[z], dev(zz, y, x, c)))
        for d in range(1, nz):
            zz = lax.rem(z + d, nz)
            last.append(go(out3.at[zz], hot_land.at[z], dev(zz, y, x, c)))
        cold_land[z] = in2[:, 3, z]
        hot_land[z] = out3[z]
        yield
        for cp in last:
            cp.wait_recv()

    def weight_grad(k):
        if k % 2 == 0:
            part = slice(w2.shape[0] // 4 * (k // 2), w2.shape[0] // 4 * (k // 2 + 1))
            g2_ref[part, :] = dot(h_ref[:, part], dys_ref[...], 0, 0)
            save(6, (part, full))
        else:
            part = slice(w1.shape[1] // 4 * (k // 2), w1.shape[1] // 4 * (k // 2 + 1))
            g1_ref[:, part] = dot(xs_ref[...], da_ref[:, part], 0, 0)
            save(5, (full, part))

    ys, dxs = [back(0), back(1)], [back(2), back(3)]

    def advance(plans):
        for g in plans:
            next(g, None)

    todo = list(range(8))

    for turn in 'y x w y x ww yy w xx y w x y w y w xx w y'.replace(' ', ''):
        if turn == 'w':
            weight_grad(todo.pop(0))
        else:
            advance(ys if turn == 'y' else dxs)

    r0, r1 = ids[0:1].astype(F32), ids[1:2].astype(F32)
    i0, i1 = as_col(r0), as_col(r1)
    tokens = tok[...]
    g0, g1 = gates(tokens, i0, i1, wg[...])
    n_tok = tok.shape[0]
    earlier = iota((n_tok, n_tok), 1) < iota((n_tok, n_tok), 0)
    n_exp = wg.shape[1]

    def where_from(i):
        rank = jnp.sum(jnp.where(earlier & ((i == r0) | (i == r1)), 1.0, 0.0), axis=1, keepdims=True)
        slot = jnp.full((n_tok, 1), -1.0, F32)
        for j in range(3):
            slot = jnp.where(i == hot_ref[j:j + 1, 0:1], CAP * j + rank, slot)
        e = i.astype(jnp.int32)
        core, xx, yy, zz = e % nc, (e // nc) % nx, (e // (nc * nx)) % ny, e // (nc * nx * ny)
        lane, single = iota((n_tok, n_exp), 1), slot < 0.0
        pick = lambda m: m.astype(F32).astype(BF16)
        return pick(iota((n_tok, 32), 1).astype(F32) == slot), (pick((lane == e) & single), pick((lane == ((zz * nx + xx) * ny + yy) * nc + core) & single))

    chosen = [where_from(i0), where_from(i1)]

    def rows_of(kind):
        parts = []
        for half in range(2):
            hot_land, cold_land = works[9 * (kind + half) + 7:9 * (kind + half) + 9]
            hot = jnp.sum(hot_land[...].astype(F32), axis=0).reshape(24, 128)
            hot = jnp.concatenate([hot, jnp.zeros((8, 128), F32)], axis=0).astype(BF16)
            cold = cold_land[...].astype(F32).reshape(n_exp, 128).astype(BF16)
            parts.append([dot(by_slot, hot, 1, 0) + dot(by_place[half], cold, 1, 0) for by_slot, by_place in chosen])
        return [jnp.concatenate([parts[0][k], parts[1][k]], axis=1) for k in range(2)]

    y0, y1 = rows_of(0)
    out_ref[...] = (g0 * y0 + g1 * y1).astype(BF16)
    save(0)
    grad = dout[...].astype(F32)
    dg0, dg1 = (jnp.sum(grad * v, axis=1, keepdims=True) for v in (y0, y1))
    mean = g0 * dg0 + g1 * dg1
    d0, d1 = ((g * (dg - mean)).astype(BF16).astype(F32) for g, dg in ((g0, dg0), (g1, dg1)))
    d_row[...] = jnp.concatenate([as_row(d0), as_row(d1), jnp.zeros((1, 2 * n_tok), F32)], axis=1)
    place = pltpu.make_async_copy(d_row, d_land.at[z, y, x, c], keep_sem.at[1])
    place.start()
    place.wait()
    d_plan = gather_rows(links[7], d_land, (1, 2, 0, 3))
    next(d_plan)
    advance(dxs)
    expert = iota((n_tok, n_exp), 1).astype(F32)
    spread = jnp.where(expert == i0, d0, jnp.where(expert == i1, d1, 0.0)).astype(BF16)
    through_gate = dot(spread, wg[...], 1, 1)
    for _ in range(6):
        next(d_plan)
    advance(dxs)
    dx0, dx1 = rows_of(2)
    gx_ref[...] = (dx0 + dx1 + through_gate).astype(BF16)
    save(1)
    take_turns([d_plan])
    save(4)
    for cp in sent:
        cp.wait_send()
    for cp in saves:
        cp.wait()


def block_call(dims, tokens, grad_out, ids, w_gate, w1, w2):
    nz, ny, nx, nc = dims
    d_model, d_hidden = w1.shape
    n_tok = tokens.shape[0]
    n_dev = nz * ny * nx * nc
    n_row = n_dev * CAP
    tile = (CAP, 128)
    hbm = pl.BlockSpec(memory_space=pltpu.HBM)
    out = jax.ShapeDtypeStruct
    work = [(4, 4, nz), (4, 2, 4, nz), (2, 2, 2, nz), (4, 4, nz), (2, 4, nz // 2), (4, 4, nz), (nz, 3), (nz, 3), (nz, 4)]
    counts = [nz - 1 + 4 + 16 + 16] * 2 + [nz - 1 + 3 + 3 + 1] + [1 + 12 + 6 + 2 * (nz - 1)] * 4 + [nz - 1 + 3 + 3 + 1]
    sems = []
    for k in counts:
        sems += [pltpu.SemaphoreType.DMA((k,))] * 2
    results = [(tokens.shape, BF16), (tokens.shape, BF16), (dims + tokens.shape, BF16), ((n_dev, 128), F32), (dims + (1, 128), F32),
               ((d_model, d_hidden), F32), ((d_hidden, d_model), F32)]
    row, n_dma = (1, 128), 16
    kept = [(tokens.shape, BF16), (tokens.shape, BF16), (ids.shape, jnp.int32), (w_gate.shape, BF16), (w1.shape, BF16), (w2.shape, BF16), (row, F32), (dims + row, F32),
            (dims + tokens.shape, BF16), ((n_row, d_model), BF16), ((n_row, d_model), BF16), ((n_row, d_hidden), BF16), ((n_row, d_hidden), BF16), (tile, F32), (row, F32)]
    return pl.pallas_call(
        functools.partial(block_kernel, dims, (6, len(results), len(results), len(kept), 4, 4 * len(work), 3, len(sems))),
        out_shape=[out(*r) for r in results],
        in_specs=[hbm] * 6,
        out_specs=[hbm] * 7,
        scratch_shapes=[pltpu.VMEM(*r) for r in results + kept] + [pltpu.VMEM((nc, nx, ny, nz) + tile, BF16)] * 4 + [pltpu.VMEM(w + tile, BF16) for w in work] * 4
        + [pltpu.SemaphoreType.DMA((n_dma,))] * 3 + sems,
        compiler_params=pltpu.CompilerParams(collective_id=0, has_side_effects=True, vmem_limit_bytes=VMEM_LIMIT),
        name='block',
    )(tokens, grad_out, ids, w_gate, w1, w2)


VMEM_LIMIT = 67043328


def gate_kernel(x_ref, m_ref, d_ref, g1_ref, g2_ref, out_ref, gx_ref, o_ref, o1_ref, o2_ref, o3_ref, o4_ref, acc):
    o1_ref[...] = g1_ref[...]
    o2_ref[...] = g2_ref[...]
    o3_ref[...] = out_ref[...]
    o4_ref[...] = gx_ref[...]
    n_quad = m_ref.shape[0] // 4
    i0, i1 = (plain_id(pair_rows(token_lanes(m_ref, k, 0, n_quad))) for k in range(2))
    d0, d1 = (pair_rows(token_lanes(d_ref, k, 0, n_quad)) for k in range(2))
    expert = iota((acc.shape[0], 256), 0).astype(F32)

    @pl.when(pl.program_id(0) == 0)
    def _():
        acc[...] = jnp.zeros_like(acc)

    total = acc[...]
    for p in range(n_quad // 2):
        q = slice(p, p + 1)
        spread = jnp.where(expert == i0[q], d0[q], jnp.where(expert == i1[q], d1[q], 0.0))
        total += dot(spread.astype(BF16), x_ref[256 * p:256 * (p + 1)], 1, 0)
    acc[...] = total

    @pl.when(pl.program_id(0) == pl.num_programs(0) - 1)
    def _():
        o_ref[...] = total.T


def gate_grad(x_all, m_all, d_all, *through):
    n_src = m_all.shape[0]
    steps = 4 if n_src == 256 else 2
    d_model = x_all.shape[1]
    part = lambda shape: pl.BlockSpec((shape[0] // steps,) + shape[1:], lambda i: (i, 0))
    whole = lambda shape: pl.BlockSpec(shape, lambda i: (0, 0))
    specs = [part(v.shape) if v.shape[0] >= 64 else whole(v.shape) for v in through]
    out = jax.ShapeDtypeStruct
    return pl.pallas_call(
        gate_kernel,
        grid=(steps,),
        out_shape=[out((d_model, n_src), F32)] + [out(v.shape, v.dtype) for v in through],
        in_specs=[part(x_all.shape), part(m_all.shape), part(d_all.shape)] + specs,
        out_specs=[whole((d_model, n_src))] + specs,
        scratch_shapes=[pltpu.VMEM((n_src, d_model), F32)],
        compiler_params=pltpu.CompilerParams(dimension_semantics=('arbitrary',), vmem_limit_bytes=VMEM_LIMIT),
        name='gate_grad',
    )(x_all, m_all, d_all, *through)


def local_block(dims, tokens, grad_out, expert_ids, w_gate, w_in, w_out):
    n_exp = w_gate.shape[1]
    y_out, grad_x, x_all, m_all, d_all, g1, g2 = block_call(dims, tokens, grad_out, expert_ids.T, w_gate, w_in[0], w_out[0])
    grad_w_gate, g1, g2, y_out, grad_x = gate_grad(x_all.reshape(-1, tokens.shape[1]), m_all, d_all.reshape(n_exp, 128), g1, g2, y_out, grad_x)
    return y_out, grad_x, g1[None], g2[None], grad_w_gate


def solution(mesh):
    dims = (8, 4, 4, 2)
    return jax.shard_map(functools.partial(local_block, dims), mesh=mesh, in_specs=(P('ep'), P('ep'), P('ep'), P(), P('ep'), P('ep')), out_specs=(P('ep'), P('ep'), P('ep'), P('ep'), P()), check_vma=False)
```

```python
import functools
import itertools

import jax
import jax.numpy as jnp
from jax import lax
from jax.experimental import pallas as pl
from jax.experimental.pallas import tpu as pltpu
from jax.sharding import PartitionSpec as P

MESH = pl.DeviceIdType.MESH
F32 = jnp.float32
BF16 = jnp.bfloat16
CAP = 8


def coords(dims):
    nz, ny, nx, nc = dims
    me = lax.axis_index('ep')
    c = lax.rem(me, nc)
    x = lax.rem(me // nc, nx)
    y = lax.rem(me // (nc * nx), ny)
    z = me // (nc * nx * ny)

    def dev(z, y, x, c):
        return (((z * ny + y) * nx + x) * nc + c,)

    return z, y, x, c, dev


def meet(peers):
    barrier = pltpu.get_barrier_semaphore()
    for peer in peers:
        pl.semaphore_signal(barrier, inc=1, device_id=peer, device_id_type=MESH)
    pl.semaphore_wait(barrier, len(peers))


def dot(a, b, ca, cb):
    return lax.dot_general(a, b, (((ca,), (cb,)), ((), ())), preferred_element_type=F32)


def iota(shape, axis):
    return lax.broadcasted_iota(jnp.int32, shape, axis)


def as_row(col):
    n = col.shape[0]
    return jnp.sum(jnp.where(iota((n, n), 0) == iota((n, n), 1), col, 0.0), axis=0, keepdims=True)


def as_col(row):
    n = row.shape[1]
    return jnp.sum(jnp.where(iota((n, n), 0) == iota((n, n), 1), row, 0.0), axis=1, keepdims=True)


def gates(tok, i0, i1, w_gate):
    logits = dot(tok, w_gate, 1, 0)
    expert = iota(logits.shape, 1).astype(F32)
    l0, l1 = (jnp.sum(jnp.where(expert == i, logits, 0.0), axis=1, keepdims=True) for i in (i0, i1))
    top = jnp.maximum(l0, l1)
    p0, p1 = jnp.exp(l0 - top), jnp.exp(l1 - top)
    total = p0 + p1
    return p0 / total, p1 / total


def choice_row(tok, ids, w_gate):
    r0, r1 = ids[0:1].astype(F32), ids[1:2].astype(F32)
    i0, i1 = as_col(r0), as_col(r1)
    g0, g1 = gates(tok, i0, i1, w_gate)

    def code(i):
        n = jnp.sum((i == r0).astype(F32) + (i == r1).astype(F32), axis=1, keepdims=True)
        return as_row(jnp.where(n > 1.5, i + 256.0, i))

    return jnp.concatenate([code(i0), code(i1), as_row(g0), as_row(g1)], axis=1)


def gelu_parts(a):
    k = 0.7978845608028654
    sq = a * a
    t = jnp.tanh(a * (k + (k * 0.044715) * sq))
    half = 0.5 + 0.5 * t
    slope = half + (0.5 * a) * (1.0 - t * t) * (k + (3 * k * 0.044715) * sq)
    return a * half, slope


def token_lanes(ref, k, start, n):
    lane = iota((n, 128), 1) // 32
    out = jnp.zeros((n, 128), F32)
    for j in range(4):
        r = ref[pl.ds(start + j, n, stride=4), :]
        out = jnp.where(lane == j, r if j == k else pltpu.roll(r, 32 * (j - k) % 128, 1), out)
    return out


def pair_rows(v):
    return jnp.concatenate([jnp.concatenate([v[2 * i:2 * i + 1], v[2 * i + 1:2 * i + 2]], axis=1) for i in range(v.shape[0] // 2)], axis=0)


def plain_id(code):
    return jnp.where(code >= 256.0, code - 256.0, code)


class Links:
    def __init__(self, send, recv, sent):
        self.send, self.recv, self.sent, self.k = send, recv, sent, 0

    def go(self, src, dst, to):
        cp = pltpu.make_async_remote_copy(src_ref=src, dst_ref=dst, send_sem=self.send.at[self.k], recv_sem=self.recv.at[self.k], device_id=to, device_id_type=MESH)
        self.k += 1
        cp.start()
        self.sent.append(cp)
        return cp


def take_turns(plans):
    live = list(plans)
    while live:
        for g in list(live):
            if next(g, 'end') == 'end':
                live.remove(g)


def block_kernel(dims, sizes, *refs):
    nz, ny, nx, nc = dims
    refs = iter(refs)
    refs = [list(itertools.islice(refs, n)) for n in sizes]
    (tok_hbm, dout_hbm, ids_hbm, wg_hbm, w1_hbm, w2_hbm), outs, held, kept, rows, works, (load_sem, keep_sem, save_sem), sems = refs
    out_ref, gx_ref, x_all, m_all, d_land, g1_ref, g2_ref = held
    tok, dout, ids, wg, w1, w2, row, m_land, g_all, xs_ref, dys_ref, h_ref, da_ref, slope_ref, hot_ref, d_row = kept
    z, y, x, c, dev = coords(dims)
    sent, saves = [], []

    def save(k, part=None):
        src, dst = (held[k], outs[k]) if part is None else (held[k].at[part], outs[k].at[part])
        cp = pltpu.make_async_copy(src, dst, save_sem.at[len(saves)])
        cp.start()
        saves.append(cp)

    links = iter([Links(send, recv, sent) for send, recv in zip(sems[::2], sems[1::2])])

    loads = [pltpu.make_async_copy(s, d, load_sem.at[k]) for k, (s, d) in enumerate(
        [(tok_hbm, x_all.at[z, y, x, c]), (dout_hbm, g_all.at[z, y, x, c]), (tok_hbm, tok), (ids_hbm, ids), (wg_hbm, wg), (dout_hbm, dout), (w1_hbm, w1), (w2_hbm, w2)])]
    for ld in loads:
        ld.start()
    peers = [dev(lax.rem(z + d, nz), y, x, c) for d in range(1, nz)]
    for d in (1, 2, 3):
        peers.append(dev(z, lax.rem(y + d, ny), x, c))
        peers.append(dev(z, y, lax.rem(x + d, nx), c))
    mate = dev(z, y, x, 1 - c)
    peers.append(mate)
    meet(peers)

    full = slice(None)

    def step(v, d, m=4):
        return lax.rem(v + d, m)

    def by_lines(link, ref, rows, x_last):
        p0, q0 = (y, x) if x_last else (x, y)
        low, high = pl.ds(0, nz // 2), pl.ds(nz // 2, nz // 2)

        def at(zs, p, q):
            return ref.at[(zs, p, q, c, rows) if x_last else (zs, q, p, c, rows)]

        def go(part, p, q):
            return link.go(part, part, dev(z, p, q, c) if x_last else dev(z, q, p, c))

        cross = []

        def over(q):
            part = at(full, full, q)
            cross.append(link.go(part, part, mate))

        own = at(z, p0, q0)
        first = [link.go(own, own, dev(step(z, d, nz), y, x, c)) for d in range(1, nz)]
        yield
        for cp in first:
            cp.wait_recv()
        pm, pp, po = step(p0, 3), step(p0, 1), step(p0, 2)
        qm, qp, qo = step(q0, 3), step(q0, 1), step(q0, 2)
        qs, relays = [], []

        def spread(p):
            part = at(full, p, q0)
            qs.append((p, go(part, p0, qp), go(part, p0, qm)))

        def relay(i):
            p, up, dn = qs[i]
            up.wait_recv()
            relays.append(go(at(low, p, qm), p0, qp))
            dn.wait_recv()
            relays.append(go(at(high, p, qp), p0, qm))

        p_up, p_dn = go(at(full, p0, q0), pp, q0), go(at(full, p0, q0), pm, q0)
        spread(p0)
        yield
        p_up.wait_recv()
        f_up = go(at(low, pm, q0), pp, q0)
        p_dn.wait_recv()
        f_dn = go(at(high, pp, q0), pm, q0)
        spread(pm)
        spread(pp)
        yield
        relay(0)
        yield
        f_up.wait_recv()
        f_dn.wait_recv()
        spread(po)
        over(q0)
        for i in range(1, 4):
            yield
            relay(i)
        over(qm)
        over(qp)
        yield
        for cp in relays:
            cp.wait_recv()
        over(qo)
        yield
        for cp in cross:
            cp.wait_recv()

    def by_planes(link, ref, rows):
        go = lambda part, *to: link.go(part, part, dev(*to))
        at = lambda zz, ys=full: ref.at[zz, ys, full, c, rows]
        own = ref.at[z, y, x, c, rows]
        xs = [go(own, z, y, step(x, d), c) for d in range(1, nx)]
        yield
        for cp in xs:
            cp.wait_recv()
        line = ref.at[z, y, full, c, rows]
        ys = [go(line, z, step(y, d), x, c) for d in range(1, ny)]
        yield
        for cp in ys:
            cp.wait_recv()
        cross = []

        def over(*planes):
            for zz in planes:
                cross.append(link.go(at(zz), at(zz), mate))

        half = nz // 2
        lower, upper = pl.ds(0, ny // 2), pl.ds(ny // 2, ny // 2)

        def pair(d):
            a, b = (full, full) if d + 1 < half else (lower, upper)
            return go(at(step(z, nz - d, nz), a), step(z, 1, nz), y, x, c), go(at(step(z, d, nz), b), step(z, nz - 1, nz), y, x, c)

        up, dn = pair(0)
        over(z)
        for d in range(1, half + 1):
            yield
            up.wait_recv()
            dn.wait_recv()
            if d < half:
                up, dn = pair(d)
                over(step(z, d, nz), step(z, nz - d, nz))
            else:
                over(step(z, d, nz))
        yield
        for cp in cross:
            cp.wait_recv()

    def gather_rows(link, held, order):
        have = [z, y, x, c]
        for axis in order:
            size = (nz, ny, nx, nc)[axis]
            part = held.at[tuple(have)]
            copies = []
            for d in range(1, size):
                there = [z, y, x, c]
                there[axis] = lax.rem(there[axis] + d, size)
                copies.append(link.go(part, part, dev(*there)))
            have[axis] = full
            yield
            for cp in copies:
                cp.wait_recv()

    def advance(plans):
        for g in plans:
            next(g, None)

    def streams(ref, cuts):
        a, b, c, d = cuts
        return [by_lines(next(links), ref, slice(a, b), True), by_lines(next(links), ref, slice(b, c), False), by_planes(next(links), ref, slice(c, d))]

    tok_plans, grad_plans = streams(x_all, (0, 16, 24, 32)), streams(g_all, (0, 8, 24, 32))
    loads[0].wait()
    advance(tok_plans)
    loads[1].wait()
    advance(grad_plans)
    for ld in loads[2:5]:
        ld.wait()
    row[...] = choice_row(tok[...], ids[...], wg[...])
    place = pltpu.make_async_copy(row, m_land.at[z, y, x, c], keep_sem.at[0])
    place.start()
    place.wait()
    row_plan = [gather_rows(next(links), m_land, range(4))]
    for turn in FIRST:
        advance({'t': tok_plans, 'g': grad_plans, 'm': row_plan}[turn])
    take_turns(row_plan)
    take_turns(tok_plans)

    def flatten(zz, carry):
        for k in range(ny * nx * nc):
            m_all[pl.ds(zz * (ny * nx * nc) + k, 1), :] = m_land[zz, k // (nx * nc), k // nc % nx, k % nc]
        return carry

    lax.fori_loop(0, nz, flatten, 0)
    for ld in loads[5:]:
        ld.wait()

    me = lax.axis_index('ep').astype(F32)
    code = m_all[...]
    left = jnp.where((iota(code.shape, 1) < 64) & (code >= 256.0), code - 256.0, 999.0)
    found = []
    for _ in range(3):
        best = jnp.min(jnp.min(left, axis=0, keepdims=True), axis=1, keepdims=True)
        left = jnp.where(left == best, 999.0, left)
        found.append(jnp.broadcast_to(best, (1, 128)))
    hot_ref[...] = jnp.concatenate(found + [jnp.full((5, 128), 999.0, F32)], axis=0)
    steps = 4 if nz == 8 else 1
    per = nz // steps
    n_quad = per * ny * nx * nc // 4
    n_pair = n_quad // 2
    n_slot = n_pair * 8 * CAP

    places = [(cc, xx, yy, zz) for cc in range(nc) for xx in range(nx) for yy in range(ny) for zz in range(per)]

    def select(i, ref, with_gate):
        c0, c1, g0, g1 = (pair_rows(token_lanes(m_all, k, pl.multiple_of(4 * n_quad * i, 4 * n_quad), n_quad)) for k in range(4))
        hit0, hit1 = plain_id(c0) == me, plain_id(c1) == me
        hit = (hit0 | hit1).astype(F32)
        gate = jnp.where(hit0, g0, 0.0) + jnp.where(hit1, g1, 0.0)
        before, after = iota((256, 256), 0), iota((256, 256), 1)
        tri = ((before < after) & (before // 32 == after // 32)).astype(F32).astype(BF16)
        rank = dot(hit.astype(BF16), tri, 1, 0)
        src = (iota((n_pair, 256), 1) // 32).astype(F32)
        key = jnp.where(hit > 0.0, src * CAP + rank, -1.0)
        slot = iota((8 * CAP, 256), 0).astype(F32)
        parts = []
        for p in range(n_pair):
            sel = (slot == key[p:p + 1]).astype(F32)
            v = dot(sel.astype(BF16), ref[i * per + p // ny, p % ny].reshape(256, 256), 1, 0)
            parts.append(v * jnp.sum(sel * gate[p:p + 1], axis=1, keepdims=True) if with_gate else v)
        return jnp.concatenate([parts[zz * ny + yy][CAP * (xx * nc + cc):CAP * (xx * nc + cc + 1)] for cc, xx, yy, zz in places], axis=0).astype(BF16)

    def put(i, v, to):
        for k, (cc, xx, yy, zz) in enumerate(places):
            for half in range(2):
                to[half][cc, xx, yy, i * per + zz] = v[CAP * k:CAP * (k + 1), 128 * half:128 * (half + 1)].astype(BF16)

    def forward(i):
        here = pl.ds(i * n_slot, n_slot)
        xs = select(i, x_all, False)
        h, slope = gelu_parts(dot(xs, w1[...], 1, 0))
        h = h.astype(BF16)
        xs_ref[here], h_ref[here], slope_ref[here] = xs, h, slope
        put(i, dot(h, w2[...], 1, 0), rows[:2])

    def backward(i):
        here = pl.ds(i * n_slot, n_slot)
        dys = select(i, g_all, True)
        da = (dot(dys, w2[...], 1, 1) * slope_ref[here]).astype(BF16)
        dys_ref[here], da_ref[here] = dys, da
        put(i, dot(da, w1[...], 1, 1), rows[2:])

    for i in range(steps):
        forward(i)
        advance(grad_plans)

    def back(i):
        h = rows[i]
        other, near, via, out2, via2, in2, out3, hot_land, cold_land = works[9 * i:9 * i + 9]
        go = next(links).go
        x_first = i % 2 == 0
        a, b = (x, y) if x_first else (y, x)

        def to(a, b):
            return dev(z, b, a, c) if x_first else dev(z, a, b, c)

        def index(lead, a, bs):
            return lead + ((a, bs) if x_first else (bs, a))

        up, dn, far = step(a, 1), step(a, 3), step(a, 2)
        lo, hi = pl.ds(0, 2), pl.ds(2, 2)
        cross = go(h.at[1 - c], other, mate)

        def spread(ref, lead, e):
            return [go(ref.at[index(lead, far, lo)], via.at[0, e], to(up, b)), go(ref.at[index(lead, far, hi)], via.at[1, e], to(dn, b)),
                    go(ref.at[index(lead, up, full)], near.at[a, e], to(up, b)), go(ref.at[index(lead, dn, full)], near.at[a, e], to(dn, b))]

        def relay(cps, e):
            cps[0].wait_recv()
            r_up = go(via.at[0, e], near.at[dn, e, lo], to(up, b))
            cps[1].wait_recv()
            r_dn = go(via.at[1, e], near.at[up, e, hi], to(dn, b))
            return [cps[2], cps[3], r_up, r_dn]

        own = spread(h, (c,), c)
        yield
        cross.wait_recv()
        his = spread(other, (), 1 - c)
        yield
        waits = relay(own, c)
        yield
        waits += relay(his, 1 - c)
        yield
        for cp in waits:
            cp.wait_recv()

        def expert(s, e):
            return ((z * ny + y) * nx + s) * nc + e if x_first else ((z * ny + s) * nx + x) * nc + e

        places = [(step(a, d), e) for d in range(4) for e in (c, 1 - c)]
        is_hot = [[(hot_ref[j:j + 1, :] == expert(s, e).astype(F32)).astype(F32) for s, e in places] for j in range(3)]
        wide = lambda v: jnp.broadcast_to(v, (8, 128))
        weight = [[wide(v).astype(BF16) for v in r] for r in is_hot]
        line = iota((8, 128), 0)
        mine = [(wide(is_hot[0][k] + is_hot[1][k] + is_hot[2][k]) < 0.5) & (line == s * nc + e) for k, (s, e) in enumerate(places)]

        def squeeze(bb, carry):
            parts = [h[index((c,), a, bb)], other[index((), a, bb)]] + [near[s, e, bb] for s, e in places[2:]]
            for j in range(3):
                out2[bb, j] = sum(parts[k] * weight[j][k] for k in range(8))
            singles = jnp.zeros((nz, 8, 128), F32)
            for k in range(8):
                singles = jnp.where(mine[k], jnp.sum(parts[k].astype(F32), axis=1, keepdims=True), singles)
            out2[bb, 3] = singles.astype(BF16)
            return carry

        lax.fori_loop(0, 4, squeeze, 0)
        up, dn, far = step(b, 1), step(b, 3), step(b, 2)
        lo, hi = pl.ds(0, nz // 2), pl.ds(nz // 2, nz // 2)
        f_up, f_dn = go(out2.at[far, :, lo], via2.at[0], to(a, up)), go(out2.at[far, :, hi], via2.at[1], to(a, dn))
        n_up, n_dn = go(out2.at[up], in2.at[b], to(a, up)), go(out2.at[dn], in2.at[b], to(a, dn))
        in2[b] = out2[b]
        yield
        f_up.wait_recv()
        r_up = go(via2.at[0], in2.at[dn, :, lo], to(a, up))
        f_dn.wait_recv()
        r_dn = go(via2.at[1], in2.at[up, :, hi], to(a, dn))
        yield
        for cp in (n_up, n_dn, r_up, r_dn):
            cp.wait_recv()
        for j in range(3):
            out3[:, j] = (in2[0, j] + in2[1, j]) + (in2[2, j] + in2[3, j])
        last = []
        for d in range(1, nz):
            zz = lax.rem(z + d, nz)
            last.append(go(in2.at[:, 3, zz], cold_land.at[z], dev(zz, y, x, c)))
        for d in range(1, nz):
            zz = lax.rem(z + d, nz)
            last.append(go(out3.at[zz], hot_land.at[z], dev(zz, y, x, c)))
        cold_land[z] = in2[:, 3, z]
        hot_land[z] = out3[z]
        yield
        for cp in last:
            cp.wait_recv()

    def weight_grad(k):
        if k % 2 == 0:
            part = slice(w2.shape[0] // 4 * (k // 2), w2.shape[0] // 4 * (k // 2 + 1))
            g2_ref[part, :] = dot(h_ref[:, part], dys_ref[...], 0, 0)
            save(6, (part, full))
        else:
            part = slice(w1.shape[1] // 4 * (k // 2), w1.shape[1] // 4 * (k // 2 + 1))
            g1_ref[:, part] = dot(xs_ref[...], da_ref[:, part], 0, 0)
            save(5, (full, part))

    ys, dxs = [back(0), back(1)], [back(2), back(3)]
    todo = [functools.partial(weight_grad, k) for k in range(8)]
    undone = [functools.partial(backward, i) for i in range(steps)]

    def turns(text):
        for turn in text:
            if turn == 'y':
                advance(ys)
            elif turn == 'x':
                advance(dxs)
            elif turn == 'd':
                advance(d_plans)
            elif turn == 'g':
                take_turns(grad_plans)
            elif turn == 'b' and undone:
                undone.pop(0)()
            elif turn == 'w':
                todo.pop(0)()

    turns(SECOND)
    save(2)
    save(3)

    r0, r1 = ids[0:1].astype(F32), ids[1:2].astype(F32)
    i0, i1 = as_col(r0), as_col(r1)
    tokens = tok[...]
    g0, g1 = gates(tokens, i0, i1, wg[...])
    n_tok = tok.shape[0]
    earlier = iota((n_tok, n_tok), 1) < iota((n_tok, n_tok), 0)
    n_exp = wg.shape[1]

    def where_from(i):
        rank = jnp.sum(jnp.where(earlier & ((i == r0) | (i == r1)), 1.0, 0.0), axis=1, keepdims=True)
        slot = jnp.full((n_tok, 1), -1.0, F32)
        for j in range(3):
            slot = jnp.where(i == hot_ref[j:j + 1, 0:1], CAP * j + rank, slot)
        e = i.astype(jnp.int32)
        core, xx, yy, zz = e % nc, (e // nc) % nx, (e // (nc * nx)) % ny, e // (nc * nx * ny)
        lane, single = iota((n_tok, n_exp), 1), slot < 0.0
        pick = lambda m: m.astype(F32).astype(BF16)
        return pick(iota((n_tok, 32), 1).astype(F32) == slot), (pick((lane == e) & single), pick((lane == ((zz * nx + xx) * ny + yy) * nc + core) & single))

    chosen = [where_from(i0), where_from(i1)]

    def rows_of(kind):
        parts = []
        for half in range(2):
            hot_land, cold_land = works[9 * (kind + half) + 7:9 * (kind + half) + 9]
            hot = jnp.sum(hot_land[...].astype(F32), axis=0).reshape(24, 128)
            hot = jnp.concatenate([hot, jnp.zeros((8, 128), F32)], axis=0).astype(BF16)
            cold = cold_land[...].astype(F32).reshape(n_exp, 128).astype(BF16)
            parts.append([dot(by_slot, hot, 1, 0) + dot(by_place[half], cold, 1, 0) for by_slot, by_place in chosen])
        return [jnp.concatenate([parts[0][k], parts[1][k]], axis=1) for k in range(2)]

    y0, y1 = rows_of(0)
    out_ref[...] = (g0 * y0 + g1 * y1).astype(BF16)
    save(0)
    grad = dout[...].astype(F32)
    dg0, dg1 = (jnp.sum(grad * v, axis=1, keepdims=True) for v in (y0, y1))
    mean = g0 * dg0 + g1 * dg1
    d0, d1 = ((g * (dg - mean)).astype(BF16).astype(F32) for g, dg in ((g0, dg0), (g1, dg1)))
    d_row[...] = jnp.concatenate([as_row(d0), as_row(d1), jnp.zeros((1, 2 * n_tok), F32)], axis=1)
    place = pltpu.make_async_copy(d_row, d_land.at[z, y, x, c], keep_sem.at[1])
    place.start()
    place.wait()
    d_plans = [gather_rows(next(links), d_land, (1, 2, 0, 3))]
    expert = iota((n_tok, n_exp), 1).astype(F32)
    spread = jnp.where(expert == i0, d0, jnp.where(expert == i1, d1, 0.0)).astype(BF16)
    through_gate = dot(spread, wg[...], 1, 1)
    turns(THIRD)
    dx0, dx1 = rows_of(2)
    gx_ref[...] = (dx0 + dx1 + through_gate).astype(BF16)
    save(1)
    take_turns(d_plans)
    save(4)
    for cp in sent:
        cp.wait_send()
    for cp in saves:
        cp.wait()


def block_call(dims, tokens, grad_out, ids, w_gate, w1, w2):
    nz, ny, nx, nc = dims
    d_model, d_hidden = w1.shape
    n_tok = tokens.shape[0]
    n_dev = nz * ny * nx * nc
    n_row = n_dev * CAP
    tile = (CAP, 128)
    hbm = pl.BlockSpec(memory_space=pltpu.HBM)
    out = jax.ShapeDtypeStruct
    work = [(4, 4, nz), (4, 2, 4, nz), (2, 2, 2, nz), (4, 4, nz), (2, 4, nz // 2), (4, 4, nz), (nz, 3), (nz, 3), (nz, 4)]
    lines, planes = nz - 1 + 4 + 16 + 4, 3 + 3 + nz + nz
    counts = [lines, lines, planes] * 2 + [nz - 1 + 3 + 3 + 1] + [1 + 12 + 6 + 2 * (nz - 1)] * 4 + [nz - 1 + 3 + 3 + 1]
    sems = []
    for k in counts:
        sems += [pltpu.SemaphoreType.DMA((k,))] * 2
    results = [(tokens.shape, BF16), (tokens.shape, BF16), (dims + tokens.shape, BF16), ((n_dev, 128), F32), (dims + (1, 128), F32),
               ((d_model, d_hidden), F32), ((d_hidden, d_model), F32)]
    row, n_dma = (1, 128), 16
    kept = [(tokens.shape, BF16), (tokens.shape, BF16), (ids.shape, jnp.int32), (w_gate.shape, BF16), (w1.shape, BF16), (w2.shape, BF16), (row, F32), (dims + row, F32),
            (dims + tokens.shape, BF16), ((n_row, d_model), BF16), ((n_row, d_model), BF16), ((n_row, d_hidden), BF16), ((n_row, d_hidden), BF16), ((n_row, d_hidden), F32), (tile, F32), (row, F32)]
    return pl.pallas_call(
        functools.partial(block_kernel, dims, (6, len(results), len(results), len(kept), 4, 4 * len(work), 3, len(sems))),
        out_shape=[out(*r) for r in results],
        in_specs=[hbm] * 6,
        out_specs=[hbm] * 7,
        scratch_shapes=[pltpu.VMEM(*r) for r in results + kept] + [pltpu.VMEM((nc, nx, ny, nz) + tile, BF16)] * 4 + [pltpu.VMEM(w + tile, BF16) for w in work] * 4
        + [pltpu.SemaphoreType.DMA((n_dma,))] * 3 + sems,
        compiler_params=pltpu.CompilerParams(collective_id=0, has_side_effects=True, vmem_limit_bytes=VMEM_LIMIT),
        name='block',
    )(tokens, grad_out, ids, w_gate, w1, w2)


VMEM_LIMIT = 67043328
FIRST = 'tmtgmtmtgmtmtgmtmtg'
SECOND = 'gybbyybybxyxxwyxwyxwy'
THIRD = 'dxwdxwdwwdwx'


def gate_kernel(n, x_hbm, m_hbm, d_hbm, *refs):
    refs = iter(refs)
    through, (o_ref,), passed, (x, m, d), held, (load_sem, save_sem) = [tuple(itertools.islice(refs, k)) for k in (n, 1, n, 3, n, 2)]
    n_part = x.shape[0]
    loads = [pltpu.make_async_copy(s, t, load_sem.at[k]) for k, (s, t) in enumerate(zip((m_hbm, d_hbm) + through, (m, d) + held))]
    chunks = [pltpu.make_async_copy(x_hbm.at[k], x.at[k], load_sem.at[len(loads) + k]) for k in range(n_part)]
    for cp in loads[:2] + chunks[:1] + loads[2:] + chunks[1:]:
        cp.start()
    for cp in loads[:2]:
        cp.wait()
    n_quad = m.shape[0] // 4
    i0, i1 = (plain_id(pair_rows(token_lanes(m, k, 0, n_quad))) for k in range(2))
    d0, d1 = (pair_rows(token_lanes(d, k, 0, n_quad)) for k in range(2))
    expert = iota((m.shape[0], 256), 0).astype(F32)
    total = jnp.zeros(o_ref.shape[::-1], F32)
    per = n_quad // 2 // n_part
    saves = []
    for k in range(n_part):
        chunks[k].wait()
        for p in range(per * k, per * (k + 1)):
            q = slice(p, p + 1)
            spread = jnp.where(expert == i0[q], d0[q], jnp.where(expert == i1[q], d1[q], 0.0))
            at = 256 * (p - per * k)
            total += dot(spread.astype(BF16), x[k, at:at + 256], 1, 0)
        if k < n:
            loads[2 + k].wait()
            saves.append(pltpu.make_async_copy(held[k], passed[k], save_sem.at[k]))
            saves[k].start()
    o_ref[...] = total.T
    for cp in saves:
        cp.wait()


def gate_grad(x_all, m_all, d_all, *through):
    n_src, d_model, parts = m_all.shape[0], x_all.shape[1], 4
    x_all = x_all.reshape(parts, -1, d_model)
    hbm, vmem = pl.BlockSpec(memory_space=pltpu.HBM), pl.BlockSpec(memory_space=pltpu.VMEM)
    out = jax.ShapeDtypeStruct
    return pl.pallas_call(
        functools.partial(gate_kernel, len(through)),
        out_shape=[out((d_model, n_src), F32)] + [out(v.shape, v.dtype) for v in through],
        in_specs=[hbm] * (len(through) + 3),
        out_specs=[vmem] + [hbm] * len(through),
        scratch_shapes=[pltpu.VMEM(v.shape, v.dtype) for v in (x_all, m_all, d_all) + through] + [pltpu.SemaphoreType.DMA((16,))] * 2,
        compiler_params=pltpu.CompilerParams(vmem_limit_bytes=VMEM_LIMIT),
        name='gate_grad',
    )(x_all, m_all, d_all, *through)


def local_block(dims, tokens, grad_out, expert_ids, w_gate, w_in, w_out):
    n_exp = w_gate.shape[1]
    y_out, grad_x, x_all, m_all, d_all, g1, g2 = block_call(dims, tokens, grad_out, expert_ids.T, w_gate, w_in[0], w_out[0])
    grad_w_gate, g1, g2, y_out, grad_x = gate_grad(x_all.reshape(-1, tokens.shape[1]), m_all, d_all.reshape(n_exp, 128), g1, g2, y_out, grad_x)
    return y_out, grad_x, g1[None], g2[None], grad_w_gate


def solution(mesh):
    dims = (8, 4, 4, 2)
    return jax.shard_map(functools.partial(local_block, dims), mesh=mesh, in_specs=(P('ep'), P('ep'), P('ep'), P(), P('ep'), P('ep')), out_specs=(P('ep'), P('ep'), P('ep'), P('ep'), P()), check_vma=False)
```

```python
import functools
import itertools

import jax
import jax.numpy as jnp
from jax import lax
from jax.experimental import pallas as pl
from jax.experimental.pallas import tpu as pltpu
from jax.sharding import PartitionSpec as P

MESH = pl.DeviceIdType.MESH
F32 = jnp.float32
BF16 = jnp.bfloat16
CAP = 8


def coords(dims):
    nz, ny, nx, nc = dims
    me = lax.axis_index('ep')
    c = lax.rem(me, nc)
    x = lax.rem(me // nc, nx)
    y = lax.rem(me // (nc * nx), ny)
    z = me // (nc * nx * ny)

    def dev(z, y, x, c):
        return (((z * ny + y) * nx + x) * nc + c,)

    return z, y, x, c, dev


def meet(peers):
    barrier = pltpu.get_barrier_semaphore()
    for peer in peers:
        pl.semaphore_signal(barrier, inc=1, device_id=peer, device_id_type=MESH)
    pl.semaphore_wait(barrier, len(peers))


def dot(a, b, ca, cb):
    return lax.dot_general(a, b, (((ca,), (cb,)), ((), ())), preferred_element_type=F32)


def iota(shape, axis):
    return lax.broadcasted_iota(jnp.int32, shape, axis)


def as_row(col):
    n = col.shape[0]
    return jnp.sum(jnp.where(iota((n, n), 0) == iota((n, n), 1), col, 0.0), axis=0, keepdims=True)


def as_col(row):
    n = row.shape[1]
    return jnp.sum(jnp.where(iota((n, n), 0) == iota((n, n), 1), row, 0.0), axis=1, keepdims=True)


def gates(tok, i0, i1, w_gate):
    logits = dot(tok, w_gate, 1, 0)
    expert = iota(logits.shape, 1).astype(F32)
    l0, l1 = (jnp.sum(jnp.where(expert == i, logits, 0.0), axis=1, keepdims=True) for i in (i0, i1))
    top = jnp.maximum(l0, l1)
    p0, p1 = jnp.exp(l0 - top), jnp.exp(l1 - top)
    total = p0 + p1
    return p0 / total, p1 / total


def choice_row(tok, ids, w_gate):
    r0, r1 = ids[0:1].astype(F32), ids[1:2].astype(F32)
    i0, i1 = as_col(r0), as_col(r1)
    g0, g1 = gates(tok, i0, i1, w_gate)

    def code(i):
        n = jnp.sum((i == r0).astype(F32) + (i == r1).astype(F32), axis=1, keepdims=True)
        return as_row(jnp.where(n > 1.5, i + 256.0, i))

    return jnp.concatenate([code(i0), code(i1), as_row(g0), as_row(g1)], axis=1)


def gelu_tanh(a):
    k = 0.7978845608028654
    sq = a * a
    return jnp.tanh(a * (k + (k * 0.044715) * sq)), sq


def gelu(a):
    half = 0.5 * a
    return half + half * gelu_tanh(a)[0]


def gelu_slope(a):
    k = 0.7978845608028654
    t, sq = gelu_tanh(a)
    return (0.5 + 0.5 * t) + (0.5 * a) * (1.0 - t * t) * (k + (3 * k * 0.044715) * sq)


def token_lanes(ref, k, start, n):
    lane = iota((n, 128), 1) // 32
    out = jnp.zeros((n, 128), F32)
    for j in range(4):
        r = ref[pl.ds(start + j, n, stride=4), :]
        out = jnp.where(lane == j, r if j == k else pltpu.roll(r, 32 * (j - k) % 128, 1), out)
    return out


def pair_rows(v):
    return jnp.concatenate([jnp.concatenate([v[2 * i:2 * i + 1], v[2 * i + 1:2 * i + 2]], axis=1) for i in range(v.shape[0] // 2)], axis=0)


def plain_id(code):
    return jnp.where(code >= 256.0, code - 256.0, code)


class Links:
    def __init__(self, send, recv, sent):
        self.send, self.recv, self.sent, self.k = send, recv, sent, 0

    def go(self, src, dst, to):
        cp = pltpu.make_async_remote_copy(src_ref=src, dst_ref=dst, send_sem=self.send.at[self.k], recv_sem=self.recv.at[self.k], device_id=to, device_id_type=MESH)
        self.k += 1
        cp.start()
        self.sent.append(cp)
        return cp


def take_turns(plans):
    live = list(plans)
    while live:
        for g in list(live):
            if next(g, 'end') == 'end':
                live.remove(g)


def block_kernel(dims, sizes, *refs):
    nz, ny, nx, nc = dims
    refs = iter(refs)
    refs = [list(itertools.islice(refs, n)) for n in sizes]
    (tok_hbm, dout_hbm, ids_hbm, wg_hbm, w1_hbm, w2_hbm), outs, held, kept, rows, works, (load_sem, keep_sem, save_sem), sems = refs
    out_ref, gx_ref, gate_ref, g1_ref, g2_ref = held
    tok, dout, ids, wg, w1, w2, row, m_land, x_all, g_all, xs_ref, dys_ref, h_ref, da_ref, a_ref, m_all, hot_ref, d_row, d_land, d_all = kept
    z, y, x, c, dev = coords(dims)
    sent, saves = [], []

    def save(k, part=None):
        src, dst = (held[k], outs[k]) if part is None else (held[k].at[part], outs[k].at[part])
        cp = pltpu.make_async_copy(src, dst, save_sem.at[len(saves)])
        cp.start()
        saves.append(cp)

    links = iter([Links(send, recv, sent) for send, recv in zip(sems[::2], sems[1::2])])

    loads = [pltpu.make_async_copy(s, d, load_sem.at[k]) for k, (s, d) in enumerate(
        [(tok_hbm, x_all.at[z, y, x, c]), (dout_hbm, g_all.at[z, y, x, c]), (tok_hbm, tok), (ids_hbm, ids), (wg_hbm, wg), (dout_hbm, dout), (w1_hbm, w1), (w2_hbm, w2)])]
    for ld in loads:
        ld.start()
    peers = [dev(lax.rem(z + d, nz), y, x, c) for d in range(1, nz)]
    for d in (1, 2, 3):
        peers.append(dev(z, lax.rem(y + d, ny), x, c))
        peers.append(dev(z, y, lax.rem(x + d, nx), c))
    mate = dev(z, y, x, 1 - c)
    peers.append(mate)
    meet(peers)

    full = slice(None)
    by_distance = sorted(range(1, nz), key=lambda d: abs(d - nz // 2))

    def step(v, d, m=4):
        return lax.rem(v + d, m)

    def by_lines(link, ref, rows, x_last):
        p0, q0 = (y, x) if x_last else (x, y)
        low, high = pl.ds(0, nz // 2), pl.ds(nz // 2, nz // 2)

        def at(zs, p, q):
            return ref.at[(zs, p, q, c, rows) if x_last else (zs, q, p, c, rows)]

        def go(part, p, q):
            return link.go(part, part, dev(z, p, q, c) if x_last else dev(z, q, p, c))

        cross = []

        def over(q):
            part = at(full, full, q)
            cross.append(link.go(part, part, mate))

        own = at(z, p0, q0)
        first = [link.go(own, own, dev(step(z, d, nz), y, x, c)) for d in by_distance]
        yield
        for cp in first:
            cp.wait_recv()
        pm, pp, po = step(p0, 3), step(p0, 1), step(p0, 2)
        qm, qp, qo = step(q0, 3), step(q0, 1), step(q0, 2)
        qs, relays = [], []

        def spread(p):
            part = at(full, p, q0)
            qs.append((p, go(part, p0, qp), go(part, p0, qm)))

        def relay(i):
            p, up, dn = qs[i]
            up.wait_recv()
            relays.append(go(at(low, p, qm), p0, qp))
            dn.wait_recv()
            relays.append(go(at(high, p, qp), p0, qm))

        p_up, p_dn = go(at(full, p0, q0), pp, q0), go(at(full, p0, q0), pm, q0)
        spread(p0)
        yield
        p_up.wait_recv()
        f_up = go(at(low, pm, q0), pp, q0)
        p_dn.wait_recv()
        f_dn = go(at(high, pp, q0), pm, q0)
        spread(pm)
        spread(pp)
        yield
        relay(0)
        yield
        f_up.wait_recv()
        f_dn.wait_recv()
        spread(po)
        over(q0)
        for i in range(1, 4):
            yield
            relay(i)
        over(qm)
        over(qp)
        yield
        for cp in relays:
            cp.wait_recv()
        over(qo)
        yield
        for cp in cross:
            cp.wait_recv()

    def by_planes(link, ref, rows):
        go = lambda part, *to: link.go(part, part, dev(*to))
        at = lambda zz, ys=full: ref.at[zz, ys, full, c, rows]
        own = ref.at[z, y, x, c, rows]
        xs = [go(own, z, y, step(x, d), c) for d in range(1, nx)]
        yield
        for cp in xs:
            cp.wait_recv()
        line = ref.at[z, y, full, c, rows]
        ys = [go(line, z, step(y, d), x, c) for d in range(1, ny)]
        yield
        for cp in ys:
            cp.wait_recv()
        cross = []

        def over(*planes):
            for zz in planes:
                cross.append(link.go(at(zz), at(zz), mate))

        half = nz // 2
        lower, upper = pl.ds(0, ny // 2), pl.ds(ny // 2, ny // 2)

        def pair(d):
            a, b = (full, full) if d + 1 < half else (lower, upper)
            return go(at(step(z, nz - d, nz), a), step(z, 1, nz), y, x, c), go(at(step(z, d, nz), b), step(z, nz - 1, nz), y, x, c)

        up, dn = pair(0)
        over(z)
        for d in range(1, half + 1):
            yield
            up.wait_recv()
            dn.wait_recv()
            if d < half:
                up, dn = pair(d)
                over(step(z, d, nz), step(z, nz - d, nz))
            else:
                over(step(z, d, nz))
        yield
        for cp in cross:
            cp.wait_recv()

    def gather_rows(link, held, order):
        have = [z, y, x, c]
        for axis in order:
            size = (nz, ny, nx, nc)[axis]
            part = held.at[tuple(have)]
            copies = []
            for d in sorted(range(1, size), key=lambda d: abs(d - size // 2)):
                there = [z, y, x, c]
                there[axis] = lax.rem(there[axis] + d, size)
                copies.append(link.go(part, part, dev(*there)))
            have[axis] = full
            yield
            for cp in copies:
                cp.wait_recv()

    def advance(plans):
        for g in plans:
            next(g, None)

    tok_plans = [by_lines(next(links), x_all, slice(0, 16), True), by_lines(next(links), x_all, slice(16, 32), False)]
    grad_plans = [by_lines(next(links), g_all, slice(0, 8), True), by_lines(next(links), g_all, slice(8, 16), False)]
    plane_plan = [by_planes(next(links), g_all, slice(16, 32))]
    loads[0].wait()
    advance(tok_plans)
    loads[1].wait()
    advance(plane_plan)
    advance(grad_plans)
    for ld in loads[2:5]:
        ld.wait()
    row[...] = choice_row(tok[...], ids[...], wg[...])
    place = pltpu.make_async_copy(row, m_land.at[z, y, x, c], keep_sem.at[0])
    place.start()
    place.wait()
    row_plan = [gather_rows(next(links), m_land, range(4))]
    for turn in FIRST:
        advance({'t': tok_plans, 'g': grad_plans, 'c': plane_plan, 'm': row_plan}[turn])
    take_turns(row_plan)
    take_turns(tok_plans)

    def flatten(land, flat):
        def lines(zz, carry):
            for k in range(ny * nx * nc):
                flat[pl.ds(zz * (ny * nx * nc) + k, 1), :] = land[zz, k // (nx * nc), k // nc % nx, k % nc]
            return carry

        lax.fori_loop(0, nz, lines, 0)

    flatten(m_land, m_all)
    for ld in loads[5:]:
        ld.wait()

    me = lax.axis_index('ep').astype(F32)
    code = m_all[...]
    left = jnp.where((iota(code.shape, 1) < 64) & (code >= 256.0), code - 256.0, 999.0)
    found = []
    for _ in range(3):
        best = jnp.min(jnp.min(left, axis=0, keepdims=True), axis=1, keepdims=True)
        left = jnp.where(left == best, 999.0, left)
        found.append(jnp.broadcast_to(best, (1, 128)))
    hot_ref[...] = jnp.concatenate(found + [jnp.full((5, 128), 999.0, F32)], axis=0)
    steps = 4 if nz == 8 else 1
    per = nz // steps
    n_quad = per * ny * nx * nc // 4
    n_pair = n_quad // 2
    n_slot = n_pair * 8 * CAP

    places = [(cc, xx, yy, zz) for cc in range(nc) for xx in range(nx) for yy in range(ny) for zz in range(per)]

    def select(i, ref, with_gate):
        c0, c1, g0, g1 = (pair_rows(token_lanes(m_all, k, pl.multiple_of(4 * n_quad * i, 4 * n_quad), n_quad)) for k in range(4))
        hit0, hit1 = plain_id(c0) == me, plain_id(c1) == me
        hit = (hit0 | hit1).astype(F32)
        gate = jnp.where(hit0, g0, 0.0) + jnp.where(hit1, g1, 0.0)
        before, after = iota((256, 256), 0), iota((256, 256), 1)
        tri = ((before < after) & (before // 32 == after // 32)).astype(F32).astype(BF16)
        rank = dot(hit.astype(BF16), tri, 1, 0)
        src = (iota((n_pair, 256), 1) // 32).astype(F32)
        key = jnp.where(hit > 0.0, src * CAP + rank, -1.0)
        slot = iota((8 * CAP, 256), 0).astype(F32)
        parts = []
        for p in range(n_pair):
            sel = (slot == key[p:p + 1]).astype(F32)
            v = dot(sel.astype(BF16), ref[i * per + p // ny, p % ny].reshape(256, 256), 1, 0)
            parts.append(v * jnp.sum(sel * gate[p:p + 1], axis=1, keepdims=True) if with_gate else v)
        return jnp.concatenate([parts[zz * ny + yy][CAP * (xx * nc + cc):CAP * (xx * nc + cc + 1)] for cc, xx, yy, zz in places], axis=0).astype(BF16)

    def put(i, v, to):
        for k, (cc, xx, yy, zz) in enumerate(places):
            for half in range(2):
                to[half][cc, xx, yy, i * per + zz] = v[CAP * k:CAP * (k + 1), 128 * half:128 * (half + 1)].astype(BF16)

    def forward(i):
        here = pl.ds(i * n_slot, n_slot)
        xs = select(i, x_all, False)
        a = dot(xs, w1[...], 1, 0)
        h = gelu(a).astype(BF16)
        xs_ref[here], h_ref[here], a_ref[here] = xs, h, a
        put(i, dot(h, w2[...], 1, 0), rows[:2])

    def backward(i):
        here = pl.ds(i * n_slot, n_slot)
        dys = select(i, g_all, True)
        da = (dot(dys, w2[...], 1, 1) * gelu_slope(a_ref[here])).astype(BF16)
        dys_ref[here], da_ref[here] = dys, da
        put(i, dot(da, w1[...], 1, 1), rows[2:])

    for i in range(steps):
        forward(i)
        advance(grad_plans + plane_plan)

    def back(i):
        h = rows[i]
        other, near, via, out2, via2, in2, out3, hot_land, cold_land = works[9 * i:9 * i + 9]
        go = next(links).go
        x_first = i % 2 == 0
        a, b = (x, y) if x_first else (y, x)

        def to(a, b):
            return dev(z, b, a, c) if x_first else dev(z, a, b, c)

        def index(lead, a, bs):
            return lead + ((a, bs) if x_first else (bs, a))

        up, dn, far = step(a, 1), step(a, 3), step(a, 2)
        lo, hi = pl.ds(0, 2), pl.ds(2, 2)
        cross = go(h.at[1 - c], other, mate)

        def spread(ref, lead, e):
            return [go(ref.at[index(lead, far, lo)], via.at[0, e], to(up, b)), go(ref.at[index(lead, far, hi)], via.at[1, e], to(dn, b)),
                    go(ref.at[index(lead, up, full)], near.at[a, e], to(up, b)), go(ref.at[index(lead, dn, full)], near.at[a, e], to(dn, b))]

        def relay(cps, e):
            cps[0].wait_recv()
            r_up = go(via.at[0, e], near.at[dn, e, lo], to(up, b))
            cps[1].wait_recv()
            r_dn = go(via.at[1, e], near.at[up, e, hi], to(dn, b))
            return [cps[2], cps[3], r_up, r_dn]

        own = spread(h, (c,), c)
        yield
        cross.wait_recv()
        his = spread(other, (), 1 - c)
        yield
        waits = relay(own, c)
        yield
        waits += relay(his, 1 - c)
        yield
        for cp in waits:
            cp.wait_recv()

        def expert(s, e):
            return ((z * ny + y) * nx + s) * nc + e if x_first else ((z * ny + s) * nx + x) * nc + e

        places = [(step(a, d), e) for d in range(4) for e in (c, 1 - c)]
        is_hot = [[(hot_ref[j:j + 1, :] == expert(s, e).astype(F32)).astype(F32) for s, e in places] for j in range(3)]
        wide = lambda v: jnp.broadcast_to(v, (8, 128))
        weight = [[wide(v).astype(BF16) for v in r] for r in is_hot]
        line = iota((8, 128), 0)
        mine = [(wide(is_hot[0][k] + is_hot[1][k] + is_hot[2][k]) < 0.5) & (line == s * nc + e) for k, (s, e) in enumerate(places)]

        def squeeze(bb, carry):
            parts = [h[index((c,), a, bb)], other[index((), a, bb)]] + [near[s, e, bb] for s, e in places[2:]]
            for j in range(3):
                out2[bb, j] = sum(parts[k] * weight[j][k] for k in range(8))
            singles = jnp.zeros((nz, 8, 128), F32)
            for k in range(8):
                singles = jnp.where(mine[k], jnp.sum(parts[k].astype(F32), axis=1, keepdims=True), singles)
            out2[bb, 3] = singles.astype(BF16)
            return carry

        lax.fori_loop(0, 4, squeeze, 0)
        up, dn, far = step(b, 1), step(b, 3), step(b, 2)
        lo, hi = pl.ds(0, nz // 2), pl.ds(nz // 2, nz // 2)
        f_up, f_dn = go(out2.at[far, :, lo], via2.at[0], to(a, up)), go(out2.at[far, :, hi], via2.at[1], to(a, dn))
        n_up, n_dn = go(out2.at[up], in2.at[b], to(a, up)), go(out2.at[dn], in2.at[b], to(a, dn))
        in2[b] = out2[b]
        yield
        f_up.wait_recv()
        r_up = go(via2.at[0], in2.at[dn, :, lo], to(a, up))
        f_dn.wait_recv()
        r_dn = go(via2.at[1], in2.at[up, :, hi], to(a, dn))
        yield
        for cp in (n_up, n_dn, r_up, r_dn):
            cp.wait_recv()
        for j in range(3):
            out3[:, j] = (in2[0, j] + in2[1, j]) + (in2[2, j] + in2[3, j])
        last = []
        for d in by_distance:
            zz = lax.rem(z + d, nz)
            last.append(go(in2.at[:, 3, zz], cold_land.at[z], dev(zz, y, x, c)))
        for d in by_distance:
            zz = lax.rem(z + d, nz)
            last.append(go(out3.at[zz], hot_land.at[z], dev(zz, y, x, c)))
        cold_land[z] = in2[:, 3, z]
        hot_land[z] = out3[z]
        yield
        for cp in last:
            cp.wait_recv()

    def weight_grad(k):
        if k % 2 == 0:
            part = slice(w2.shape[0] // 4 * (k // 2), w2.shape[0] // 4 * (k // 2 + 1))
            g2_ref[part, :] = dot(h_ref[:, part], dys_ref[...], 0, 0)
            save(4, (part, full))
        else:
            part = slice(w1.shape[1] // 4 * (k // 2), w1.shape[1] // 4 * (k // 2 + 1))
            g1_ref[:, part] = dot(xs_ref[...], da_ref[:, part], 0, 0)
            save(3, (full, part))

    ys, dxs = [back(0), back(1)], [back(2), back(3)]
    todo = [functools.partial(weight_grad, k) for k in range(8)]
    undone = [functools.partial(backward, i) for i in range(steps)]

    def turns(text):
        for turn in text:
            if turn == 'y':
                advance(ys)
            elif turn == 'x':
                advance(dxs)
            elif turn == 'd':
                advance(d_plans)
            elif turn == 'g':
                take_turns(grad_plans + plane_plan)
            elif turn == 'b' and undone:
                undone.pop(0)()
            elif turn == 'w':
                todo.pop(0)()

    turns(SECOND)

    r0, r1 = ids[0:1].astype(F32), ids[1:2].astype(F32)
    i0, i1 = as_col(r0), as_col(r1)
    tokens = tok[...]
    g0, g1 = gates(tokens, i0, i1, wg[...])
    n_tok = tok.shape[0]
    earlier = iota((n_tok, n_tok), 1) < iota((n_tok, n_tok), 0)
    n_exp = wg.shape[1]

    def where_from(i):
        rank = jnp.sum(jnp.where(earlier & ((i == r0) | (i == r1)), 1.0, 0.0), axis=1, keepdims=True)
        slot = jnp.full((n_tok, 1), -1.0, F32)
        for j in range(3):
            slot = jnp.where(i == hot_ref[j:j + 1, 0:1], CAP * j + rank, slot)
        e = i.astype(jnp.int32)
        core, xx, yy, zz = e % nc, (e // nc) % nx, (e // (nc * nx)) % ny, e // (nc * nx * ny)
        lane, single = iota((n_tok, n_exp), 1), slot < 0.0
        pick = lambda m: m.astype(F32).astype(BF16)
        return pick(iota((n_tok, 32), 1).astype(F32) == slot), (pick((lane == e) & single), pick((lane == ((zz * nx + xx) * ny + yy) * nc + core) & single))

    chosen = [where_from(i0), where_from(i1)]

    def rows_of(kind):
        parts = []
        for half in range(2):
            hot_land, cold_land = works[9 * (kind + half) + 7:9 * (kind + half) + 9]
            hot = jnp.sum(hot_land[...].astype(F32), axis=0).reshape(24, 128)
            hot = jnp.concatenate([hot, jnp.zeros((8, 128), F32)], axis=0).astype(BF16)
            cold = cold_land[...].astype(F32).reshape(n_exp, 128).astype(BF16)
            parts.append([dot(by_slot, hot, 1, 0) + dot(by_place[half], cold, 1, 0) for by_slot, by_place in chosen])
        return [jnp.concatenate([parts[0][k], parts[1][k]], axis=1) for k in range(2)]

    y0, y1 = rows_of(0)
    out_ref[...] = (g0 * y0 + g1 * y1).astype(BF16)
    save(0)
    grad = dout[...].astype(F32)
    dg0, dg1 = (jnp.sum(grad * v, axis=1, keepdims=True) for v in (y0, y1))
    mean = g0 * dg0 + g1 * dg1
    d0, d1 = ((g * (dg - mean)).astype(BF16).astype(F32) for g, dg in ((g0, dg0), (g1, dg1)))
    d_row[...] = jnp.concatenate([as_row(d0), as_row(d1), jnp.zeros((1, 2 * n_tok), F32)], axis=1)
    place = pltpu.make_async_copy(d_row, d_land.at[z, y, x, c], keep_sem.at[1])
    place.start()
    place.wait()
    d_plans = [gather_rows(next(links), d_land, range(4))]
    expert = iota((n_tok, n_exp), 1).astype(F32)
    spread = jnp.where(expert == i0, d0, jnp.where(expert == i1, d1, 0.0)).astype(BF16)
    through_gate = dot(spread, wg[...], 1, 1)
    turns(THIRD)
    dx0, dx1 = rows_of(2)
    gx_ref[...] = (dx0 + dx1 + through_gate).astype(BF16)
    save(1)
    take_turns(d_plans)
    flatten(d_land, d_all)
    expert = iota((n_exp, 256), 0).astype(F32)
    n_tok_z = ny * nx * nc * n_tok
    def gate_part(zz, carry):
        start = pl.multiple_of(zz * (ny * nx * nc), ny * nx * nc)
        c0, c1 = (plain_id(pair_rows(token_lanes(m_all, k, start, n_tok_z // 128))) for k in range(2))
        e0, e1 = (pair_rows(token_lanes(d_all, k, start, n_tok_z // 128)) for k in range(2))
        spread = [jnp.where(expert == c0[p:p + 1], e0[p:p + 1], jnp.where(expert == c1[p:p + 1], e1[p:p + 1], 0.0)).astype(BF16) for p in range(n_tok_z // 256)]
        return carry + dot(jnp.concatenate(spread, axis=1), x_all[zz].reshape(n_tok_z, x_all.shape[-1]), 1, 0)

    gate_ref[...] = lax.fori_loop(0, nz, gate_part, jnp.zeros((n_exp, x_all.shape[-1]), F32)).T
    save(2)
    for cp in sent:
        cp.wait_send()
    for cp in saves:
        cp.wait()


def block_call(dims, tokens, grad_out, ids, w_gate, w1, w2):
    nz, ny, nx, nc = dims
    d_model, d_hidden = w1.shape
    n_tok = tokens.shape[0]
    n_dev = nz * ny * nx * nc
    n_row = n_dev * CAP
    tile = (CAP, 128)
    hbm = pl.BlockSpec(memory_space=pltpu.HBM)
    out = jax.ShapeDtypeStruct
    work = [(4, 4, nz), (4, 2, 4, nz), (2, 2, 2, nz), (4, 4, nz), (2, 4, nz // 2), (4, 4, nz), (nz, 3), (nz, 3), (nz, 4)]
    lines, planes = nz - 1 + 4 + 16 + 4, 3 + 3 + nz + nz
    counts = [lines] * 4 + [planes] + [nz - 1 + 3 + 3 + 1] + [1 + 12 + 6 + 2 * (nz - 1)] * 4 + [nz - 1 + 3 + 3 + 1]
    sems = []
    for k in counts:
        sems += [pltpu.SemaphoreType.DMA((k,))] * 2
    results = [(tokens.shape, BF16), (tokens.shape, BF16), ((d_model, n_dev), F32), ((d_model, d_hidden), F32), ((d_hidden, d_model), F32)]
    row, n_dma = (1, 128), 16
    kept = [(tokens.shape, BF16), (tokens.shape, BF16), (ids.shape, jnp.int32), (w_gate.shape, BF16), (w1.shape, BF16), (w2.shape, BF16), (row, F32), (dims + row, F32),
            (dims + tokens.shape, BF16), (dims + tokens.shape, BF16), ((n_row, d_model), BF16), ((n_row, d_model), BF16), ((n_row, d_hidden), BF16), ((n_row, d_hidden), BF16), ((n_row, d_hidden), F32), ((n_dev, 128), F32), (tile, F32), (row, F32),
            (dims + row, F32), ((n_dev, 128), F32)]
    return pl.pallas_call(
        functools.partial(block_kernel, dims, (6, len(results), len(results), len(kept), 4, 4 * len(work), 3, len(sems))),
        out_shape=[out(*r) for r in results],
        in_specs=[hbm] * 6,
        out_specs=[hbm] * len(results),
        scratch_shapes=[pltpu.VMEM(*r) for r in results + kept] + [pltpu.VMEM((nc, nx, ny, nz) + tile, BF16)] * 4 + [pltpu.VMEM(w + tile, BF16) for w in work] * 4
        + [pltpu.SemaphoreType.DMA((n_dma,))] * 3 + sems,
        compiler_params=pltpu.CompilerParams(collective_id=0, has_side_effects=True, vmem_limit_bytes=VMEM_LIMIT),
        name='block',
    )(tokens, grad_out, ids, w_gate, w1, w2)


VMEM_LIMIT = 67043328
FIRST = 'ctcgmttcgtmtcgtgmtcgt'
SECOND = 'gybybyybybyxwwyxxwxwy'
THIRD = 'dxwdxwdxwdwx'


def pass_kernel(n, *refs):
    refs = iter(refs)
    given, passed, held, (load_sem, save_sem) = [list(itertools.islice(refs, k)) for k in (n, n, n, 2)]
    loads = [pltpu.make_async_copy(given[k], held[k], load_sem.at[k]) for k in range(n)]
    saves = [pltpu.make_async_copy(held[k], passed[k], save_sem.at[k]) for k in range(n)]
    for cp in loads:
        cp.start()
    for load, save in zip(loads, saves):
        load.wait()
        save.start()
    for cp in saves:
        cp.wait()


def pass_on(*arrays):
    n = len(arrays)
    return pl.pallas_call(
        functools.partial(pass_kernel, n),
        out_shape=[jax.ShapeDtypeStruct(v.shape, v.dtype) for v in arrays],
        in_specs=[pl.BlockSpec(memory_space=pltpu.HBM)] * n,
        out_specs=[pl.BlockSpec(memory_space=pltpu.HBM)] * n,
        scratch_shapes=[pltpu.VMEM(v.shape, v.dtype) for v in arrays] + [pltpu.SemaphoreType.DMA((n,))] * 2,
        compiler_params=pltpu.CompilerParams(vmem_limit_bytes=VMEM_LIMIT),
        name='pass_on',
    )(*arrays)


def local_block(dims, tokens, grad_out, expert_ids, w_gate, w_in, w_out):
    y_out, grad_x, grad_w_gate, g1, g2 = pass_on(*block_call(dims, tokens, grad_out, expert_ids.T, w_gate, w_in[0], w_out[0]))
    return y_out, grad_x, g1[None], g2[None], grad_w_gate


def solution(mesh):
    dims = (8, 4, 4, 2)
    return jax.shard_map(functools.partial(local_block, dims), mesh=mesh, in_specs=(P('ep'), P('ep'), P('ep'), P(), P('ep'), P('ep')), out_specs=(P('ep'), P('ep'), P('ep'), P('ep'), P()), check_vma=False)
```

```python
import functools
import itertools
import math

import jax
import jax.numpy as jnp
from jax import lax
from jax.experimental import pallas as pl
from jax.experimental.pallas import tpu as pltpu
from jax.sharding import PartitionSpec as P

MESH = pl.DeviceIdType.MESH
F32 = jnp.float32
BF16 = jnp.bfloat16
CAP = 8


def coords(dims):
    nz, ny, nx, nc = dims
    me = lax.axis_index('ep')
    c = lax.rem(me, nc)
    x = lax.rem(me // nc, nx)
    y = lax.rem(me // (nc * nx), ny)
    z = me // (nc * nx * ny)

    def dev(z, y, x, c):
        return (((z * ny + y) * nx + x) * nc + c,)

    return z, y, x, c, dev


def meet(peers):
    barrier = pltpu.get_barrier_semaphore()
    for peer in peers:
        pl.semaphore_signal(barrier, inc=1, device_id=peer, device_id_type=MESH)
    pl.semaphore_wait(barrier, len(peers))


def dot(a, b, ca, cb):
    return lax.dot_general(a, b, (((ca,), (cb,)), ((), ())), preferred_element_type=F32)


def iota(shape, axis):
    return lax.broadcasted_iota(jnp.int32, shape, axis)


def as_row(col):
    n = col.shape[0]
    return jnp.sum(jnp.where(iota((n, n), 0) == iota((n, n), 1), col, 0.0), axis=0, keepdims=True)


def as_col(row):
    n = row.shape[1]
    return jnp.sum(jnp.where(iota((n, n), 0) == iota((n, n), 1), row, 0.0), axis=1, keepdims=True)


def gates(tok, i0, i1, w_gate):
    logits = dot(tok, w_gate, 1, 0)
    expert = iota(logits.shape, 1).astype(F32)
    l0, l1 = (jnp.sum(jnp.where(expert == i, logits, 0.0), axis=1, keepdims=True) for i in (i0, i1))
    top = jnp.maximum(l0, l1)
    p0, p1 = jnp.exp(l0 - top), jnp.exp(l1 - top)
    total = p0 + p1
    return p0 / total, p1 / total


def choice_row(tok, ids, w_gate):
    r0, r1 = ids[0:1].astype(F32), ids[1:2].astype(F32)
    i0, i1 = as_col(r0), as_col(r1)
    g0, g1 = gates(tok, i0, i1, w_gate)

    def code(i):
        n = jnp.sum((i == r0).astype(F32) + (i == r1).astype(F32), axis=1, keepdims=True)
        return as_row(jnp.where(n > 1.5, i + 256.0, i))

    return jnp.concatenate([code(i0), code(i1), as_row(g0), as_row(g1)], axis=1)


def gelu_tanh(a):
    k = 0.7978845608028654
    sq = a * a
    return jnp.tanh(a * (k + (k * 0.044715) * sq)), sq


def gelu(a):
    half = 0.5 * a
    return half + half * gelu_tanh(a)[0]


def gelu_slope(a):
    k = 0.7978845608028654
    t, sq = gelu_tanh(a)
    return (0.5 + 0.5 * t) + (0.5 * a) * (1.0 - t * t) * (k + (3 * k * 0.044715) * sq)


def token_lanes(ref, k, start, n):
    lane = iota((n, 128), 1) // 32
    out = jnp.zeros((n, 128), F32)
    for j in range(4):
        r = ref[pl.ds(start + j, n, stride=4), :]
        out = jnp.where(lane == j, r if j == k else pltpu.roll(r, 32 * (j - k) % 128, 1), out)
    return out


def pair_rows(v):
    return jnp.concatenate([jnp.concatenate([v[2 * i:2 * i + 1], v[2 * i + 1:2 * i + 2]], axis=1) for i in range(v.shape[0] // 2)], axis=0)


def plain_id(code):
    return jnp.where(code >= 256.0, code - 256.0, code)


class Links:
    def __init__(self, send, recv, pool):
        self.send, self.recv, self.pool, self.bytes = send, recv, pool, 0

    def group(self):
        return self.recv.at[next(self.pool)]

    def go(self, src, dst, to, group):
        pltpu.make_async_remote_copy(src_ref=src, dst_ref=dst, send_sem=self.send, recv_sem=group, device_id=to, device_id_type=MESH).start()
        self.bytes += math.prod(src.shape) * jnp.dtype(src.dtype).itemsize

    def wait(self, group, ref):
        pltpu.make_async_copy(ref, ref, group).wait()

    def finish(self, *pads):
        for pad in pads:
            unit = math.prod(pad.shape[1:]) * jnp.dtype(pad.dtype).itemsize
            if self.bytes % unit == 0:
                return self.wait(self.send, pad.at[pl.ds(0, self.bytes // unit)])
        raise ValueError(self.bytes)


def take_turns(plans):
    live = list(plans)
    while live:
        for g in list(live):
            if next(g, 'end') == 'end':
                live.remove(g)


def block_kernel(dims, sizes, *refs):
    nz, ny, nx, nc = dims
    refs = iter(refs)
    refs = [list(itertools.islice(refs, n)) for n in sizes]
    (tok_hbm, dout_hbm, ids_hbm, wg_hbm, w1_hbm, w2_hbm), outs, held, kept, rows, works, (load_sem, keep_sem, save_sem), sems = refs
    out_ref, gx_ref, gate_ref, g1_ref, g2_ref = held
    tok, dout, ids, wg, w1, w2, row, m_land, x_all, g_all, xs_ref, dys_ref, h_ref, da_ref, a_ref, m_all, hot_ref, d_row, d_land, d_all, pad, pad_row = kept
    z, y, x, c, dev = coords(dims)
    saves = []

    def save(k, part=None):
        src, dst = (held[k], outs[k]) if part is None else (held[k].at[part], outs[k].at[part])
        cp = pltpu.make_async_copy(src, dst, save_sem.at[len(saves)])
        cp.start()
        saves.append(cp)

    send_sem, recv_sem = sems
    pool = itertools.count()
    all_links = [Links(send_sem.at[k], recv_sem, pool) for k in range(send_sem.shape[0])]
    links = iter(all_links)

    loads = [pltpu.make_async_copy(s, d, load_sem.at[k]) for k, (s, d) in enumerate(
        [(tok_hbm, x_all.at[z, y, x, c]), (dout_hbm, g_all.at[z, y, x, c]), (tok_hbm, tok), (ids_hbm, ids), (wg_hbm, wg), (dout_hbm, dout), (w1_hbm, w1), (w2_hbm, w2)])]
    for ld in loads:
        ld.start()
    peers = [dev(lax.rem(z + d, nz), y, x, c) for d in range(1, nz)]
    for d in (1, 2, 3):
        peers.append(dev(z, lax.rem(y + d, ny), x, c))
        peers.append(dev(z, y, lax.rem(x + d, nx), c))
    mate = dev(z, y, x, 1 - c)
    peers.append(mate)
    meet(peers)

    full = slice(None)
    by_distance = sorted(range(1, nz), key=lambda d: abs(d - nz // 2))

    def step(v, d, m=4):
        return lax.rem(v + d, m)

    def by_lines(link, ref, rows, x_last):
        p0, q0 = (y, x) if x_last else (x, y)
        low, high = pl.ds(0, nz // 2), pl.ds(nz // 2, nz // 2)

        def at(zs, p, q):
            return ref.at[(zs, p, q, c, rows) if x_last else (zs, q, p, c, rows)]

        def go(part, p, q, group):
            link.go(part, part, dev(z, p, q, c) if x_last else dev(z, q, p, c), group)

        in_z, in_p, in_m, in_f, in_r, in_c = [link.group() for _ in range(6)]
        line = at(full, p0, q0)

        def over(q):
            part = at(full, full, q)
            link.go(part, part, mate, in_c)

        own = at(z, p0, q0)
        for d in by_distance:
            link.go(own, own, dev(step(z, d, nz), y, x, c), in_z)
        yield
        link.wait(in_z, at(pl.ds(0, nz - 1), p0, q0))
        pm, pp, po = step(p0, 3), step(p0, 1), step(p0, 2)
        qm, qp, qo = step(q0, 3), step(q0, 1), step(q0, 2)
        qs = []

        def spread(p):
            part = at(full, p, q0)
            qs.append((p, link.group(), link.group()))
            go(part, p0, qp, qs[-1][1])
            go(part, p0, qm, qs[-1][2])

        def relay(i):
            p, up, dn = qs[i]
            link.wait(up, line)
            go(at(low, p, qm), p0, qp, in_r)
            link.wait(dn, line)
            go(at(high, p, qp), p0, qm, in_r)

        go(line, pp, q0, in_p)
        go(line, pm, q0, in_m)
        spread(p0)
        yield
        link.wait(in_p, line)
        go(at(low, pm, q0), pp, q0, in_f)
        link.wait(in_m, line)
        go(at(high, pp, q0), pm, q0, in_f)
        spread(pm)
        spread(pp)
        yield
        relay(0)
        yield
        link.wait(in_f, line)
        spread(po)
        over(q0)
        for i in range(1, 4):
            yield
            relay(i)
        over(qm)
        over(qp)
        yield
        link.wait(in_r, at(full, full, q0))
        over(qo)
        yield
        link.wait(in_c, ref.at[full, full, full, c, rows])

    def by_planes(link, ref, rows):
        go = lambda part, group, *to: link.go(part, part, dev(*to), group)
        at = lambda zz, ys=full: ref.at[zz, ys, full, c, rows]
        in_x, in_y, in_c = [link.group() for _ in range(3)]
        own = ref.at[z, y, x, c, rows]
        for d in range(1, nx):
            go(own, in_x, z, y, step(x, d), c)
        yield
        link.wait(in_x, ref.at[z, y, pl.ds(0, nx - 1), c, rows])
        line = ref.at[z, y, full, c, rows]
        for d in range(1, ny):
            go(line, in_y, z, step(y, d), x, c)
        yield
        link.wait(in_y, ref.at[z, pl.ds(0, ny - 1), full, c, rows])

        def over(*planes):
            for zz in planes:
                link.go(at(zz), at(zz), mate, in_c)

        half = nz // 2
        lower, upper = pl.ds(0, ny // 2), pl.ds(ny // 2, ny // 2)

        def pair(d):
            a, b = (full, full) if d + 1 < half else (lower, upper)
            group = link.group()
            go(at(step(z, nz - d, nz), a), group, step(z, 1, nz), y, x, c)
            go(at(step(z, d, nz), b), group, step(z, nz - 1, nz), y, x, c)
            return group

        group = pair(0)
        over(z)
        for d in range(1, half + 1):
            yield
            link.wait(group, at(pl.ds(0, 2) if d < half else z))
            if d < half:
                group = pair(d)
                over(step(z, d, nz), step(z, nz - d, nz))
            else:
                over(step(z, d, nz))
        yield
        link.wait(in_c, ref.at[full, full, full, c, rows])

    def gather_rows(link, held, order):
        have = [z, y, x, c]
        for axis in order:
            size = (nz, ny, nx, nc)[axis]
            part = held.at[tuple(have)]
            group = link.group()
            for d in sorted(range(1, size), key=lambda d: abs(d - size // 2)):
                there = [z, y, x, c]
                there[axis] = lax.rem(there[axis] + d, size)
                link.go(part, part, dev(*there), group)
            have[axis] = pl.ds(0, size - 1)
            yield
            link.wait(group, held.at[tuple(have)])
            have[axis] = full

    def advance(plans):
        for g in plans:
            next(g, None)

    tok_plans = [by_lines(next(links), x_all, slice(0, 16), True), by_lines(next(links), x_all, slice(16, 32), False)]
    grad_plans = [by_lines(next(links), g_all, slice(0, 8), True), by_lines(next(links), g_all, slice(8, 16), False)]
    plane_plan = [by_planes(next(links), g_all, slice(16, 32))]
    loads[0].wait()
    advance(tok_plans)
    for ld in loads[2:5]:
        ld.wait()
    row[...] = choice_row(tok[...], ids[...], wg[...])
    place = pltpu.make_async_copy(row, m_land.at[z, y, x, c], keep_sem.at[0])
    place.start()
    place.wait()
    row_plan = [gather_rows(next(links), m_land, range(4))]
    loads[1].wait()
    advance(row_plan + plane_plan + grad_plans)
    for turn in FIRST:
        advance({'t': tok_plans, 'g': grad_plans, 'c': plane_plan, 'm': row_plan}[turn])
    take_turns(row_plan)
    take_turns(tok_plans)

    def flatten(land, flat):
        def lines(zz, carry):
            for k in range(ny * nx * nc):
                flat[pl.ds(zz * (ny * nx * nc) + k, 1), :] = land[zz, k // (nx * nc), k // nc % nx, k % nc]
            return carry

        lax.fori_loop(0, nz, lines, 0)

    flatten(m_land, m_all)
    for ld in loads[5:]:
        ld.wait()

    me = lax.axis_index('ep').astype(F32)
    code = m_all[...]
    left = jnp.where((iota(code.shape, 1) < 64) & (code >= 256.0), code - 256.0, 999.0)
    found = []
    for _ in range(3):
        best = jnp.min(jnp.min(left, axis=0, keepdims=True), axis=1, keepdims=True)
        left = jnp.where(left == best, 999.0, left)
        found.append(jnp.broadcast_to(best, (1, 128)))
    hot_ref[...] = jnp.concatenate(found + [jnp.full((5, 128), 999.0, F32)], axis=0)
    steps = 4 if nz == 8 else 1
    per = nz // steps
    n_quad = per * ny * nx * nc // 4
    n_pair = n_quad // 2
    n_slot = n_pair * 8 * CAP

    places = [(cc, xx, yy, zz) for cc in range(nc) for xx in range(nx) for yy in range(ny) for zz in range(per)]

    def select(i, ref, with_gate):
        c0, c1, g0, g1 = (pair_rows(token_lanes(m_all, k, pl.multiple_of(4 * n_quad * i, 4 * n_quad), n_quad)) for k in range(4))
        hit0, hit1 = plain_id(c0) == me, plain_id(c1) == me
        hit = (hit0 | hit1).astype(F32)
        gate = jnp.where(hit0, g0, 0.0) + jnp.where(hit1, g1, 0.0)
        before, after = iota((256, 256), 0), iota((256, 256), 1)
        tri = ((before < after) & (before // 32 == after // 32)).astype(F32).astype(BF16)
        rank = dot(hit.astype(BF16), tri, 1, 0)
        src = (iota((n_pair, 256), 1) // 32).astype(F32)
        key = jnp.where(hit > 0.0, src * CAP + rank, -1.0)
        slot = iota((8 * CAP, 256), 0).astype(F32)
        parts = []
        for p in range(n_pair):
            sel = (slot == key[p:p + 1]).astype(F32)
            v = dot(sel.astype(BF16), ref[i * per + p // ny, p % ny].reshape(256, 256), 1, 0)
            parts.append(v * jnp.sum(sel * gate[p:p + 1], axis=1, keepdims=True) if with_gate else v)
        return jnp.concatenate([parts[zz * ny + yy][CAP * (xx * nc + cc):CAP * (xx * nc + cc + 1)] for cc, xx, yy, zz in places], axis=0).astype(BF16)

    def put(i, v, to):
        for k, (cc, xx, yy, zz) in enumerate(places):
            for half in range(2):
                to[half][cc, xx, yy, i * per + zz] = v[CAP * k:CAP * (k + 1), 128 * half:128 * (half + 1)].astype(BF16)

    def forward(i):
        here = pl.ds(i * n_slot, n_slot)
        xs = select(i, x_all, False)
        a = dot(xs, w1[...], 1, 0)
        h = gelu(a).astype(BF16)
        xs_ref[here], h_ref[here], a_ref[here] = xs, h, a
        put(i, dot(h, w2[...], 1, 0), rows[:2])

    def backward(i):
        here = pl.ds(i * n_slot, n_slot)
        dys = select(i, g_all, True)
        dys_ref[here] = dys
        da_ref[here] = (dot(dys, w2[...], 1, 1) * gelu_slope(a_ref[here])).astype(BF16)

    def backward_rows(i):
        put(i, dot(da_ref[pl.ds(i * n_slot, n_slot)], w1[...], 1, 1), rows[2:])

    for i in range(steps):
        forward(i)
        advance(grad_plans + plane_plan if i else grad_plans)

    def back(i):
        h = rows[i]
        other, near, via, out2, via2, in2, out3, hot_land, cold_land = works[9 * i:9 * i + 9]
        link = next(links)
        go = link.go
        in_c, in_e, in_h, in_n, in_v, in_2, in_l, in_s = [link.group() for _ in range(8)]
        x_first = i % 2 == 0
        a, b = (x, y) if x_first else (y, x)

        def to(a, b):
            return dev(z, b, a, c) if x_first else dev(z, a, b, c)

        def index(lead, a, bs):
            return lead + ((a, bs) if x_first else (bs, a))

        up, dn, far = step(a, 1), step(a, 3), step(a, 2)
        lo, hi = pl.ds(0, 2), pl.ds(2, 2)
        go(h.at[1 - c], other, mate, in_c)

        def spread(ref, lead, e, group):
            go(ref.at[index(lead, far, lo)], via.at[0, e], to(up, b), group)
            go(ref.at[index(lead, far, hi)], via.at[1, e], to(dn, b), group)
            go(ref.at[index(lead, up, full)], near.at[a, e], to(up, b), in_n)
            go(ref.at[index(lead, dn, full)], near.at[a, e], to(dn, b), in_n)

        def relay(e, group):
            link.wait(group, via.at[:, e])
            go(via.at[0, e], near.at[dn, e, lo], to(up, b), in_n)
            go(via.at[1, e], near.at[up, e, hi], to(dn, b), in_n)

        spread(h, (c,), c, in_e)
        yield
        link.wait(in_c, other)
        spread(other, (), 1 - c, in_h)
        yield
        relay(c, in_e)
        yield
        relay(1 - c, in_h)
        yield
        link.wait(in_n, near.at[pl.ds(0, 3)])

        def expert(s, e):
            return ((z * ny + y) * nx + s) * nc + e if x_first else ((z * ny + s) * nx + x) * nc + e

        places = [(step(a, d), e) for d in range(4) for e in (c, 1 - c)]
        is_hot = [[(hot_ref[j:j + 1, :] == expert(s, e).astype(F32)).astype(F32) for s, e in places] for j in range(3)]
        wide = lambda v: jnp.broadcast_to(v, (8, 128))
        weight = [[wide(v).astype(BF16) for v in r] for r in is_hot]
        line = iota((8, 128), 0)
        mine = [(wide(is_hot[0][k] + is_hot[1][k] + is_hot[2][k]) < 0.5) & (line == s * nc + e) for k, (s, e) in enumerate(places)]

        def squeeze(bb, carry):
            parts = [h[index((c,), a, bb)], other[index((), a, bb)]] + [near[s, e, bb] for s, e in places[2:]]
            for j in range(3):
                out2[bb, j] = sum(parts[k] * weight[j][k] for k in range(8))
            singles = jnp.zeros((nz, 8, 128), F32)
            for k in range(8):
                singles = jnp.where(mine[k], jnp.sum(parts[k].astype(F32), axis=1, keepdims=True), singles)
            out2[bb, 3] = singles.astype(BF16)
            return carry

        lax.fori_loop(0, 4, squeeze, 0)
        up, dn, far = step(b, 1), step(b, 3), step(b, 2)
        lo, hi = pl.ds(0, nz // 2), pl.ds(nz // 2, nz // 2)
        go(out2.at[far, :, lo], via2.at[0], to(a, up), in_v)
        go(out2.at[far, :, hi], via2.at[1], to(a, dn), in_v)
        go(out2.at[up], in2.at[b], to(a, up), in_2)
        go(out2.at[dn], in2.at[b], to(a, dn), in_2)
        in2[b] = out2[b]
        yield
        link.wait(in_v, via2)
        go(via2.at[0], in2.at[dn, :, lo], to(a, up), in_2)
        go(via2.at[1], in2.at[up, :, hi], to(a, dn), in_2)
        yield
        link.wait(in_2, in2.at[pl.ds(0, 3)])
        for j in range(3):
            out3[:, j] = (in2[0, j] + in2[1, j]) + (in2[2, j] + in2[3, j])
        for d in by_distance:
            zz = lax.rem(z + d, nz)
            go(in2.at[:, 3, zz], cold_land.at[z], dev(zz, y, x, c), in_s)
            go(out3.at[zz], hot_land.at[z], dev(zz, y, x, c), in_l)
        cold_land[z] = in2[:, 3, z]
        hot_land[z] = out3[z]
        yield
        link.wait(in_s, cold_land.at[pl.ds(0, nz - 1)])
        link.wait(in_l, hot_land.at[pl.ds(0, nz - 1)])

    def weight_grad(k):
        if k % 2 == 0:
            part = slice(w2.shape[0] // 4 * (k // 2), w2.shape[0] // 4 * (k // 2 + 1))
            g2_ref[part, :] = dot(h_ref[:, part], dys_ref[...], 0, 0)
            save(4, (part, full))
        else:
            part = slice(w1.shape[1] // 4 * (k // 2), w1.shape[1] // 4 * (k // 2 + 1))
            g1_ref[:, part] = dot(xs_ref[...], da_ref[:, part], 0, 0)
            save(3, (full, part))

    ys, dxs = [back(0), back(1)], [back(2), back(3)]
    todo = [functools.partial(weight_grad, k) for k in range(8)]
    undone = [functools.partial(backward, i) for i in range(steps)]
    unsent = [functools.partial(backward_rows, i) for i in range(steps)]

    def turns(text):
        for turn in text:
            if turn == 'y':
                advance(ys)
            elif turn == 'x':
                advance(dxs)
            elif turn == 'd':
                advance(d_plans)
            elif turn == 'g':
                take_turns(grad_plans + plane_plan)
            elif turn == 'b' and undone:
                undone.pop(0)()
            elif turn == 'B' and unsent:
                unsent.pop(0)()
            elif turn == 'w':
                todo.pop(0)()

    turns(SECOND)

    r0, r1 = ids[0:1].astype(F32), ids[1:2].astype(F32)
    i0, i1 = as_col(r0), as_col(r1)
    tokens = tok[...]
    g0, g1 = gates(tokens, i0, i1, wg[...])
    n_tok = tok.shape[0]
    earlier = iota((n_tok, n_tok), 1) < iota((n_tok, n_tok), 0)
    n_exp = wg.shape[1]

    def where_from(i):
        rank = jnp.sum(jnp.where(earlier & ((i == r0) | (i == r1)), 1.0, 0.0), axis=1, keepdims=True)
        slot = jnp.full((n_tok, 1), -1.0, F32)
        for j in range(3):
            slot = jnp.where(i == hot_ref[j:j + 1, 0:1], CAP * j + rank, slot)
        e = i.astype(jnp.int32)
        core, xx, yy, zz = e % nc, (e // nc) % nx, (e // (nc * nx)) % ny, e // (nc * nx * ny)
        lane, single = iota((n_tok, n_exp), 1), slot < 0.0
        pick = lambda m: m.astype(F32).astype(BF16)
        return pick(iota((n_tok, 32), 1).astype(F32) == slot), (pick((lane == e) & single), pick((lane == ((zz * nx + xx) * ny + yy) * nc + core) & single))

    chosen = [where_from(i0), where_from(i1)]

    def rows_of(kind):
        parts = []
        for half in range(2):
            hot_land, cold_land = works[9 * (kind + half) + 7:9 * (kind + half) + 9]
            hot = jnp.sum(hot_land[...].astype(F32), axis=0).reshape(24, 128)
            hot = jnp.concatenate([hot, jnp.zeros((8, 128), F32)], axis=0).astype(BF16)
            cold = cold_land[...].astype(F32).reshape(n_exp, 128).astype(BF16)
            parts.append([dot(by_slot, hot, 1, 0) + dot(by_place[half], cold, 1, 0) for by_slot, by_place in chosen])
        return [jnp.concatenate([parts[0][k], parts[1][k]], axis=1) for k in range(2)]

    y0, y1 = rows_of(0)
    out_ref[...] = (g0 * y0 + g1 * y1).astype(BF16)
    save(0)
    grad = dout[...].astype(F32)
    dg0, dg1 = (jnp.sum(grad * v, axis=1, keepdims=True) for v in (y0, y1))
    mean = g0 * dg0 + g1 * dg1
    d0, d1 = ((g * (dg - mean)).astype(BF16).astype(F32) for g, dg in ((g0, dg0), (g1, dg1)))
    d_row[...] = jnp.concatenate([as_row(d0), as_row(d1), jnp.zeros((1, 2 * n_tok), F32)], axis=1)
    place = pltpu.make_async_copy(d_row, d_land.at[z, y, x, c], keep_sem.at[1])
    place.start()
    place.wait()
    d_plans = [gather_rows(next(links), d_land, range(4))]
    expert = iota((n_tok, n_exp), 1).astype(F32)
    spread = jnp.where(expert == i0, d0, jnp.where(expert == i1, d1, 0.0)).astype(BF16)
    through_gate = dot(spread, wg[...], 1, 1)
    turns(THIRD)
    dx0, dx1 = rows_of(2)
    gx_ref[...] = (dx0 + dx1 + through_gate).astype(BF16)
    save(1)
    take_turns(d_plans)
    n_dev = nz * ny * nx * nc
    flatten(d_land, d_all)
    expert = iota((n_exp, 256), 0).astype(F32)
    some = n_dev // 4
    codes = [plain_id(pair_rows(token_lanes(m_all, k, 0, some))) for k in range(2)]
    grads = [pair_rows(token_lanes(d_all, k, 0, some)) for k in range(2)]
    total = jnp.zeros((n_exp, x_all.shape[-1]), F32)
    zs = nz // 4 or 1
    for z0 in range(0, nz, zs):
        spread = []
        for p in range(z0 * ny, (z0 + zs) * ny):
            q = slice(p, p + 1)
            spread.append(jnp.where(expert == codes[0][q], grads[0][q], jnp.where(expert == codes[1][q], grads[1][q], 0.0)).astype(BF16))
        total += dot(jnp.concatenate(spread, axis=1), x_all[z0:z0 + zs].reshape(zs * ny * 256, x_all.shape[-1]), 1, 0)
    gate_ref[...] = total.T
    save(2)
    for link in all_links:
        link.finish(pad, pad_row)
    for cp in saves:
        cp.wait()


def block_call(dims, tokens, grad_out, ids, w_gate, w1, w2):
    nz, ny, nx, nc = dims
    d_model, d_hidden = w1.shape
    n_tok = tokens.shape[0]
    n_dev = nz * ny * nx * nc
    n_row = n_dev * CAP
    tile = (CAP, 128)
    hbm = pl.BlockSpec(memory_space=pltpu.HBM)
    out = jax.ShapeDtypeStruct
    work = [(4, 4, nz), (4, 2, 4, nz), (2, 2, 2, nz), (4, 4, nz), (2, 4, nz // 2), (4, 4, nz), (nz, 3), (nz, 3), (nz, 4)]
    n_group = 4 * 14 + 3 + nz // 2 + 4 + 4 * 8 + 4
    sems = [pltpu.SemaphoreType.DMA((11,)), pltpu.SemaphoreType.DMA((n_group,))]
    results = [(tokens.shape, BF16), (tokens.shape, BF16), ((d_model, n_dev), F32), ((d_model, d_hidden), F32), ((d_hidden, d_model), F32)]
    row = (1, 128)
    kept = [(tokens.shape, BF16), (tokens.shape, BF16), (ids.shape, jnp.int32), (w_gate.shape, BF16), (w1.shape, BF16), (w2.shape, BF16), (row, F32), (dims + row, F32),
            (dims + tokens.shape, BF16), (dims + tokens.shape, BF16), ((n_row, d_model), BF16), ((n_row, d_model), BF16), ((n_row, d_hidden), BF16), ((n_row, d_hidden), BF16), ((n_row, d_hidden), F32), ((n_dev, 128), F32), (tile, F32), (row, F32),
            (dims + row, F32), ((n_dev, 128), F32), ((1024,) + tile, BF16), ((n_dev,) + row, F32)]
    return pl.pallas_call(
        functools.partial(block_kernel, dims, (6, len(results), len(results), len(kept), 4, 4 * len(work), 3, len(sems))),
        out_shape=[out(*r) for r in results],
        in_specs=[hbm] * 6,
        out_specs=[hbm] * len(results),
        scratch_shapes=[pltpu.VMEM(*r) for r in results + kept] + [pltpu.VMEM((nc, nx, ny, nz) + tile, BF16)] * 4 + [pltpu.VMEM(w + tile, BF16) for w in work] * 4
        + [pltpu.SemaphoreType.DMA((k,)) for k in (8, 2, 11)] + sems,
        compiler_params=pltpu.CompilerParams(collective_id=0, has_side_effects=True, vmem_limit_bytes=VMEM_LIMIT),
        name='block',
    )(tokens, grad_out, ids, w_gate, w1, w2)


VMEM_LIMIT = 67043328
FIRST = 'tmcgttmctgtmtgtcmgt'
SECOND = 'ygbybyBybBybByBxwwyxwxxwy'
THIRD = 'dxwwdxdxwdwx'


def pass_kernel(n, *refs):
    refs = iter(refs)
    given, passed, held, (load_sem, save_sem) = [list(itertools.islice(refs, k)) for k in (n, n, n, 2)]
    loads = [pltpu.make_async_copy(given[k], held[k], load_sem.at[k]) for k in range(n)]
    saves = [pltpu.make_async_copy(held[k], passed[k], save_sem.at[k]) for k in range(n)]
    for cp in loads:
        cp.start()
    for load, save in zip(loads, saves):
        load.wait()
        save.start()
    for cp in saves:
        cp.wait()


def pass_on(*arrays):
    n = len(arrays)
    return pl.pallas_call(
        functools.partial(pass_kernel, n),
        out_shape=[jax.ShapeDtypeStruct(v.shape, v.dtype) for v in arrays],
        in_specs=[pl.BlockSpec(memory_space=pltpu.HBM)] * n,
        out_specs=[pl.BlockSpec(memory_space=pltpu.HBM)] * n,
        scratch_shapes=[pltpu.VMEM(v.shape, v.dtype) for v in arrays] + [pltpu.SemaphoreType.DMA((n,))] * 2,
        compiler_params=pltpu.CompilerParams(vmem_limit_bytes=VMEM_LIMIT),
        name='pass_on',
    )(*arrays)


def local_block(dims, tokens, grad_out, expert_ids, w_gate, w_in, w_out):
    y_out, grad_x, grad_w_gate, g1, g2 = pass_on(*block_call(dims, tokens, grad_out, expert_ids.T, w_gate, w_in[0], w_out[0]))
    return y_out, grad_x, g1[None], g2[None], grad_w_gate


def solution(mesh):
    dims = (8, 4, 4, 2)
    return jax.shard_map(functools.partial(local_block, dims), mesh=mesh, in_specs=(P('ep'), P('ep'), P('ep'), P(), P('ep'), P('ep')), out_specs=(P('ep'), P('ep'), P('ep'), P('ep'), P()), check_vma=False)
```

```python
import functools
import itertools
import math

import jax
import jax.numpy as jnp
from jax import lax
from jax.experimental import pallas as pl
from jax.experimental.pallas import tpu as pltpu
from jax.sharding import PartitionSpec as P

MESH = pl.DeviceIdType.MESH
F32 = jnp.float32
BF16 = jnp.bfloat16
CAP = 8


def coords(dims):
    nz, ny, nx, nc = dims
    me = lax.axis_index('ep')
    c = lax.rem(me, nc)
    x = lax.rem(me // nc, nx)
    y = lax.rem(me // (nc * nx), ny)
    z = me // (nc * nx * ny)

    def dev(z, y, x, c):
        return (((z * ny + y) * nx + x) * nc + c,)

    return z, y, x, c, dev


def meet(peers):
    barrier = pltpu.get_barrier_semaphore()
    for peer in peers:
        pl.semaphore_signal(barrier, inc=1, device_id=peer, device_id_type=MESH)
    pl.semaphore_wait(barrier, len(peers))


def dot(a, b, ca, cb):
    return lax.dot_general(a, b, (((ca,), (cb,)), ((), ())), preferred_element_type=F32)


def iota(shape, axis):
    return lax.broadcasted_iota(jnp.int32, shape, axis)


def as_row(col):
    n = col.shape[0]
    return jnp.sum(jnp.where(iota((n, n), 0) == iota((n, n), 1), col, 0.0), axis=0, keepdims=True)


def as_col(row):
    n = row.shape[1]
    return jnp.sum(jnp.where(iota((n, n), 0) == iota((n, n), 1), row, 0.0), axis=1, keepdims=True)


def gates(tok, i0, i1, w_gate):
    logits = dot(tok, w_gate, 1, 0)
    expert = iota(logits.shape, 1).astype(F32)
    l0, l1 = (jnp.sum(jnp.where(expert == i, logits, 0.0), axis=1, keepdims=True) for i in (i0, i1))
    top = jnp.maximum(l0, l1)
    p0, p1 = jnp.exp(l0 - top), jnp.exp(l1 - top)
    total = p0 + p1
    return p0 / total, p1 / total


def choice_row(tok, ids, w_gate):
    r0, r1 = ids[0:1].astype(F32), ids[1:2].astype(F32)
    i0, i1 = as_col(r0), as_col(r1)
    g0, g1 = gates(tok, i0, i1, w_gate)

    def code(i):
        n = jnp.sum((i == r0).astype(F32) + (i == r1).astype(F32), axis=1, keepdims=True)
        return as_row(jnp.where(n > 1.5, i + 256.0, i))

    return jnp.concatenate([code(i0), code(i1), as_row(g0), as_row(g1)], axis=1)


def gelu_tanh(a):
    k = 0.7978845608028654
    sq = a * a
    return jnp.tanh(a * (k + (k * 0.044715) * sq)), sq


def gelu(a):
    half = 0.5 * a
    return half + half * gelu_tanh(a)[0]


def gelu_slope(a):
    k = 0.7978845608028654
    t, sq = gelu_tanh(a)
    return (0.5 + 0.5 * t) + (0.5 * a) * (1.0 - t * t) * (k + (3 * k * 0.044715) * sq)


def token_lanes(ref, k, start, n):
    lane = iota((n, 128), 1) // 32
    out = jnp.zeros((n, 128), F32)
    for j in range(4):
        r = ref[pl.ds(start + j, n, stride=4), :]
        out = jnp.where(lane == j, r if j == k else pltpu.roll(r, 32 * (j - k) % 128, 1), out)
    return out


def pair_rows(v):
    return jnp.concatenate([jnp.concatenate([v[2 * i:2 * i + 1], v[2 * i + 1:2 * i + 2]], axis=1) for i in range(v.shape[0] // 2)], axis=0)


def plain_id(code):
    return jnp.where(code >= 256.0, code - 256.0, code)


class Links:
    def __init__(self, send, recv, pool):
        self.send, self.recv, self.pool, self.bytes = send, recv, pool, 0

    def group(self):
        return self.recv.at[next(self.pool)]

    def go(self, src, dst, to, group):
        pltpu.make_async_remote_copy(src_ref=src, dst_ref=dst, send_sem=self.send, recv_sem=group, device_id=to, device_id_type=MESH).start()
        self.bytes += math.prod(src.shape) * jnp.dtype(src.dtype).itemsize

    def wait(self, group, ref):
        pltpu.make_async_copy(ref, ref, group).wait()

    def finish(self, *pads):
        for pad in pads:
            unit = math.prod(pad.shape[1:]) * jnp.dtype(pad.dtype).itemsize
            if self.bytes % unit == 0:
                return self.wait(self.send, pad.at[pl.ds(0, self.bytes // unit)])
        raise ValueError(self.bytes)


def block_kernel(dims, sizes, *refs):
    nz, ny, nx, nc = dims
    refs = iter(refs)
    refs = [list(itertools.islice(refs, n)) for n in sizes]
    (tok_hbm, dout_hbm, ids_hbm, wg_hbm, w1_hbm, w2_hbm), outs, held, kept, rows, areas, (load_sem, keep_sem, save_sem), sems = refs
    out_ref, gx_ref, gate_ref, g1_ref, g2_ref = held
    tok, dout, ids, wg, w1, w2, row, m_land, x_all, g_all, xs_ref, dys_ref, h_ref, da_ref, a_ref, m_all, hot_ref, d_row, d_land, d_all, pad, pad_row = kept
    z, y, x, c, dev = coords(dims)
    saves = []

    def save(k, part=None):
        src, dst = (held[k], outs[k]) if part is None else (held[k].at[part], outs[k].at[part])
        cp = pltpu.make_async_copy(src, dst, save_sem.at[len(saves)])
        cp.start()
        saves.append(cp)

    send_sem, recv_sem = sems
    pool = itertools.count()
    all_links = [Links(send_sem.at[k], recv_sem, pool) for k in range(send_sem.shape[0])]
    links = iter(all_links)

    loads = [pltpu.make_async_copy(s, d, load_sem.at[k]) for k, (s, d) in enumerate(
        [(tok_hbm, x_all.at[z, y, x, c]), (dout_hbm, g_all.at[z, y, x, c]), (tok_hbm, tok), (ids_hbm, ids), (wg_hbm, wg), (dout_hbm, dout), (w1_hbm, w1), (w2_hbm, w2)])]
    for ld in loads:
        ld.start()
    peers = [dev(lax.rem(z + d, nz), y, x, c) for d in range(1, nz)]
    for d in (1, 2, 3):
        peers.append(dev(z, lax.rem(y + d, ny), x, c))
        peers.append(dev(z, y, lax.rem(x + d, nx), c))
    mate = dev(z, y, x, 1 - c)
    peers.append(mate)
    meet(peers)

    full = slice(None)
    by_distance = sorted(range(1, nz), key=lambda d: abs(d - nz // 2))

    def step(v, d, m=4):
        return lax.rem(v + d, m)

    def by_lines(link, ref, rows, x_last):
        p0, q0 = (y, x) if x_last else (x, y)
        low, high = pl.ds(0, nz // 2), pl.ds(nz // 2, nz // 2)

        def at(zs, p, q):
            return ref.at[(zs, p, q, c, rows) if x_last else (zs, q, p, c, rows)]

        def go(part, p, q, group):
            link.go(part, part, dev(z, p, q, c) if x_last else dev(z, q, p, c), group)

        in_z, in_p, in_m, in_f, in_r, in_c = [link.group() for _ in range(6)]
        line = at(full, p0, q0)

        def over(q):
            part = at(full, full, q)
            link.go(part, part, mate, in_c)

        own = at(z, p0, q0)
        for d in by_distance:
            link.go(own, own, dev(step(z, d, nz), y, x, c), in_z)
        yield
        link.wait(in_z, at(pl.ds(0, nz - 1), p0, q0))
        pm, pp, po = step(p0, 3), step(p0, 1), step(p0, 2)
        qm, qp, qo = step(q0, 3), step(q0, 1), step(q0, 2)
        qs = []

        def spread(p):
            part = at(full, p, q0)
            qs.append((p, link.group(), link.group()))
            go(part, p0, qp, qs[-1][1])
            go(part, p0, qm, qs[-1][2])

        def relay(i):
            p, up, dn = qs[i]
            link.wait(up, line)
            go(at(low, p, qm), p0, qp, in_r)
            link.wait(dn, line)
            go(at(high, p, qp), p0, qm, in_r)

        go(line, pp, q0, in_p)
        go(line, pm, q0, in_m)
        spread(p0)
        yield
        link.wait(in_p, line)
        go(at(low, pm, q0), pp, q0, in_f)
        link.wait(in_m, line)
        go(at(high, pp, q0), pm, q0, in_f)
        spread(pm)
        spread(pp)
        yield
        relay(0)
        yield
        link.wait(in_f, line)
        spread(po)
        over(q0)
        for i in range(1, 4):
            yield
            relay(i)
        over(qm)
        over(qp)
        yield
        link.wait(in_r, at(full, full, q0))
        over(qo)
        yield
        link.wait(in_c, ref.at[full, full, full, c, rows])

    def gather_rows(link, held, order):
        have = [z, y, x, c]
        for axis in order:
            size = (nz, ny, nx, nc)[axis]
            part = held.at[tuple(have)]
            group = link.group()
            for d in sorted(range(1, size), key=lambda d: abs(d - size // 2)):
                there = [z, y, x, c]
                there[axis] = lax.rem(there[axis] + d, size)
                link.go(part, part, dev(*there), group)
            have[axis] = pl.ds(0, size - 1)
            yield
            link.wait(group, held.at[tuple(have)])
            have[axis] = full

    def advance(plans):
        for g in plans:
            next(g, None)

    halves = [slice(0, 16), slice(16, 32)]
    tok_plans, grad_plans = [[by_lines(next(links), ref, half, half.start == 0) for half in halves] for ref in (x_all, g_all)]
    loads[0].wait()
    advance(tok_plans)
    for ld in loads[2:5]:
        ld.wait()
    row[...] = choice_row(tok[...], ids[...], wg[...])
    place = pltpu.make_async_copy(row, m_land.at[z, y, x, c], keep_sem.at[0])
    place.start()
    place.wait()
    row_plan = [gather_rows(next(links), m_land, range(4))]
    loads[1].wait()
    advance(row_plan + grad_plans)
    def flatten(land, flat):
        def lines(zz, carry):
            for k in range(ny * nx * nc):
                flat[pl.ds(zz * (ny * nx * nc) + k, 1), :] = land[zz, k // (nx * nc), k // nc % nx, k % nc]
            return carry

        lax.fori_loop(0, nz, lines, 0)


    me = lax.axis_index('ep').astype(F32)
    def read_rows():
        flatten(m_land, m_all)
        for ld in loads[5:]:
            ld.wait()
        code = m_all[...]
        left = jnp.where((iota(code.shape, 1) < 64) & (code >= 256.0), code - 256.0, 999.0)
        found = []
        for _ in range(3):
            best = jnp.min(jnp.min(left, axis=0, keepdims=True), axis=1, keepdims=True)
            left = jnp.where(left == best, 999.0, left)
            found.append(jnp.broadcast_to(best, (1, 128)))
        hot_ref[...] = jnp.concatenate(found + [jnp.full((5, 128), 999.0, F32)], axis=0)

    steps = 4 if nz == 8 else 1
    per = nz // steps
    n_quad = per * ny * nx * nc // 4
    n_pair = n_quad // 2
    n_slot = n_pair * 8 * CAP

    places = [(cc, xx, yy, zz) for cc in range(nc) for xx in range(nx) for yy in range(ny) for zz in range(per)]

    def select(i, ref, with_gate):
        c0, c1, g0, g1 = (pair_rows(token_lanes(m_all, k, pl.multiple_of(4 * n_quad * i, 4 * n_quad), n_quad)) for k in range(4))
        hit0, hit1 = plain_id(c0) == me, plain_id(c1) == me
        hit = (hit0 | hit1).astype(F32)
        gate = jnp.where(hit0, g0, 0.0) + jnp.where(hit1, g1, 0.0)
        before, after = iota((256, 256), 0), iota((256, 256), 1)
        tri = ((before < after) & (before // 32 == after // 32)).astype(F32).astype(BF16)
        rank = dot(hit.astype(BF16), tri, 1, 0)
        src = (iota((n_pair, 256), 1) // 32).astype(F32)
        key = jnp.where(hit > 0.0, src * CAP + rank, -1.0)
        slot = iota((8 * CAP, 256), 0).astype(F32)
        parts = []
        for p in range(n_pair):
            sel = (slot == key[p:p + 1]).astype(F32)
            v = dot(sel.astype(BF16), ref[i * per + p // ny, p % ny].reshape(256, 256), 1, 0)
            parts.append(v * jnp.sum(sel * gate[p:p + 1], axis=1, keepdims=True) if with_gate else v)
        return jnp.concatenate([parts[zz * ny + yy][CAP * (xx * nc + cc):CAP * (xx * nc + cc + 1)] for cc, xx, yy, zz in places], axis=0).astype(BF16)

    def put(i, v, to):
        for k, (cc, xx, yy, zz) in enumerate(places):
            for half in range(2):
                to[half][cc, xx, yy, i * per + zz] = v[CAP * k:CAP * (k + 1), 128 * half:128 * (half + 1)].astype(BF16)

    def forward(i):
        here = pl.ds(i * n_slot, n_slot)
        xs = select(i, x_all, False)
        a = dot(xs, w1[...], 1, 0)
        h = gelu(a).astype(BF16)
        xs_ref[here], h_ref[here], a_ref[here] = xs, h, a
        put(i, dot(h, w2[...], 1, 0), rows[:2])

    def backward(i):
        here = pl.ds(i * n_slot, n_slot)
        dys = select(i, g_all, True)
        dys_ref[here] = dys
        da_ref[here] = (dot(dys, w2[...], 1, 1) * gelu_slope(a_ref[here])).astype(BF16)

    def backward_rows(i):
        put(i, dot(da_ref[pl.ds(i * n_slot, n_slot)], w1[...], 1, 1), rows[2:])

    def back(i):
        h = rows[i]
        other, near, via, out2, via2, in2, out3, hot_land, cold_land = areas[9 * i:9 * i + 9]
        link = next(links)
        go = link.go
        in_c, in_e, in_h = [[link.group(), link.group()] for _ in range(3)]
        in_n, in_v, in_2, in_l, in_s = [link.group() for _ in range(5)]
        x_first = i % 2 == 0
        a, b = (x, y) if x_first else (y, x)

        def to(a, b):
            return dev(z, b, a, c) if x_first else dev(z, a, b, c)

        def index(lead, a, bs):
            return lead + ((a, bs) if x_first else (bs, a))

        up, dn, far = step(a, 1), step(a, 3), step(a, 2)
        lo, hi = pl.ds(0, 2), pl.ds(2, 2)
        parts = [pl.ds(0, nz // 2), pl.ds(nz // 2, nz // 2)]

        def start(k):
            zs = parts[k]
            go(h.at[1 - c, :, :, zs], other.at[:, :, zs], mate, in_c[k])
            spread(h, (c,), c, zs, in_e[k])

        def follow(k):
            link.wait(in_c[k], other.at[:, :, parts[k]])
            spread(other, (), 1 - c, parts[k], in_h[k])

        def spread(ref, lead, e, zs, group):
            go(ref.at[index(lead, far, lo) + (zs,)], via.at[0, e, :, zs], to(up, b), group)
            go(ref.at[index(lead, far, hi) + (zs,)], via.at[1, e, :, zs], to(dn, b), group)
            go(ref.at[index(lead, up, full) + (zs,)], near.at[a, e, :, zs], to(up, b), in_n)
            go(ref.at[index(lead, dn, full) + (zs,)], near.at[a, e, :, zs], to(dn, b), in_n)

        def relay(e, zs, group):
            link.wait(group, via.at[:, e, :, zs])
            go(via.at[0, e, :, zs], near.at[dn, e, lo, zs], to(up, b), in_n)
            go(via.at[1, e, :, zs], near.at[up, e, hi, zs], to(dn, b), in_n)

        start(0)
        yield
        follow(0)
        yield
        start(1)
        yield
        relay(c, parts[0], in_e[0])
        relay(1 - c, parts[0], in_h[0])
        yield
        follow(1)
        yield
        relay(c, parts[1], in_e[1])
        yield
        relay(1 - c, parts[1], in_h[1])
        yield
        link.wait(in_n, near.at[pl.ds(0, 3)])

        def expert(s, e):
            return ((z * ny + y) * nx + s) * nc + e if x_first else ((z * ny + s) * nx + x) * nc + e

        places = [(step(a, d), e) for d in range(4) for e in (c, 1 - c)]
        is_hot = [[(hot_ref[j:j + 1, :] == expert(s, e).astype(F32)).astype(F32) for s, e in places] for j in range(3)]
        wide = lambda v: jnp.broadcast_to(v, (8, 128))
        weight = [[wide(v).astype(BF16) for v in r] for r in is_hot]
        line = iota((8, 128), 0)
        mine = [(wide(is_hot[0][k] + is_hot[1][k] + is_hot[2][k]) < 0.5) & (line == s * nc + e) for k, (s, e) in enumerate(places)]

        def squeeze(bb, carry):
            given = [h[index((c,), a, bb)], other[index((), a, bb)]] + [near[s, e, bb] for s, e in places[2:]]
            for j in range(3):
                out2[bb, j] = sum(given[k] * weight[j][k] for k in range(8))
            singles = jnp.zeros((nz, 8, 128), F32)
            for k in range(8):
                singles = jnp.where(mine[k], jnp.sum(given[k].astype(F32), axis=1, keepdims=True), singles)
            out2[bb, 3] = singles.astype(BF16)
            return carry

        lax.fori_loop(0, 4, squeeze, 0)
        up, dn, far = step(b, 1), step(b, 3), step(b, 2)
        lo, hi = pl.ds(0, nz // 2), pl.ds(nz // 2, nz // 2)
        go(out2.at[far, :, lo], via2.at[0], to(a, up), in_v)
        go(out2.at[far, :, hi], via2.at[1], to(a, dn), in_v)
        go(out2.at[up], in2.at[b], to(a, up), in_2)
        go(out2.at[dn], in2.at[b], to(a, dn), in_2)
        in2[b] = out2[b]
        yield
        link.wait(in_v, via2)
        go(via2.at[0], in2.at[dn, :, lo], to(a, up), in_2)
        go(via2.at[1], in2.at[up, :, hi], to(a, dn), in_2)
        yield
        link.wait(in_2, in2.at[pl.ds(0, 3)])
        for j in range(3):
            out3[:, j] = (in2[0, j] + in2[1, j]) + (in2[2, j] + in2[3, j])
        for d in by_distance:
            zz = lax.rem(z + d, nz)
            go(in2.at[:, 3, zz], cold_land.at[z], dev(zz, y, x, c), in_s)
            go(out3.at[zz], hot_land.at[z], dev(zz, y, x, c), in_l)
        cold_land[z] = in2[:, 3, z]
        hot_land[z] = out3[z]
        yield
        link.wait(in_s, cold_land.at[pl.ds(0, nz - 1)])
        link.wait(in_l, hot_land.at[pl.ds(0, nz - 1)])

    def weight_grad(k):
        if k % 2 == 0:
            part = slice(w2.shape[0] // 4 * (k // 2), w2.shape[0] // 4 * (k // 2 + 1))
            g2_ref[part, :] = dot(h_ref[:, part], dys_ref[...], 0, 0)
            save(4, (part, full))
        else:
            part = slice(w1.shape[1] // 4 * (k // 2), w1.shape[1] // 4 * (k // 2 + 1))
            g1_ref[:, part] = dot(xs_ref[...], da_ref[:, part], 0, 0)
            save(3, (full, part))

    ys, dxs = [back(0), back(1)], [back(2), back(3)]
    n_tok = tok.shape[0]
    memo = {}
    earlier = iota((n_tok, n_tok), 1) < iota((n_tok, n_tok), 0)
    n_exp = wg.shape[1]

    def where_from(i, r0, r1):
        rank = jnp.sum(jnp.where(earlier & ((i == r0) | (i == r1)), 1.0, 0.0), axis=1, keepdims=True)
        slot = jnp.full((n_tok, 1), -1.0, F32)
        for j in range(3):
            slot = jnp.where(i == hot_ref[j:j + 1, 0:1], CAP * j + rank, slot)
        e = i.astype(jnp.int32)
        core, xx, yy, zz = e % nc, (e // nc) % nx, (e // (nc * nx)) % ny, e // (nc * nx * ny)
        lane, single = iota((n_tok, n_exp), 1), slot < 0.0
        pick = lambda m: m.astype(F32).astype(BF16)
        return pick(iota((n_tok, 32), 1).astype(F32) == slot), (pick((lane == e) & single), pick((lane == ((zz * nx + xx) * ny + yy) * nc + core) & single))

    def rows_of(kind, chosen):
        parts = []
        for half in range(2):
            hot_land, cold_land = areas[9 * (kind + half) + 7:9 * (kind + half) + 9]
            hot = jnp.sum(hot_land[...].astype(F32), axis=0).reshape(24, 128)
            hot = jnp.concatenate([hot, jnp.zeros((8, 128), F32)], axis=0).astype(BF16)
            cold = cold_land[...].astype(F32).reshape(n_exp, 128).astype(BF16)
            parts.append([dot(by_slot, hot, 1, 0) + dot(by_place[half], cold, 1, 0) for by_slot, by_place in chosen])
        return [jnp.concatenate([parts[0][k], parts[1][k]], axis=1) for k in range(2)]

    def combine():
        r0, r1 = ids[0:1].astype(F32), ids[1:2].astype(F32)
        i0, i1 = as_col(r0), as_col(r1)
        g0, g1 = gates(tok[...], i0, i1, wg[...])
        chosen = [where_from(i, r0, r1) for i in (i0, i1)]
        y0, y1 = rows_of(0, chosen)
        grad = dout[...].astype(F32)
        dg0, dg1 = (jnp.sum(grad * v, axis=1, keepdims=True) for v in (y0, y1))
        mean = g0 * dg0 + g1 * dg1
        d0, d1 = ((g * (dg - mean)).astype(BF16).astype(F32) for g, dg in ((g0, dg0), (g1, dg1)))
        d_row[...] = jnp.concatenate([as_row(d0), as_row(d1), jnp.zeros((1, 2 * n_tok), F32)], axis=1)
        place = pltpu.make_async_copy(d_row, d_land.at[z, y, x, c], keep_sem.at[1])
        place.start()
        out_ref[...] = (g0 * y0 + g1 * y1).astype(BF16)
        save(0)
        place.wait()
        d_plans.append(gather_rows(next(links), d_land, range(4)))
        advance(d_plans)
        expert = iota((n_tok, n_exp), 1).astype(F32)
        spread = jnp.where(expert == i0, d0, jnp.where(expert == i1, d1, 0.0)).astype(BF16)
        memo.update(chosen=chosen, through=dot(spread, wg[...], 1, 1))

    def finish():
        dx0, dx1 = rows_of(2, memo['chosen'])
        gx_ref[...] = (dx0 + dx1 + memo['through']).astype(BF16)
        save(1)

    n_dev = nz * ny * nx * nc

    def gate_grad():
        flatten(d_land, d_all)
        expert = iota((n_exp, 256), 0).astype(F32)
        codes = [plain_id(pair_rows(token_lanes(m_all, k, 0, n_dev // 4))) for k in range(2)]
        grads = [pair_rows(token_lanes(d_all, k, 0, n_dev // 4)) for k in range(2)]
        total = jnp.zeros((n_exp, x_all.shape[-1]), F32)
        zs = nz // 4 or 1
        for z0 in range(0, nz, zs):
            spread = []
            for p in range(z0 * ny, (z0 + zs) * ny):
                q = slice(p, p + 1)
                spread.append(jnp.where(expert == codes[0][q], grads[0][q], jnp.where(expert == codes[1][q], grads[1][q], 0.0)).astype(BF16))
            total += dot(jnp.concatenate(spread, axis=1), x_all[z0:z0 + zs].reshape(zs * ny * 256, x_all.shape[-1]), 1, 0)
        gate_ref[...] = total.T
        save(2)

    d_plans = []
    moves = {'t': tok_plans, 'g': grad_plans, 'm': row_plan, 'y': ys, 'x': dxs, 'd': d_plans}
    works = {'f': [functools.partial(forward, i) for i in range(steps)], 'b': [functools.partial(backward, i) for i in range(steps)],
             'B': [functools.partial(backward_rows, i) for i in range(steps)], 'w': [functools.partial(weight_grad, k) for k in range(8)],
             'h': [read_rows], 'c': [combine], 'k': [gate_grad], 'e': [finish]}
    for turn in SCHEDULE:
        if turn in moves:
            advance(moves[turn])
        elif works[turn]:
            works[turn].pop(0)()
    for link in all_links:
        link.finish(pad, pad_row)
    for cp in saves:
        cp.wait()


def block_call(dims, tokens, grad_out, ids, w_gate, w1, w2):
    nz, ny, nx, nc = dims
    d_model, d_hidden = w1.shape
    n_tok = tokens.shape[0]
    n_dev = nz * ny * nx * nc
    n_row = n_dev * CAP
    tile = (CAP, 128)
    hbm = pl.BlockSpec(memory_space=pltpu.HBM)
    out = jax.ShapeDtypeStruct
    work = [(4, 4, nz), (4, 2, 4, nz), (2, 2, 2, nz), (4, 4, nz), (2, 4, nz // 2), (4, 4, nz), (nz, 3), (nz, 3), (nz, 4)]
    n_group = 4 * 14 + 4 + 4 * 11 + 4
    sems = [pltpu.SemaphoreType.DMA((10,)), pltpu.SemaphoreType.DMA((n_group,))]
    results = [(tokens.shape, BF16), (tokens.shape, BF16), ((d_model, n_dev), F32), ((d_model, d_hidden), F32), ((d_hidden, d_model), F32)]
    row = (1, 128)
    kept = [(tokens.shape, BF16), (tokens.shape, BF16), (ids.shape, jnp.int32), (w_gate.shape, BF16), (w1.shape, BF16), (w2.shape, BF16), (row, F32), (dims + row, F32),
            (dims + tokens.shape, BF16), (dims + tokens.shape, BF16), ((n_row, d_model), BF16), ((n_row, d_model), BF16), ((n_row, d_hidden), BF16), ((n_row, d_hidden), BF16), ((n_row, d_hidden), F32), ((n_dev, 128), F32), (tile, F32), (row, F32),
            (dims + row, F32), ((n_dev, 128), F32), ((1024,) + tile, BF16), ((n_dev,) + row, F32)]
    return pl.pallas_call(
        functools.partial(block_kernel, dims, (6, len(results), len(results), len(kept), 4, 4 * len(work), 3, len(sems))),
        out_shape=[out(*r) for r in results],
        in_specs=[hbm] * 6,
        out_specs=[hbm] * len(results),
        scratch_shapes=[pltpu.VMEM(*r) for r in results + kept] + [pltpu.VMEM((nc, nx, ny, nz) + tile, BF16)] * 4 + [pltpu.VMEM(w + tile, BF16) for w in work] * 4
        + [pltpu.SemaphoreType.DMA((k,)) for k in (8, 2, 11)] + sems,
        compiler_params=pltpu.CompilerParams(collective_id=0, has_side_effects=True, vmem_limit_bytes=VMEM_LIMIT),
        name='block',
    )(tokens, grad_out, ids, w_gate, w1, w2)


VMEM_LIMIT = 67043328
SCHEDULE = 'tmttmgttmgttgmtgth' + 'fgfgyfgyf' + 'ygygybyybyBBxbybBBxxyx' + 'wxwwxwxyc' + 'wxwwdxdwxddkx' + 'e'


def pass_kernel(n, *refs):
    refs = iter(refs)
    given, passed, held, (load_sem, save_sem) = [list(itertools.islice(refs, k)) for k in (n, n, n, 2)]
    loads = [pltpu.make_async_copy(given[k], held[k], load_sem.at[k]) for k in range(n)]
    saves = [pltpu.make_async_copy(held[k], passed[k], save_sem.at[k]) for k in range(n)]
    for cp in loads:
        cp.start()
    for load, save in zip(loads, saves):
        load.wait()
        save.start()
    for cp in saves:
        cp.wait()


def pass_on(*arrays):
    n = len(arrays)
    return pl.pallas_call(
        functools.partial(pass_kernel, n),
        out_shape=[jax.ShapeDtypeStruct(v.shape, v.dtype) for v in arrays],
        in_specs=[pl.BlockSpec(memory_space=pltpu.HBM)] * n,
        out_specs=[pl.BlockSpec(memory_space=pltpu.HBM)] * n,
        scratch_shapes=[pltpu.VMEM(v.shape, v.dtype) for v in arrays] + [pltpu.SemaphoreType.DMA((n,))] * 2,
        compiler_params=pltpu.CompilerParams(vmem_limit_bytes=VMEM_LIMIT),
        name='pass_on',
    )(*arrays)


def local_block(dims, tokens, grad_out, expert_ids, w_gate, w_in, w_out):
    y_out, grad_x, grad_w_gate, g1, g2 = pass_on(*block_call(dims, tokens, grad_out, expert_ids.T, w_gate, w_in[0], w_out[0]))
    return y_out, grad_x, g1[None], g2[None], grad_w_gate


def solution(mesh):
    dims = (8, 4, 4, 2)
    return jax.shard_map(functools.partial(local_block, dims), mesh=mesh, in_specs=(P('ep'), P('ep'), P('ep'), P(), P('ep'), P('ep')), out_specs=(P('ep'), P('ep'), P('ep'), P('ep'), P()), check_vma=False)
```

```python
import functools
import itertools
import math

import jax
import jax.numpy as jnp
from jax import lax
from jax.experimental import pallas as pl
from jax.experimental.pallas import tpu as pltpu
from jax.sharding import PartitionSpec as P

MESH = pl.DeviceIdType.MESH
F32 = jnp.float32
BF16 = jnp.bfloat16
CAP = 8


def coords(dims):
    nz, ny, nx, nc = dims
    me = lax.axis_index('ep')
    c = lax.rem(me, nc)
    x = lax.rem(me // nc, nx)
    y = lax.rem(me // (nc * nx), ny)
    z = me // (nc * nx * ny)

    def dev(z, y, x, c):
        return (((z * ny + y) * nx + x) * nc + c,)

    return z, y, x, c, dev


def dot(a, b, ca, cb):
    return lax.dot_general(a, b, (((ca,), (cb,)), ((), ())), preferred_element_type=F32)


def iota(shape, axis):
    return lax.broadcasted_iota(jnp.int32, shape, axis)


def as_row(col):
    n = col.shape[0]
    return jnp.sum(jnp.where(iota((n, n), 0) == iota((n, n), 1), col, 0.0), axis=0, keepdims=True)


def as_col(row):
    n = row.shape[1]
    return jnp.sum(jnp.where(iota((n, n), 0) == iota((n, n), 1), row, 0.0), axis=1, keepdims=True)


def gates(tok, i0, i1, w_gate):
    logits = dot(tok, w_gate, 1, 0)
    expert = iota(logits.shape, 1).astype(F32)
    l0, l1 = (jnp.sum(jnp.where(expert == i, logits, 0.0), axis=1, keepdims=True) for i in (i0, i1))
    top = jnp.maximum(l0, l1)
    p0, p1 = jnp.exp(l0 - top), jnp.exp(l1 - top)
    total = p0 + p1
    return p0 / total, p1 / total


def choice_row(tok, ids, w_gate):
    r0, r1 = ids[0:1].astype(F32), ids[1:2].astype(F32)
    i0, i1 = as_col(r0), as_col(r1)
    g0, g1 = gates(tok, i0, i1, w_gate)

    def code(i):
        n = jnp.sum((i == r0).astype(F32) + (i == r1).astype(F32), axis=1, keepdims=True)
        return as_row(jnp.where(n > 1.5, i + 256.0, i))

    return jnp.concatenate([code(i0), code(i1), as_row(g0), as_row(g1)], axis=1)


def gelu_tanh(a):
    k = 0.7978845608028654
    sq = a * a
    return jnp.tanh(a * (k + (k * 0.044715) * sq)), sq


def gelu(a):
    half = 0.5 * a
    return half + half * gelu_tanh(a)[0]


def gelu_slope(a):
    k = 0.7978845608028654
    t, sq = gelu_tanh(a)
    return (0.5 + 0.5 * t) + (0.5 * a) * (1.0 - t * t) * (k + (3 * k * 0.044715) * sq)


def token_lanes(ref, k, start, n):
    lane = iota((n, 128), 1) // 32
    out = jnp.zeros((n, 128), F32)
    for j in range(4):
        r = ref[pl.ds(start + j, n, stride=4), :]
        out = jnp.where(lane == j, r if j == k else pltpu.roll(r, 32 * (j - k) % 128, 1), out)
    return out


def pair_rows(v):
    return jnp.concatenate([jnp.concatenate([v[2 * i:2 * i + 1], v[2 * i + 1:2 * i + 2]], axis=1) for i in range(v.shape[0] // 2)], axis=0)


def plain_id(code):
    return jnp.where(code >= 256.0, code - 256.0, code)


class Links:
    def __init__(self, send, recv, pool):
        self.send, self.recv, self.pool, self.bytes = send, recv, pool, 0

    def group(self):
        return self.recv.at[next(self.pool)]

    def go(self, src, dst, to, group):
        pltpu.make_async_remote_copy(src_ref=src, dst_ref=dst, send_sem=self.send, recv_sem=group, device_id=to, device_id_type=MESH).start()
        self.bytes += math.prod(src.shape) * jnp.dtype(src.dtype).itemsize

    def wait(self, group, ref):
        pltpu.make_async_copy(ref, ref, group).wait()

    def finish(self, *pads):
        for pad in pads:
            unit = math.prod(pad.shape[1:]) * jnp.dtype(pad.dtype).itemsize
            if self.bytes % unit == 0:
                return self.wait(self.send, pad.at[pl.ds(0, self.bytes // unit)])
        raise ValueError(self.bytes)


def block_kernel(dims, sizes, *refs):
    nz, ny, nx, nc = dims
    refs = iter(refs)
    refs = [list(itertools.islice(refs, n)) for n in sizes]
    (tok_hbm, dout_hbm, ids_hbm, wg_hbm, w1_hbm, w2_hbm), outs, held, kept, rows, areas, (load_sem, keep_sem, save_sem), sems = refs
    out_ref, gx_ref, gate_ref, g1_ref, g2_ref = held
    tok, dout, ids, wg, w1, w2, row, m_land, x_all, g_all, xs_ref, dys_ref, h_ref, da_ref, a_ref, m_all, hot_ref, d_row, d_land, d_all, pad, pad_row = kept
    z, y, x, c, dev = coords(dims)
    saves = []

    def save(k, part=None):
        src, dst = (held[k], outs[k]) if part is None else (held[k].at[part], outs[k].at[part])
        cp = pltpu.make_async_copy(src, dst, save_sem.at[len(saves)])
        cp.start()
        saves.append(cp)

    send_sem, recv_sem = sems
    pool = itertools.count()
    all_links = [Links(send_sem.at[k], recv_sem, pool) for k in range(send_sem.shape[0])]
    links = iter(all_links)

    loads = [pltpu.make_async_copy(s, d, load_sem.at[k]) for k, (s, d) in enumerate(
        [(tok_hbm, x_all.at[z, y, x, c]), (dout_hbm, g_all.at[z, y, x, c]), (tok_hbm, tok), (ids_hbm, ids), (wg_hbm, wg), (dout_hbm, dout), (w1_hbm, w1), (w2_hbm, w2)])]
    for ld in loads:
        ld.start()
    peers = [dev(lax.rem(z + d, nz), y, x, c) for d in range(1, nz)]
    for d in (1, 2, 3):
        peers.append(dev(z, lax.rem(y + d, ny), x, c))
        peers.append(dev(z, y, lax.rem(x + d, nx), c))
    mate = dev(z, y, x, 1 - c)
    peers.append(mate)
    barrier = pltpu.get_barrier_semaphore()
    for peer in peers:
        pl.semaphore_signal(barrier, inc=1, device_id=peer, device_id_type=MESH)
    for ld in loads[2:5]:
        ld.wait()
    row[...] = choice_row(tok[...], ids[...], wg[...])
    place = pltpu.make_async_copy(row, m_land.at[z, y, x, c], keep_sem.at[0])
    place.start()
    loads[0].wait()
    loads[1].wait()
    place.wait()
    pl.semaphore_wait(barrier, len(peers))

    full = slice(None)
    by_distance = sorted(range(1, nz), key=lambda d: abs(d - nz // 2))

    def step(v, d, m=4):
        return lax.rem(v + d, m)

    def by_lines(link, ref, rows, x_last):
        p0, q0 = (y, x) if x_last else (x, y)
        low, high = pl.ds(0, nz // 2), pl.ds(nz // 2, nz // 2)

        def at(zs, p, q):
            return ref.at[(zs, p, q, c, rows) if x_last else (zs, q, p, c, rows)]

        def go(part, p, q, group):
            link.go(part, part, dev(z, p, q, c) if x_last else dev(z, q, p, c), group)

        in_z, in_p, in_m, in_f, in_r, in_c = [link.group() for _ in range(6)]
        line = at(full, p0, q0)

        def over(q):
            part = at(full, full, q)
            link.go(part, part, mate, in_c)

        own = at(z, p0, q0)
        for d in by_distance:
            link.go(own, own, dev(step(z, d, nz), y, x, c), in_z)
        yield
        link.wait(in_z, at(pl.ds(0, nz - 1), p0, q0))
        pm, pp, po = step(p0, 3), step(p0, 1), step(p0, 2)
        qm, qp, qo = step(q0, 3), step(q0, 1), step(q0, 2)
        qs = []

        def spread(p):
            part = at(full, p, q0)
            qs.append((p, link.group(), link.group()))
            go(part, p0, qp, qs[-1][1])
            go(part, p0, qm, qs[-1][2])

        def relay(i):
            p, up, dn = qs[i]
            link.wait(up, line)
            go(at(low, p, qm), p0, qp, in_r)
            link.wait(dn, line)
            go(at(high, p, qp), p0, qm, in_r)

        go(line, pp, q0, in_p)
        go(line, pm, q0, in_m)
        spread(p0)
        yield
        link.wait(in_p, line)
        go(at(low, pm, q0), pp, q0, in_f)
        link.wait(in_m, line)
        go(at(high, pp, q0), pm, q0, in_f)
        spread(pm)
        spread(pp)
        yield
        relay(0)
        yield
        link.wait(in_f, line)
        spread(po)
        over(q0)
        for i in range(1, 4):
            yield
            relay(i)
        over(qm)
        over(qp)
        yield
        link.wait(in_r, at(full, full, q0))
        over(qo)
        yield
        link.wait(in_c, ref.at[full, full, full, c, rows])

    def gather_rows(link, held, order):
        have = [z, y, x, c]
        for axis in order:
            size = (nz, ny, nx, nc)[axis]
            part = held.at[tuple(have)]
            group = link.group()
            for d in sorted(range(1, size), key=lambda d: abs(d - size // 2)):
                there = [z, y, x, c]
                there[axis] = lax.rem(there[axis] + d, size)
                link.go(part, part, dev(*there), group)
            have[axis] = pl.ds(0, size - 1)
            yield
            link.wait(group, held.at[tuple(have)])
            have[axis] = full

    def advance(plans):
        for g in plans:
            next(g, None)

    halves = [slice(0, 16), slice(16, 32)]
    tok_plans, grad_plans = [[by_lines(next(links), ref, half, half.start == 0) for half in halves] for ref in (x_all, g_all)]
    row_plan = [gather_rows(next(links), m_land, range(4))]
    advance(tok_plans)
    advance(row_plan + grad_plans)
    def flatten(land, flat):
        def lines(zz, carry):
            for k in range(ny * nx * nc):
                flat[pl.ds(zz * (ny * nx * nc) + k, 1), :] = land[zz, k // (nx * nc), k // nc % nx, k % nc]
            return carry

        lax.fori_loop(0, nz, lines, 0)


    me = lax.axis_index('ep').astype(F32)
    def read_rows():
        flatten(m_land, m_all)
        for ld in loads[5:]:
            ld.wait()
        code = m_all[...]
        left = jnp.where((iota(code.shape, 1) < 64) & (code >= 256.0), code - 256.0, 999.0)
        found = []
        for _ in range(3):
            best = jnp.min(jnp.min(left, axis=0, keepdims=True), axis=1, keepdims=True)
            left = jnp.where(left == best, 999.0, left)
            found.append(jnp.broadcast_to(best, (1, 128)))
        hot_ref[...] = jnp.concatenate(found + [jnp.full((5, 128), 999.0, F32)], axis=0)

    steps = 4 if nz == 8 else 1
    per = nz // steps
    n_quad = per * ny * nx * nc // 4
    n_pair = n_quad // 2
    n_slot = n_pair * 8 * CAP

    places = [(cc, xx, yy, zz) for cc in range(nc) for xx in range(nx) for yy in range(ny) for zz in range(per)]

    def select(i, ref, with_gate):
        c0, c1, g0, g1 = (pair_rows(token_lanes(m_all, k, pl.multiple_of(4 * n_quad * i, 4 * n_quad), n_quad)) for k in range(4))
        hit0, hit1 = plain_id(c0) == me, plain_id(c1) == me
        hit = (hit0 | hit1).astype(F32)
        gate = jnp.where(hit0, g0, 0.0) + jnp.where(hit1, g1, 0.0)
        before, after = iota((256, 256), 0), iota((256, 256), 1)
        tri = ((before < after) & (before // 32 == after // 32)).astype(F32).astype(BF16)
        rank = dot(hit.astype(BF16), tri, 1, 0)
        src = (iota((n_pair, 256), 1) // 32).astype(F32)
        key = jnp.where(hit > 0.0, src * CAP + rank, -1.0)
        slot = iota((8 * CAP, 256), 0).astype(F32)
        parts = []
        for p in range(n_pair):
            sel = (slot == key[p:p + 1]).astype(F32)
            v = dot(sel.astype(BF16), ref[i * per + p // ny, p % ny].reshape(256, 256), 1, 0)
            parts.append(v * jnp.sum(sel * gate[p:p + 1], axis=1, keepdims=True) if with_gate else v)
        return jnp.concatenate([parts[zz * ny + yy][CAP * (xx * nc + cc):CAP * (xx * nc + cc + 1)] for cc, xx, yy, zz in places], axis=0).astype(BF16)

    def put(i, v, to):
        for k, (cc, xx, yy, zz) in enumerate(places):
            for half in range(2):
                to[half][cc, xx, yy, i * per + zz] = v[CAP * k:CAP * (k + 1), 128 * half:128 * (half + 1)].astype(BF16)

    def forward(i):
        here = pl.ds(i * n_slot, n_slot)
        xs = select(i, x_all, False)
        a = dot(xs, w1[...], 1, 0)
        h = gelu(a).astype(BF16)
        xs_ref[here], h_ref[here], a_ref[here] = xs, h, a
        put(i, dot(h, w2[...], 1, 0), rows[:2])

    def backward(i):
        here = pl.ds(i * n_slot, n_slot)
        dys = select(i, g_all, True)
        dys_ref[here] = dys
        da_ref[here] = (dot(dys, w2[...], 1, 1) * gelu_slope(a_ref[here])).astype(BF16)

    def backward_rows(i):
        put(i, dot(da_ref[pl.ds(i * n_slot, n_slot)], w1[...], 1, 1), rows[2:])

    def back(i):
        h = rows[i]
        other, near, via, out2, via2, in2, out3, hot_land, cold_land = areas[9 * i:9 * i + 9]
        link = next(links)
        go = link.go
        in_c, in_e, in_h = [[link.group(), link.group()] for _ in range(3)]
        in_n, in_v, in_2, in_l, in_s = [link.group() for _ in range(5)]
        x_first = i % 2 == 0
        a, b = (x, y) if x_first else (y, x)

        def to(a, b):
            return dev(z, b, a, c) if x_first else dev(z, a, b, c)

        def index(lead, a, bs):
            return lead + ((a, bs) if x_first else (bs, a))

        up, dn, far = step(a, 1), step(a, 3), step(a, 2)
        lo, hi = pl.ds(0, 2), pl.ds(2, 2)
        parts = [pl.ds(0, nz // 2), pl.ds(nz // 2, nz // 2)]

        def start(k):
            zs = parts[k]
            go(h.at[1 - c, :, :, zs], other.at[:, :, zs], mate, in_c[k])
            spread(h, (c,), c, zs, in_e[k])

        def follow(k):
            link.wait(in_c[k], other.at[:, :, parts[k]])
            spread(other, (), 1 - c, parts[k], in_h[k])

        def spread(ref, lead, e, zs, group):
            go(ref.at[index(lead, far, lo) + (zs,)], via.at[0, e, :, zs], to(up, b), group)
            go(ref.at[index(lead, far, hi) + (zs,)], via.at[1, e, :, zs], to(dn, b), group)
            go(ref.at[index(lead, up, full) + (zs,)], near.at[a, e, :, zs], to(up, b), in_n)
            go(ref.at[index(lead, dn, full) + (zs,)], near.at[a, e, :, zs], to(dn, b), in_n)

        def relay(e, zs, group):
            link.wait(group, via.at[:, e, :, zs])
            go(via.at[0, e, :, zs], near.at[dn, e, lo, zs], to(up, b), in_n)
            go(via.at[1, e, :, zs], near.at[up, e, hi, zs], to(dn, b), in_n)

        start(0)
        yield
        follow(0)
        yield
        start(1)
        yield
        relay(c, parts[0], in_e[0])
        relay(1 - c, parts[0], in_h[0])
        yield
        follow(1)
        yield
        relay(c, parts[1], in_e[1])
        yield
        relay(1 - c, parts[1], in_h[1])
        yield
        link.wait(in_n, near.at[pl.ds(0, 3)])

        def expert(s, e):
            return ((z * ny + y) * nx + s) * nc + e if x_first else ((z * ny + s) * nx + x) * nc + e

        places = [(step(a, d), e) for d in range(4) for e in (c, 1 - c)]
        is_hot = [[(hot_ref[j:j + 1, :] == expert(s, e).astype(F32)).astype(F32) for s, e in places] for j in range(3)]
        wide = lambda v: jnp.broadcast_to(v, (8, 128))
        weight = [[wide(v).astype(BF16) for v in r] for r in is_hot]
        line = iota((8, 128), 0)
        mine = [(wide(is_hot[0][k] + is_hot[1][k] + is_hot[2][k]) < 0.5) & (line == s * nc + e) for k, (s, e) in enumerate(places)]

        def squeeze(bb, carry):
            given = [h[index((c,), a, bb)], other[index((), a, bb)]] + [near[s, e, bb] for s, e in places[2:]]
            for j in range(3):
                out2[bb, j] = sum(given[k] * weight[j][k] for k in range(8))
            singles = jnp.zeros((nz, 8, 128), F32)
            for k in range(8):
                singles = jnp.where(mine[k], jnp.sum(given[k].astype(F32), axis=1, keepdims=True), singles)
            out2[bb, 3] = singles.astype(BF16)
            return carry

        lax.fori_loop(0, 4, squeeze, 0)
        up, dn, far = step(b, 1), step(b, 3), step(b, 2)
        lo, hi = pl.ds(0, nz // 2), pl.ds(nz // 2, nz // 2)
        go(out2.at[far, :, lo], via2.at[0], to(a, up), in_v)
        go(out2.at[far, :, hi], via2.at[1], to(a, dn), in_v)
        go(out2.at[up], in2.at[b], to(a, up), in_2)
        go(out2.at[dn], in2.at[b], to(a, dn), in_2)
        in2[b] = out2[b]
        yield
        link.wait(in_v, via2)
        go(via2.at[0], in2.at[dn, :, lo], to(a, up), in_2)
        go(via2.at[1], in2.at[up, :, hi], to(a, dn), in_2)
        yield
        link.wait(in_2, in2.at[pl.ds(0, 3)])
        for j in range(3):
            out3[:, j] = (in2[0, j] + in2[1, j]) + (in2[2, j] + in2[3, j])
        for d in by_distance:
            zz = lax.rem(z + d, nz)
            go(in2.at[:, 3, zz], cold_land.at[z], dev(zz, y, x, c), in_s)
            go(out3.at[zz], hot_land.at[z], dev(zz, y, x, c), in_l)
        cold_land[z] = in2[:, 3, z]
        hot_land[z] = out3[z]
        yield
        link.wait(in_s, cold_land.at[pl.ds(0, nz - 1)])
        link.wait(in_l, hot_land.at[pl.ds(0, nz - 1)])

    def weight_grad(k):
        if k % 2 == 0:
            part = slice(w2.shape[0] // 4 * (k // 2), w2.shape[0] // 4 * (k // 2 + 1))
            g2_ref[part, :] = dot(h_ref[:, part], dys_ref[...], 0, 0)
            save(4, (part, full))
        else:
            part = slice(w1.shape[1] // 4 * (k // 2), w1.shape[1] // 4 * (k // 2 + 1))
            g1_ref[:, part] = dot(xs_ref[...], da_ref[:, part], 0, 0)
            save(3, (full, part))

    ys, dxs = [back(0), back(1)], [back(2), back(3)]
    n_tok = tok.shape[0]
    memo = {}
    earlier = iota((n_tok, n_tok), 1) < iota((n_tok, n_tok), 0)
    n_exp = wg.shape[1]

    def where_from(i, r0, r1):
        rank = jnp.sum(jnp.where(earlier & ((i == r0) | (i == r1)), 1.0, 0.0), axis=1, keepdims=True)
        slot = jnp.full((n_tok, 1), -1.0, F32)
        for j in range(3):
            slot = jnp.where(i == hot_ref[j:j + 1, 0:1], CAP * j + rank, slot)
        e = i.astype(jnp.int32)
        core, xx, yy, zz = e % nc, (e // nc) % nx, (e // (nc * nx)) % ny, e // (nc * nx * ny)
        lane, single = iota((n_tok, n_exp), 1), slot < 0.0
        pick = lambda m: m.astype(F32).astype(BF16)
        return pick(iota((n_tok, 32), 1).astype(F32) == slot), (pick((lane == e) & single), pick((lane == ((zz * nx + xx) * ny + yy) * nc + core) & single))

    def rows_of(kind, chosen):
        parts = []
        for half in range(2):
            hot_land, cold_land = areas[9 * (kind + half) + 7:9 * (kind + half) + 9]
            hot = jnp.sum(hot_land[...].astype(F32), axis=0).reshape(24, 128)
            hot = jnp.concatenate([hot, jnp.zeros((8, 128), F32)], axis=0).astype(BF16)
            cold = cold_land[...].astype(F32).reshape(n_exp, 128).astype(BF16)
            parts.append([dot(by_slot, hot, 1, 0) + dot(by_place[half], cold, 1, 0) for by_slot, by_place in chosen])
        return [jnp.concatenate([parts[0][k], parts[1][k]], axis=1) for k in range(2)]

    def combine():
        r0, r1 = ids[0:1].astype(F32), ids[1:2].astype(F32)
        i0, i1 = as_col(r0), as_col(r1)
        g0, g1 = gates(tok[...], i0, i1, wg[...])
        chosen = [where_from(i, r0, r1) for i in (i0, i1)]
        y0, y1 = rows_of(0, chosen)
        grad = dout[...].astype(F32)
        dg0, dg1 = (jnp.sum(grad * v, axis=1, keepdims=True) for v in (y0, y1))
        mean = g0 * dg0 + g1 * dg1
        d0, d1 = ((g * (dg - mean)).astype(BF16).astype(F32) for g, dg in ((g0, dg0), (g1, dg1)))
        d_row[...] = jnp.concatenate([as_row(d0), as_row(d1), jnp.zeros((1, 2 * n_tok), F32)], axis=1)
        place = pltpu.make_async_copy(d_row, d_land.at[z, y, x, c], keep_sem.at[1])
        place.start()
        out_ref[...] = (g0 * y0 + g1 * y1).astype(BF16)
        save(0)
        place.wait()
        d_plans.append(gather_rows(next(links), d_land, range(4)))
        advance(d_plans)
        expert = iota((n_tok, n_exp), 1).astype(F32)
        spread = jnp.where(expert == i0, d0, jnp.where(expert == i1, d1, 0.0)).astype(BF16)
        memo.update(chosen=chosen, through=dot(spread, wg[...], 1, 1))

    def finish():
        dx0, dx1 = rows_of(2, memo['chosen'])
        gx_ref[...] = (dx0 + dx1 + memo['through']).astype(BF16)
        save(1)

    n_dev = nz * ny * nx * nc

    def gate_grad():
        flatten(d_land, d_all)
        expert = iota((n_exp, 256), 0).astype(F32)
        codes = [plain_id(pair_rows(token_lanes(m_all, k, 0, n_dev // 4))) for k in range(2)]
        grads = [pair_rows(token_lanes(d_all, k, 0, n_dev // 4)) for k in range(2)]
        total = jnp.zeros((n_exp, x_all.shape[-1]), F32)
        zs = nz // 4 or 1
        for z0 in range(0, nz, zs):
            spread = []
            for p in range(z0 * ny, (z0 + zs) * ny):
                q = slice(p, p + 1)
                spread.append(jnp.where(expert == codes[0][q], grads[0][q], jnp.where(expert == codes[1][q], grads[1][q], 0.0)).astype(BF16))
            total += dot(jnp.concatenate(spread, axis=1), x_all[z0:z0 + zs].reshape(zs * ny * 256, x_all.shape[-1]), 1, 0)
        gate_ref[...] = total.T
        save(2)

    d_plans = []
    moves = {'t': tok_plans, 'g': grad_plans, 'm': row_plan, 'y': ys, 'x': dxs, 'd': d_plans}
    works = {'f': [functools.partial(forward, i) for i in range(steps)], 'b': [functools.partial(backward, i) for i in range(steps)],
             'B': [functools.partial(backward_rows, i) for i in range(steps)], 'w': [functools.partial(weight_grad, k) for k in range(8)],
             'h': [read_rows], 'c': [combine], 'k': [gate_grad], 'e': [finish]}
    for turn in SCHEDULE:
        if turn in moves:
            advance(moves[turn])
        elif works[turn]:
            works[turn].pop(0)()
    for link in all_links:
        link.finish(pad, pad_row)
    for cp in saves:
        cp.wait()


def block_call(dims, tokens, grad_out, ids, w_gate, w1, w2):
    nz, ny, nx, nc = dims
    d_model, d_hidden = w1.shape
    n_tok = tokens.shape[0]
    n_dev = nz * ny * nx * nc
    n_row = n_dev * CAP
    tile = (CAP, 128)
    hbm = pl.BlockSpec(memory_space=pltpu.HBM)
    out = jax.ShapeDtypeStruct
    work = [(4, 4, nz), (4, 2, 4, nz), (2, 2, 2, nz), (4, 4, nz), (2, 4, nz // 2), (4, 4, nz), (nz, 3), (nz, 3), (nz, 4)]
    n_group = 4 * 14 + 4 + 4 * 11 + 4
    sems = [pltpu.SemaphoreType.DMA((10,)), pltpu.SemaphoreType.DMA((n_group,))]
    results = [(tokens.shape, BF16), (tokens.shape, BF16), ((d_model, n_dev), F32), ((d_model, d_hidden), F32), ((d_hidden, d_model), F32)]
    row = (1, 128)
    kept = [(tokens.shape, BF16), (tokens.shape, BF16), (ids.shape, jnp.int32), (w_gate.shape, BF16), (w1.shape, BF16), (w2.shape, BF16), (row, F32), (dims + row, F32),
            (dims + tokens.shape, BF16), (dims + tokens.shape, BF16), ((n_row, d_model), BF16), ((n_row, d_model), BF16), ((n_row, d_hidden), BF16), ((n_row, d_hidden), BF16), ((n_row, d_hidden), F32), ((n_dev, 128), F32), (tile, F32), (row, F32),
            (dims + row, F32), ((n_dev, 128), F32), ((1024,) + tile, BF16), ((n_dev,) + row, F32)]
    return pl.pallas_call(
        functools.partial(block_kernel, dims, (6, len(results), len(results), len(kept), 4, 4 * len(work), 3, len(sems))),
        out_shape=[out(*r) for r in results],
        in_specs=[hbm] * 6,
        out_specs=[hbm] * len(results),
        scratch_shapes=[pltpu.VMEM(*r) for r in results + kept] + [pltpu.VMEM((nc, nx, ny, nz) + tile, BF16)] * 4 + [pltpu.VMEM(w + tile, BF16) for w in work] * 4
        + [pltpu.SemaphoreType.DMA((k,)) for k in (8, 2, 11)] + sems,
        compiler_params=pltpu.CompilerParams(collective_id=0, has_side_effects=True, vmem_limit_bytes=VMEM_LIMIT),
        name='block',
    )(tokens, grad_out, ids, w_gate, w1, w2)


VMEM_LIMIT = 67043328
SCHEDULE = 'ttmttmttmtgtmgtgh' + 'fgfgyfgyf' + 'ygygygbyybyBBxbyxbBBxyx' + 'wxwwxxwxyc' + 'wwxdwxdwddkx' + 'e'


def pass_kernel(n, *refs):
    refs = iter(refs)
    given, passed, held, (load_sem, save_sem) = [list(itertools.islice(refs, k)) for k in (n, n, n, 2)]
    loads = [pltpu.make_async_copy(given[k], held[k], load_sem.at[k]) for k in range(n)]
    saves = [pltpu.make_async_copy(held[k], passed[k], save_sem.at[k]) for k in range(n)]
    for cp in loads:
        cp.start()
    for load, save in zip(loads, saves):
        load.wait()
        save.start()
    for cp in saves:
        cp.wait()


def pass_on(*arrays):
    n = len(arrays)
    return pl.pallas_call(
        functools.partial(pass_kernel, n),
        out_shape=[jax.ShapeDtypeStruct(v.shape, v.dtype) for v in arrays],
        in_specs=[pl.BlockSpec(memory_space=pltpu.HBM)] * n,
        out_specs=[pl.BlockSpec(memory_space=pltpu.HBM)] * n,
        scratch_shapes=[pltpu.VMEM(v.shape, v.dtype) for v in arrays] + [pltpu.SemaphoreType.DMA((n,))] * 2,
        compiler_params=pltpu.CompilerParams(vmem_limit_bytes=VMEM_LIMIT),
        name='pass_on',
    )(*arrays)


def local_block(dims, tokens, grad_out, expert_ids, w_gate, w_in, w_out):
    y_out, grad_x, grad_w_gate, g1, g2 = pass_on(*block_call(dims, tokens, grad_out, expert_ids.T, w_gate, w_in[0], w_out[0]))
    return y_out, grad_x, g1[None], g2[None], grad_w_gate


def solution(mesh):
    dims = (8, 4, 4, 2)
    return jax.shard_map(functools.partial(local_block, dims), mesh=mesh, in_specs=(P('ep'), P('ep'), P('ep'), P(), P('ep'), P('ep')), out_specs=(P('ep'), P('ep'), P('ep'), P('ep'), P()), check_vma=False)
```

```python
import functools
import itertools
import math

import jax
import jax.numpy as jnp
from jax import lax
from jax.experimental import pallas as pl
from jax.experimental.pallas import tpu as pltpu
from jax.sharding import PartitionSpec as P

MESH = pl.DeviceIdType.MESH
F32 = jnp.float32
BF16 = jnp.bfloat16
CAP = 8


def coords(dims):
    nz, ny, nx, nc = dims
    me = lax.axis_index('ep')
    c = lax.rem(me, nc)
    x = lax.rem(me // nc, nx)
    y = lax.rem(me // (nc * nx), ny)
    z = me // (nc * nx * ny)

    def dev(z, y, x, c):
        return (((z * ny + y) * nx + x) * nc + c,)

    return z, y, x, c, dev


def dot(a, b, ca, cb):
    return lax.dot_general(a, b, (((ca,), (cb,)), ((), ())), preferred_element_type=F32)


def iota(shape, axis):
    return lax.broadcasted_iota(jnp.int32, shape, axis)


def as_row(col):
    n = col.shape[0]
    return jnp.sum(jnp.where(iota((n, n), 0) == iota((n, n), 1), col, 0.0), axis=0, keepdims=True)


def as_col(row):
    n = row.shape[1]
    return jnp.sum(jnp.where(iota((n, n), 0) == iota((n, n), 1), row, 0.0), axis=1, keepdims=True)


def gates(tok, i0, i1, w_gate):
    logits = dot(tok, w_gate, 1, 0)
    expert = iota(logits.shape, 1).astype(F32)
    l0, l1 = (jnp.sum(jnp.where(expert == i, logits, 0.0), axis=1, keepdims=True) for i in (i0, i1))
    top = jnp.maximum(l0, l1)
    p0, p1 = jnp.exp(l0 - top), jnp.exp(l1 - top)
    total = p0 + p1
    return p0 / total, p1 / total


def choice_row(tok, ids, w_gate):
    r0, r1 = ids[0:1].astype(F32), ids[1:2].astype(F32)
    i0, i1 = as_col(r0), as_col(r1)
    g0, g1 = gates(tok, i0, i1, w_gate)

    def code(i):
        n = jnp.sum((i == r0).astype(F32) + (i == r1).astype(F32), axis=1, keepdims=True)
        return as_row(jnp.where(n > 1.5, i + 256.0, i))

    return jnp.concatenate([code(i0), code(i1), as_row(g0), as_row(g1)], axis=1)


def gelu_tanh(a):
    k = 0.7978845608028654
    sq = a * a
    return jnp.tanh(a * (k + (k * 0.044715) * sq)), sq


def gelu(a):
    half = 0.5 * a
    return half + half * gelu_tanh(a)[0]


def gelu_slope(a):
    k = 0.7978845608028654
    t, sq = gelu_tanh(a)
    return (0.5 + 0.5 * t) + (0.5 * a) * (1.0 - t * t) * (k + (3 * k * 0.044715) * sq)


def token_lanes(ref, k, start, n):
    lane = iota((n, 128), 1) // 32
    out = jnp.zeros((n, 128), F32)
    for j in range(4):
        r = ref[pl.ds(start + j, n, stride=4), :]
        out = jnp.where(lane == j, r if j == k else pltpu.roll(r, 32 * (j - k) % 128, 1), out)
    return out


def pair_rows(v):
    return jnp.concatenate([jnp.concatenate([v[2 * i:2 * i + 1], v[2 * i + 1:2 * i + 2]], axis=1) for i in range(v.shape[0] // 2)], axis=0)


def plain_id(code):
    return jnp.where(code >= 256.0, code - 256.0, code)


class Links:
    def __init__(self, send, recv, pool):
        self.send, self.recv, self.pool, self.bytes = send, recv, pool, 0

    def group(self):
        return self.recv.at[next(self.pool)]

    def go(self, src, dst, to, group):
        pltpu.make_async_remote_copy(src_ref=src, dst_ref=dst, send_sem=self.send, recv_sem=group, device_id=to, device_id_type=MESH).start()
        self.bytes += math.prod(src.shape) * jnp.dtype(src.dtype).itemsize

    def wait(self, group, ref):
        pltpu.make_async_copy(ref, ref, group).wait()

    def finish(self, *pads):
        for pad in pads:
            unit = math.prod(pad.shape[1:]) * jnp.dtype(pad.dtype).itemsize
            if self.bytes % unit == 0:
                return self.wait(self.send, pad.at[pl.ds(0, self.bytes // unit)])
        raise ValueError(self.bytes)


def block_kernel(dims, sizes, *refs):
    nz, ny, nx, nc = dims
    refs = iter(refs)
    refs = [list(itertools.islice(refs, n)) for n in sizes]
    (tok_hbm, dout_hbm, ids_hbm, wg_hbm, w1_hbm, w2_hbm), outs, held, kept, rows, areas, (load_sem, keep_sem, save_sem), sems = refs
    out_ref, gx_ref, gate_ref, g1_ref, g2_ref = held
    tok, dout, ids, wg, w1, w2, row, m_land, x_all, g_all, xs_ref, dys_ref, h_ref, da_ref, a_ref, m_all, hot_ref, d_row, d_land, d_all, pad, pad_row = kept
    z, y, x, c, dev = coords(dims)
    saves = []

    def save(k, part=None):
        src, dst = (held[k], outs[k]) if part is None else (held[k].at[part], outs[k].at[part])
        cp = pltpu.make_async_copy(src, dst, save_sem.at[len(saves)])
        cp.start()
        saves.append(cp)

    send_sem, recv_sem = sems
    pool = itertools.count()
    all_links = [Links(send_sem.at[k], recv_sem, pool) for k in range(send_sem.shape[0])]
    links = iter(all_links)

    loads = [pltpu.make_async_copy(s, d, load_sem.at[k]) for k, (s, d) in enumerate(
        [(tok_hbm, x_all.at[z, y, x, c]), (dout_hbm, g_all.at[z, y, x, c]), (tok_hbm, tok), (ids_hbm, ids), (wg_hbm, wg), (dout_hbm, dout), (w1_hbm, w1), (w2_hbm, w2)])]
    for ld in loads:
        ld.start()
    peers = [dev(lax.rem(z + d, nz), y, x, c) for d in range(1, nz)]
    for d in (1, 2, 3):
        peers.append(dev(z, lax.rem(y + d, ny), x, c))
        peers.append(dev(z, y, lax.rem(x + d, nx), c))
    mate = dev(z, y, x, 1 - c)
    peers.append(mate)
    barrier = pltpu.get_barrier_semaphore()
    for peer in peers:
        pl.semaphore_signal(barrier, inc=1, device_id=peer, device_id_type=MESH)
    for ld in loads[2:5]:
        ld.wait()
    row[...] = choice_row(tok[...], ids[...], wg[...])
    place = pltpu.make_async_copy(row, m_land.at[z, y, x, c], keep_sem.at[0])
    place.start()
    loads[0].wait()
    loads[1].wait()
    place.wait()
    pl.semaphore_wait(barrier, len(peers))

    full = slice(None)
    by_distance = sorted(range(1, nz), key=lambda d: abs(d - nz // 2))

    def step(v, d, m=4):
        return lax.rem(v + d, m)

    def by_lines(link, ref, rows, x_last):
        p0, q0 = (y, x) if x_last else (x, y)
        low, high = pl.ds(0, nz // 2), pl.ds(nz // 2, nz // 2)

        def at(zs, p, q):
            return ref.at[(zs, p, q, c, rows) if x_last else (zs, q, p, c, rows)]

        def go(part, p, q, group):
            link.go(part, part, dev(z, p, q, c) if x_last else dev(z, q, p, c), group)

        in_z, in_p, in_m, in_f, in_r, in_c = [link.group() for _ in range(6)]
        line = at(full, p0, q0)

        def over(q):
            part = at(full, full, q)
            link.go(part, part, mate, in_c)

        own = at(z, p0, q0)
        for d in by_distance:
            link.go(own, own, dev(step(z, d, nz), y, x, c), in_z)
        yield
        link.wait(in_z, at(pl.ds(0, nz - 1), p0, q0))
        pm, pp, po = step(p0, 3), step(p0, 1), step(p0, 2)
        qm, qp, qo = step(q0, 3), step(q0, 1), step(q0, 2)
        qs = []

        def spread(p):
            part = at(full, p, q0)
            qs.append((p, link.group(), link.group()))
            go(part, p0, qp, qs[-1][1])
            go(part, p0, qm, qs[-1][2])

        def relay(i):
            p, up, dn = qs[i]
            link.wait(up, line)
            go(at(low, p, qm), p0, qp, in_r)
            link.wait(dn, line)
            go(at(high, p, qp), p0, qm, in_r)

        go(line, pp, q0, in_p)
        go(line, pm, q0, in_m)
        spread(p0)
        yield
        link.wait(in_p, line)
        go(at(low, pm, q0), pp, q0, in_f)
        link.wait(in_m, line)
        go(at(high, pp, q0), pm, q0, in_f)
        spread(pm)
        spread(pp)
        yield
        relay(0)
        yield
        link.wait(in_f, line)
        spread(po)
        over(q0)
        for i in range(1, 4):
            yield
            relay(i)
        over(qm)
        over(qp)
        yield
        link.wait(in_r, at(full, full, q0))
        over(qo)
        yield
        link.wait(in_c, ref.at[full, full, full, c, rows])

    def gather_rows(link, held, order):
        have = [z, y, x, c]
        for axis in order:
            size = (nz, ny, nx, nc)[axis]
            part = held.at[tuple(have)]
            group = link.group()
            for d in sorted(range(1, size), key=lambda d: abs(d - size // 2)):
                there = [z, y, x, c]
                there[axis] = lax.rem(there[axis] + d, size)
                link.go(part, part, dev(*there), group)
            have[axis] = pl.ds(0, size - 1)
            yield
            link.wait(group, held.at[tuple(have)])
            have[axis] = full

    def advance(plans):
        for g in plans:
            next(g, None)

    halves = [slice(0, 16), slice(16, 32)]
    tok_plans, grad_plans = [[by_lines(next(links), ref, half, half.start == 0) for half in halves] for ref in (x_all, g_all)]
    row_plan = [gather_rows(next(links), m_land, range(4))]
    advance(row_plan + tok_plans + grad_plans)
    def flatten(land, flat):
        def lines(zz, carry):
            for k in range(ny * nx * nc):
                flat[pl.ds(zz * (ny * nx * nc) + k, 1), :] = land[zz, k // (nx * nc), k // nc % nx, k % nc]
            return carry

        lax.fori_loop(0, nz, lines, 0)


    me = lax.axis_index('ep').astype(F32)
    def read_rows():
        flatten(m_land, m_all)
        for ld in loads[5:]:
            ld.wait()
        code = m_all[...]
        left = jnp.where((iota(code.shape, 1) < 64) & (code >= 256.0), code - 256.0, 999.0)
        found = []
        for _ in range(3):
            best = jnp.min(jnp.min(left, axis=0, keepdims=True), axis=1, keepdims=True)
            left = jnp.where(left == best, 999.0, left)
            found.append(jnp.broadcast_to(best, (1, 128)))
        hot_ref[...] = jnp.concatenate(found + [jnp.full((5, 128), 999.0, F32)], axis=0)

    steps = 4 if nz == 8 else 1
    per = nz // steps
    n_quad = per * ny * nx * nc // 4
    n_pair = n_quad // 2
    n_slot = n_pair * 8 * CAP

    places = [(cc, xx, yy, zz) for cc in range(nc) for xx in range(nx) for yy in range(ny) for zz in range(per)]

    def select(i, ref, with_gate):
        c0, c1, g0, g1 = (pair_rows(token_lanes(m_all, k, pl.multiple_of(4 * n_quad * i, 4 * n_quad), n_quad)) for k in range(4))
        hit0, hit1 = plain_id(c0) == me, plain_id(c1) == me
        hit = (hit0 | hit1).astype(F32)
        gate = jnp.where(hit0, g0, 0.0) + jnp.where(hit1, g1, 0.0)
        before, after = iota((256, 256), 0), iota((256, 256), 1)
        tri = ((before < after) & (before // 32 == after // 32)).astype(F32).astype(BF16)
        rank = dot(hit.astype(BF16), tri, 1, 0)
        src = (iota((n_pair, 256), 1) // 32).astype(F32)
        key = jnp.where(hit > 0.0, src * CAP + rank, -1.0)
        slot = iota((8 * CAP, 256), 0).astype(F32)
        parts = []
        for p in range(n_pair):
            sel = (slot == key[p:p + 1]).astype(F32)
            v = dot(sel.astype(BF16), ref[i * per + p // ny, p % ny].reshape(256, 256), 1, 0)
            parts.append(v * jnp.sum(sel * gate[p:p + 1], axis=1, keepdims=True) if with_gate else v)
        return jnp.concatenate([parts[zz * ny + yy][CAP * (xx * nc + cc):CAP * (xx * nc + cc + 1)] for cc, xx, yy, zz in places], axis=0).astype(BF16)

    def put(i, v, to):
        for k, (cc, xx, yy, zz) in enumerate(places):
            for half in range(2):
                to[half][cc, xx, yy, i * per + zz] = v[CAP * k:CAP * (k + 1), 128 * half:128 * (half + 1)].astype(BF16)

    def forward(i):
        here = pl.ds(i * n_slot, n_slot)
        xs = select(i, x_all, False)
        a = dot(xs, w1[...], 1, 0)
        h = gelu(a).astype(BF16)
        xs_ref[here], h_ref[here], a_ref[here] = xs, h, a
        put(i, dot(h, w2[...], 1, 0), rows[:2])

    def backward(i):
        here = pl.ds(i * n_slot, n_slot)
        dys = select(i, g_all, True)
        dys_ref[here] = dys
        da_ref[here] = (dot(dys, w2[...], 1, 1) * gelu_slope(a_ref[here])).astype(BF16)

    def backward_rows(i):
        put(i, dot(da_ref[pl.ds(i * n_slot, n_slot)], w1[...], 1, 1), rows[2:])

    def back(i):
        h = rows[i]
        other, near, via, out2, via2, in2, out3, hot_land, cold_land = areas[9 * i:9 * i + 9]
        link = next(links)
        go = link.go
        in_c, in_e, in_h = [[link.group(), link.group()] for _ in range(3)]
        in_n, in_v, in_2, in_l, in_s = [link.group() for _ in range(5)]
        x_first = i % 2 == 0
        a, b = (x, y) if x_first else (y, x)

        def to(a, b):
            return dev(z, b, a, c) if x_first else dev(z, a, b, c)

        def index(lead, a, bs):
            return lead + ((a, bs) if x_first else (bs, a))

        up, dn, far = step(a, 1), step(a, 3), step(a, 2)
        lo, hi = pl.ds(0, 2), pl.ds(2, 2)
        parts = [pl.ds(0, nz // 2), pl.ds(nz // 2, nz // 2)]

        def start(k):
            zs = parts[k]
            go(h.at[1 - c, :, :, zs], other.at[:, :, zs], mate, in_c[k])
            spread(h, (c,), c, zs, in_e[k])

        def follow(k):
            link.wait(in_c[k], other.at[:, :, parts[k]])
            spread(other, (), 1 - c, parts[k], in_h[k])

        def spread(ref, lead, e, zs, group):
            go(ref.at[index(lead, far, lo) + (zs,)], via.at[0, e, :, zs], to(up, b), group)
            go(ref.at[index(lead, far, hi) + (zs,)], via.at[1, e, :, zs], to(dn, b), group)
            go(ref.at[index(lead, up, full) + (zs,)], near.at[a, e, :, zs], to(up, b), in_n)
            go(ref.at[index(lead, dn, full) + (zs,)], near.at[a, e, :, zs], to(dn, b), in_n)

        def relay(e, zs, group):
            link.wait(group, via.at[:, e, :, zs])
            go(via.at[0, e, :, zs], near.at[dn, e, lo, zs], to(up, b), in_n)
            go(via.at[1, e, :, zs], near.at[up, e, hi, zs], to(dn, b), in_n)

        start(0)
        yield
        follow(0)
        yield
        start(1)
        yield
        relay(c, parts[0], in_e[0])
        relay(1 - c, parts[0], in_h[0])
        yield
        follow(1)
        yield
        relay(c, parts[1], in_e[1])
        yield
        relay(1 - c, parts[1], in_h[1])
        yield
        link.wait(in_n, near.at[pl.ds(0, 3)])

        def expert(s, e):
            return ((z * ny + y) * nx + s) * nc + e if x_first else ((z * ny + s) * nx + x) * nc + e

        places = [(step(a, d), e) for d in range(4) for e in (c, 1 - c)]
        is_hot = [[(hot_ref[j:j + 1, :] == expert(s, e).astype(F32)).astype(F32) for s, e in places] for j in range(3)]
        wide = lambda v: jnp.broadcast_to(v, (8, 128))
        weight = [[wide(v).astype(BF16) for v in r] for r in is_hot]
        line = iota((8, 128), 0)
        mine = [(wide(is_hot[0][k] + is_hot[1][k] + is_hot[2][k]) < 0.5) & (line == s * nc + e) for k, (s, e) in enumerate(places)]

        def squeeze(bb, carry):
            given = [h[index((c,), a, bb)], other[index((), a, bb)]] + [near[s, e, bb] for s, e in places[2:]]
            for j in range(3):
                out2[bb, j] = sum(given[k] * weight[j][k] for k in range(8))
            singles = jnp.zeros((nz, 8, 128), F32)
            for k in range(8):
                singles = jnp.where(mine[k], jnp.sum(given[k].astype(F32), axis=1, keepdims=True), singles)
            out2[bb, 3] = singles.astype(BF16)
            return carry

        lax.fori_loop(0, 4, squeeze, 0)
        up, dn, far = step(b, 1), step(b, 3), step(b, 2)
        lo, hi = pl.ds(0, nz // 2), pl.ds(nz // 2, nz // 2)
        go(out2.at[far, :, lo], via2.at[0], to(a, up), in_v)
        go(out2.at[far, :, hi], via2.at[1], to(a, dn), in_v)
        go(out2.at[up], in2.at[b], to(a, up), in_2)
        go(out2.at[dn], in2.at[b], to(a, dn), in_2)
        in2[b] = out2[b]
        yield
        link.wait(in_v, via2)
        go(via2.at[0], in2.at[dn, :, lo], to(a, up), in_2)
        go(via2.at[1], in2.at[up, :, hi], to(a, dn), in_2)
        yield
        link.wait(in_2, in2.at[pl.ds(0, 3)])
        for j in range(3):
            out3[:, j] = (in2[0, j] + in2[1, j]) + (in2[2, j] + in2[3, j])
        for d in by_distance:
            zz = lax.rem(z + d, nz)
            go(in2.at[:, 3, zz], cold_land.at[z], dev(zz, y, x, c), in_s)
            go(out3.at[zz], hot_land.at[z], dev(zz, y, x, c), in_l)
        cold_land[z] = in2[:, 3, z]
        hot_land[z] = out3[z]
        yield
        link.wait(in_s, cold_land.at[pl.ds(0, nz - 1)])
        link.wait(in_l, hot_land.at[pl.ds(0, nz - 1)])

    def weight_grad(k):
        if k % 2 == 0:
            part = slice(w2.shape[0] // 4 * (k // 2), w2.shape[0] // 4 * (k // 2 + 1))
            g2_ref[part, :] = dot(h_ref[:, part], dys_ref[...], 0, 0)
            save(4, (part, full))
        else:
            part = slice(w1.shape[1] // 4 * (k // 2), w1.shape[1] // 4 * (k // 2 + 1))
            g1_ref[:, part] = dot(xs_ref[...], da_ref[:, part], 0, 0)
            save(3, (full, part))

    ys, dxs = [back(0), back(1)], [back(2), back(3)]
    n_tok = tok.shape[0]
    memo = {}
    earlier = iota((n_tok, n_tok), 1) < iota((n_tok, n_tok), 0)
    n_exp = wg.shape[1]

    def where_from(i, r0, r1):
        rank = jnp.sum(jnp.where(earlier & ((i == r0) | (i == r1)), 1.0, 0.0), axis=1, keepdims=True)
        slot = jnp.full((n_tok, 1), -1.0, F32)
        for j in range(3):
            slot = jnp.where(i == hot_ref[j:j + 1, 0:1], CAP * j + rank, slot)
        e = i.astype(jnp.int32)
        core, xx, yy, zz = e % nc, (e // nc) % nx, (e // (nc * nx)) % ny, e // (nc * nx * ny)
        lane, single = iota((n_tok, n_exp), 1), slot < 0.0
        pick = lambda m: m.astype(F32).astype(BF16)
        return pick(iota((n_tok, 32), 1).astype(F32) == slot), (pick((lane == e) & single), pick((lane == ((zz * nx + xx) * ny + yy) * nc + core) & single))

    def rows_of(kind, chosen):
        parts = []
        for half in range(2):
            hot_land, cold_land = areas[9 * (kind + half) + 7:9 * (kind + half) + 9]
            hot = jnp.sum(hot_land[...].astype(F32), axis=0).reshape(24, 128)
            hot = jnp.concatenate([hot, jnp.zeros((8, 128), F32)], axis=0).astype(BF16)
            cold = cold_land[...].astype(F32).reshape(n_exp, 128).astype(BF16)
            parts.append([dot(by_slot, hot, 1, 0) + dot(by_place[half], cold, 1, 0) for by_slot, by_place in chosen])
        return [jnp.concatenate([parts[0][k], parts[1][k]], axis=1) for k in range(2)]

    def combine():
        r0, r1 = ids[0:1].astype(F32), ids[1:2].astype(F32)
        i0, i1 = as_col(r0), as_col(r1)
        g0, g1 = gates(tok[...], i0, i1, wg[...])
        chosen = [where_from(i, r0, r1) for i in (i0, i1)]
        y0, y1 = rows_of(0, chosen)
        grad = dout[...].astype(F32)
        dg0, dg1 = (jnp.sum(grad * v, axis=1, keepdims=True) for v in (y0, y1))
        mean = g0 * dg0 + g1 * dg1
        d0, d1 = ((g * (dg - mean)).astype(BF16).astype(F32) for g, dg in ((g0, dg0), (g1, dg1)))
        d_row[...] = jnp.concatenate([as_row(d0), as_row(d1), jnp.zeros((1, 2 * n_tok), F32)], axis=1)
        place = pltpu.make_async_copy(d_row, d_land.at[z, y, x, c], keep_sem.at[1])
        place.start()
        out_ref[...] = (g0 * y0 + g1 * y1).astype(BF16)
        save(0)
        place.wait()
        d_plans.append(gather_rows(next(links), d_land, range(4)))
        advance(d_plans)
        expert = iota((n_tok, n_exp), 1).astype(F32)
        spread = jnp.where(expert == i0, d0, jnp.where(expert == i1, d1, 0.0)).astype(BF16)
        memo.update(chosen=chosen, through=dot(spread, wg[...], 1, 1))

    def finish():
        dx0, dx1 = rows_of(2, memo['chosen'])
        gx_ref[...] = (dx0 + dx1 + memo['through']).astype(BF16)
        save(1)

    n_dev = nz * ny * nx * nc

    def gate_grad():
        flatten(d_land, d_all)
        expert = iota((n_exp, 256), 0).astype(F32)
        codes = [plain_id(pair_rows(token_lanes(m_all, k, 0, n_dev // 4))) for k in range(2)]
        grads = [pair_rows(token_lanes(d_all, k, 0, n_dev // 4)) for k in range(2)]
        total = jnp.zeros((n_exp, x_all.shape[-1]), F32)
        zs = nz // 4 or 1
        for z0 in range(0, nz, zs):
            spread = []
            for p in range(z0 * ny, (z0 + zs) * ny):
                q = slice(p, p + 1)
                spread.append(jnp.where(expert == codes[0][q], grads[0][q], jnp.where(expert == codes[1][q], grads[1][q], 0.0)).astype(BF16))
            total += dot(jnp.concatenate(spread, axis=1), x_all[z0:z0 + zs].reshape(zs * ny * 256, x_all.shape[-1]), 1, 0)
        gate_ref[...] = total.T
        save(2)

    d_plans = []
    moves = {'t': tok_plans, 'g': grad_plans, 'm': row_plan, 'y': ys, 'x': dxs, 'd': d_plans}
    works = {'f': [functools.partial(forward, i) for i in range(steps)], 'b': [functools.partial(backward, i) for i in range(steps)],
             'B': [functools.partial(backward_rows, i) for i in range(steps)], 'w': [functools.partial(weight_grad, k) for k in range(8)],
             'h': [read_rows], 'c': [combine], 'k': [gate_grad], 'e': [finish]}
    for turn in SCHEDULE:
        if turn in moves:
            advance(moves[turn])
        elif works[turn]:
            works[turn].pop(0)()
    for link in all_links:
        link.finish(pad, pad_row)
    for cp in saves:
        cp.wait()


def block_call(dims, tokens, grad_out, ids, w_gate, w1, w2):
    nz, ny, nx, nc = dims
    d_model, d_hidden = w1.shape
    n_tok = tokens.shape[0]
    n_dev = nz * ny * nx * nc
    n_row = n_dev * CAP
    tile = (CAP, 128)
    hbm = pl.BlockSpec(memory_space=pltpu.HBM)
    out = jax.ShapeDtypeStruct
    work = [(4, 4, nz), (4, 2, 4, nz), (2, 2, 2, nz), (4, 4, nz), (2, 4, nz // 2), (4, 4, nz), (nz, 3), (nz, 3), (nz, 4)]
    n_group = 4 * 14 + 4 + 4 * 11 + 4
    sems = [pltpu.SemaphoreType.DMA((10,)), pltpu.SemaphoreType.DMA((n_group,))]
    results = [(tokens.shape, BF16), (tokens.shape, BF16), ((d_model, n_dev), F32), ((d_model, d_hidden), F32), ((d_hidden, d_model), F32)]
    row = (1, 128)
    kept = [(tokens.shape, BF16), (tokens.shape, BF16), (ids.shape, jnp.int32), (w_gate.shape, BF16), (w1.shape, BF16), (w2.shape, BF16), (row, F32), (dims + row, F32),
            (dims + tokens.shape, BF16), (dims + tokens.shape, BF16), ((n_row, d_model), BF16), ((n_row, d_model), BF16), ((n_row, d_hidden), BF16), ((n_row, d_hidden), BF16), ((n_row, d_hidden), F32), ((n_dev, 128), F32), (tile, F32), (row, F32),
            (dims + row, F32), ((n_dev, 128), F32), ((1024,) + tile, BF16), ((n_dev,) + row, F32)]
    return pl.pallas_call(
        functools.partial(block_kernel, dims, (6, len(results), len(results), len(kept), 4, 4 * len(work), 3, len(sems))),
        out_shape=[out(*r) for r in results],
        in_specs=[hbm] * 6,
        out_specs=[hbm] * len(results),
        scratch_shapes=[pltpu.VMEM(*r) for r in results + kept] + [pltpu.VMEM((nc, nx, ny, nz) + tile, BF16)] * 4 + [pltpu.VMEM(w + tile, BF16) for w in work] * 4
        + [pltpu.SemaphoreType.DMA((k,)) for k in (8, 2, 11)] + sems,
        compiler_params=pltpu.CompilerParams(collective_id=0, has_side_effects=True, vmem_limit_bytes=VMEM_LIMIT),
        name='block',
    )(tokens, grad_out, ids, w_gate, w1, w2)


VMEM_LIMIT = 67043328
SCHEDULE = 'mttmttmtmttgtth' + 'fggfgyfgyf' + 'yggygyg' + 'bybybyBBxbyxBBxy' + 'wwxxwwxwxyc' + 'xwwdxdxwddkxe'


def pass_kernel(n, *refs):
    refs = iter(refs)
    given, passed, held, (load_sem, save_sem) = [list(itertools.islice(refs, k)) for k in (n, n, n, 2)]
    loads = [pltpu.make_async_copy(given[k], held[k], load_sem.at[k]) for k in range(n)]
    saves = [pltpu.make_async_copy(held[k], passed[k], save_sem.at[k]) for k in range(n)]
    for cp in loads:
        cp.start()
    for load, save in zip(loads, saves):
        load.wait()
        save.start()
    for cp in saves:
        cp.wait()


def pass_on(*arrays):
    n = len(arrays)
    return pl.pallas_call(
        functools.partial(pass_kernel, n),
        out_shape=[jax.ShapeDtypeStruct(v.shape, v.dtype) for v in arrays],
        in_specs=[pl.BlockSpec(memory_space=pltpu.HBM)] * n,
        out_specs=[pl.BlockSpec(memory_space=pltpu.HBM)] * n,
        scratch_shapes=[pltpu.VMEM(v.shape, v.dtype) for v in arrays] + [pltpu.SemaphoreType.DMA((n,))] * 2,
        compiler_params=pltpu.CompilerParams(vmem_limit_bytes=VMEM_LIMIT),
        name='pass_on',
    )(*arrays)


def local_block(dims, tokens, grad_out, expert_ids, w_gate, w_in, w_out):
    y_out, grad_x, grad_w_gate, g1, g2 = pass_on(*block_call(dims, tokens, grad_out, expert_ids.T, w_gate, w_in[0], w_out[0]))
    return y_out, grad_x, g1[None], g2[None], grad_w_gate


def solution(mesh):
    dims = (8, 4, 4, 2)
    return jax.shard_map(functools.partial(local_block, dims), mesh=mesh, in_specs=(P('ep'), P('ep'), P('ep'), P(), P('ep'), P('ep')), out_specs=(P('ep'), P('ep'), P('ep'), P('ep'), P()), check_vma=False)
```

```python
import functools
import itertools
import math

import jax
import jax.numpy as jnp
from jax import lax
from jax.experimental import pallas as pl
from jax.experimental.pallas import tpu as pltpu
from jax.sharding import PartitionSpec as P

MESH = pl.DeviceIdType.MESH
F32 = jnp.float32
BF16 = jnp.bfloat16
CAP = 8


def coords(dims):
    nz, ny, nx, nc = dims
    me = lax.axis_index('ep')
    c = lax.rem(me, nc)
    x = lax.rem(me // nc, nx)
    y = lax.rem(me // (nc * nx), ny)
    z = me // (nc * nx * ny)

    def dev(z, y, x, c):
        return (((z * ny + y) * nx + x) * nc + c,)

    return z, y, x, c, dev


def dot(a, b, ca, cb):
    return lax.dot_general(a, b, (((ca,), (cb,)), ((), ())), preferred_element_type=F32)


def iota(shape, axis):
    return lax.broadcasted_iota(jnp.int32, shape, axis)


def as_row(col):
    n = col.shape[0]
    return jnp.sum(jnp.where(iota((n, n), 0) == iota((n, n), 1), col, 0.0), axis=0, keepdims=True)


def as_col(row):
    n = row.shape[1]
    return jnp.sum(jnp.where(iota((n, n), 0) == iota((n, n), 1), row, 0.0), axis=1, keepdims=True)


def gates(tok, i0, i1, w_gate):
    logits = dot(tok, w_gate, 1, 0)
    expert = iota(logits.shape, 1).astype(F32)
    l0, l1 = (jnp.sum(jnp.where(expert == i, logits, 0.0), axis=1, keepdims=True) for i in (i0, i1))
    top = jnp.maximum(l0, l1)
    p0, p1 = jnp.exp(l0 - top), jnp.exp(l1 - top)
    total = p0 + p1
    return p0 / total, p1 / total


def choice_row(tok, ids, w_gate):
    r0, r1 = ids[0:1].astype(F32), ids[1:2].astype(F32)
    i0, i1 = as_col(r0), as_col(r1)
    g0, g1 = gates(tok, i0, i1, w_gate)

    def code(i):
        n = jnp.sum((i == r0).astype(F32) + (i == r1).astype(F32), axis=1, keepdims=True)
        return as_row(jnp.where(n > 1.5, i + 256.0, i))

    return jnp.concatenate([code(i0), code(i1), as_row(g0), as_row(g1)], axis=1)


def gelu_tanh(a):
    k = 0.7978845608028654
    sq = a * a
    return jnp.tanh(a * (k + (k * 0.044715) * sq)), sq


def gelu(a):
    half = 0.5 * a
    return half + half * gelu_tanh(a)[0]


def gelu_slope(a):
    k = 0.7978845608028654
    t, sq = gelu_tanh(a)
    return (0.5 + 0.5 * t) + (0.5 * a) * (1.0 - t * t) * (k + (3 * k * 0.044715) * sq)


def token_lanes(ref, k, start, n):
    lane = iota((n, 128), 1) // 32
    out = jnp.zeros((n, 128), F32)
    for j in range(4):
        r = ref[pl.ds(start + j, n, stride=4), :]
        out = jnp.where(lane == j, r if j == k else pltpu.roll(r, 32 * (j - k) % 128, 1), out)
    return out


def pair_rows(v):
    return jnp.concatenate([jnp.concatenate([v[2 * i:2 * i + 1], v[2 * i + 1:2 * i + 2]], axis=1) for i in range(v.shape[0] // 2)], axis=0)


def plain_id(code):
    return jnp.where(code >= 256.0, code - 256.0, code)


class Links:
    def __init__(self, send, recv, pool):
        self.send, self.recv, self.pool, self.bytes = send, recv, pool, 0

    def group(self):
        return self.recv.at[next(self.pool)]

    def go(self, src, dst, to, group):
        pltpu.make_async_remote_copy(src_ref=src, dst_ref=dst, send_sem=self.send, recv_sem=group, device_id=to, device_id_type=MESH).start()
        self.bytes += math.prod(src.shape) * jnp.dtype(src.dtype).itemsize

    def wait(self, group, ref):
        pltpu.make_async_copy(ref, ref, group).wait()

    def finish(self, *pads):
        for pad in pads:
            unit = math.prod(pad.shape[1:]) * jnp.dtype(pad.dtype).itemsize
            if self.bytes % unit == 0:
                return self.wait(self.send, pad.at[pl.ds(0, self.bytes // unit)])
        raise ValueError(self.bytes)


def block_kernel(dims, sizes, *refs):
    nz, ny, nx, nc = dims
    refs = iter(refs)
    refs = [list(itertools.islice(refs, n)) for n in sizes]
    (tok_hbm, dout_hbm, ids_hbm, wg_hbm, w1_hbm, w2_hbm), outs, held, kept, rows, areas, (load_sem, keep_sem, save_sem), sems = refs
    out_ref, gx_ref, gate_ref, g1_ref, g2_ref = held
    tok, dout, ids, wg, w1, w2, row, m_land, x_all, g_all, xs_ref, dys_ref, h_ref, da_ref, a_ref, m_all, hot_ref, d_row, d_land, d_all, pad, pad_row = kept
    z, y, x, c, dev = coords(dims)
    saves = []

    def save(k, part=None):
        src, dst = (held[k], outs[k]) if part is None else (held[k].at[part], outs[k].at[part])
        cp = pltpu.make_async_copy(src, dst, save_sem.at[len(saves)])
        cp.start()
        saves.append(cp)

    send_sem, recv_sem = sems
    pool = itertools.count()
    all_links = [Links(send_sem.at[k], recv_sem, pool) for k in range(send_sem.shape[0])]
    links = iter(all_links)

    loads = [pltpu.make_async_copy(s, d, load_sem.at[k]) for k, (s, d) in enumerate(
        [(tok_hbm, x_all.at[z, y, x, c]), (dout_hbm, g_all.at[z, y, x, c]), (tok_hbm, tok), (ids_hbm, ids), (wg_hbm, wg), (dout_hbm, dout), (w1_hbm, w1), (w2_hbm, w2)])]
    for ld in loads:
        ld.start()
    peers = [dev(lax.rem(z + d, nz), y, x, c) for d in range(1, nz)]
    for d in (1, 2, 3):
        peers.append(dev(z, lax.rem(y + d, ny), x, c))
        peers.append(dev(z, y, lax.rem(x + d, nx), c))
    mate = dev(z, y, x, 1 - c)
    peers.append(mate)
    barrier = pltpu.get_barrier_semaphore()
    for peer in peers:
        pl.semaphore_signal(barrier, inc=1, device_id=peer, device_id_type=MESH)
    for ld in loads[2:5]:
        ld.wait()
    row[...] = choice_row(tok[...], ids[...], wg[...])
    place = pltpu.make_async_copy(row, m_land.at[z, y, x, c], keep_sem.at[0])
    place.start()
    loads[0].wait()
    loads[1].wait()
    place.wait()
    pl.semaphore_wait(barrier, len(peers))

    full = slice(None)
    by_distance = sorted(range(1, nz), key=lambda d: abs(d - nz // 2))

    def step(v, d, m=4):
        return lax.rem(v + d, m)

    def by_lines(link, ref, rows, x_last, late):
        p0, q0 = (y, x) if x_last else (x, y)
        low, high = pl.ds(0, nz // 2), pl.ds(nz // 2, nz // 2)

        def at(zs, p, q):
            return ref.at[(zs, p, q, c, rows) if x_last else (zs, q, p, c, rows)]

        def go(part, p, q, group):
            link.go(part, part, dev(z, p, q, c) if x_last else dev(z, q, p, c), group)

        in_z, in_p, in_m, in_f, in_r, in_c = [link.group() for _ in range(6)]
        line = at(full, p0, q0)

        def over(q):
            part = at(full, full, q)
            link.go(part, part, mate, in_c)

        own = at(z, p0, q0)
        for d in by_distance:
            link.go(own, own, dev(step(z, d, nz), y, x, c), in_z)
        yield
        link.wait(in_z, at(pl.ds(0, nz - 1), p0, q0))
        pm, pp, po = step(p0, 3), step(p0, 1), step(p0, 2)
        qm, qp, qo = step(q0, 3), step(q0, 1), step(q0, 2)
        qs = []

        def spread(p):
            part = at(full, p, q0)
            qs.append((p, link.group(), link.group()))
            go(part, p0, qp, qs[-1][1])
            go(part, p0, qm, qs[-1][2])

        def relay(i):
            p, up, dn = qs[i]
            link.wait(up, line)
            go(at(low, p, qm), p0, qp, in_r)
            link.wait(dn, line)
            go(at(high, p, qp), p0, qm, in_r)

        def pass_one():
            link.wait(in_p, line)
            go(at(low, pm, q0), pp, q0, in_f)
            link.wait(in_m, line)
            go(at(high, pp, q0), pm, q0, in_f)

        go(line, pp, q0, in_p)
        go(line, pm, q0, in_m)
        if late:
            yield
            pass_one()
            yield
            link.wait(in_f, line)
            for p in (p0, pm, pp, po):
                spread(p)
            over(q0)
            yield
            relay(0)
        else:
            spread(p0)
            yield
            pass_one()
            spread(pm)
            spread(pp)
            yield
            relay(0)
            yield
            link.wait(in_f, line)
            spread(po)
            over(q0)
        for i in range(1, 4):
            yield
            relay(i)
        over(qm)
        over(qp)
        yield
        link.wait(in_r, at(full, full, q0))
        over(qo)
        yield
        link.wait(in_c, ref.at[full, full, full, c, rows])

    def gather_rows(link, held, order):
        have = [z, y, x, c]
        for axis in order:
            size = (nz, ny, nx, nc)[axis]
            part = held.at[tuple(have)]
            group = link.group()
            for d in sorted(range(1, size), key=lambda d: abs(d - size // 2)):
                there = [z, y, x, c]
                there[axis] = lax.rem(there[axis] + d, size)
                link.go(part, part, dev(*there), group)
            have[axis] = pl.ds(0, size - 1)
            yield
            link.wait(group, held.at[tuple(have)])
            have[axis] = full

    def advance(plans):
        for g in plans:
            next(g, None)

    halves = [slice(0, 16), slice(16, 32)]
    tok_plans, grad_plans = [[by_lines(next(links), ref, half, half.start == 0, ref is g_all) for half in halves] for ref in (x_all, g_all)]
    row_plan = [gather_rows(next(links), m_land, range(4))]
    advance(row_plan + tok_plans + grad_plans)
    def flatten(land, flat):
        def lines(zz, carry):
            for k in range(ny * nx * nc):
                flat[pl.ds(zz * (ny * nx * nc) + k, 1), :] = land[zz, k // (nx * nc), k // nc % nx, k % nc]
            return carry

        lax.fori_loop(0, nz, lines, 0)


    me = lax.axis_index('ep').astype(F32)
    def read_rows():
        flatten(m_land, m_all)
        for ld in loads[5:]:
            ld.wait()
        code = m_all[...]
        left = jnp.where((iota(code.shape, 1) < 64) & (code >= 256.0), code - 256.0, 999.0)
        found = []
        for _ in range(3):
            best = jnp.min(jnp.min(left, axis=0, keepdims=True), axis=1, keepdims=True)
            left = jnp.where(left == best, 999.0, left)
            found.append(jnp.broadcast_to(best, (1, 128)))
        hot_ref[...] = jnp.concatenate(found + [jnp.full((5, 128), 999.0, F32)], axis=0)

    steps = 4 if nz == 8 else 1
    per = nz // steps
    n_quad = per * ny * nx * nc // 4
    n_pair = n_quad // 2
    n_slot = n_pair * 8 * CAP

    places = [(cc, xx, yy, zz) for cc in range(nc) for xx in range(nx) for yy in range(ny) for zz in range(per)]

    def select(i, ref, with_gate):
        c0, c1, g0, g1 = (pair_rows(token_lanes(m_all, k, pl.multiple_of(4 * n_quad * i, 4 * n_quad), n_quad)) for k in range(4))
        hit0, hit1 = plain_id(c0) == me, plain_id(c1) == me
        hit = (hit0 | hit1).astype(F32)
        gate = jnp.where(hit0, g0, 0.0) + jnp.where(hit1, g1, 0.0)
        before, after = iota((256, 256), 0), iota((256, 256), 1)
        tri = ((before < after) & (before // 32 == after // 32)).astype(F32).astype(BF16)
        rank = dot(hit.astype(BF16), tri, 1, 0)
        src = (iota((n_pair, 256), 1) // 32).astype(F32)
        key = jnp.where(hit > 0.0, src * CAP + rank, -1.0)
        slot = iota((8 * CAP, 256), 0).astype(F32)
        parts = []
        for p in range(n_pair):
            sel = (slot == key[p:p + 1]).astype(F32)
            v = dot(sel.astype(BF16), ref[i * per + p // ny, p % ny].reshape(256, 256), 1, 0)
            parts.append(v * jnp.sum(sel * gate[p:p + 1], axis=1, keepdims=True) if with_gate else v)
        return jnp.concatenate([parts[zz * ny + yy][CAP * (xx * nc + cc):CAP * (xx * nc + cc + 1)] for cc, xx, yy, zz in places], axis=0).astype(BF16)

    def put(i, v, to):
        for k, (cc, xx, yy, zz) in enumerate(places):
            for half in range(2):
                to[half][cc, xx, yy, i * per + zz] = v[CAP * k:CAP * (k + 1), 128 * half:128 * (half + 1)].astype(BF16)

    def forward(i):
        here = pl.ds(i * n_slot, n_slot)
        xs = select(i, x_all, False)
        a = dot(xs, w1[...], 1, 0)
        h = gelu(a).astype(BF16)
        xs_ref[here], h_ref[here], a_ref[here] = xs, h, a
        put(i, dot(h, w2[...], 1, 0), rows[:2])

    def backward(i):
        here = pl.ds(i * n_slot, n_slot)
        dys = select(i, g_all, True)
        dys_ref[here] = dys
        da_ref[here] = (dot(dys, w2[...], 1, 1) * gelu_slope(a_ref[here])).astype(BF16)

    def backward_rows(i):
        put(i, dot(da_ref[pl.ds(i * n_slot, n_slot)], w1[...], 1, 1), rows[2:])

    def back(i):
        h = rows[i]
        other, near, via, out2, via2, in2, out3, hot_land, cold_land = areas[9 * i:9 * i + 9]
        link = next(links)
        go = link.go
        in_c, in_e, in_h = [[link.group(), link.group()] for _ in range(3)]
        in_n, in_v, in_2, in_l, in_s = [link.group() for _ in range(5)]
        x_first = i % 2 == 0
        a, b = (x, y) if x_first else (y, x)

        def to(a, b):
            return dev(z, b, a, c) if x_first else dev(z, a, b, c)

        def index(lead, a, bs):
            return lead + ((a, bs) if x_first else (bs, a))

        up, dn, far = step(a, 1), step(a, 3), step(a, 2)
        lo, hi = pl.ds(0, 2), pl.ds(2, 2)
        parts = [pl.ds(0, nz // 2), pl.ds(nz // 2, nz // 2)]

        def start(k):
            zs = parts[k]
            go(h.at[1 - c, :, :, zs], other.at[:, :, zs], mate, in_c[k])
            spread(h, (c,), c, zs, in_e[k])

        def follow(k):
            link.wait(in_c[k], other.at[:, :, parts[k]])
            spread(other, (), 1 - c, parts[k], in_h[k])

        def spread(ref, lead, e, zs, group):
            go(ref.at[index(lead, far, lo) + (zs,)], via.at[0, e, :, zs], to(up, b), group)
            go(ref.at[index(lead, far, hi) + (zs,)], via.at[1, e, :, zs], to(dn, b), group)
            go(ref.at[index(lead, up, full) + (zs,)], near.at[a, e, :, zs], to(up, b), in_n)
            go(ref.at[index(lead, dn, full) + (zs,)], near.at[a, e, :, zs], to(dn, b), in_n)

        def relay(e, zs, group):
            link.wait(group, via.at[:, e, :, zs])
            go(via.at[0, e, :, zs], near.at[dn, e, lo, zs], to(up, b), in_n)
            go(via.at[1, e, :, zs], near.at[up, e, hi, zs], to(dn, b), in_n)

        start(0)
        yield
        follow(0)
        yield
        start(1)
        yield
        relay(c, parts[0], in_e[0])
        relay(1 - c, parts[0], in_h[0])
        yield
        follow(1)
        yield
        relay(c, parts[1], in_e[1])
        yield
        relay(1 - c, parts[1], in_h[1])
        yield
        link.wait(in_n, near.at[pl.ds(0, 3)])

        def expert(s, e):
            return ((z * ny + y) * nx + s) * nc + e if x_first else ((z * ny + s) * nx + x) * nc + e

        places = [(step(a, d), e) for d in range(4) for e in (c, 1 - c)]
        is_hot = [[(hot_ref[j:j + 1, :] == expert(s, e).astype(F32)).astype(F32) for s, e in places] for j in range(3)]
        wide = lambda v: jnp.broadcast_to(v, (8, 128))
        weight = [[wide(v).astype(BF16) for v in r] for r in is_hot]
        line = iota((8, 128), 0)
        mine = [(wide(is_hot[0][k] + is_hot[1][k] + is_hot[2][k]) < 0.5) & (line == s * nc + e) for k, (s, e) in enumerate(places)]

        def squeeze(bb, carry):
            given = [h[index((c,), a, bb)], other[index((), a, bb)]] + [near[s, e, bb] for s, e in places[2:]]
            for j in range(3):
                out2[bb, j] = sum(given[k] * weight[j][k] for k in range(8))
            singles = jnp.zeros((nz, 8, 128), F32)
            for k in range(8):
                singles = jnp.where(mine[k], jnp.sum(given[k].astype(F32), axis=1, keepdims=True), singles)
            out2[bb, 3] = singles.astype(BF16)
            return carry

        lax.fori_loop(0, 4, squeeze, 0)
        up, dn, far = step(b, 1), step(b, 3), step(b, 2)
        lo, hi = pl.ds(0, nz // 2), pl.ds(nz // 2, nz // 2)
        go(out2.at[far, :, lo], via2.at[0], to(a, up), in_v)
        go(out2.at[far, :, hi], via2.at[1], to(a, dn), in_v)
        go(out2.at[up], in2.at[b], to(a, up), in_2)
        go(out2.at[dn], in2.at[b], to(a, dn), in_2)
        in2[b] = out2[b]
        yield
        link.wait(in_v, via2)
        go(via2.at[0], in2.at[dn, :, lo], to(a, up), in_2)
        go(via2.at[1], in2.at[up, :, hi], to(a, dn), in_2)
        yield
        link.wait(in_2, in2.at[pl.ds(0, 3)])
        for j in range(3):
            out3[:, j] = (in2[0, j] + in2[1, j]) + (in2[2, j] + in2[3, j])
        for d in by_distance:
            zz = lax.rem(z + d, nz)
            go(in2.at[:, 3, zz], cold_land.at[z], dev(zz, y, x, c), in_s)
            go(out3.at[zz], hot_land.at[z], dev(zz, y, x, c), in_l)
        cold_land[z] = in2[:, 3, z]
        hot_land[z] = out3[z]
        yield
        link.wait(in_s, cold_land.at[pl.ds(0, nz - 1)])
        link.wait(in_l, hot_land.at[pl.ds(0, nz - 1)])

    def weight_grad(k):
        if k % 2 == 0:
            part = slice(w2.shape[0] // 4 * (k // 2), w2.shape[0] // 4 * (k // 2 + 1))
            g2_ref[part, :] = dot(h_ref[:, part], dys_ref[...], 0, 0)
            save(4, (part, full))
        else:
            part = slice(w1.shape[1] // 4 * (k // 2), w1.shape[1] // 4 * (k // 2 + 1))
            g1_ref[:, part] = dot(xs_ref[...], da_ref[:, part], 0, 0)
            save(3, (full, part))

    ys, dxs = [back(0), back(1)], [back(2), back(3)]
    n_tok = tok.shape[0]
    memo = {}
    earlier = iota((n_tok, n_tok), 1) < iota((n_tok, n_tok), 0)
    n_exp = wg.shape[1]

    def where_from(i, r0, r1):
        rank = jnp.sum(jnp.where(earlier & ((i == r0) | (i == r1)), 1.0, 0.0), axis=1, keepdims=True)
        slot = jnp.full((n_tok, 1), -1.0, F32)
        for j in range(3):
            slot = jnp.where(i == hot_ref[j:j + 1, 0:1], CAP * j + rank, slot)
        e = i.astype(jnp.int32)
        core, xx, yy, zz = e % nc, (e // nc) % nx, (e // (nc * nx)) % ny, e // (nc * nx * ny)
        lane, single = iota((n_tok, n_exp), 1), slot < 0.0
        pick = lambda m: m.astype(F32).astype(BF16)
        return pick(iota((n_tok, 32), 1).astype(F32) == slot), (pick((lane == e) & single), pick((lane == ((zz * nx + xx) * ny + yy) * nc + core) & single))

    def rows_of(kind, chosen):
        parts = []
        for half in range(2):
            hot_land, cold_land = areas[9 * (kind + half) + 7:9 * (kind + half) + 9]
            hot = jnp.sum(hot_land[...].astype(F32), axis=0).reshape(24, 128)
            hot = jnp.concatenate([hot, jnp.zeros((8, 128), F32)], axis=0).astype(BF16)
            cold = cold_land[...].astype(F32).reshape(n_exp, 128).astype(BF16)
            parts.append([dot(by_slot, hot, 1, 0) + dot(by_place[half], cold, 1, 0) for by_slot, by_place in chosen])
        return [jnp.concatenate([parts[0][k], parts[1][k]], axis=1) for k in range(2)]

    def combine():
        r0, r1 = ids[0:1].astype(F32), ids[1:2].astype(F32)
        i0, i1 = as_col(r0), as_col(r1)
        g0, g1 = gates(tok[...], i0, i1, wg[...])
        chosen = [where_from(i, r0, r1) for i in (i0, i1)]
        y0, y1 = rows_of(0, chosen)
        grad = dout[...].astype(F32)
        dg0, dg1 = (jnp.sum(grad * v, axis=1, keepdims=True) for v in (y0, y1))
        mean = g0 * dg0 + g1 * dg1
        d0, d1 = ((g * (dg - mean)).astype(BF16).astype(F32) for g, dg in ((g0, dg0), (g1, dg1)))
        d_row[...] = jnp.concatenate([as_row(d0), as_row(d1), jnp.zeros((1, 2 * n_tok), F32)], axis=1)
        place = pltpu.make_async_copy(d_row, d_land.at[z, y, x, c], keep_sem.at[1])
        place.start()
        out_ref[...] = (g0 * y0 + g1 * y1).astype(BF16)
        save(0)
        place.wait()
        d_plans.append(gather_rows(next(links), d_land, range(4)))
        advance(d_plans)
        expert = iota((n_tok, n_exp), 1).astype(F32)
        spread = jnp.where(expert == i0, d0, jnp.where(expert == i1, d1, 0.0)).astype(BF16)
        memo.update(chosen=chosen, through=dot(spread, wg[...], 1, 1))

    def finish():
        dx0, dx1 = rows_of(2, memo['chosen'])
        gx_ref[...] = (dx0 + dx1 + memo['through']).astype(BF16)
        save(1)

    n_dev = nz * ny * nx * nc

    def gate_grad():
        flatten(d_land, d_all)
        expert = iota((n_exp, 256), 0).astype(F32)
        codes = [plain_id(pair_rows(token_lanes(m_all, k, 0, n_dev // 4))) for k in range(2)]
        grads = [pair_rows(token_lanes(d_all, k, 0, n_dev // 4)) for k in range(2)]
        total = jnp.zeros((n_exp, x_all.shape[-1]), F32)
        zs = nz // 4 or 1
        for z0 in range(0, nz, zs):
            spread = []
            for p in range(z0 * ny, (z0 + zs) * ny):
                q = slice(p, p + 1)
                spread.append(jnp.where(expert == codes[0][q], grads[0][q], jnp.where(expert == codes[1][q], grads[1][q], 0.0)).astype(BF16))
            total += dot(jnp.concatenate(spread, axis=1), x_all[z0:z0 + zs].reshape(zs * ny * 256, x_all.shape[-1]), 1, 0)
        gate_ref[...] = total.T
        save(2)

    d_plans = []
    moves = {'t': tok_plans, 'g': grad_plans, 'm': row_plan, 'y': ys, 'x': dxs, 'd': d_plans}
    works = {'f': [functools.partial(forward, i) for i in range(steps)], 'b': [functools.partial(backward, i) for i in range(steps)],
             'B': [functools.partial(backward_rows, i) for i in range(steps)], 'w': [functools.partial(weight_grad, k) for k in range(8)],
             'h': [read_rows], 'c': [combine], 'k': [gate_grad], 'e': [finish]}
    for turn in SCHEDULE:
        if turn in moves:
            advance(moves[turn])
        elif works[turn]:
            works[turn].pop(0)()
    for link in all_links:
        link.finish(pad, pad_row)
    for cp in saves:
        cp.wait()


def block_call(dims, tokens, grad_out, ids, w_gate, w1, w2):
    nz, ny, nx, nc = dims
    d_model, d_hidden = w1.shape
    n_tok = tokens.shape[0]
    n_dev = nz * ny * nx * nc
    n_row = n_dev * CAP
    tile = (CAP, 128)
    hbm = pl.BlockSpec(memory_space=pltpu.HBM)
    out = jax.ShapeDtypeStruct
    work = [(4, 4, nz), (4, 2, 4, nz), (2, 2, 2, nz), (4, 4, nz), (2, 4, nz // 2), (4, 4, nz), (nz, 3), (nz, 3), (nz, 4)]
    n_group = 4 * 14 + 4 + 4 * 11 + 4
    sems = [pltpu.SemaphoreType.DMA((10,)), pltpu.SemaphoreType.DMA((n_group,))]
    results = [(tokens.shape, BF16), (tokens.shape, BF16), ((d_model, n_dev), F32), ((d_model, d_hidden), F32), ((d_hidden, d_model), F32)]
    row = (1, 128)
    kept = [(tokens.shape, BF16), (tokens.shape, BF16), (ids.shape, jnp.int32), (w_gate.shape, BF16), (w1.shape, BF16), (w2.shape, BF16), (row, F32), (dims + row, F32),
            (dims + tokens.shape, BF16), (dims + tokens.shape, BF16), ((n_row, d_model), BF16), ((n_row, d_model), BF16), ((n_row, d_hidden), BF16), ((n_row, d_hidden), BF16), ((n_row, d_hidden), F32), ((n_dev, 128), F32), (tile, F32), (row, F32),
            (dims + row, F32), ((n_dev, 128), F32), ((1024,) + tile, BF16), ((n_dev,) + row, F32)]
    return pl.pallas_call(
        functools.partial(block_kernel, dims, (6, len(results), len(results), len(kept), 4, 4 * len(work), 3, len(sems))),
        out_shape=[out(*r) for r in results],
        in_specs=[hbm] * 6,
        out_specs=[hbm] * len(results),
        scratch_shapes=[pltpu.VMEM(*r) for r in results + kept] + [pltpu.VMEM((nc, nx, ny, nz) + tile, BF16)] * 4 + [pltpu.VMEM(w + tile, BF16) for w in work] * 4
        + [pltpu.SemaphoreType.DMA((k,)) for k in (8, 2, 11)] + sems,
        compiler_params=pltpu.CompilerParams(collective_id=0, has_side_effects=True, vmem_limit_bytes=VMEM_LIMIT),
        name='block',
    )(tokens, grad_out, ids, w_gate, w1, w2)


VMEM_LIMIT = 67043328
SCHEDULE = 'mttgmttmgtmttgtth' + 'fgfgyfgyfgy' + 'yygg' + 'bybybyBBxbyxBBxy' + 'wwxxwwxwxyc' + 'xwwdxdxwddkxe'


def pass_kernel(n, *refs):
    refs = iter(refs)
    given, passed, held, (load_sem, save_sem) = [list(itertools.islice(refs, k)) for k in (n, n, n, 2)]
    loads = [pltpu.make_async_copy(given[k], held[k], load_sem.at[k]) for k in range(n)]
    saves = [pltpu.make_async_copy(held[k], passed[k], save_sem.at[k]) for k in range(n)]
    for cp in loads:
        cp.start()
    for load, save in zip(loads, saves):
        load.wait()
        save.start()
    for cp in saves:
        cp.wait()


def pass_on(*arrays):
    n = len(arrays)
    return pl.pallas_call(
        functools.partial(pass_kernel, n),
        out_shape=[jax.ShapeDtypeStruct(v.shape, v.dtype) for v in arrays],
        in_specs=[pl.BlockSpec(memory_space=pltpu.HBM)] * n,
        out_specs=[pl.BlockSpec(memory_space=pltpu.HBM)] * n,
        scratch_shapes=[pltpu.VMEM(v.shape, v.dtype) for v in arrays] + [pltpu.SemaphoreType.DMA((n,))] * 2,
        compiler_params=pltpu.CompilerParams(vmem_limit_bytes=VMEM_LIMIT),
        name='pass_on',
    )(*arrays)


def local_block(dims, tokens, grad_out, expert_ids, w_gate, w_in, w_out):
    y_out, grad_x, grad_w_gate, g1, g2 = pass_on(*block_call(dims, tokens, grad_out, expert_ids.T, w_gate, w_in[0], w_out[0]))
    return y_out, grad_x, g1[None], g2[None], grad_w_gate


def solution(mesh):
    dims = (8, 4, 4, 2)
    return jax.shard_map(functools.partial(local_block, dims), mesh=mesh, in_specs=(P('ep'), P('ep'), P('ep'), P(), P('ep'), P('ep')), out_specs=(P('ep'), P('ep'), P('ep'), P('ep'), P()), check_vma=False)
```

```python
import functools
import itertools
import math

import jax
import jax.numpy as jnp
from jax import lax
from jax.experimental import pallas as pl
from jax.experimental.pallas import tpu as pltpu
from jax.sharding import PartitionSpec as P

MESH = pl.DeviceIdType.MESH
F32 = jnp.float32
BF16 = jnp.bfloat16
CAP = 8


def coords(dims):
    nz, ny, nx, nc = dims
    me = lax.axis_index('ep')
    c = lax.rem(me, nc)
    x = lax.rem(me // nc, nx)
    y = lax.rem(me // (nc * nx), ny)
    z = me // (nc * nx * ny)

    def dev(z, y, x, c):
        return (((z * ny + y) * nx + x) * nc + c,)

    return z, y, x, c, dev


def dot(a, b, ca, cb):
    return lax.dot_general(a, b, (((ca,), (cb,)), ((), ())), preferred_element_type=F32)


def iota(shape, axis):
    return lax.broadcasted_iota(jnp.int32, shape, axis)


def as_row(col):
    n = col.shape[0]
    return jnp.sum(jnp.where(iota((n, n), 0) == iota((n, n), 1), col, 0.0), axis=0, keepdims=True)


def as_col(row):
    n = row.shape[1]
    return jnp.sum(jnp.where(iota((n, n), 0) == iota((n, n), 1), row, 0.0), axis=1, keepdims=True)


def gates(tok, i0, i1, w_gate):
    logits = dot(tok, w_gate, 1, 0)
    expert = iota(logits.shape, 1).astype(F32)
    l0, l1 = (jnp.sum(jnp.where(expert == i, logits, 0.0), axis=1, keepdims=True) for i in (i0, i1))
    top = jnp.maximum(l0, l1)
    p0, p1 = jnp.exp(l0 - top), jnp.exp(l1 - top)
    total = p0 + p1
    return p0 / total, p1 / total


def choice_row(tok, ids, w_gate):
    r0, r1 = ids[0:1].astype(F32), ids[1:2].astype(F32)
    i0, i1 = as_col(r0), as_col(r1)
    g0, g1 = gates(tok, i0, i1, w_gate)

    def code(i):
        n = jnp.sum((i == r0).astype(F32) + (i == r1).astype(F32), axis=1, keepdims=True)
        return as_row(jnp.where(n > 1.5, i + 256.0, i))

    return jnp.concatenate([code(i0), code(i1), as_row(g0), as_row(g1)], axis=1)


def gelu_tanh(a):
    k = 0.7978845608028654
    sq = a * a
    return jnp.tanh(a * (k + (k * 0.044715) * sq)), sq


def gelu(a):
    half = 0.5 * a
    return half + half * gelu_tanh(a)[0]


def gelu_slope(a):
    k = 0.7978845608028654
    t, sq = gelu_tanh(a)
    return (0.5 + 0.5 * t) + (0.5 * a) * (1.0 - t * t) * (k + (3 * k * 0.044715) * sq)


def token_lanes(ref, k, start, n):
    lane = iota((n, 128), 1) // 32
    out = jnp.zeros((n, 128), F32)
    for j in range(4):
        r = ref[pl.ds(start + j, n, stride=4), :]
        out = jnp.where(lane == j, r if j == k else pltpu.roll(r, 32 * (j - k) % 128, 1), out)
    return out


def pair_rows(v):
    return jnp.concatenate([jnp.concatenate([v[2 * i:2 * i + 1], v[2 * i + 1:2 * i + 2]], axis=1) for i in range(v.shape[0] // 2)], axis=0)


def plain_id(code):
    return jnp.where(code >= 256.0, code - 256.0, code)


class Links:
    def __init__(self, send, recv, pool):
        self.send, self.recv, self.pool, self.bytes = send, recv, pool, 0

    def group(self):
        return self.recv.at[next(self.pool)]

    def go(self, src, dst, to, group):
        pltpu.make_async_remote_copy(src_ref=src, dst_ref=dst, send_sem=self.send, recv_sem=group, device_id=to, device_id_type=MESH).start()
        self.bytes += math.prod(src.shape) * jnp.dtype(src.dtype).itemsize

    def wait(self, group, ref):
        pltpu.make_async_copy(ref, ref, group).wait()

    def finish(self, *pads):
        for pad in pads:
            unit = math.prod(pad.shape[1:]) * jnp.dtype(pad.dtype).itemsize
            if self.bytes % unit == 0:
                return self.wait(self.send, pad.at[pl.ds(0, self.bytes // unit)])
        raise ValueError(self.bytes)


def block_kernel(dims, sizes, *refs):
    nz, ny, nx, nc = dims
    refs = iter(refs)
    refs = [list(itertools.islice(refs, n)) for n in sizes]
    (tok_hbm, dout_hbm, ids_hbm, wg_hbm, w1_hbm, w2_hbm), outs, held, kept, rows, areas, (load_sem, keep_sem, save_sem), sems = refs
    out_ref, gx_ref, gate_ref, g1_ref, g2_ref = held
    tok, dout, ids, wg, w1, w2, row, m_land, x_all, g_all, xs_ref, dys_ref, h_ref, da_ref, a_ref, m_all, hot_ref, d_row, d_land, d_all, pad, pad_row = kept
    z, y, x, c, dev = coords(dims)
    saves = []

    def save(k, part=None):
        src, dst = (held[k], outs[k]) if part is None else (held[k].at[part], outs[k].at[part])
        cp = pltpu.make_async_copy(src, dst, save_sem.at[len(saves)])
        cp.start()
        saves.append(cp)

    send_sem, recv_sem = sems
    pool = itertools.count()
    all_links = [Links(send_sem.at[k], recv_sem, pool) for k in range(send_sem.shape[0])]
    links = iter(all_links)

    loads = [pltpu.make_async_copy(s, d, load_sem.at[k]) for k, (s, d) in enumerate(
        [(tok_hbm, x_all.at[z, y, x, c]), (dout_hbm, g_all.at[z, y, x, c]), (tok_hbm, tok), (ids_hbm, ids), (wg_hbm, wg), (dout_hbm, dout), (w1_hbm, w1), (w2_hbm, w2)])]
    for ld in loads:
        ld.start()
    peers = [dev(lax.rem(z + d, nz), y, x, c) for d in range(1, nz)]
    for d in (1, 2, 3):
        peers.append(dev(z, lax.rem(y + d, ny), x, c))
        peers.append(dev(z, y, lax.rem(x + d, nx), c))
    mate = dev(z, y, x, 1 - c)
    peers.append(mate)
    barrier = pltpu.get_barrier_semaphore()
    for peer in peers:
        pl.semaphore_signal(barrier, inc=1, device_id=peer, device_id_type=MESH)
    for ld in loads[2:5]:
        ld.wait()
    row[...] = choice_row(tok[...], ids[...], wg[...])
    place = pltpu.make_async_copy(row, m_land.at[z, y, x, c], keep_sem.at[0])
    place.start()
    loads[0].wait()
    loads[1].wait()
    place.wait()
    pl.semaphore_wait(barrier, len(peers))

    full = slice(None)
    by_distance = sorted(range(1, nz), key=lambda d: abs(d - nz // 2))

    def step(v, d, m=4):
        return lax.rem(v + d, m)

    def by_lines(link, ref, rows, x_last, late):
        p0, q0 = (y, x) if x_last else (x, y)
        low, high = pl.ds(0, nz // 2), pl.ds(nz // 2, nz // 2)

        def at(zs, p, q):
            return ref.at[(zs, p, q, c, rows) if x_last else (zs, q, p, c, rows)]

        def go(part, p, q, group):
            link.go(part, part, dev(z, p, q, c) if x_last else dev(z, q, p, c), group)

        in_z, in_p, in_m, in_f, in_r, in_c = [link.group() for _ in range(6)]
        line = at(full, p0, q0)

        def over(q):
            part = at(full, full, q)
            link.go(part, part, mate, in_c)

        own = at(z, p0, q0)
        for d in by_distance:
            link.go(own, own, dev(step(z, d, nz), y, x, c), in_z)
        yield
        link.wait(in_z, at(pl.ds(0, nz - 1), p0, q0))
        pm, pp, po = step(p0, 3), step(p0, 1), step(p0, 2)
        qm, qp, qo = step(q0, 3), step(q0, 1), step(q0, 2)
        qs = []

        def spread(p):
            part = at(full, p, q0)
            qs.append((p, link.group(), link.group()))
            go(part, p0, qp, qs[-1][1])
            go(part, p0, qm, qs[-1][2])

        def relay(i):
            p, up, dn = qs[i]
            link.wait(up, line)
            go(at(low, p, qm), p0, qp, in_r)
            link.wait(dn, line)
            go(at(high, p, qp), p0, qm, in_r)

        def pass_one():
            link.wait(in_p, line)
            go(at(low, pm, q0), pp, q0, in_f)
            link.wait(in_m, line)
            go(at(high, pp, q0), pm, q0, in_f)

        go(line, pp, q0, in_p)
        go(line, pm, q0, in_m)
        if late:
            yield
            pass_one()
            yield
            link.wait(in_f, line)
            for p in (p0, pm, pp, po):
                spread(p)
            over(q0)
            yield
            relay(0)
        else:
            yield
            spread(p0)
            yield
            pass_one()
            yield
            spread(pm)
            spread(pp)
            yield
            relay(0)
            yield
            link.wait(in_f, line)
            spread(po)
            over(q0)
        for i in range(1, 4):
            yield
            relay(i)
        over(qm)
        over(qp)
        yield
        link.wait(in_r, at(full, full, q0))
        over(qo)
        yield
        link.wait(in_c, ref.at[full, full, full, c, rows])

    def gather_rows(link, held, order):
        have = [z, y, x, c]
        for axis in order:
            size = (nz, ny, nx, nc)[axis]
            part = held.at[tuple(have)]
            group = link.group()
            for d in sorted(range(1, size), key=lambda d: abs(d - size // 2)):
                there = [z, y, x, c]
                there[axis] = lax.rem(there[axis] + d, size)
                link.go(part, part, dev(*there), group)
            have[axis] = pl.ds(0, size - 1)
            yield
            link.wait(group, held.at[tuple(have)])
            have[axis] = full

    def advance(plans):
        for g in plans:
            next(g, None)

    halves = [slice(0, 16), slice(16, 32)]
    tok_plans, grad_plans = [[by_lines(next(links), ref, half, half.start == 0, ref is g_all) for half in halves] for ref in (x_all, g_all)]
    row_plan = [gather_rows(next(links), m_land, range(4))]
    advance(row_plan + tok_plans + grad_plans)
    def flatten(land, flat):
        def lines(zz, carry):
            for k in range(ny * nx * nc):
                flat[pl.ds(zz * (ny * nx * nc) + k, 1), :] = land[zz, k // (nx * nc), k // nc % nx, k % nc]
            return carry

        lax.fori_loop(0, nz, lines, 0)


    me = lax.axis_index('ep').astype(F32)
    def read_rows():
        flatten(m_land, m_all)
        for ld in loads[5:]:
            ld.wait()
        code = m_all[...]
        left = jnp.where((iota(code.shape, 1) < 64) & (code >= 256.0), code - 256.0, 999.0)
        found = []
        for _ in range(3):
            best = jnp.min(jnp.min(left, axis=0, keepdims=True), axis=1, keepdims=True)
            left = jnp.where(left == best, 999.0, left)
            found.append(jnp.broadcast_to(best, (1, 128)))
        hot_ref[...] = jnp.concatenate(found + [jnp.full((5, 128), 999.0, F32)], axis=0)

    steps = 4 if nz == 8 else 1
    per = nz // steps
    n_quad = per * ny * nx * nc // 4
    n_pair = n_quad // 2
    n_slot = n_pair * 8 * CAP

    places = [(cc, xx, yy, zz) for cc in range(nc) for xx in range(nx) for yy in range(ny) for zz in range(per)]

    def select(i, ref, with_gate):
        c0, c1, g0, g1 = (pair_rows(token_lanes(m_all, k, pl.multiple_of(4 * n_quad * i, 4 * n_quad), n_quad)) for k in range(4))
        hit0, hit1 = plain_id(c0) == me, plain_id(c1) == me
        hit = (hit0 | hit1).astype(F32)
        gate = jnp.where(hit0, g0, 0.0) + jnp.where(hit1, g1, 0.0)
        before, after = iota((256, 256), 0), iota((256, 256), 1)
        tri = ((before < after) & (before // 32 == after // 32)).astype(F32).astype(BF16)
        rank = dot(hit.astype(BF16), tri, 1, 0)
        src = (iota((n_pair, 256), 1) // 32).astype(F32)
        key = jnp.where(hit > 0.0, src * CAP + rank, -1.0)
        slot = iota((8 * CAP, 256), 0).astype(F32)
        parts = []
        for p in range(n_pair):
            sel = (slot == key[p:p + 1]).astype(F32)
            v = dot(sel.astype(BF16), ref[i * per + p // ny, p % ny].reshape(256, 256), 1, 0)
            parts.append(v * jnp.sum(sel * gate[p:p + 1], axis=1, keepdims=True) if with_gate else v)
        return jnp.concatenate([parts[zz * ny + yy][CAP * (xx * nc + cc):CAP * (xx * nc + cc + 1)] for cc, xx, yy, zz in places], axis=0).astype(BF16)

    def put(i, v, to):
        for k, (cc, xx, yy, zz) in enumerate(places):
            for half in range(2):
                to[half][cc, xx, yy, i * per + zz] = v[CAP * k:CAP * (k + 1), 128 * half:128 * (half + 1)].astype(BF16)

    def forward(i):
        here = pl.ds(i * n_slot, n_slot)
        xs = select(i, x_all, False)
        a = dot(xs, w1[...], 1, 0)
        h = gelu(a).astype(BF16)
        xs_ref[here], h_ref[here], a_ref[here] = xs, h, a
        put(i, dot(h, w2[...], 1, 0), rows[:2])

    def backward(i):
        here = pl.ds(i * n_slot, n_slot)
        dys = select(i, g_all, True)
        dys_ref[here] = dys
        da_ref[here] = (dot(dys, w2[...], 1, 1) * gelu_slope(a_ref[here])).astype(BF16)

    def backward_rows(i):
        put(i, dot(da_ref[pl.ds(i * n_slot, n_slot)], w1[...], 1, 1), rows[2:])

    def back(i):
        h = rows[i]
        other, near, via, out2, via2, in2, out3, hot_land, cold_land = areas[9 * i:9 * i + 9]
        link = next(links)
        go = link.go
        in_c, in_e, in_h = [[link.group(), link.group()] for _ in range(3)]
        in_n, in_v, in_2, in_l, in_s = [link.group() for _ in range(5)]
        x_first = i % 2 == 0
        a, b = (x, y) if x_first else (y, x)

        def to(a, b):
            return dev(z, b, a, c) if x_first else dev(z, a, b, c)

        def index(lead, a, bs):
            return lead + ((a, bs) if x_first else (bs, a))

        up, dn, far = step(a, 1), step(a, 3), step(a, 2)
        lo, hi = pl.ds(0, 2), pl.ds(2, 2)
        parts = [pl.ds(0, nz // 2), pl.ds(nz // 2, nz // 2)]

        def start(k):
            zs = parts[k]
            go(h.at[1 - c, :, :, zs], other.at[:, :, zs], mate, in_c[k])
            spread(h, (c,), c, zs, in_e[k])

        def follow(k):
            link.wait(in_c[k], other.at[:, :, parts[k]])
            spread(other, (), 1 - c, parts[k], in_h[k])

        def spread(ref, lead, e, zs, group):
            go(ref.at[index(lead, far, lo) + (zs,)], via.at[0, e, :, zs], to(up, b), group)
            go(ref.at[index(lead, far, hi) + (zs,)], via.at[1, e, :, zs], to(dn, b), group)
            go(ref.at[index(lead, up, full) + (zs,)], near.at[a, e, :, zs], to(up, b), in_n)
            go(ref.at[index(lead, dn, full) + (zs,)], near.at[a, e, :, zs], to(dn, b), in_n)

        def relay(e, zs, group):
            link.wait(group, via.at[:, e, :, zs])
            go(via.at[0, e, :, zs], near.at[dn, e, lo, zs], to(up, b), in_n)
            go(via.at[1, e, :, zs], near.at[up, e, hi, zs], to(dn, b), in_n)

        start(0)
        yield
        follow(0)
        yield
        start(1)
        yield
        follow(1)
        yield
        relay(c, parts[0], in_e[0])
        relay(1 - c, parts[0], in_h[0])
        yield
        relay(c, parts[1], in_e[1])
        yield
        relay(1 - c, parts[1], in_h[1])
        yield
        link.wait(in_n, near.at[pl.ds(0, 3)])

        def expert(s, e):
            return ((z * ny + y) * nx + s) * nc + e if x_first else ((z * ny + s) * nx + x) * nc + e

        places = [(step(a, d), e) for d in range(4) for e in (c, 1 - c)]
        is_hot = [[(hot_ref[j:j + 1, :] == expert(s, e).astype(F32)).astype(F32) for s, e in places] for j in range(3)]
        wide = lambda v: jnp.broadcast_to(v, (8, 128))
        weight = [[wide(v).astype(BF16) for v in r] for r in is_hot]
        line = iota((8, 128), 0)
        mine = [(wide(is_hot[0][k] + is_hot[1][k] + is_hot[2][k]) < 0.5) & (line == s * nc + e) for k, (s, e) in enumerate(places)]

        def squeeze(bb, carry):
            given = [h[index((c,), a, bb)], other[index((), a, bb)]] + [near[s, e, bb] for s, e in places[2:]]
            for j in range(3):
                out2[bb, j] = sum(given[k] * weight[j][k] for k in range(8))
            singles = jnp.zeros((nz, 8, 128), F32)
            for k in range(8):
                singles = jnp.where(mine[k], jnp.sum(given[k].astype(F32), axis=1, keepdims=True), singles)
            out2[bb, 3] = singles.astype(BF16)
            return carry

        lax.fori_loop(0, 4, squeeze, 0)
        up, dn, far = step(b, 1), step(b, 3), step(b, 2)
        lo, hi = pl.ds(0, nz // 2), pl.ds(nz // 2, nz // 2)
        go(out2.at[far, :, lo], via2.at[0], to(a, up), in_v)
        go(out2.at[far, :, hi], via2.at[1], to(a, dn), in_v)
        go(out2.at[up], in2.at[b], to(a, up), in_2)
        go(out2.at[dn], in2.at[b], to(a, dn), in_2)
        in2[b] = out2[b]
        yield
        link.wait(in_v, via2)
        go(via2.at[0], in2.at[dn, :, lo], to(a, up), in_2)
        go(via2.at[1], in2.at[up, :, hi], to(a, dn), in_2)
        yield
        link.wait(in_2, in2.at[pl.ds(0, 3)])
        for j in range(3):
            out3[:, j] = (in2[0, j] + in2[1, j]) + (in2[2, j] + in2[3, j])
        for d in by_distance:
            zz = lax.rem(z + d, nz)
            go(in2.at[:, 3, zz], cold_land.at[z], dev(zz, y, x, c), in_s)
            go(out3.at[zz], hot_land.at[z], dev(zz, y, x, c), in_l)
        cold_land[z] = in2[:, 3, z]
        hot_land[z] = out3[z]
        yield
        link.wait(in_s, cold_land.at[pl.ds(0, nz - 1)])
        link.wait(in_l, hot_land.at[pl.ds(0, nz - 1)])

    def weight_grad(k):
        if k % 2 == 0:
            part = slice(w2.shape[0] // 4 * (k // 2), w2.shape[0] // 4 * (k // 2 + 1))
            g2_ref[part, :] = dot(h_ref[:, part], dys_ref[...], 0, 0)
            save(4, (part, full))
        else:
            part = slice(w1.shape[1] // 4 * (k // 2), w1.shape[1] // 4 * (k // 2 + 1))
            g1_ref[:, part] = dot(xs_ref[...], da_ref[:, part], 0, 0)
            save(3, (full, part))

    ys, dxs = [back(0), back(1)], [back(2), back(3)]
    n_tok = tok.shape[0]
    memo = {}
    earlier = iota((n_tok, n_tok), 1) < iota((n_tok, n_tok), 0)
    n_exp = wg.shape[1]

    def where_from(i, r0, r1):
        rank = jnp.sum(jnp.where(earlier & ((i == r0) | (i == r1)), 1.0, 0.0), axis=1, keepdims=True)
        slot = jnp.full((n_tok, 1), -1.0, F32)
        for j in range(3):
            slot = jnp.where(i == hot_ref[j:j + 1, 0:1], CAP * j + rank, slot)
        e = i.astype(jnp.int32)
        core, xx, yy, zz = e % nc, (e // nc) % nx, (e // (nc * nx)) % ny, e // (nc * nx * ny)
        lane, single = iota((n_tok, n_exp), 1), slot < 0.0
        pick = lambda m: m.astype(F32).astype(BF16)
        return pick(iota((n_tok, 32), 1).astype(F32) == slot), (pick((lane == e) & single), pick((lane == ((zz * nx + xx) * ny + yy) * nc + core) & single))

    def rows_of(kind, chosen):
        parts = []
        for half in range(2):
            hot_land, cold_land = areas[9 * (kind + half) + 7:9 * (kind + half) + 9]
            hot = jnp.sum(hot_land[...].astype(F32), axis=0).reshape(24, 128)
            hot = jnp.concatenate([hot, jnp.zeros((8, 128), F32)], axis=0).astype(BF16)
            cold = cold_land[...].astype(F32).reshape(n_exp, 128).astype(BF16)
            parts.append([dot(by_slot, hot, 1, 0) + dot(by_place[half], cold, 1, 0) for by_slot, by_place in chosen])
        return [jnp.concatenate([parts[0][k], parts[1][k]], axis=1) for k in range(2)]

    def combine():
        r0, r1 = ids[0:1].astype(F32), ids[1:2].astype(F32)
        i0, i1 = as_col(r0), as_col(r1)
        g0, g1 = gates(tok[...], i0, i1, wg[...])
        chosen = [where_from(i, r0, r1) for i in (i0, i1)]
        y0, y1 = rows_of(0, chosen)
        grad = dout[...].astype(F32)
        dg0, dg1 = (jnp.sum(grad * v, axis=1, keepdims=True) for v in (y0, y1))
        mean = g0 * dg0 + g1 * dg1
        d0, d1 = ((g * (dg - mean)).astype(BF16).astype(F32) for g, dg in ((g0, dg0), (g1, dg1)))
        d_row[...] = jnp.concatenate([as_row(d0), as_row(d1), jnp.zeros((1, 2 * n_tok), F32)], axis=1)
        place = pltpu.make_async_copy(d_row, d_land.at[z, y, x, c], keep_sem.at[1])
        place.start()
        out_ref[...] = (g0 * y0 + g1 * y1).astype(BF16)
        save(0)
        place.wait()
        d_plans.append(gather_rows(next(links), d_land, range(4)))
        advance(d_plans)
        expert = iota((n_tok, n_exp), 1).astype(F32)
        spread = jnp.where(expert == i0, d0, jnp.where(expert == i1, d1, 0.0)).astype(BF16)
        memo.update(chosen=chosen, through=dot(spread, wg[...], 1, 1))

    def finish():
        dx0, dx1 = rows_of(2, memo['chosen'])
        gx_ref[...] = (dx0 + dx1 + memo['through']).astype(BF16)
        save(1)

    n_dev = nz * ny * nx * nc

    def gate_grad():
        flatten(d_land, d_all)
        expert = iota((n_exp, 256), 0).astype(F32)
        codes = [plain_id(pair_rows(token_lanes(m_all, k, 0, n_dev // 4))) for k in range(2)]
        grads = [pair_rows(token_lanes(d_all, k, 0, n_dev // 4)) for k in range(2)]
        total = jnp.zeros((n_exp, x_all.shape[-1]), F32)
        zs = nz // 4 or 1
        for z0 in range(0, nz, zs):
            spread = []
            for p in range(z0 * ny, (z0 + zs) * ny):
                q = slice(p, p + 1)
                spread.append(jnp.where(expert == codes[0][q], grads[0][q], jnp.where(expert == codes[1][q], grads[1][q], 0.0)).astype(BF16))
            total += dot(jnp.concatenate(spread, axis=1), x_all[z0:z0 + zs].reshape(zs * ny * 256, x_all.shape[-1]), 1, 0)
        gate_ref[...] = total.T
        save(2)

    d_plans = []
    moves = {'t': tok_plans, 'g': grad_plans, 'm': row_plan, 'y': ys, 'x': dxs, 'd': d_plans}
    works = {'f': [functools.partial(forward, i) for i in range(steps)], 'b': [functools.partial(backward, i) for i in range(steps)],
             'B': [functools.partial(backward_rows, i) for i in range(steps)], 'w': [functools.partial(weight_grad, k) for k in range(8)],
             'h': [read_rows], 'c': [combine], 'k': [gate_grad], 'e': [finish]}
    for turn in SCHEDULE:
        if turn in moves:
            advance(moves[turn])
        elif works[turn]:
            works[turn].pop(0)()
    for link in all_links:
        link.finish(pad, pad_row)
    for cp in saves:
        cp.wait()


def block_call(dims, tokens, grad_out, ids, w_gate, w1, w2):
    nz, ny, nx, nc = dims
    d_model, d_hidden = w1.shape
    n_tok = tokens.shape[0]
    n_dev = nz * ny * nx * nc
    n_row = n_dev * CAP
    tile = (CAP, 128)
    hbm = pl.BlockSpec(memory_space=pltpu.HBM)
    out = jax.ShapeDtypeStruct
    work = [(4, 4, nz), (4, 2, 4, nz), (2, 2, 2, nz), (4, 4, nz), (2, 4, nz // 2), (4, 4, nz), (nz, 3), (nz, 3), (nz, 4)]
    n_group = 4 * 14 + 4 + 4 * 11 + 4
    sems = [pltpu.SemaphoreType.DMA((10,)), pltpu.SemaphoreType.DMA((n_group,))]
    results = [(tokens.shape, BF16), (tokens.shape, BF16), ((d_model, n_dev), F32), ((d_model, d_hidden), F32), ((d_hidden, d_model), F32)]
    row = (1, 128)
    kept = [(tokens.shape, BF16), (tokens.shape, BF16), (ids.shape, jnp.int32), (w_gate.shape, BF16), (w1.shape, BF16), (w2.shape, BF16), (row, F32), (dims + row, F32),
            (dims + tokens.shape, BF16), (dims + tokens.shape, BF16), ((n_row, d_model), BF16), ((n_row, d_model), BF16), ((n_row, d_hidden), BF16), ((n_row, d_hidden), BF16), ((n_row, d_hidden), F32), ((n_dev, 128), F32), (tile, F32), (row, F32),
            (dims + row, F32), ((n_dev, 128), F32), ((1024,) + tile, BF16), ((n_dev,) + row, F32)]
    return pl.pallas_call(
        functools.partial(block_kernel, dims, (6, len(results), len(results), len(kept), 4, 4 * len(work), 3, len(sems))),
        out_shape=[out(*r) for r in results],
        in_specs=[hbm] * 6,
        out_specs=[hbm] * len(results),
        scratch_shapes=[pltpu.VMEM(*r) for r in results + kept] + [pltpu.VMEM((nc, nx, ny, nz) + tile, BF16)] * 4 + [pltpu.VMEM(w + tile, BF16) for w in work] * 4
        + [pltpu.SemaphoreType.DMA((k,)) for k in (8, 2, 11)] + sems,
        compiler_params=pltpu.CompilerParams(collective_id=0, has_side_effects=True, vmem_limit_bytes=VMEM_LIMIT),
        name='block',
    )(tokens, grad_out, ids, w_gate, w1, w2)


VMEM_LIMIT = 67043328
SCHEDULE = 'mttttmgttmgtttgtmth' + 'fgfgyfgyfgy' + 'gygy' + 'bybybyBBxbyxBBxy' + 'wwxxwxwwxxyc' + 'wwxdxwdddkxe'


def pass_kernel(n, *refs):
    refs = iter(refs)
    given, passed, held, (load_sem, save_sem) = [list(itertools.islice(refs, k)) for k in (n, n, n, 2)]
    loads = [pltpu.make_async_copy(given[k], held[k], load_sem.at[k]) for k in range(n)]
    saves = [pltpu.make_async_copy(held[k], passed[k], save_sem.at[k]) for k in range(n)]
    for cp in loads:
        cp.start()
    for load, save in zip(loads, saves):
        load.wait()
        save.start()
    for cp in saves:
        cp.wait()


def pass_on(*arrays):
    n = len(arrays)
    return pl.pallas_call(
        functools.partial(pass_kernel, n),
        out_shape=[jax.ShapeDtypeStruct(v.shape, v.dtype) for v in arrays],
        in_specs=[pl.BlockSpec(memory_space=pltpu.HBM)] * n,
        out_specs=[pl.BlockSpec(memory_space=pltpu.HBM)] * n,
        scratch_shapes=[pltpu.VMEM(v.shape, v.dtype) for v in arrays] + [pltpu.SemaphoreType.DMA((n,))] * 2,
        compiler_params=pltpu.CompilerParams(vmem_limit_bytes=VMEM_LIMIT),
        name='pass_on',
    )(*arrays)


def local_block(dims, tokens, grad_out, expert_ids, w_gate, w_in, w_out):
    y_out, grad_x, grad_w_gate, g1, g2 = pass_on(*block_call(dims, tokens, grad_out, expert_ids.T, w_gate, w_in[0], w_out[0]))
    return y_out, grad_x, g1[None], g2[None], grad_w_gate


def solution(mesh):
    dims = (8, 4, 4, 2)
    return jax.shard_map(functools.partial(local_block, dims), mesh=mesh, in_specs=(P('ep'), P('ep'), P('ep'), P(), P('ep'), P('ep')), out_specs=(P('ep'), P('ep'), P('ep'), P('ep'), P()), check_vma=False)
```

```python
import functools
import itertools
import math

import jax
import jax.numpy as jnp
from jax import lax
from jax.experimental import pallas as pl
from jax.experimental.pallas import tpu as pltpu
from jax.sharding import PartitionSpec as P

MESH = pl.DeviceIdType.MESH
F32 = jnp.float32
BF16 = jnp.bfloat16
CAP = 8


def coords(dims):
    nz, ny, nx, nc = dims
    me = lax.axis_index('ep')
    c = lax.rem(me, nc)
    x = lax.rem(me // nc, nx)
    y = lax.rem(me // (nc * nx), ny)
    z = me // (nc * nx * ny)

    def dev(z, y, x, c):
        return (((z * ny + y) * nx + x) * nc + c,)

    return z, y, x, c, dev


def dot(a, b, ca, cb):
    return lax.dot_general(a, b, (((ca,), (cb,)), ((), ())), preferred_element_type=F32)


def iota(shape, axis):
    return lax.broadcasted_iota(jnp.int32, shape, axis)


def as_row(col):
    n = col.shape[0]
    return jnp.sum(jnp.where(iota((n, n), 0) == iota((n, n), 1), col, 0.0), axis=0, keepdims=True)


def as_col(row):
    n = row.shape[1]
    return jnp.sum(jnp.where(iota((n, n), 0) == iota((n, n), 1), row, 0.0), axis=1, keepdims=True)


def gates(tok, i0, i1, w_gate):
    logits = dot(tok, w_gate, 1, 0)
    expert = iota(logits.shape, 1).astype(F32)
    l0, l1 = (jnp.sum(jnp.where(expert == i, logits, 0.0), axis=1, keepdims=True) for i in (i0, i1))
    top = jnp.maximum(l0, l1)
    p0, p1 = jnp.exp(l0 - top), jnp.exp(l1 - top)
    total = p0 + p1
    return p0 / total, p1 / total


def choice_row(tok, ids, w_gate):
    r0, r1 = ids[0:1].astype(F32), ids[1:2].astype(F32)
    i0, i1 = as_col(r0), as_col(r1)
    g0, g1 = gates(tok, i0, i1, w_gate)

    def code(i):
        n = jnp.sum((i == r0).astype(F32) + (i == r1).astype(F32), axis=1, keepdims=True)
        return as_row(jnp.where(n > 1.5, i + 256.0, i))

    return jnp.concatenate([code(i0), code(i1), as_row(g0), as_row(g1)], axis=1)


def gelu_tanh(a):
    k = 0.7978845608028654
    sq = a * a
    return jnp.tanh(a * (k + (k * 0.044715) * sq)), sq


def gelu(a):
    half = 0.5 * a
    return half + half * gelu_tanh(a)[0]


def gelu_slope(a):
    k = 0.7978845608028654
    t, sq = gelu_tanh(a)
    return (0.5 + 0.5 * t) + (0.5 * a) * (1.0 - t * t) * (k + (3 * k * 0.044715) * sq)


def token_lanes(ref, k, start, n):
    lane = iota((n, 128), 1) // 32
    out = jnp.zeros((n, 128), F32)
    for j in range(4):
        r = ref[pl.ds(start + j, n, stride=4), :]
        out = jnp.where(lane == j, r if j == k else pltpu.roll(r, 32 * (j - k) % 128, 1), out)
    return out


def pair_rows(v):
    return jnp.concatenate([jnp.concatenate([v[2 * i:2 * i + 1], v[2 * i + 1:2 * i + 2]], axis=1) for i in range(v.shape[0] // 2)], axis=0)


def plain_id(code):
    return jnp.where(code >= 256.0, code - 256.0, code)


class Links:
    def __init__(self, send, recv, pool):
        self.send, self.recv, self.pool, self.bytes = send, recv, pool, 0

    def group(self):
        return self.recv.at[next(self.pool)]

    def go(self, src, dst, to, group):
        pltpu.make_async_remote_copy(src_ref=src, dst_ref=dst, send_sem=self.send, recv_sem=group, device_id=to, device_id_type=MESH).start()
        self.bytes += math.prod(src.shape) * jnp.dtype(src.dtype).itemsize

    def wait(self, group, ref):
        pltpu.make_async_copy(ref, ref, group).wait()

    def finish(self, *pads):
        for pad in pads:
            unit = math.prod(pad.shape[1:]) * jnp.dtype(pad.dtype).itemsize
            if self.bytes % unit == 0:
                return self.wait(self.send, pad.at[pl.ds(0, self.bytes // unit)])
        raise ValueError(self.bytes)


def block_kernel(dims, sizes, *refs):
    nz, ny, nx, nc = dims
    refs = iter(refs)
    refs = [list(itertools.islice(refs, n)) for n in sizes]
    (tok_hbm, dout_hbm, ids_hbm, wg_hbm, w1_hbm, w2_hbm), outs, held, kept, rows, areas, (load_sem, keep_sem, save_sem), sems = refs
    out_ref, gx_ref, gate_ref, g1_ref, g2_ref = held
    tok, dout, ids, wg, w1, w2, row, m_land, x_all, g_all, xs_ref, dys_ref, h_ref, da_ref, a_ref, m_all, hot_ref, d_row, d_land, d_all, pad, pad_row = kept
    z, y, x, c, dev = coords(dims)
    saves = []

    def save(k, part=None):
        src, dst = (held[k], outs[k]) if part is None else (held[k].at[part], outs[k].at[part])
        cp = pltpu.make_async_copy(src, dst, save_sem.at[len(saves)])
        cp.start()
        saves.append(cp)

    send_sem, recv_sem = sems
    pool = itertools.count()
    all_links = [Links(send_sem.at[k], recv_sem, pool) for k in range(send_sem.shape[0])]
    links = iter(all_links)

    loads = [pltpu.make_async_copy(s, d, load_sem.at[k]) for k, (s, d) in enumerate(
        [(tok_hbm, x_all.at[z, y, x, c]), (dout_hbm, g_all.at[z, y, x, c]), (tok_hbm, tok), (ids_hbm, ids), (wg_hbm, wg), (dout_hbm, dout), (w1_hbm, w1), (w2_hbm, w2)])]
    for ld in loads:
        ld.start()
    peers = [dev(lax.rem(z + d, nz), y, x, c) for d in range(1, nz)]
    for d in (1, 2, 3):
        peers.append(dev(z, lax.rem(y + d, ny), x, c))
        peers.append(dev(z, y, lax.rem(x + d, nx), c))
    mate = dev(z, y, x, 1 - c)
    peers.append(mate)
    barrier = pltpu.get_barrier_semaphore()
    for peer in peers:
        pl.semaphore_signal(barrier, inc=1, device_id=peer, device_id_type=MESH)
    for ld in loads[2:5]:
        ld.wait()
    row[...] = choice_row(tok[...], ids[...], wg[...])
    place = pltpu.make_async_copy(row, m_land.at[z, y, x, c], keep_sem.at[0])
    place.start()
    loads[0].wait()
    loads[1].wait()
    place.wait()
    pl.semaphore_wait(barrier, len(peers))

    full = slice(None)
    by_distance = sorted(range(1, nz), key=lambda d: abs(d - nz // 2))

    def step(v, d, m=4):
        return lax.rem(v + d, m)

    def by_lines(link, ref, rows, x_last, late):
        p0, q0 = (y, x) if x_last else (x, y)
        low, high = pl.ds(0, nz // 2), pl.ds(nz // 2, nz // 2)

        def at(zs, p, q):
            return ref.at[(zs, p, q, c, rows) if x_last else (zs, q, p, c, rows)]

        def go(part, p, q, group):
            link.go(part, part, dev(z, p, q, c) if x_last else dev(z, q, p, c), group)

        in_z, in_p, in_m, in_f, in_r, in_c = [link.group() for _ in range(6)]
        line = at(full, p0, q0)

        def over(q):
            part = at(full, full, q)
            link.go(part, part, mate, in_c)

        own = at(z, p0, q0)
        for d in by_distance:
            link.go(own, own, dev(step(z, d, nz), y, x, c), in_z)
        yield
        link.wait(in_z, at(pl.ds(0, nz - 1), p0, q0))
        pm, pp, po = step(p0, 3), step(p0, 1), step(p0, 2)
        qm, qp, qo = step(q0, 3), step(q0, 1), step(q0, 2)
        qs = []

        def spread(p):
            part = at(full, p, q0)
            qs.append((p, link.group(), link.group()))
            go(part, p0, qp, qs[-1][1])
            go(part, p0, qm, qs[-1][2])

        def relay(i):
            p, up, dn = qs[i]
            link.wait(up, line)
            go(at(low, p, qm), p0, qp, in_r)
            link.wait(dn, line)
            go(at(high, p, qp), p0, qm, in_r)

        def pass_one():
            link.wait(in_p, line)
            go(at(low, pm, q0), pp, q0, in_f)
            link.wait(in_m, line)
            go(at(high, pp, q0), pm, q0, in_f)

        go(line, pp, q0, in_p)
        go(line, pm, q0, in_m)
        if late:
            yield
            pass_one()
            yield
            link.wait(in_f, line)
            for p in (p0, pm, pp, po):
                spread(p)
            over(q0)
            yield
            relay(0)
        else:
            yield
            spread(p0)
            yield
            pass_one()
            yield
            spread(pm)
            spread(pp)
            yield
            relay(0)
            yield
            link.wait(in_f, line)
            spread(po)
            over(q0)
        for i in range(1, 4):
            yield
            relay(i)
        over(qm)
        over(qp)
        yield
        link.wait(in_r, at(full, full, q0))
        over(qo)
        yield
        link.wait(in_c, ref.at[full, full, full, c, rows])

    def gather_rows(link, held, order):
        have = [z, y, x, c]
        for axis in order:
            size = (nz, ny, nx, nc)[axis]
            part = held.at[tuple(have)]
            group = link.group()
            for d in sorted(range(1, size), key=lambda d: abs(d - size // 2)):
                there = [z, y, x, c]
                there[axis] = lax.rem(there[axis] + d, size)
                link.go(part, part, dev(*there), group)
            have[axis] = pl.ds(0, size - 1)
            yield
            link.wait(group, held.at[tuple(have)])
            have[axis] = full

    def advance(plans):
        for g in plans:
            next(g, None)

    halves = [slice(0, 16), slice(16, 32)]
    tok_plans, grad_plans = [[by_lines(next(links), ref, half, half.start == 0, ref is g_all) for half in halves] for ref in (x_all, g_all)]
    row_plan = [gather_rows(next(links), m_land, range(4))]
    advance(row_plan + tok_plans + grad_plans)
    def flatten(land, flat):
        def lines(zz, carry):
            for k in range(ny * nx * nc):
                flat[pl.ds(zz * (ny * nx * nc) + k, 1), :] = land[zz, k // (nx * nc), k // nc % nx, k % nc]
            return carry

        lax.fori_loop(0, nz, lines, 0)


    me = lax.axis_index('ep').astype(F32)
    def read_rows():
        flatten(m_land, m_all)
        for ld in loads[5:]:
            ld.wait()
        code = m_all[...]
        left = jnp.where((iota(code.shape, 1) < 64) & (code >= 256.0), code - 256.0, 999.0)
        found = []
        for _ in range(3):
            best = jnp.min(jnp.min(left, axis=0, keepdims=True), axis=1, keepdims=True)
            left = jnp.where(left == best, 999.0, left)
            found.append(jnp.broadcast_to(best, (1, 128)))
        hot_ref[...] = jnp.concatenate(found + [jnp.full((5, 128), 999.0, F32)], axis=0)

    steps = 4 if nz == 8 else 1
    per = nz // steps
    n_quad = per * ny * nx * nc // 4
    n_pair = n_quad // 2
    n_slot = n_pair * 8 * CAP

    places = [(cc, xx, yy, zz) for cc in range(nc) for xx in range(nx) for yy in range(ny) for zz in range(per)]

    def select(i, ref, with_gate):
        c0, c1, g0, g1 = (pair_rows(token_lanes(m_all, k, pl.multiple_of(4 * n_quad * i, 4 * n_quad), n_quad)) for k in range(4))
        hit0, hit1 = plain_id(c0) == me, plain_id(c1) == me
        hit = (hit0 | hit1).astype(F32)
        gate = jnp.where(hit0, g0, 0.0) + jnp.where(hit1, g1, 0.0)
        before, after = iota((256, 256), 0), iota((256, 256), 1)
        tri = ((before < after) & (before // 32 == after // 32)).astype(F32).astype(BF16)
        rank = dot(hit.astype(BF16), tri, 1, 0)
        src = (iota((n_pair, 256), 1) // 32).astype(F32)
        key = jnp.where(hit > 0.0, src * CAP + rank, -1.0)
        slot = iota((8 * CAP, 256), 0).astype(F32)
        parts = []
        for p in range(n_pair):
            sel = (slot == key[p:p + 1]).astype(F32)
            v = dot(sel.astype(BF16), ref[i * per + p // ny, p % ny].reshape(256, 256), 1, 0)
            parts.append(v * jnp.sum(sel * gate[p:p + 1], axis=1, keepdims=True) if with_gate else v)
        return jnp.concatenate([parts[zz * ny + yy][CAP * (xx * nc + cc):CAP * (xx * nc + cc + 1)] for cc, xx, yy, zz in places], axis=0).astype(BF16)

    def put(i, v, to):
        for k, (cc, xx, yy, zz) in enumerate(places):
            for half in range(2):
                to[half][cc, xx, yy, i * per + zz] = v[CAP * k:CAP * (k + 1), 128 * half:128 * (half + 1)].astype(BF16)

    def forward(i):
        here = pl.ds(i * n_slot, n_slot)
        xs = select(i, x_all, False)
        a = dot(xs, w1[...], 1, 0)
        h = gelu(a).astype(BF16)
        xs_ref[here], h_ref[here], a_ref[here] = xs, h, a
        put(i, dot(h, w2[...], 1, 0), rows[:2])

    def backward(i):
        here = pl.ds(i * n_slot, n_slot)
        dys = select(i, g_all, True)
        dys_ref[here] = dys
        da_ref[here] = (dot(dys, w2[...], 1, 1) * gelu_slope(a_ref[here])).astype(BF16)

    def backward_rows(i):
        put(i, dot(da_ref[pl.ds(i * n_slot, n_slot)], w1[...], 1, 1), rows[2:])

    def back(i):
        h = rows[i]
        other, near, via, out2, via2, in2, out3, hot_land, cold_land = areas[9 * i:9 * i + 9]
        link = next(links)
        go = link.go
        in_c, in_e, in_h = [[link.group(), link.group()] for _ in range(3)]
        in_n, in_v, in_2, in_l, in_s = [link.group() for _ in range(5)]
        x_first = i % 2 == 0
        a, b = (x, y) if x_first else (y, x)

        def to(a, b):
            return dev(z, b, a, c) if x_first else dev(z, a, b, c)

        def index(lead, a, bs):
            return lead + ((a, bs) if x_first else (bs, a))

        up, dn, far = step(a, 1), step(a, 3), step(a, 2)
        lo, hi = pl.ds(0, 2), pl.ds(2, 2)
        parts = [pl.ds(0, nz // 2), pl.ds(nz // 2, nz // 2)]

        def start(k):
            zs = parts[k]
            go(h.at[1 - c, :, :, zs], other.at[:, :, zs], mate, in_c[k])
            spread(h, (c,), c, zs, in_e[k])

        def follow(k):
            link.wait(in_c[k], other.at[:, :, parts[k]])
            spread(other, (), 1 - c, parts[k], in_h[k])

        def spread(ref, lead, e, zs, group):
            go(ref.at[index(lead, far, lo) + (zs,)], via.at[0, e, :, zs], to(up, b), group)
            go(ref.at[index(lead, far, hi) + (zs,)], via.at[1, e, :, zs], to(dn, b), group)
            go(ref.at[index(lead, up, full) + (zs,)], near.at[a, e, :, zs], to(up, b), in_n)
            go(ref.at[index(lead, dn, full) + (zs,)], near.at[a, e, :, zs], to(dn, b), in_n)

        def relay(e, zs, group):
            link.wait(group, via.at[:, e, :, zs])
            go(via.at[0, e, :, zs], near.at[dn, e, lo, zs], to(up, b), in_n)
            go(via.at[1, e, :, zs], near.at[up, e, hi, zs], to(dn, b), in_n)

        start(0)
        yield
        follow(0)
        yield
        start(1)
        yield
        follow(1)
        yield
        relay(c, parts[0], in_e[0])
        relay(1 - c, parts[0], in_h[0])
        yield
        relay(c, parts[1], in_e[1])
        yield
        relay(1 - c, parts[1], in_h[1])
        yield
        link.wait(in_n, near.at[pl.ds(0, 3)])

        def expert(s, e):
            return ((z * ny + y) * nx + s) * nc + e if x_first else ((z * ny + s) * nx + x) * nc + e

        places = [(step(a, d), e) for d in range(4) for e in (c, 1 - c)]
        is_hot = [[(hot_ref[j:j + 1, :] == expert(s, e).astype(F32)).astype(F32) for s, e in places] for j in range(3)]
        wide = lambda v: jnp.broadcast_to(v, (8, 128))
        weight = [[wide(v).astype(BF16) for v in r] for r in is_hot]
        line = iota((8, 128), 0)
        mine = [(wide(is_hot[0][k] + is_hot[1][k] + is_hot[2][k]) < 0.5) & (line == s * nc + e) for k, (s, e) in enumerate(places)]

        def squeeze(bb, carry):
            given = [h[index((c,), a, bb)], other[index((), a, bb)]] + [near[s, e, bb] for s, e in places[2:]]
            for j in range(3):
                out2[bb, j] = sum(given[k] * weight[j][k] for k in range(8))
            singles = jnp.zeros((nz, 8, 128), F32)
            for k in range(8):
                singles = jnp.where(mine[k], jnp.sum(given[k].astype(F32), axis=1, keepdims=True), singles)
            out2[bb, 3] = singles.astype(BF16)
            return carry

        lax.fori_loop(0, 4, squeeze, 0)
        up, dn, far = step(b, 1), step(b, 3), step(b, 2)
        lo, hi = pl.ds(0, nz // 2), pl.ds(nz // 2, nz // 2)
        go(out2.at[far, :, lo], via2.at[0], to(a, up), in_v)
        go(out2.at[far, :, hi], via2.at[1], to(a, dn), in_v)
        go(out2.at[up], in2.at[b], to(a, up), in_2)
        go(out2.at[dn], in2.at[b], to(a, dn), in_2)
        in2[b] = out2[b]
        yield
        link.wait(in_v, via2)
        go(via2.at[0], in2.at[dn, :, lo], to(a, up), in_2)
        go(via2.at[1], in2.at[up, :, hi], to(a, dn), in_2)
        yield
        link.wait(in_2, in2.at[pl.ds(0, 3)])
        for j in range(3):
            out3[:, j] = (in2[0, j] + in2[1, j]) + (in2[2, j] + in2[3, j])
        for d in by_distance:
            zz = lax.rem(z + d, nz)
            go(in2.at[:, 3, zz], cold_land.at[z], dev(zz, y, x, c), in_s)
            go(out3.at[zz], hot_land.at[z], dev(zz, y, x, c), in_l)
        cold_land[z] = in2[:, 3, z]
        hot_land[z] = out3[z]
        yield
        link.wait(in_s, cold_land.at[pl.ds(0, nz - 1)])
        link.wait(in_l, hot_land.at[pl.ds(0, nz - 1)])

    def weight_grad(k):
        if k % 2 == 0:
            part = slice(w2.shape[0] // 4 * (k // 2), w2.shape[0] // 4 * (k // 2 + 1))
            g2_ref[part, :] = dot(h_ref[:, part], dys_ref[...], 0, 0)
            save(4, (part, full))
        else:
            part = slice(w1.shape[1] // 4 * (k // 2), w1.shape[1] // 4 * (k // 2 + 1))
            g1_ref[:, part] = dot(xs_ref[...], da_ref[:, part], 0, 0)
            save(3, (full, part))

    ys, dxs = [back(0), back(1)], [back(2), back(3)]
    n_tok = tok.shape[0]
    memo = {}
    earlier = iota((n_tok, n_tok), 1) < iota((n_tok, n_tok), 0)
    n_exp = wg.shape[1]

    def where_from(i, r0, r1):
        rank = jnp.sum(jnp.where(earlier & ((i == r0) | (i == r1)), 1.0, 0.0), axis=1, keepdims=True)
        slot = jnp.full((n_tok, 1), -1.0, F32)
        for j in range(3):
            slot = jnp.where(i == hot_ref[j:j + 1, 0:1], CAP * j + rank, slot)
        e = i.astype(jnp.int32)
        core, xx, yy, zz = e % nc, (e // nc) % nx, (e // (nc * nx)) % ny, e // (nc * nx * ny)
        lane, single = iota((n_tok, n_exp), 1), slot < 0.0
        pick = lambda m: m.astype(F32).astype(BF16)
        return pick(iota((n_tok, 32), 1).astype(F32) == slot), (pick((lane == e) & single), pick((lane == ((zz * nx + xx) * ny + yy) * nc + core) & single))

    def rows_of(kind, chosen):
        parts = []
        for half in range(2):
            hot_land, cold_land = areas[9 * (kind + half) + 7:9 * (kind + half) + 9]
            hot = jnp.sum(hot_land[...].astype(F32), axis=0).reshape(24, 128)
            hot = jnp.concatenate([hot, jnp.zeros((8, 128), F32)], axis=0).astype(BF16)
            cold = cold_land[...].astype(F32).reshape(n_exp, 128).astype(BF16)
            parts.append([dot(by_slot, hot, 1, 0) + dot(by_place[half], cold, 1, 0) for by_slot, by_place in chosen])
        return [jnp.concatenate([parts[0][k], parts[1][k]], axis=1) for k in range(2)]

    def combine():
        r0, r1 = ids[0:1].astype(F32), ids[1:2].astype(F32)
        i0, i1 = as_col(r0), as_col(r1)
        g0, g1 = gates(tok[...], i0, i1, wg[...])
        chosen = [where_from(i, r0, r1) for i in (i0, i1)]
        y0, y1 = rows_of(0, chosen)
        grad = dout[...].astype(F32)
        dg0, dg1 = (jnp.sum(grad * v, axis=1, keepdims=True) for v in (y0, y1))
        mean = g0 * dg0 + g1 * dg1
        d0, d1 = ((g * (dg - mean)).astype(BF16).astype(F32) for g, dg in ((g0, dg0), (g1, dg1)))
        d_row[...] = jnp.concatenate([as_row(d0), as_row(d1), jnp.zeros((1, 2 * n_tok), F32)], axis=1)
        place = pltpu.make_async_copy(d_row, d_land.at[z, y, x, c], keep_sem.at[1])
        place.start()
        out_ref[...] = (g0 * y0 + g1 * y1).astype(BF16)
        save(0)
        place.wait()
        d_plans.append(gather_rows(next(links), d_land, range(4)))
        advance(d_plans)
        expert = iota((n_tok, n_exp), 1).astype(F32)
        spread = jnp.where(expert == i0, d0, jnp.where(expert == i1, d1, 0.0)).astype(BF16)
        memo.update(chosen=chosen, through=dot(spread, wg[...], 1, 1))

    def finish():
        dx0, dx1 = rows_of(2, memo['chosen'])
        gx_ref[...] = (dx0 + dx1 + memo['through']).astype(BF16)
        save(1)

    n_dev = nz * ny * nx * nc

    def gate_grad():
        flatten(d_land, d_all)
        expert = iota((n_exp, 256), 0).astype(F32)
        codes = [plain_id(pair_rows(token_lanes(m_all, k, 0, n_dev // 4))) for k in range(2)]
        grads = [pair_rows(token_lanes(d_all, k, 0, n_dev // 4)) for k in range(2)]
        total = jnp.zeros((n_exp, x_all.shape[-1]), F32)
        zs = nz // 4 or 1
        for z0 in range(0, nz, zs):
            spread = []
            for p in range(z0 * ny, (z0 + zs) * ny):
                q = slice(p, p + 1)
                spread.append(jnp.where(expert == codes[0][q], grads[0][q], jnp.where(expert == codes[1][q], grads[1][q], 0.0)).astype(BF16))
            total += dot(jnp.concatenate(spread, axis=1), x_all[z0:z0 + zs].reshape(zs * ny * 256, x_all.shape[-1]), 1, 0)
        gate_ref[...] = total.T
        save(2)

    d_plans = []
    moves = {'t': tok_plans, 'g': grad_plans, 'm': row_plan, 'y': ys, 'x': dxs, 'd': d_plans}
    works = {'f': [functools.partial(forward, i) for i in range(steps)], 'b': [functools.partial(backward, i) for i in range(steps)],
             'B': [functools.partial(backward_rows, i) for i in range(steps)], 'w': [functools.partial(weight_grad, k) for k in range(8)],
             'h': [read_rows], 'c': [combine], 'k': [gate_grad], 'e': [finish]}
    for turn in SCHEDULE:
        if turn in moves:
            advance(moves[turn])
        elif works[turn]:
            works[turn].pop(0)()
    for link in all_links:
        link.finish(pad, pad_row)
    for cp in saves:
        cp.wait()


def block_call(dims, tokens, grad_out, ids, w_gate, w1, w2):
    nz, ny, nx, nc = dims
    d_model, d_hidden = w1.shape
    n_tok = tokens.shape[0]
    n_dev = nz * ny * nx * nc
    n_row = n_dev * CAP
    tile = (CAP, 128)
    hbm = pl.BlockSpec(memory_space=pltpu.HBM)
    out = jax.ShapeDtypeStruct
    work = [(4, 4, nz), (4, 2, 4, nz), (2, 2, 2, nz), (4, 4, nz), (2, 4, nz // 2), (4, 4, nz), (nz, 3), (nz, 3), (nz, 4)]
    n_group = 4 * 14 + 4 + 4 * 11 + 4
    sems = [pltpu.SemaphoreType.DMA((10,)), pltpu.SemaphoreType.DMA((n_group,))]
    results = [(tokens.shape, BF16), (tokens.shape, BF16), ((d_model, n_dev), F32), ((d_model, d_hidden), F32), ((d_hidden, d_model), F32)]
    row = (1, 128)
    kept = [(tokens.shape, BF16), (tokens.shape, BF16), (ids.shape, jnp.int32), (w_gate.shape, BF16), (w1.shape, BF16), (w2.shape, BF16), (row, F32), (dims + row, F32),
            (dims + tokens.shape, BF16), (dims + tokens.shape, BF16), ((n_row, d_model), BF16), ((n_row, d_model), BF16), ((n_row, d_hidden), BF16), ((n_row, d_hidden), BF16), ((n_row, d_hidden), F32), ((n_dev, 128), F32), (tile, F32), (row, F32),
            (dims + row, F32), ((n_dev, 128), F32), ((1024,) + tile, BF16), ((n_dev,) + row, F32)]
    return pl.pallas_call(
        functools.partial(block_kernel, dims, (6, len(results), len(results), len(kept), 4, 4 * len(work), 3, len(sems))),
        out_shape=[out(*r) for r in results],
        in_specs=[hbm] * 6,
        out_specs=[hbm] * len(results),
        scratch_shapes=[pltpu.VMEM(*r) for r in results + kept] + [pltpu.VMEM((nc, nx, ny, nz) + tile, BF16)] * 4 + [pltpu.VMEM(w + tile, BF16) for w in work] * 4
        + [pltpu.SemaphoreType.DMA((k,)) for k in (8, 2, 11)] + sems,
        compiler_params=pltpu.CompilerParams(collective_id=0, has_side_effects=True, vmem_limit_bytes=VMEM_LIMIT),
        name='block',
    )(tokens, grad_out, ids, w_gate, w1, w2)


VMEM_LIMIT = 67043328
SCHEDULE = 'mttmttmgttgtttgtmth' + 'fgfgyfgyfgy' + 'gygy' + 'bybybyBBxbyxBBxy' + 'wwxxwxwwxyc' + 'xwwdxdxwddkxe'


def pass_kernel(n, *refs):
    refs = iter(refs)
    given, passed, held, (load_sem, save_sem) = [list(itertools.islice(refs, k)) for k in (n, n, n, 2)]
    loads = [pltpu.make_async_copy(given[k], held[k], load_sem.at[k]) for k in range(n)]
    saves = [pltpu.make_async_copy(held[k], passed[k], save_sem.at[k]) for k in range(n)]
    for cp in loads:
        cp.start()
    for load, save in zip(loads, saves):
        load.wait()
        save.start()
    for cp in saves:
        cp.wait()


def pass_on(*arrays):
    n = len(arrays)
    return pl.pallas_call(
        functools.partial(pass_kernel, n),
        out_shape=[jax.ShapeDtypeStruct(v.shape, v.dtype) for v in arrays],
        in_specs=[pl.BlockSpec(memory_space=pltpu.HBM)] * n,
        out_specs=[pl.BlockSpec(memory_space=pltpu.HBM)] * n,
        scratch_shapes=[pltpu.VMEM(v.shape, v.dtype) for v in arrays] + [pltpu.SemaphoreType.DMA((n,))] * 2,
        compiler_params=pltpu.CompilerParams(vmem_limit_bytes=VMEM_LIMIT),
        name='pass_on',
    )(*arrays)


def local_block(dims, tokens, grad_out, expert_ids, w_gate, w_in, w_out):
    y_out, grad_x, grad_w_gate, g1, g2 = pass_on(*block_call(dims, tokens, grad_out, expert_ids.T, w_gate, w_in[0], w_out[0]))
    return y_out, grad_x, g1[None], g2[None], grad_w_gate


def solution(mesh):
    dims = (8, 4, 4, 2)
    return jax.shard_map(functools.partial(local_block, dims), mesh=mesh, in_specs=(P('ep'), P('ep'), P('ep'), P(), P('ep'), P('ep')), out_specs=(P('ep'), P('ep'), P('ep'), P('ep'), P()), check_vma=False)
```

```python
import functools
import itertools
import math

import jax
import jax.numpy as jnp
from jax import lax
from jax.experimental import pallas as pl
from jax.experimental.pallas import tpu as pltpu
from jax.sharding import PartitionSpec as P

MESH = pl.DeviceIdType.MESH
F32 = jnp.float32
BF16 = jnp.bfloat16
CAP = 8


def coords(dims):
    nz, ny, nx, nc = dims
    me = lax.axis_index('ep')
    c = lax.rem(me, nc)
    x = lax.rem(me // nc, nx)
    y = lax.rem(me // (nc * nx), ny)
    z = me // (nc * nx * ny)

    def dev(z, y, x, c):
        return (((z * ny + y) * nx + x) * nc + c,)

    return z, y, x, c, dev


def dot(a, b, ca, cb):
    return lax.dot_general(a, b, (((ca,), (cb,)), ((), ())), preferred_element_type=F32)


def iota(shape, axis):
    return lax.broadcasted_iota(jnp.int32, shape, axis)


def as_row(col):
    n = col.shape[0]
    return jnp.sum(jnp.where(iota((n, n), 0) == iota((n, n), 1), col, 0.0), axis=0, keepdims=True)


def as_col(row):
    n = row.shape[1]
    return jnp.sum(jnp.where(iota((n, n), 0) == iota((n, n), 1), row, 0.0), axis=1, keepdims=True)


def gates(tok, i0, i1, w_gate):
    logits = dot(tok, w_gate, 1, 0)
    expert = iota(logits.shape, 1).astype(F32)
    l0, l1 = (jnp.sum(jnp.where(expert == i, logits, 0.0), axis=1, keepdims=True) for i in (i0, i1))
    top = jnp.maximum(l0, l1)
    p0, p1 = jnp.exp(l0 - top), jnp.exp(l1 - top)
    total = p0 + p1
    return p0 / total, p1 / total


def choice_row(tok, ids, w_gate):
    r0, r1 = ids[0:1].astype(F32), ids[1:2].astype(F32)
    i0, i1 = as_col(r0), as_col(r1)
    g0, g1 = gates(tok, i0, i1, w_gate)

    def code(i):
        n = jnp.sum((i == r0).astype(F32) + (i == r1).astype(F32), axis=1, keepdims=True)
        return as_row(jnp.where(n > 1.5, i + 256.0, i))

    return jnp.concatenate([code(i0), code(i1), as_row(g0), as_row(g1)], axis=1)


def gelu_tanh(a):
    k = 0.7978845608028654
    sq = a * a
    return jnp.tanh(a * (k + (k * 0.044715) * sq)), sq


def gelu(a):
    half = 0.5 * a
    return half + half * gelu_tanh(a)[0]


def gelu_slope(a):
    k = 0.7978845608028654
    t, sq = gelu_tanh(a)
    return (0.5 + 0.5 * t) + (0.5 * a) * (1.0 - t * t) * (k + (3 * k * 0.044715) * sq)


def token_lanes(ref, k, start, n):
    lane = iota((n, 128), 1) // 32
    out = jnp.zeros((n, 128), F32)
    for j in range(4):
        r = ref[pl.ds(start + j, n, stride=4), :]
        out = jnp.where(lane == j, r if j == k else pltpu.roll(r, 32 * (j - k) % 128, 1), out)
    return out


def pair_rows(v):
    return jnp.concatenate([jnp.concatenate([v[2 * i:2 * i + 1], v[2 * i + 1:2 * i + 2]], axis=1) for i in range(v.shape[0] // 2)], axis=0)


def plain_id(code):
    return jnp.where(code >= 256.0, code - 256.0, code)


class Links:
    def __init__(self, send, recv, pool):
        self.send, self.recv, self.pool, self.bytes = send, recv, pool, 0

    def group(self):
        return self.recv.at[next(self.pool)]

    def go(self, src, dst, to, group):
        pltpu.make_async_remote_copy(src_ref=src, dst_ref=dst, send_sem=self.send, recv_sem=group, device_id=to, device_id_type=MESH).start()
        self.bytes += math.prod(src.shape) * jnp.dtype(src.dtype).itemsize

    def wait(self, group, ref):
        pltpu.make_async_copy(ref, ref, group).wait()

    def finish(self, *pads):
        for pad in pads:
            unit = math.prod(pad.shape[1:]) * jnp.dtype(pad.dtype).itemsize
            if self.bytes % unit == 0:
                return self.wait(self.send, pad.at[pl.ds(0, self.bytes // unit)])
        raise ValueError(self.bytes)


def block_kernel(dims, sizes, *refs):
    nz, ny, nx, nc = dims
    refs = iter(refs)
    refs = [list(itertools.islice(refs, n)) for n in sizes]
    (tok_hbm, dout_hbm, ids_hbm, wg_hbm, w1_hbm, w2_hbm), outs, held, kept, rows, areas, (load_sem, keep_sem, save_sem), sems = refs
    out_ref, gx_ref, gate_ref, g1_ref, g2_ref = held
    tok, dout, ids, wg, w1, w2, row, m_land, x_all, g_all, xs_ref, dys_ref, h_ref, da_ref, a_ref, m_all, hot_ref, d_row, d_land, d_all, pad, pad_row = kept
    z, y, x, c, dev = coords(dims)
    saves = [pltpu.make_async_copy(held[k], outs[k], save_sem.at[k]) for k in range(len(held))]

    def save(k, part):
        pltpu.make_async_copy(held[k].at[part], outs[k].at[part], save_sem.at[k]).start()

    send_sem, recv_sem = sems
    pool = itertools.count()
    all_links = [Links(send_sem.at[k], recv_sem, pool) for k in range(send_sem.shape[0])]
    links = iter(all_links)

    loads = [pltpu.make_async_copy(s, d, load_sem.at[k]) for k, (s, d) in enumerate(
        [(tok_hbm, x_all.at[z, y, x, c]), (dout_hbm, g_all.at[z, y, x, c]), (tok_hbm, tok), (ids_hbm, ids), (wg_hbm, wg), (dout_hbm, dout), (w1_hbm, w1), (w2_hbm, w2)])]
    for ld in loads:
        ld.start()
    peers = [dev(lax.rem(z + d, nz), y, x, c) for d in range(1, nz)]
    for d in (1, 2, 3):
        peers.append(dev(z, lax.rem(y + d, ny), x, c))
        peers.append(dev(z, y, lax.rem(x + d, nx), c))
    mate = dev(z, y, x, 1 - c)
    peers.append(mate)
    barrier = pltpu.get_barrier_semaphore()
    for peer in peers:
        pl.semaphore_signal(barrier, inc=1, device_id=peer, device_id_type=MESH)
    for ld in loads[2:5]:
        ld.wait()
    row[...] = choice_row(tok[...], ids[...], wg[...])
    place = pltpu.make_async_copy(row, m_land.at[z, y, x, c], keep_sem.at[0])
    place.start()
    loads[0].wait()
    loads[1].wait()
    place.wait()
    pl.semaphore_wait(barrier, len(peers))

    full = slice(None)
    by_distance = sorted(range(1, nz), key=lambda d: abs(d - nz // 2))

    def step(v, d, m=4):
        return lax.rem(v + d, m)

    def by_lines(link, ref, rows, x_last, late):
        p0, q0 = (y, x) if x_last else (x, y)
        low, high = pl.ds(0, nz // 2), pl.ds(nz // 2, nz // 2)

        def at(zs, p, q):
            return ref.at[(zs, p, q, c, rows) if x_last else (zs, q, p, c, rows)]

        def go(part, p, q, group):
            link.go(part, part, dev(z, p, q, c) if x_last else dev(z, q, p, c), group)

        in_z, in_p, in_m, in_f, in_r, in_c = [link.group() for _ in range(6)]
        line = at(full, p0, q0)

        def over(q):
            part = at(full, full, q)
            link.go(part, part, mate, in_c)

        own = at(z, p0, q0)
        for d in by_distance:
            link.go(own, own, dev(step(z, d, nz), y, x, c), in_z)
        yield
        link.wait(in_z, at(pl.ds(0, nz - 1), p0, q0))
        pm, pp, po = step(p0, 3), step(p0, 1), step(p0, 2)
        qm, qp, qo = step(q0, 3), step(q0, 1), step(q0, 2)
        qs = []

        def spread(p):
            part = at(full, p, q0)
            qs.append((p, link.group()))
            go(part, p0, qp, qs[-1][1])
            go(part, p0, qm, qs[-1][1])

        def relay(i):
            p, group = qs[i]
            link.wait(group, at(full, pl.ds(0, 2), q0))
            go(at(low, p, qm), p0, qp, in_r)
            go(at(high, p, qp), p0, qm, in_r)

        def pass_one():
            link.wait(in_p, line)
            go(at(low, pm, q0), pp, q0, in_f)
            link.wait(in_m, line)
            go(at(high, pp, q0), pm, q0, in_f)

        go(line, pp, q0, in_p)
        go(line, pm, q0, in_m)
        if late:
            yield
            pass_one()
            yield
            link.wait(in_f, line)
            for p in (p0, pm, pp, po):
                spread(p)
            over(q0)
            yield
            relay(0)
        else:
            yield
            spread(p0)
            yield
            pass_one()
            yield
            spread(pm)
            spread(pp)
            yield
            relay(0)
            yield
            link.wait(in_f, line)
            spread(po)
            over(q0)
        for i in range(1, 4):
            yield
            relay(i)
        over(qm)
        over(qp)
        yield
        link.wait(in_r, at(full, full, q0))
        over(qo)
        yield
        link.wait(in_c, ref.at[full, full, full, c, rows])

    def gather_rows(link, held, order):
        have = [z, y, x, c]
        for axis in order:
            size = (nz, ny, nx, nc)[axis]
            part = held.at[tuple(have)]
            group = link.group()
            for d in sorted(range(1, size), key=lambda d: abs(d - size // 2)):
                there = [z, y, x, c]
                there[axis] = lax.rem(there[axis] + d, size)
                link.go(part, part, dev(*there), group)
            have[axis] = pl.ds(0, size - 1)
            yield
            link.wait(group, held.at[tuple(have)])
            have[axis] = full

    def advance(plans):
        for g in plans:
            next(g, None)

    halves = [slice(0, 16), slice(16, 32)]
    tok_plans, grad_plans = [[by_lines(next(links), ref, half, half.start == 0, ref is g_all) for half in halves] for ref in (x_all, g_all)]
    row_plan = [gather_rows(next(links), m_land, range(4))]
    advance(row_plan + tok_plans + grad_plans)
    def flatten(land, flat):
        def lines(zz, carry):
            for k in range(ny * nx * nc):
                flat[pl.ds(zz * (ny * nx * nc) + k, 1), :] = land[zz, k // (nx * nc), k // nc % nx, k % nc]
            return carry

        lax.fori_loop(0, nz, lines, 0)


    me = lax.axis_index('ep').astype(F32)
    def read_rows():
        flatten(m_land, m_all)
        for ld in loads[5:]:
            ld.wait()
        code = m_all[...]
        left = jnp.where((iota(code.shape, 1) < 64) & (code >= 256.0), code - 256.0, 999.0)
        found = []
        for _ in range(3):
            best = jnp.min(jnp.min(left, axis=0, keepdims=True), axis=1, keepdims=True)
            left = jnp.where(left == best, 999.0, left)
            found.append(jnp.broadcast_to(best, (1, 128)))
        hot_ref[...] = jnp.concatenate(found + [jnp.full((5, 128), 999.0, F32)], axis=0)

    steps = 4 if nz == 8 else 1
    per = nz // steps
    n_quad = per * ny * nx * nc // 4
    n_pair = n_quad // 2
    n_slot = n_pair * 8 * CAP

    places = [(cc, xx, yy, zz) for cc in range(nc) for xx in range(nx) for yy in range(ny) for zz in range(per)]

    def select(i, ref, with_gate):
        c0, c1, g0, g1 = (pair_rows(token_lanes(m_all, k, pl.multiple_of(4 * n_quad * i, 4 * n_quad), n_quad)) for k in range(4))
        hit0, hit1 = plain_id(c0) == me, plain_id(c1) == me
        hit = (hit0 | hit1).astype(F32)
        gate = jnp.where(hit0, g0, 0.0) + jnp.where(hit1, g1, 0.0)
        before, after = iota((256, 256), 0), iota((256, 256), 1)
        tri = ((before < after) & (before // 32 == after // 32)).astype(F32).astype(BF16)
        rank = dot(hit.astype(BF16), tri, 1, 0)
        src = (iota((n_pair, 256), 1) // 32).astype(F32)
        key = jnp.where(hit > 0.0, src * CAP + rank, -1.0)
        slot = iota((8 * CAP, 256), 0).astype(F32)
        parts = []
        for p in range(n_pair):
            sel = (slot == key[p:p + 1]).astype(F32)
            v = dot(sel.astype(BF16), ref[i * per + p // ny, p % ny].reshape(256, 256), 1, 0)
            parts.append(v * jnp.sum(sel * gate[p:p + 1], axis=1, keepdims=True) if with_gate else v)
        return jnp.concatenate([parts[zz * ny + yy][CAP * (xx * nc + cc):CAP * (xx * nc + cc + 1)] for cc, xx, yy, zz in places], axis=0).astype(BF16)

    def put(i, v, to):
        for k, (cc, xx, yy, zz) in enumerate(places):
            for half in range(2):
                to[half][cc, xx, yy, i * per + zz] = v[CAP * k:CAP * (k + 1), 128 * half:128 * (half + 1)].astype(BF16)

    def forward(i):
        here = pl.ds(i * n_slot, n_slot)
        xs = select(i, x_all, False)
        a = dot(xs, w1[...], 1, 0)
        h = gelu(a).astype(BF16)
        xs_ref[here], h_ref[here], a_ref[here] = xs, h, a
        put(i, dot(h, w2[...], 1, 0), rows[:2])

    def backward(i):
        here = pl.ds(i * n_slot, n_slot)
        dys = select(i, g_all, True)
        dys_ref[here] = dys
        da_ref[here] = (dot(dys, w2[...], 1, 1) * gelu_slope(a_ref[here])).astype(BF16)

    def backward_rows(i):
        put(i, dot(da_ref[pl.ds(i * n_slot, n_slot)], w1[...], 1, 1), rows[2:])

    def back(i):
        h = rows[i]
        other, near, via, out2, via2, in2, out3, hot_land, cold_land = areas[9 * i:9 * i + 9]
        link = next(links)
        go = link.go
        in_c, in_e, in_h = [[link.group(), link.group()] for _ in range(3)]
        in_n, in_v, in_2, in_l, in_s = [link.group() for _ in range(5)]
        x_first = i % 2 == 0
        a, b = (x, y) if x_first else (y, x)

        def to(a, b):
            return dev(z, b, a, c) if x_first else dev(z, a, b, c)

        def index(lead, a, bs):
            return lead + ((a, bs) if x_first else (bs, a))

        up, dn, far = step(a, 1), step(a, 3), step(a, 2)
        lo, hi = pl.ds(0, 2), pl.ds(2, 2)
        parts = [pl.ds(0, nz // 2), pl.ds(nz // 2, nz // 2)]

        def start(k):
            zs = parts[k]
            go(h.at[1 - c, :, :, zs], other.at[:, :, zs], mate, in_c[k])
            spread(h, (c,), c, zs, in_e[k])

        def follow(k):
            link.wait(in_c[k], other.at[:, :, parts[k]])
            spread(other, (), 1 - c, parts[k], in_h[k])

        def spread(ref, lead, e, zs, group):
            go(ref.at[index(lead, far, lo) + (zs,)], via.at[0, e, :, zs], to(up, b), group)
            go(ref.at[index(lead, far, hi) + (zs,)], via.at[1, e, :, zs], to(dn, b), group)
            go(ref.at[index(lead, up, full) + (zs,)], near.at[a, e, :, zs], to(up, b), in_n)
            go(ref.at[index(lead, dn, full) + (zs,)], near.at[a, e, :, zs], to(dn, b), in_n)

        def relay(e, zs, group):
            link.wait(group, via.at[:, e, :, zs])
            go(via.at[0, e, :, zs], near.at[dn, e, lo, zs], to(up, b), in_n)
            go(via.at[1, e, :, zs], near.at[up, e, hi, zs], to(dn, b), in_n)

        start(0)
        yield
        follow(0)
        yield
        start(1)
        yield
        follow(1)
        yield
        relay(c, parts[0], in_e[0])
        relay(1 - c, parts[0], in_h[0])
        yield
        relay(c, parts[1], in_e[1])
        yield
        relay(1 - c, parts[1], in_h[1])
        yield
        link.wait(in_n, near.at[pl.ds(0, 3)])

        def expert(s, e):
            return ((z * ny + y) * nx + s) * nc + e if x_first else ((z * ny + s) * nx + x) * nc + e

        places = [(step(a, d), e) for d in range(4) for e in (c, 1 - c)]
        is_hot = [[(hot_ref[j:j + 1, :] == expert(s, e).astype(F32)).astype(F32) for s, e in places] for j in range(3)]
        wide = lambda v: jnp.broadcast_to(v, (8, 128))
        weight = [[wide(v).astype(BF16) for v in r] for r in is_hot]
        line = iota((8, 128), 0)
        mine = [(wide(is_hot[0][k] + is_hot[1][k] + is_hot[2][k]) < 0.5) & (line == s * nc + e) for k, (s, e) in enumerate(places)]

        def squeeze(bb, carry):
            given = [h[index((c,), a, bb)], other[index((), a, bb)]] + [near[s, e, bb] for s, e in places[2:]]
            for j in range(3):
                out2[bb, j] = sum(given[k] * weight[j][k] for k in range(8))
            singles = jnp.zeros((nz, 8, 128), F32)
            for k in range(8):
                singles = jnp.where(mine[k], jnp.sum(given[k].astype(F32), axis=1, keepdims=True), singles)
            out2[bb, 3] = singles.astype(BF16)
            return carry

        lax.fori_loop(0, 4, squeeze, 0)
        up, dn, far = step(b, 1), step(b, 3), step(b, 2)
        lo, hi = pl.ds(0, nz // 2), pl.ds(nz // 2, nz // 2)
        go(out2.at[far, :, lo], via2.at[0], to(a, up), in_v)
        go(out2.at[far, :, hi], via2.at[1], to(a, dn), in_v)
        go(out2.at[up], in2.at[b], to(a, up), in_2)
        go(out2.at[dn], in2.at[b], to(a, dn), in_2)
        in2[b] = out2[b]
        yield
        link.wait(in_v, via2)
        go(via2.at[0], in2.at[dn, :, lo], to(a, up), in_2)
        go(via2.at[1], in2.at[up, :, hi], to(a, dn), in_2)
        yield
        link.wait(in_2, in2.at[pl.ds(0, 3)])
        for j in range(3):
            out3[:, j] = (in2[0, j] + in2[1, j]) + (in2[2, j] + in2[3, j])
        for d in by_distance:
            zz = lax.rem(z + d, nz)
            go(in2.at[:, 3, zz], cold_land.at[z], dev(zz, y, x, c), in_s)
            go(out3.at[zz], hot_land.at[z], dev(zz, y, x, c), in_l)
        cold_land[z] = in2[:, 3, z]
        hot_land[z] = out3[z]
        yield
        link.wait(in_s, cold_land.at[pl.ds(0, nz - 1)])
        link.wait(in_l, hot_land.at[pl.ds(0, nz - 1)])

    def weight_grad(k):
        if k % 2 == 0:
            part = slice(w2.shape[0] // 4 * (k // 2), w2.shape[0] // 4 * (k // 2 + 1))
            g2_ref[part, :] = dot(h_ref[:, part], dys_ref[...], 0, 0)
            save(4, (part, full))
        else:
            part = slice(w1.shape[1] // 4 * (k // 2), w1.shape[1] // 4 * (k // 2 + 1))
            g1_ref[:, part] = dot(xs_ref[...], da_ref[:, part], 0, 0)
            save(3, (full, part))

    ys, dxs = [back(0), back(1)], [back(2), back(3)]
    n_tok = tok.shape[0]
    memo = {}
    earlier = iota((n_tok, n_tok), 1) < iota((n_tok, n_tok), 0)
    n_exp = wg.shape[1]

    def where_from(i, r0, r1):
        rank = jnp.sum(jnp.where(earlier & ((i == r0) | (i == r1)), 1.0, 0.0), axis=1, keepdims=True)
        slot = jnp.full((n_tok, 1), -1.0, F32)
        for j in range(3):
            slot = jnp.where(i == hot_ref[j:j + 1, 0:1], CAP * j + rank, slot)
        e = i.astype(jnp.int32)
        core, xx, yy, zz = e % nc, (e // nc) % nx, (e // (nc * nx)) % ny, e // (nc * nx * ny)
        lane, single = iota((n_tok, n_exp), 1), slot < 0.0
        pick = lambda m: m.astype(F32).astype(BF16)
        return pick(iota((n_tok, 32), 1).astype(F32) == slot), (pick((lane == e) & single), pick((lane == ((zz * nx + xx) * ny + yy) * nc + core) & single))

    def rows_of(kind, chosen):
        parts = []
        for half in range(2):
            hot_land, cold_land = areas[9 * (kind + half) + 7:9 * (kind + half) + 9]
            hot = jnp.sum(hot_land[...].astype(F32), axis=0).reshape(24, 128)
            hot = jnp.concatenate([hot, jnp.zeros((8, 128), F32)], axis=0).astype(BF16)
            cold = cold_land[...].astype(F32).reshape(n_exp, 128).astype(BF16)
            parts.append([dot(by_slot, hot, 1, 0) + dot(by_place[half], cold, 1, 0) for by_slot, by_place in chosen])
        return [jnp.concatenate([parts[0][k], parts[1][k]], axis=1) for k in range(2)]

    def combine():
        r0, r1 = ids[0:1].astype(F32), ids[1:2].astype(F32)
        i0, i1 = as_col(r0), as_col(r1)
        g0, g1 = gates(tok[...], i0, i1, wg[...])
        chosen = [where_from(i, r0, r1) for i in (i0, i1)]
        y0, y1 = rows_of(0, chosen)
        grad = dout[...].astype(F32)
        dg0, dg1 = (jnp.sum(grad * v, axis=1, keepdims=True) for v in (y0, y1))
        mean = g0 * dg0 + g1 * dg1
        d0, d1 = ((g * (dg - mean)).astype(BF16).astype(F32) for g, dg in ((g0, dg0), (g1, dg1)))
        d_row[...] = jnp.concatenate([as_row(d0), as_row(d1), jnp.zeros((1, 2 * n_tok), F32)], axis=1)
        place = pltpu.make_async_copy(d_row, d_land.at[z, y, x, c], keep_sem.at[1])
        place.start()
        out_ref[...] = (g0 * y0 + g1 * y1).astype(BF16)
        saves[0].start()
        place.wait()
        d_plans.append(gather_rows(next(links), d_land, range(4)))
        advance(d_plans)
        expert = iota((n_tok, n_exp), 1).astype(F32)
        spread = jnp.where(expert == i0, d0, jnp.where(expert == i1, d1, 0.0)).astype(BF16)
        memo.update(chosen=chosen, through=dot(spread, wg[...], 1, 1))

    def finish():
        dx0, dx1 = rows_of(2, memo['chosen'])
        gx_ref[...] = (dx0 + dx1 + memo['through']).astype(BF16)
        saves[1].start()

    n_dev = nz * ny * nx * nc

    def gate_grad():
        flatten(d_land, d_all)
        expert = iota((n_exp, 256), 0).astype(F32)
        codes = [plain_id(pair_rows(token_lanes(m_all, k, 0, n_dev // 4))) for k in range(2)]
        grads = [pair_rows(token_lanes(d_all, k, 0, n_dev // 4)) for k in range(2)]
        total = jnp.zeros((n_exp, x_all.shape[-1]), F32)
        zs = nz // 4 or 1
        for z0 in range(0, nz, zs):
            spread = []
            for p in range(z0 * ny, (z0 + zs) * ny):
                q = slice(p, p + 1)
                spread.append(jnp.where(expert == codes[0][q], grads[0][q], jnp.where(expert == codes[1][q], grads[1][q], 0.0)).astype(BF16))
            total += dot(jnp.concatenate(spread, axis=1), x_all[z0:z0 + zs].reshape(zs * ny * 256, x_all.shape[-1]), 1, 0)
        gate_ref[...] = total.T
        saves[2].start()

    d_plans = []
    moves = {'t': tok_plans, 'g': grad_plans, 'm': row_plan, 'y': ys, 'x': dxs, 'd': d_plans}
    works = {'f': [functools.partial(forward, i) for i in range(steps)], 'b': [functools.partial(backward, i) for i in range(steps)],
             'B': [functools.partial(backward_rows, i) for i in range(steps)], 'w': [functools.partial(weight_grad, k) for k in range(8)],
             'h': [read_rows], 'c': [combine], 'k': [gate_grad], 'e': [finish]}
    for turn in SCHEDULE:
        if turn in moves:
            advance(moves[turn])
        elif works[turn]:
            works[turn].pop(0)()
    for link in all_links:
        link.finish(pad, pad_row)
    for cp in saves:
        cp.wait()


def block_call(dims, tokens, grad_out, ids, w_gate, w1, w2):
    nz, ny, nx, nc = dims
    d_model, d_hidden = w1.shape
    n_tok = tokens.shape[0]
    n_dev = nz * ny * nx * nc
    n_row = n_dev * CAP
    tile = (CAP, 128)
    hbm = pl.BlockSpec(memory_space=pltpu.HBM)
    out = jax.ShapeDtypeStruct
    work = [(4, 4, nz), (4, 2, 4, nz), (2, 2, 2, nz), (4, 4, nz), (2, 4, nz // 2), (4, 4, nz), (nz, 3), (nz, 3), (nz, 4)]
    n_group = 4 * 10 + 4 + 4 * 11 + 4
    sems = [pltpu.SemaphoreType.DMA((10,)), pltpu.SemaphoreType.DMA((n_group,))]
    results = [(tokens.shape, BF16), (tokens.shape, BF16), ((d_model, n_dev), F32), ((d_model, d_hidden), F32), ((d_hidden, d_model), F32)]
    row = (1, 128)
    kept = [(tokens.shape, BF16), (tokens.shape, BF16), (ids.shape, jnp.int32), (w_gate.shape, BF16), (w1.shape, BF16), (w2.shape, BF16), (row, F32), (dims + row, F32),
            (dims + tokens.shape, BF16), (dims + tokens.shape, BF16), ((n_row, d_model), BF16), ((n_row, d_model), BF16), ((n_row, d_hidden), BF16), ((n_row, d_hidden), BF16), ((n_row, d_hidden), F32), ((n_dev, 128), F32), (tile, F32), (row, F32),
            (dims + row, F32), ((n_dev, 128), F32), ((1024,) + tile, BF16), ((n_dev,) + row, F32)]
    return pl.pallas_call(
        functools.partial(block_kernel, dims, (6, len(results), len(results), len(kept), 4, 4 * len(work), 3, len(sems))),
        out_shape=[out(*r) for r in results],
        in_specs=[hbm] * 6,
        out_specs=[hbm] * len(results),
        scratch_shapes=[pltpu.VMEM(*r) for r in results + kept] + [pltpu.VMEM((nc, nx, ny, nz) + tile, BF16)] * 4 + [pltpu.VMEM(w + tile, BF16) for w in work] * 4
        + [pltpu.SemaphoreType.DMA((k,)) for k in (8, 2, len(results))] + sems,
        compiler_params=pltpu.CompilerParams(collective_id=0, has_side_effects=True, vmem_limit_bytes=VMEM_LIMIT),
        name='block',
    )(tokens, grad_out, ids, w_gate, w1, w2)


VMEM_LIMIT = 67043328
SCHEDULE = 'mttmttmgttttgttgmth' + 'fggfgyfgyfy' + 'gygy' + 'bybybyBBxbyxBBxy' + 'wwxxwxwwxyc' + 'xwwdxdxwddkxe'


def pass_kernel(n, *refs):
    refs = iter(refs)
    given, passed, held, (load_sem, save_sem) = [list(itertools.islice(refs, k)) for k in (n, n, n, 2)]
    loads = [pltpu.make_async_copy(given[k], held[k], load_sem.at[k]) for k in range(n)]
    saves = [pltpu.make_async_copy(held[k], passed[k], save_sem.at[k]) for k in range(n)]
    for cp in loads:
        cp.start()
    for load, save in zip(loads, saves):
        load.wait()
        save.start()
    for cp in saves:
        cp.wait()


def pass_on(*arrays):
    n = len(arrays)
    return pl.pallas_call(
        functools.partial(pass_kernel, n),
        out_shape=[jax.ShapeDtypeStruct(v.shape, v.dtype) for v in arrays],
        in_specs=[pl.BlockSpec(memory_space=pltpu.HBM)] * n,
        out_specs=[pl.BlockSpec(memory_space=pltpu.HBM)] * n,
        scratch_shapes=[pltpu.VMEM(v.shape, v.dtype) for v in arrays] + [pltpu.SemaphoreType.DMA((n,))] * 2,
        compiler_params=pltpu.CompilerParams(vmem_limit_bytes=VMEM_LIMIT),
        name='pass_on',
    )(*arrays)


def local_block(dims, tokens, grad_out, expert_ids, w_gate, w_in, w_out):
    y_out, grad_x, grad_w_gate, g1, g2 = pass_on(*block_call(dims, tokens, grad_out, expert_ids.T, w_gate, w_in[0], w_out[0]))
    return y_out, grad_x, g1[None], g2[None], grad_w_gate


def solution(mesh):
    dims = (8, 4, 4, 2)
    return jax.shard_map(functools.partial(local_block, dims), mesh=mesh, in_specs=(P('ep'), P('ep'), P('ep'), P(), P('ep'), P('ep')), out_specs=(P('ep'), P('ep'), P('ep'), P('ep'), P()), check_vma=False)
```

```python
import functools
import itertools
import math

import jax
import jax.numpy as jnp
from jax import lax
from jax.experimental import pallas as pl
from jax.experimental.pallas import tpu as pltpu
from jax.sharding import PartitionSpec as P

MESH = pl.DeviceIdType.MESH
F32 = jnp.float32
BF16 = jnp.bfloat16
CAP = 8


def coords(dims):
    nz, ny, nx, nc = dims
    me = lax.axis_index('ep')
    c = lax.rem(me, nc)
    x = lax.rem(me // nc, nx)
    y = lax.rem(me // (nc * nx), ny)
    z = me // (nc * nx * ny)

    def dev(z, y, x, c):
        return (((z * ny + y) * nx + x) * nc + c,)

    return z, y, x, c, dev


def dot(a, b, ca, cb):
    return lax.dot_general(a, b, (((ca,), (cb,)), ((), ())), preferred_element_type=F32)


def iota(shape, axis):
    return lax.broadcasted_iota(jnp.int32, shape, axis)


def as_row(col):
    n = col.shape[0]
    return jnp.sum(jnp.where(iota((n, n), 0) == iota((n, n), 1), col, 0.0), axis=0, keepdims=True)


def as_col(row):
    n = row.shape[1]
    return jnp.sum(jnp.where(iota((n, n), 0) == iota((n, n), 1), row, 0.0), axis=1, keepdims=True)


def gates(tok, i0, i1, w_gate):
    logits = dot(tok, w_gate, 1, 0)
    expert = iota(logits.shape, 1).astype(F32)
    l0, l1 = (jnp.sum(jnp.where(expert == i, logits, 0.0), axis=1, keepdims=True) for i in (i0, i1))
    top = jnp.maximum(l0, l1)
    p0, p1 = jnp.exp(l0 - top), jnp.exp(l1 - top)
    total = p0 + p1
    return p0 / total, p1 / total


def choice_row(tok, ids, w_gate):
    r0, r1 = ids[0:1].astype(F32), ids[1:2].astype(F32)
    i0, i1 = as_col(r0), as_col(r1)
    g0, g1 = gates(tok, i0, i1, w_gate)

    def code(i):
        n = jnp.sum((i == r0).astype(F32) + (i == r1).astype(F32), axis=1, keepdims=True)
        return as_row(jnp.where(n > 1.5, i + 256.0, i))

    return jnp.concatenate([code(i0), code(i1), as_row(g0), as_row(g1)], axis=1)


def gelu_tanh(a):
    k = 0.7978845608028654
    sq = a * a
    return jnp.tanh(a * (k + (k * 0.044715) * sq)), sq


def gelu(a):
    half = 0.5 * a
    return half + half * gelu_tanh(a)[0]


def gelu_slope(a):
    k = 0.7978845608028654
    t, sq = gelu_tanh(a)
    return (0.5 + 0.5 * t) + (0.5 * a) * (1.0 - t * t) * (k + (3 * k * 0.044715) * sq)


def token_lanes(ref, k, start, n):
    lane = iota((n, 128), 1) // 32
    out = jnp.zeros((n, 128), F32)
    for j in range(4):
        r = ref[pl.ds(start + j, n, stride=4), :]
        out = jnp.where(lane == j, r if j == k else pltpu.roll(r, 32 * (j - k) % 128, 1), out)
    return out


def pair_rows(v):
    return jnp.concatenate([jnp.concatenate([v[2 * i:2 * i + 1], v[2 * i + 1:2 * i + 2]], axis=1) for i in range(v.shape[0] // 2)], axis=0)


def plain_id(code):
    return jnp.where(code >= 256.0, code - 256.0, code)


class Links:
    def __init__(self, send, recv, pool):
        self.send, self.recv, self.pool, self.bytes = send, recv, pool, 0

    def group(self):
        return self.recv.at[next(self.pool)]

    def go(self, src, dst, to, group):
        pltpu.make_async_remote_copy(src_ref=src, dst_ref=dst, send_sem=self.send, recv_sem=group, device_id=to, device_id_type=MESH).start()
        self.bytes += math.prod(src.shape) * jnp.dtype(src.dtype).itemsize

    def wait(self, group, ref):
        pltpu.make_async_copy(ref, ref, group).wait()

    def finish(self, *pads):
        for pad in pads:
            unit = math.prod(pad.shape[1:]) * jnp.dtype(pad.dtype).itemsize
            if self.bytes % unit == 0:
                return self.wait(self.send, pad.at[pl.ds(0, self.bytes // unit)])
        raise ValueError(self.bytes)


def block_kernel(dims, sizes, *refs):
    nz, ny, nx, nc = dims
    refs = iter(refs)
    refs = [list(itertools.islice(refs, n)) for n in sizes]
    (tok_hbm, dout_hbm, ids_hbm, wg_hbm, w1_hbm, w2_hbm), outs, held, kept, rows, areas, (load_sem, keep_sem, save_sem), sems = refs
    out_ref, gx_ref, gate_ref, g1_ref, g2_ref = held
    tok, dout, ids, wg, w1, w2, row, m_land, x_all, g_all, xs_ref, dys_ref, h_ref, da_ref, a_ref, m_all, hot_ref, d_row, d_land, d_all, pad, pad_row = kept
    z, y, x, c, dev = coords(dims)
    saves = [pltpu.make_async_copy(held[k], outs[k], save_sem.at[k]) for k in range(len(held))]

    def save(k, part):
        pltpu.make_async_copy(held[k].at[part], outs[k].at[part], save_sem.at[k]).start()

    send_sem, recv_sem = sems
    pool = itertools.count()
    all_links = [Links(send_sem.at[k], recv_sem, pool) for k in range(send_sem.shape[0])]
    links = iter(all_links)

    loads = [pltpu.make_async_copy(s, d, load_sem.at[k]) for k, (s, d) in enumerate(
        [(tok_hbm, x_all.at[z, y, x, c]), (dout_hbm, g_all.at[z, y, x, c]), (tok_hbm, tok), (ids_hbm, ids), (wg_hbm, wg), (dout_hbm, dout), (w1_hbm, w1), (w2_hbm, w2)])]
    for ld in loads:
        ld.start()
    peers = [dev(lax.rem(z + d, nz), y, x, c) for d in range(1, nz)]
    for d in (1, 2, 3):
        peers.append(dev(z, lax.rem(y + d, ny), x, c))
        peers.append(dev(z, y, lax.rem(x + d, nx), c))
    mate = dev(z, y, x, 1 - c)
    peers.append(mate)
    barrier = pltpu.get_barrier_semaphore()
    for peer in peers:
        pl.semaphore_signal(barrier, inc=1, device_id=peer, device_id_type=MESH)
    for ld in loads[2:5]:
        ld.wait()
    row[...] = choice_row(tok[...], ids[...], wg[...])
    place = pltpu.make_async_copy(row, m_land.at[z, y, x, c], keep_sem.at[0])
    place.start()
    loads[0].wait()
    loads[1].wait()
    place.wait()
    pl.semaphore_wait(barrier, len(peers))

    full = slice(None)
    by_distance = sorted(range(1, nz), key=lambda d: abs(d - nz // 2))

    def step(v, d, m=4):
        return lax.rem(v + d, m)

    def by_lines(link, ref, rows, x_last, late):
        p0, q0 = (y, x) if x_last else (x, y)
        low, high = pl.ds(0, nz // 2), pl.ds(nz // 2, nz // 2)

        def at(zs, p, q):
            return ref.at[(zs, p, q, c, rows) if x_last else (zs, q, p, c, rows)]

        def go(part, p, q, group):
            link.go(part, part, dev(z, p, q, c) if x_last else dev(z, q, p, c), group)

        in_z, in_p, in_m, in_f, in_r, in_c = [link.group() for _ in range(6)]
        line = at(full, p0, q0)

        def over(q):
            part = at(full, full, q)
            link.go(part, part, mate, in_c)

        own = at(z, p0, q0)
        for d in by_distance:
            link.go(own, own, dev(step(z, d, nz), y, x, c), in_z)
        yield
        link.wait(in_z, at(pl.ds(0, nz - 1), p0, q0))
        pm, pp, po = step(p0, 3), step(p0, 1), step(p0, 2)
        qm, qp, qo = step(q0, 3), step(q0, 1), step(q0, 2)
        qs = []

        def spread(p):
            part = at(full, p, q0)
            qs.append((p, link.group()))
            go(part, p0, qp, qs[-1][1])
            go(part, p0, qm, qs[-1][1])

        def relay(i):
            p, group = qs[i]
            link.wait(group, at(full, pl.ds(0, 2), q0))
            go(at(low, p, qm), p0, qp, in_r)
            go(at(high, p, qp), p0, qm, in_r)

        def pass_one():
            link.wait(in_p, line)
            go(at(low, pm, q0), pp, q0, in_f)
            link.wait(in_m, line)
            go(at(high, pp, q0), pm, q0, in_f)

        go(line, pp, q0, in_p)
        go(line, pm, q0, in_m)
        if late:
            yield
            pass_one()
            yield
            link.wait(in_f, line)
            for p in (p0, pm, pp, po):
                spread(p)
            over(q0)
            yield
            relay(0)
        else:
            yield
            spread(p0)
            yield
            pass_one()
            yield
            spread(pm)
            spread(pp)
            yield
            relay(0)
            yield
            link.wait(in_f, line)
            spread(po)
            over(q0)
        for i in range(1, 4):
            yield
            relay(i)
        over(qm)
        over(qp)
        yield
        link.wait(in_r, at(full, full, q0))
        over(qo)
        yield
        link.wait(in_c, ref.at[full, full, full, c, rows])

    def gather_rows(link, held, order):
        have = [z, y, x, c]
        for axis in order:
            size = (nz, ny, nx, nc)[axis]
            part = held.at[tuple(have)]
            group = link.group()
            for d in sorted(range(1, size), key=lambda d: abs(d - size // 2)):
                there = [z, y, x, c]
                there[axis] = lax.rem(there[axis] + d, size)
                link.go(part, part, dev(*there), group)
            have[axis] = pl.ds(0, size - 1)
            yield
            link.wait(group, held.at[tuple(have)])
            have[axis] = full

    def advance(plans):
        for g in plans:
            next(g, None)

    halves = [slice(0, 16), slice(16, 32)]
    tok_plans, grad_plans = [[by_lines(next(links), ref, half, half.start == 0, ref is g_all) for half in halves] for ref in (x_all, g_all)]
    row_plan = [gather_rows(next(links), m_land, range(4))]
    advance(row_plan + tok_plans + grad_plans)
    def flatten(land, flat):
        def lines(zz, carry):
            for k in range(ny * nx * nc):
                flat[pl.ds(zz * (ny * nx * nc) + k, 1), :] = land[zz, k // (nx * nc), k // nc % nx, k % nc]
            return carry

        lax.fori_loop(0, nz, lines, 0)


    me = lax.axis_index('ep').astype(F32)
    def read_rows():
        flatten(m_land, m_all)
        for ld in loads[5:]:
            ld.wait()
        code = m_all[...]
        left = jnp.where((iota(code.shape, 1) < 64) & (code >= 256.0), code - 256.0, 999.0)
        found = []
        for _ in range(3):
            best = jnp.min(jnp.min(left, axis=0, keepdims=True), axis=1, keepdims=True)
            left = jnp.where(left == best, 999.0, left)
            found.append(jnp.broadcast_to(best, (1, 128)))
        hot_ref[...] = jnp.concatenate(found + [jnp.full((5, 128), 999.0, F32)], axis=0)

    steps = 4 if nz == 8 else 1
    per = nz // steps
    n_quad = per * ny * nx * nc // 4
    n_pair = n_quad // 2
    n_slot = n_pair * 8 * CAP

    places = [(cc, xx, yy, zz) for cc in range(nc) for xx in range(nx) for yy in range(ny) for zz in range(per)]

    def select(i, ref, with_gate):
        c0, c1, g0, g1 = (pair_rows(token_lanes(m_all, k, pl.multiple_of(4 * n_quad * i, 4 * n_quad), n_quad)) for k in range(4))
        hit0, hit1 = plain_id(c0) == me, plain_id(c1) == me
        hit = (hit0 | hit1).astype(F32)
        gate = jnp.where(hit0, g0, 0.0) + jnp.where(hit1, g1, 0.0)
        before, after = iota((256, 256), 0), iota((256, 256), 1)
        tri = ((before < after) & (before // 32 == after // 32)).astype(F32).astype(BF16)
        rank = dot(hit.astype(BF16), tri, 1, 0)
        src = (iota((n_pair, 256), 1) // 32).astype(F32)
        key = jnp.where(hit > 0.0, src * CAP + rank, -1.0)
        slot = iota((8 * CAP, 256), 0).astype(F32)
        parts = []
        for p in range(n_pair):
            sel = (slot == key[p:p + 1]).astype(F32)
            v = dot(sel.astype(BF16), ref[i * per + p // ny, p % ny].reshape(256, 256), 1, 0)
            parts.append(v * jnp.sum(sel * gate[p:p + 1], axis=1, keepdims=True) if with_gate else v)
        return jnp.concatenate([parts[zz * ny + yy][CAP * (xx * nc + cc):CAP * (xx * nc + cc + 1)] for cc, xx, yy, zz in places], axis=0).astype(BF16)

    def put(i, v, to):
        for k, (cc, xx, yy, zz) in enumerate(places):
            for half in range(2):
                to[half][cc, xx, yy, i * per + zz] = v[CAP * k:CAP * (k + 1), 128 * half:128 * (half + 1)].astype(BF16)

    def forward(i):
        here = pl.ds(i * n_slot, n_slot)
        xs = select(i, x_all, False)
        a = dot(xs, w1[...], 1, 0)
        h = gelu(a).astype(BF16)
        xs_ref[here], h_ref[here], a_ref[here] = xs, h, a
        put(i, dot(h, w2[...], 1, 0), rows[:2])

    def backward(i):
        here = pl.ds(i * n_slot, n_slot)
        dys = select(i, g_all, True)
        dys_ref[here] = dys
        da_ref[here] = (dot(dys, w2[...], 1, 1) * gelu_slope(a_ref[here])).astype(BF16)

    def backward_rows(i):
        put(i, dot(da_ref[pl.ds(i * n_slot, n_slot)], w1[...], 1, 1), rows[2:])

    def back(i):
        h = rows[i]
        other, near, via, out2, via2, in2, out3, hot_land, cold_land = areas[9 * i:9 * i + 9]
        link = next(links)
        go = link.go
        in_c, in_e, in_h = [[link.group(), link.group()] for _ in range(3)]
        in_n, in_v, in_2, in_l, in_s = [link.group() for _ in range(5)]
        x_first = i % 2 == 0
        a, b = (x, y) if x_first else (y, x)

        def to(a, b):
            return dev(z, b, a, c) if x_first else dev(z, a, b, c)

        def index(lead, a, bs):
            return lead + ((a, bs) if x_first else (bs, a))

        up, dn, far = step(a, 1), step(a, 3), step(a, 2)
        lo, hi = pl.ds(0, 2), pl.ds(2, 2)
        parts = [pl.ds(0, nz // 2), pl.ds(nz // 2, nz // 2)]

        def start(k):
            zs = parts[k]
            go(h.at[1 - c, :, :, zs], other.at[:, :, zs], mate, in_c[k])
            spread(h, (c,), c, zs, in_e[k])

        def follow(k):
            link.wait(in_c[k], other.at[:, :, parts[k]])
            spread(other, (), 1 - c, parts[k], in_h[k])

        def spread(ref, lead, e, zs, group):
            go(ref.at[index(lead, far, lo) + (zs,)], via.at[0, e, :, zs], to(up, b), group)
            go(ref.at[index(lead, far, hi) + (zs,)], via.at[1, e, :, zs], to(dn, b), group)
            go(ref.at[index(lead, up, full) + (zs,)], near.at[a, e, :, zs], to(up, b), in_n)
            go(ref.at[index(lead, dn, full) + (zs,)], near.at[a, e, :, zs], to(dn, b), in_n)

        def relay(e, zs, group):
            link.wait(group, via.at[:, e, :, zs])
            go(via.at[0, e, :, zs], near.at[dn, e, lo, zs], to(up, b), in_n)
            go(via.at[1, e, :, zs], near.at[up, e, hi, zs], to(dn, b), in_n)

        start(0)
        yield
        follow(0)
        yield
        start(1)
        yield
        follow(1)
        yield
        relay(c, parts[0], in_e[0])
        relay(1 - c, parts[0], in_h[0])
        yield
        relay(c, parts[1], in_e[1])
        yield
        relay(1 - c, parts[1], in_h[1])
        yield
        link.wait(in_n, near.at[pl.ds(0, 3)])

        def expert(s, e):
            return ((z * ny + y) * nx + s) * nc + e if x_first else ((z * ny + s) * nx + x) * nc + e

        places = [(step(a, d), e) for d in range(4) for e in (c, 1 - c)]
        is_hot = [[(hot_ref[j:j + 1, :] == expert(s, e).astype(F32)).astype(F32) for s, e in places] for j in range(3)]
        wide = lambda v: jnp.broadcast_to(v, (8, 128))
        weight = [[wide(v).astype(BF16) for v in r] for r in is_hot]
        line = iota((8, 128), 0)
        mine = [(wide(is_hot[0][k] + is_hot[1][k] + is_hot[2][k]) < 0.5) & (line == s * nc + e) for k, (s, e) in enumerate(places)]

        def squeeze(bb, carry):
            given = [h[index((c,), a, bb)], other[index((), a, bb)]] + [near[s, e, bb] for s, e in places[2:]]
            for j in range(3):
                out2[bb, j] = sum(given[k] * weight[j][k] for k in range(8))
            singles = jnp.zeros((nz, 8, 128), F32)
            for k in range(8):
                singles = jnp.where(mine[k], jnp.sum(given[k].astype(F32), axis=1, keepdims=True), singles)
            out2[bb, 3] = singles.astype(BF16)
            return carry

        lax.fori_loop(0, 4, squeeze, 0)
        up, dn, far = step(b, 1), step(b, 3), step(b, 2)
        lo, hi = pl.ds(0, nz // 2), pl.ds(nz // 2, nz // 2)
        go(out2.at[far, :, lo], via2.at[0], to(a, up), in_v)
        go(out2.at[far, :, hi], via2.at[1], to(a, dn), in_v)
        go(out2.at[up], in2.at[b], to(a, up), in_2)
        go(out2.at[dn], in2.at[b], to(a, dn), in_2)
        in2[b] = out2[b]
        yield
        link.wait(in_v, via2)
        go(via2.at[0], in2.at[dn, :, lo], to(a, up), in_2)
        go(via2.at[1], in2.at[up, :, hi], to(a, dn), in_2)
        yield
        link.wait(in_2, in2.at[pl.ds(0, 3)])
        for j in range(3):
            out3[:, j] = (in2[0, j] + in2[1, j]) + (in2[2, j] + in2[3, j])
        for d in by_distance:
            zz = lax.rem(z + d, nz)
            go(in2.at[:, 3, zz], cold_land.at[z], dev(zz, y, x, c), in_s)
            go(out3.at[zz], hot_land.at[z], dev(zz, y, x, c), in_l)
        cold_land[z] = in2[:, 3, z]
        hot_land[z] = out3[z]
        yield
        link.wait(in_s, cold_land.at[pl.ds(0, nz - 1)])
        link.wait(in_l, hot_land.at[pl.ds(0, nz - 1)])

    def weight_grad(k):
        if k % 2 == 0:
            part = slice(w2.shape[0] // 4 * (k // 2), w2.shape[0] // 4 * (k // 2 + 1))
            g2_ref[part, :] = dot(h_ref[:, part], dys_ref[...], 0, 0)
            save(4, (part, full))
        else:
            part = slice(w1.shape[1] // 4 * (k // 2), w1.shape[1] // 4 * (k // 2 + 1))
            g1_ref[:, part] = dot(xs_ref[...], da_ref[:, part], 0, 0)
            save(3, (full, part))

    ys, dxs = [back(0), back(1)], [back(2), back(3)]
    n_tok = tok.shape[0]
    memo = {}
    earlier = iota((n_tok, n_tok), 1) < iota((n_tok, n_tok), 0)
    n_exp = wg.shape[1]

    def where_from(i, r0, r1):
        rank = jnp.sum(jnp.where(earlier & ((i == r0) | (i == r1)), 1.0, 0.0), axis=1, keepdims=True)
        slot = jnp.full((n_tok, 1), -1.0, F32)
        for j in range(3):
            slot = jnp.where(i == hot_ref[j:j + 1, 0:1], CAP * j + rank, slot)
        e = i.astype(jnp.int32)
        core, xx, yy, zz = e % nc, (e // nc) % nx, (e // (nc * nx)) % ny, e // (nc * nx * ny)
        lane, single = iota((n_tok, n_exp), 1), slot < 0.0
        pick = lambda m: m.astype(F32).astype(BF16)
        return pick(iota((n_tok, 32), 1).astype(F32) == slot), (pick((lane == e) & single), pick((lane == ((zz * nx + xx) * ny + yy) * nc + core) & single))

    def rows_of(kind, chosen):
        parts = []
        for half in range(2):
            hot_land, cold_land = areas[9 * (kind + half) + 7:9 * (kind + half) + 9]
            hot = jnp.sum(hot_land[...].astype(F32), axis=0).reshape(24, 128)
            hot = jnp.concatenate([hot, jnp.zeros((8, 128), F32)], axis=0).astype(BF16)
            cold = cold_land[...].astype(F32).reshape(n_exp, 128).astype(BF16)
            parts.append([dot(by_slot, hot, 1, 0) + dot(by_place[half], cold, 1, 0) for by_slot, by_place in chosen])
        return [jnp.concatenate([parts[0][k], parts[1][k]], axis=1) for k in range(2)]

    def combine():
        r0, r1 = ids[0:1].astype(F32), ids[1:2].astype(F32)
        i0, i1 = as_col(r0), as_col(r1)
        g0, g1 = gates(tok[...], i0, i1, wg[...])
        chosen = [where_from(i, r0, r1) for i in (i0, i1)]
        y0, y1 = rows_of(0, chosen)
        grad = dout[...].astype(F32)
        dg0, dg1 = (jnp.sum(grad * v, axis=1, keepdims=True) for v in (y0, y1))
        mean = g0 * dg0 + g1 * dg1
        d0, d1 = ((g * (dg - mean)).astype(BF16).astype(F32) for g, dg in ((g0, dg0), (g1, dg1)))
        d_row[...] = jnp.concatenate([as_row(d0), as_row(d1), jnp.zeros((1, 2 * n_tok), F32)], axis=1)
        place = pltpu.make_async_copy(d_row, d_land.at[z, y, x, c], keep_sem.at[1])
        place.start()
        out_ref[...] = (g0 * y0 + g1 * y1).astype(BF16)
        saves[0].start()
        place.wait()
        d_plans.append(gather_rows(next(links), d_land, range(4)))
        advance(d_plans)
        expert = iota((n_tok, n_exp), 1).astype(F32)
        spread = jnp.where(expert == i0, d0, jnp.where(expert == i1, d1, 0.0)).astype(BF16)
        memo.update(chosen=chosen, through=dot(spread, wg[...], 1, 1))

    def finish():
        dx0, dx1 = rows_of(2, memo['chosen'])
        gx_ref[...] = (dx0 + dx1 + memo['through']).astype(BF16)
        saves[1].start()

    n_dev = nz * ny * nx * nc

    def gate_grad():
        flatten(d_land, d_all)
        expert = iota((n_exp, 256), 0).astype(F32)
        codes = [plain_id(pair_rows(token_lanes(m_all, k, 0, n_dev // 4))) for k in range(2)]
        grads = [pair_rows(token_lanes(d_all, k, 0, n_dev // 4)) for k in range(2)]
        total = jnp.zeros((n_exp, x_all.shape[-1]), F32)
        zs = nz // 4 or 1
        for z0 in range(0, nz, zs):
            spread = []
            for p in range(z0 * ny, (z0 + zs) * ny):
                q = slice(p, p + 1)
                spread.append(jnp.where(expert == codes[0][q], grads[0][q], jnp.where(expert == codes[1][q], grads[1][q], 0.0)).astype(BF16))
            total += dot(jnp.concatenate(spread, axis=1), x_all[z0:z0 + zs].reshape(zs * ny * 256, x_all.shape[-1]), 1, 0)
        gate_ref[...] = total.T
        saves[2].start()

    d_plans = []
    moves = {'t': tok_plans, 'g': grad_plans, 'm': row_plan, 'y': ys, 'x': dxs, 'd': d_plans}
    works = {'f': [functools.partial(forward, i) for i in range(steps)], 'b': [functools.partial(backward, i) for i in range(steps)],
             'B': [functools.partial(backward_rows, i) for i in range(steps)], 'w': [functools.partial(weight_grad, k) for k in range(8)],
             'h': [read_rows], 'c': [combine], 'k': [gate_grad], 'e': [finish]}
    for turn in SCHEDULE:
        if turn in moves:
            advance(moves[turn])
        elif works[turn]:
            works[turn].pop(0)()
    for link in all_links:
        link.finish(pad, pad_row)
    for cp in saves:
        cp.wait()


def block_call(dims, tokens, grad_out, ids, w_gate, w1, w2):
    nz, ny, nx, nc = dims
    d_model, d_hidden = w1.shape
    n_tok = tokens.shape[0]
    n_dev = nz * ny * nx * nc
    n_row = n_dev * CAP
    tile = (CAP, 128)
    hbm = pl.BlockSpec(memory_space=pltpu.HBM)
    out = jax.ShapeDtypeStruct
    work = [(4, 4, nz), (4, 2, 4, nz), (2, 2, 2, nz), (4, 4, nz), (2, 4, nz // 2), (4, 4, nz), (nz, 3), (nz, 3), (nz, 4)]
    n_group = 4 * 10 + 4 + 4 * 11 + 4
    sems = [pltpu.SemaphoreType.DMA((10,)), pltpu.SemaphoreType.DMA((n_group,))]
    results = [(tokens.shape, BF16), (tokens.shape, BF16), ((d_model, n_dev), F32), ((d_model, d_hidden), F32), ((d_hidden, d_model), F32)]
    row = (1, 128)
    kept = [(tokens.shape, BF16), (tokens.shape, BF16), (ids.shape, jnp.int32), (w_gate.shape, BF16), (w1.shape, BF16), (w2.shape, BF16), (row, F32), (dims + row, F32),
            (dims + tokens.shape, BF16), (dims + tokens.shape, BF16), ((n_row, d_model), BF16), ((n_row, d_model), BF16), ((n_row, d_hidden), BF16), ((n_row, d_hidden), BF16), ((n_row, d_hidden), F32), ((n_dev, 128), F32), (tile, F32), (row, F32),
            (dims + row, F32), ((n_dev, 128), F32), ((1024,) + tile, BF16), ((n_dev,) + row, F32)]
    return pl.pallas_call(
        functools.partial(block_kernel, dims, (6, len(results), len(results), len(kept), 4, 4 * len(work), 3, len(sems))),
        out_shape=[out(*r) for r in results],
        in_specs=[hbm] * 6,
        out_specs=[hbm] * len(results),
        scratch_shapes=[pltpu.VMEM(*r) for r in results + kept] + [pltpu.VMEM((nc, nx, ny, nz) + tile, BF16)] * 4 + [pltpu.VMEM(w + tile, BF16) for w in work] * 4
        + [pltpu.SemaphoreType.DMA((k,)) for k in (8, 2, len(results))] + sems,
        compiler_params=pltpu.CompilerParams(collective_id=0, has_side_effects=True, vmem_limit_bytes=VMEM_LIMIT),
        name='block',
    )(tokens, grad_out, ids, w_gate, w1, w2)


VMEM_LIMIT = 67043328
SCHEDULE = 'mttmttmgttttgttgmth' + 'ffggyfggyfy' + 'gygy' + 'bybyBBxbybyBBxxwwxwyxwxxwwxyc' + 'xwxddwddkxe'


def pass_kernel(n, *refs):
    refs = iter(refs)
    given, passed, held, (load_sem, save_sem) = [list(itertools.islice(refs, k)) for k in (n, n, n, 2)]
    loads = [pltpu.make_async_copy(given[k], held[k], load_sem.at[k]) for k in range(n)]
    saves = [pltpu.make_async_copy(held[k], passed[k], save_sem.at[k]) for k in range(n)]
    for cp in loads:
        cp.start()
    for load, save in zip(loads, saves):
        load.wait()
        save.start()
    for cp in saves:
        cp.wait()


def pass_on(*arrays):
    n = len(arrays)
    return pl.pallas_call(
        functools.partial(pass_kernel, n),
        out_shape=[jax.ShapeDtypeStruct(v.shape, v.dtype) for v in arrays],
        in_specs=[pl.BlockSpec(memory_space=pltpu.HBM)] * n,
        out_specs=[pl.BlockSpec(memory_space=pltpu.HBM)] * n,
        scratch_shapes=[pltpu.VMEM(v.shape, v.dtype) for v in arrays] + [pltpu.SemaphoreType.DMA((n,))] * 2,
        compiler_params=pltpu.CompilerParams(vmem_limit_bytes=VMEM_LIMIT),
        name='pass_on',
    )(*arrays)


def local_block(dims, tokens, grad_out, expert_ids, w_gate, w_in, w_out):
    y_out, grad_x, grad_w_gate, g1, g2 = pass_on(*block_call(dims, tokens, grad_out, expert_ids.T, w_gate, w_in[0], w_out[0]))
    return y_out, grad_x, g1[None], g2[None], grad_w_gate


def solution(mesh):
    dims = (8, 4, 4, 2)
    return jax.shard_map(functools.partial(local_block, dims), mesh=mesh, in_specs=(P('ep'), P('ep'), P('ep'), P(), P('ep'), P('ep')), out_specs=(P('ep'), P('ep'), P('ep'), P('ep'), P()), check_vma=False)
```

```python
import functools
import itertools
import math

import jax
import jax.numpy as jnp
from jax import lax
from jax.experimental import pallas as pl
from jax.experimental.pallas import tpu as pltpu
from jax.sharding import PartitionSpec as P

MESH = pl.DeviceIdType.MESH
F32 = jnp.float32
BF16 = jnp.bfloat16
CAP = 8


def coords(dims):
    nz, ny, nx, nc = dims
    me = lax.axis_index('ep')
    c = lax.rem(me, nc)
    x = lax.rem(me // nc, nx)
    y = lax.rem(me // (nc * nx), ny)
    z = me // (nc * nx * ny)

    def dev(z, y, x, c):
        return (((z * ny + y) * nx + x) * nc + c,)

    return z, y, x, c, dev


def dot(a, b, ca, cb):
    return lax.dot_general(a, b, (((ca,), (cb,)), ((), ())), preferred_element_type=F32)


def iota(shape, axis):
    return lax.broadcasted_iota(jnp.int32, shape, axis)


def as_row(col):
    n = col.shape[0]
    return jnp.sum(jnp.where(iota((n, n), 0) == iota((n, n), 1), col, 0.0), axis=0, keepdims=True)


def as_col(row):
    n = row.shape[1]
    return jnp.sum(jnp.where(iota((n, n), 0) == iota((n, n), 1), row, 0.0), axis=1, keepdims=True)


def gates(tok, i0, i1, w_gate):
    logits = dot(tok, w_gate, 1, 0)
    expert = iota(logits.shape, 1).astype(F32)
    l0, l1 = (jnp.sum(jnp.where(expert == i, logits, 0.0), axis=1, keepdims=True) for i in (i0, i1))
    top = jnp.maximum(l0, l1)
    p0, p1 = jnp.exp(l0 - top), jnp.exp(l1 - top)
    total = p0 + p1
    return p0 / total, p1 / total


def choice_row(tok, ids, w_gate):
    r0, r1 = ids[0:1].astype(F32), ids[1:2].astype(F32)
    i0, i1 = as_col(r0), as_col(r1)
    g0, g1 = gates(tok, i0, i1, w_gate)

    def code(i):
        n = jnp.sum((i == r0).astype(F32) + (i == r1).astype(F32), axis=1, keepdims=True)
        return as_row(jnp.where(n > 1.5, i + 256.0, i))

    return jnp.concatenate([code(i0), code(i1), as_row(g0), as_row(g1)], axis=1)


def gelu_tanh(a):
    k = 0.7978845608028654
    sq = a * a
    return jnp.tanh(a * (k + (k * 0.044715) * sq)), sq


def gelu(a):
    half = 0.5 * a
    return half + half * gelu_tanh(a)[0]


def gelu_slope(a):
    k = 0.7978845608028654
    t, sq = gelu_tanh(a)
    return (0.5 + 0.5 * t) + (0.5 * a) * (1.0 - t * t) * (k + (3 * k * 0.044715) * sq)


def token_lanes(ref, k, start, n):
    lane = iota((n, 128), 1) // 32
    out = jnp.zeros((n, 128), F32)
    for j in range(4):
        r = ref[pl.ds(start + j, n, stride=4), :]
        out = jnp.where(lane == j, r if j == k else pltpu.roll(r, 32 * (j - k) % 128, 1), out)
    return out


def pair_rows(v):
    return jnp.concatenate([jnp.concatenate([v[2 * i:2 * i + 1], v[2 * i + 1:2 * i + 2]], axis=1) for i in range(v.shape[0] // 2)], axis=0)


def plain_id(code):
    return jnp.where(code >= 256.0, code - 256.0, code)


class Links:
    def __init__(self, send, recv, pool):
        self.send, self.recv, self.pool, self.bytes = send, recv, pool, 0

    def group(self):
        return self.recv.at[next(self.pool)]

    def go(self, src, dst, to, group):
        pltpu.make_async_remote_copy(src_ref=src, dst_ref=dst, send_sem=self.send, recv_sem=group, device_id=to, device_id_type=MESH).start()
        self.bytes += math.prod(src.shape) * jnp.dtype(src.dtype).itemsize

    def wait(self, group, ref):
        pltpu.make_async_copy(ref, ref, group).wait()

    def finish(self, *pads):
        for pad in pads:
            unit = math.prod(pad.shape[1:]) * jnp.dtype(pad.dtype).itemsize
            if self.bytes % unit == 0:
                return self.wait(self.send, pad.at[pl.ds(0, self.bytes // unit)])
        raise ValueError(self.bytes)


def block_kernel(dims, sizes, *refs):
    nz, ny, nx, nc = dims
    refs = iter(refs)
    refs = [list(itertools.islice(refs, n)) for n in sizes]
    (tok_hbm, dout_hbm, ids_hbm, wg_hbm, w1_hbm, w2_hbm), outs, held, kept, rows, areas, (load_sem, keep_sem, save_sem), sems = refs
    out_ref, gx_ref, gate_ref, g1_ref, g2_ref = held
    tok, dout, ids, wg, w1, w2, row, m_land, x_all, g_all, xs_ref, dys_ref, h_ref, da_ref, a_ref, m_all, hot_ref, d_land, d_all, pad, pad_row = kept
    z, y, x, c, dev = coords(dims)
    saves = [pltpu.make_async_copy(held[k], outs[k], save_sem.at[k]) for k in range(len(held))]

    def save(k, part):
        pltpu.make_async_copy(held[k].at[part], outs[k].at[part], save_sem.at[k]).start()

    send_sem, recv_sem = sems
    pool = itertools.count()
    all_links = [Links(send_sem.at[k], recv_sem, pool) for k in range(send_sem.shape[0])]
    links = iter(all_links)

    loads = [pltpu.make_async_copy(s, d, load_sem.at[k]) for k, (s, d) in enumerate(
        [(tok_hbm, x_all.at[z, y, x, c]), (dout_hbm, g_all.at[z, y, x, c]), (tok_hbm, tok), (ids_hbm, ids), (wg_hbm, wg), (dout_hbm, dout), (w1_hbm, w1), (w2_hbm, w2)])]
    for ld in loads:
        ld.start()
    peers = [dev(lax.rem(z + d, nz), y, x, c) for d in range(1, nz)]
    for d in (1, 2, 3):
        peers.append(dev(z, lax.rem(y + d, ny), x, c))
        peers.append(dev(z, y, lax.rem(x + d, nx), c))
    mate = dev(z, y, x, 1 - c)
    peers.append(mate)
    barrier = pltpu.get_barrier_semaphore()
    for peer in peers:
        pl.semaphore_signal(barrier, inc=1, device_id=peer, device_id_type=MESH)
    for ld in loads[2:5]:
        ld.wait()
    row[...] = choice_row(tok[...], ids[...], wg[...])
    place = pltpu.make_async_copy(row, m_land.at[z, y, x, c], keep_sem.at[0])
    place.start()
    loads[0].wait()
    loads[1].wait()
    place.wait()
    pl.semaphore_wait(barrier, len(peers))

    full = slice(None)
    by_distance = sorted(range(1, nz), key=lambda d: abs(d - nz // 2))

    def step(v, d, m=4):
        return lax.rem(v + d, m)

    def by_lines(link, ref, rows, x_last, late):
        p0, q0 = (y, x) if x_last else (x, y)
        low, high = pl.ds(0, nz // 2), pl.ds(nz // 2, nz // 2)

        def at(zs, p, q):
            return ref.at[(zs, p, q, c, rows) if x_last else (zs, q, p, c, rows)]

        def go(part, p, q, group):
            link.go(part, part, dev(z, p, q, c) if x_last else dev(z, q, p, c), group)

        in_z, in_p, in_m, in_f, in_r, in_c = [link.group() for _ in range(6)]
        line = at(full, p0, q0)

        def over(q):
            part = at(full, full, q)
            link.go(part, part, mate, in_c)

        own = at(z, p0, q0)
        for d in by_distance:
            link.go(own, own, dev(step(z, d, nz), y, x, c), in_z)
        yield
        link.wait(in_z, at(pl.ds(0, nz - 1), p0, q0))
        pm, pp, po = step(p0, 3), step(p0, 1), step(p0, 2)
        qm, qp, qo = step(q0, 3), step(q0, 1), step(q0, 2)
        qs = []

        def spread(p):
            part = at(full, p, q0)
            qs.append((p, link.group()))
            go(part, p0, qp, qs[-1][1])
            go(part, p0, qm, qs[-1][1])

        def relay(i):
            p, group = qs[i]
            link.wait(group, at(full, pl.ds(0, 2), q0))
            go(at(low, p, qm), p0, qp, in_r)
            go(at(high, p, qp), p0, qm, in_r)

        def pass_one():
            link.wait(in_p, line)
            go(at(low, pm, q0), pp, q0, in_f)
            link.wait(in_m, line)
            go(at(high, pp, q0), pm, q0, in_f)

        go(line, pp, q0, in_p)
        go(line, pm, q0, in_m)
        if late:
            yield
            pass_one()
            yield
            link.wait(in_f, line)
            for p in (p0, pm, pp, po):
                spread(p)
            over(q0)
            yield
            relay(0)
        else:
            yield
            spread(p0)
            yield
            pass_one()
            yield
            spread(pm)
            spread(pp)
            yield
            relay(0)
            yield
            link.wait(in_f, line)
            spread(po)
            over(q0)
        for i in range(1, 4):
            yield
            relay(i)
        over(qm)
        over(qp)
        yield
        link.wait(in_r, at(full, full, q0))
        over(qo)
        yield
        link.wait(in_c, ref.at[full, full, full, c, rows])

    def gather_rows(link, held, order):
        have = [z, y, x, c]
        for axis in order:
            size = (nz, ny, nx, nc)[axis]
            part = held.at[tuple(have)]
            group = link.group()
            for d in sorted(range(1, size), key=lambda d: abs(d - size // 2)):
                there = [z, y, x, c]
                there[axis] = lax.rem(there[axis] + d, size)
                link.go(part, part, dev(*there), group)
            have[axis] = pl.ds(0, size - 1)
            yield
            link.wait(group, held.at[tuple(have)])
            have[axis] = full

    def advance(plans):
        for g in plans:
            next(g, None)

    halves = [slice(0, 16), slice(16, 32)]
    tok_plans, grad_plans = [[by_lines(next(links), ref, half, half.start == 0, ref is g_all) for half in halves] for ref in (x_all, g_all)]
    row_plan = [gather_rows(next(links), m_land, range(4))]
    advance(row_plan + tok_plans + grad_plans)
    def flatten(land, flat):
        def lines(zz, carry):
            for k in range(ny * nx * nc):
                flat[pl.ds(zz * (ny * nx * nc) + k, 1), :] = land[zz, k // (nx * nc), k // nc % nx, k % nc]
            return carry

        lax.fori_loop(0, nz, lines, 0)


    me = lax.axis_index('ep').astype(F32)
    def read_rows():
        flatten(m_land, m_all)
        for ld in loads[5:]:
            ld.wait()
        code = m_all[...]
        left = jnp.where((iota(code.shape, 1) < 64) & (code >= 256.0), code - 256.0, 999.0)
        found = []
        for _ in range(3):
            best = jnp.min(jnp.min(left, axis=0, keepdims=True), axis=1, keepdims=True)
            left = jnp.where(left == best, 999.0, left)
            found.append(jnp.broadcast_to(best, (1, 128)))
        hot_ref[...] = jnp.concatenate(found + [jnp.full((5, 128), 999.0, F32)], axis=0)

    steps = 4 if nz == 8 else 1
    per = nz // steps
    n_quad = per * ny * nx * nc // 4
    n_pair = n_quad // 2
    n_slot = n_pair * 8 * CAP

    places = [(cc, xx, yy, zz) for cc in range(nc) for xx in range(nx) for yy in range(ny) for zz in range(per)]

    def select(i, ref, with_gate):
        c0, c1, g0, g1 = (pair_rows(token_lanes(m_all, k, pl.multiple_of(4 * n_quad * i, 4 * n_quad), n_quad)) for k in range(4))
        hit0, hit1 = plain_id(c0) == me, plain_id(c1) == me
        hit = (hit0 | hit1).astype(F32)
        gate = jnp.where(hit0, g0, 0.0) + jnp.where(hit1, g1, 0.0)
        before, after = iota((256, 256), 0), iota((256, 256), 1)
        tri = ((before < after) & (before // 32 == after // 32)).astype(F32).astype(BF16)
        rank = dot(hit.astype(BF16), tri, 1, 0)
        src = (iota((n_pair, 256), 1) // 32).astype(F32)
        key = jnp.where(hit > 0.0, src * CAP + rank, -1.0)
        slot = iota((8 * CAP, 256), 0).astype(F32)
        parts = []
        for p in range(n_pair):
            sel = (slot == key[p:p + 1]).astype(F32)
            v = dot(sel.astype(BF16), ref[i * per + p // ny, p % ny].reshape(256, 256), 1, 0)
            parts.append(v * jnp.sum(sel * gate[p:p + 1], axis=1, keepdims=True) if with_gate else v)
        return jnp.concatenate([parts[zz * ny + yy][CAP * (xx * nc + cc):CAP * (xx * nc + cc + 1)] for cc, xx, yy, zz in places], axis=0).astype(BF16)

    def put(i, v, to):
        for k, (cc, xx, yy, zz) in enumerate(places):
            for half in range(2):
                to[half][cc, xx, yy, i * per + zz] = v[CAP * k:CAP * (k + 1), 128 * half:128 * (half + 1)].astype(BF16)

    def forward(i):
        here = pl.ds(i * n_slot, n_slot)
        xs = select(i, x_all, False)
        a = dot(xs, w1[...], 1, 0)
        h = gelu(a).astype(BF16)
        xs_ref[here], h_ref[here], a_ref[here] = xs, h, a
        put(i, dot(h, w2[...], 1, 0), rows[:2])

    def backward(i):
        here = pl.ds(i * n_slot, n_slot)
        dys = select(i, g_all, True)
        dys_ref[here] = dys
        da_ref[here] = (dot(dys, w2[...], 1, 1) * gelu_slope(a_ref[here])).astype(BF16)

    def backward_rows(i):
        put(i, dot(da_ref[pl.ds(i * n_slot, n_slot)], w1[...], 1, 1), rows[2:])

    def back(i):
        h = rows[i]
        other, near, via, out2, via2, in2, out3, hot_land, cold_land = areas[9 * i:9 * i + 9]
        link = next(links)
        go = link.go
        in_c, in_e, in_h = [[link.group(), link.group()] for _ in range(3)]
        in_n, in_v, in_2, in_l, in_s = [link.group() for _ in range(5)]
        x_first = i % 2 == 0
        a, b = (x, y) if x_first else (y, x)

        def to(a, b):
            return dev(z, b, a, c) if x_first else dev(z, a, b, c)

        def index(lead, a, bs):
            return lead + ((a, bs) if x_first else (bs, a))

        up, dn, far = step(a, 1), step(a, 3), step(a, 2)
        lo, hi = pl.ds(0, 2), pl.ds(2, 2)
        parts = [pl.ds(0, nz // 2), pl.ds(nz // 2, nz // 2)]

        def start(k):
            zs = parts[k]
            go(h.at[1 - c, :, :, zs], other.at[:, :, zs], mate, in_c[k])
            spread(h, (c,), c, zs, in_e[k])

        def follow(k):
            link.wait(in_c[k], other.at[:, :, parts[k]])
            spread(other, (), 1 - c, parts[k], in_h[k])

        def spread(ref, lead, e, zs, group):
            go(ref.at[index(lead, far, lo) + (zs,)], via.at[0, e, :, zs], to(up, b), group)
            go(ref.at[index(lead, far, hi) + (zs,)], via.at[1, e, :, zs], to(dn, b), group)
            go(ref.at[index(lead, up, full) + (zs,)], near.at[a, e, :, zs], to(up, b), in_n)
            go(ref.at[index(lead, dn, full) + (zs,)], near.at[a, e, :, zs], to(dn, b), in_n)

        def relay(e, zs, group):
            link.wait(group, via.at[:, e, :, zs])
            go(via.at[0, e, :, zs], near.at[dn, e, lo, zs], to(up, b), in_n)
            go(via.at[1, e, :, zs], near.at[up, e, hi, zs], to(dn, b), in_n)

        start(0)
        yield
        follow(0)
        yield
        start(1)
        yield
        follow(1)
        yield
        relay(c, parts[0], in_e[0])
        relay(1 - c, parts[0], in_h[0])
        yield
        relay(c, parts[1], in_e[1])
        yield
        relay(1 - c, parts[1], in_h[1])
        yield
        link.wait(in_n, near.at[pl.ds(0, 3)])

        def expert(s, e):
            return ((z * ny + y) * nx + s) * nc + e if x_first else ((z * ny + s) * nx + x) * nc + e

        places = [(step(a, d), e) for d in range(4) for e in (c, 1 - c)]
        is_hot = [[(hot_ref[j:j + 1, :] == expert(s, e).astype(F32)).astype(F32) for s, e in places] for j in range(3)]
        wide = lambda v: jnp.broadcast_to(v, (8, 128))
        weight = [[wide(v).astype(BF16) for v in r] for r in is_hot]
        line = iota((8, 128), 0)
        mine = [(wide(is_hot[0][k] + is_hot[1][k] + is_hot[2][k]) < 0.5) & (line == s * nc + e) for k, (s, e) in enumerate(places)]

        def squeeze(bb):
            given = [h[index((c,), a, bb)], other[index((), a, bb)]] + [near[s, e, bb] for s, e in places[2:]]
            for j in range(3):
                out2[bb, j] = sum(given[k] * weight[j][k] for k in range(8))
            singles = jnp.zeros((nz, 8, 128), F32)
            for k in range(8):
                singles = jnp.where(mine[k], jnp.sum(given[k].astype(F32), axis=1, keepdims=True), singles)
            out2[bb, 3] = singles.astype(BF16)

        up, dn, far = step(b, 1), step(b, 3), step(b, 2)
        lo, hi = pl.ds(0, nz // 2), pl.ds(nz // 2, nz // 2)
        squeeze(far)
        squeeze(up)
        go(out2.at[far, :, lo], via2.at[0], to(a, up), in_v)
        go(out2.at[far, :, hi], via2.at[1], to(a, dn), in_v)
        squeeze(dn)
        go(out2.at[up], in2.at[b], to(a, up), in_2)
        squeeze(b)
        go(out2.at[dn], in2.at[b], to(a, dn), in_2)
        in2[b] = out2[b]
        yield
        link.wait(in_v, via2)
        go(via2.at[0], in2.at[dn, :, lo], to(a, up), in_2)
        go(via2.at[1], in2.at[up, :, hi], to(a, dn), in_2)
        yield
        link.wait(in_2, in2.at[pl.ds(0, 3)])
        for d in by_distance:
            zz = lax.rem(z + d, nz)
            go(in2.at[:, 3, zz], cold_land.at[z], dev(zz, y, x, c), in_s)
        for j in range(3):
            out3[:, j] = (in2[0, j] + in2[1, j]) + (in2[2, j] + in2[3, j])
        for d in by_distance:
            zz = lax.rem(z + d, nz)
            go(out3.at[zz], hot_land.at[z], dev(zz, y, x, c), in_l)
        cold_land[z] = in2[:, 3, z]
        hot_land[z] = out3[z]
        yield
        link.wait(in_s, cold_land.at[pl.ds(0, nz - 1)])
        link.wait(in_l, hot_land.at[pl.ds(0, nz - 1)])

    def weight_grad(k):
        if k % 2 == 0:
            part = slice(w2.shape[0] // 4 * (k // 2), w2.shape[0] // 4 * (k // 2 + 1))
            g2_ref[part, :] = dot(h_ref[:, part], dys_ref[...], 0, 0)
            save(4, (part, full))
        else:
            part = slice(w1.shape[1] // 4 * (k // 2), w1.shape[1] // 4 * (k // 2 + 1))
            g1_ref[:, part] = dot(xs_ref[...], da_ref[:, part], 0, 0)
            save(3, (full, part))

    ys, dxs = [back(0), back(1)], [back(2), back(3)]
    n_tok = tok.shape[0]
    memo = {}
    earlier = iota((n_tok, n_tok), 1) < iota((n_tok, n_tok), 0)
    n_exp = wg.shape[1]

    def where_from(i, r0, r1):
        rank = jnp.sum(jnp.where(earlier & ((i == r0) | (i == r1)), 1.0, 0.0), axis=1, keepdims=True)
        slot = jnp.full((n_tok, 1), -1.0, F32)
        for j in range(3):
            slot = jnp.where(i == hot_ref[j:j + 1, 0:1], CAP * j + rank, slot)
        e = i.astype(jnp.int32)
        core, xx, yy, zz = e % nc, (e // nc) % nx, (e // (nc * nx)) % ny, e // (nc * nx * ny)
        lane, single = iota((n_tok, n_exp), 1), slot < 0.0
        pick = lambda m: m.astype(F32).astype(BF16)
        return pick(iota((n_tok, 32), 1).astype(F32) == slot), (pick((lane == e) & single), pick((lane == ((zz * nx + xx) * ny + yy) * nc + core) & single))

    def rows_of(kind, chosen):
        parts = []
        for half in range(2):
            hot_land, cold_land = areas[9 * (kind + half) + 7:9 * (kind + half) + 9]
            hot = jnp.sum(hot_land[...].astype(F32), axis=0).reshape(24, 128)
            hot = jnp.concatenate([hot, jnp.zeros((8, 128), F32)], axis=0).astype(BF16)
            cold = cold_land[...].astype(F32).reshape(n_exp, 128).astype(BF16)
            parts.append([dot(by_slot, hot, 1, 0) + dot(by_place[half], cold, 1, 0) for by_slot, by_place in chosen])
        return [jnp.concatenate([parts[0][k], parts[1][k]], axis=1) for k in range(2)]

    def combine():
        r0, r1 = ids[0:1].astype(F32), ids[1:2].astype(F32)
        i0, i1 = as_col(r0), as_col(r1)
        g0, g1 = gates(tok[...], i0, i1, wg[...])
        chosen = [where_from(i, r0, r1) for i in (i0, i1)]
        y0, y1 = rows_of(0, chosen)
        grad = dout[...].astype(F32)
        dg0, dg1 = (jnp.sum(grad * v, axis=1, keepdims=True) for v in (y0, y1))
        mean = g0 * dg0 + g1 * dg1
        d0, d1 = ((g * (dg - mean)).astype(BF16).astype(F32) for g, dg in ((g0, dg0), (g1, dg1)))
        d_land[z, y, x, c] = jnp.concatenate([as_row(d0), as_row(d1), jnp.zeros((1, 2 * n_tok), F32)], axis=1)
        out_ref[...] = (g0 * y0 + g1 * y1).astype(BF16)
        saves[0].start()
        d_plans.append(gather_rows(next(links), d_land, range(4)))
        advance(d_plans)
        expert = iota((n_tok, n_exp), 1).astype(F32)
        spread = jnp.where(expert == i0, d0, jnp.where(expert == i1, d1, 0.0)).astype(BF16)
        memo.update(chosen=chosen, through=dot(spread, wg[...], 1, 1))

    def finish():
        dx0, dx1 = rows_of(2, memo['chosen'])
        gx_ref[...] = (dx0 + dx1 + memo['through']).astype(BF16)
        saves[1].start()

    n_dev = nz * ny * nx * nc

    def gate_grad():
        flatten(d_land, d_all)
        expert = iota((n_exp, 256), 0).astype(F32)
        codes = [plain_id(pair_rows(token_lanes(m_all, k, 0, n_dev // 4))) for k in range(2)]
        grads = [pair_rows(token_lanes(d_all, k, 0, n_dev // 4)) for k in range(2)]
        total = jnp.zeros((n_exp, x_all.shape[-1]), F32)
        zs = nz // 4 or 1
        for z0 in range(0, nz, zs):
            spread = []
            for p in range(z0 * ny, (z0 + zs) * ny):
                q = slice(p, p + 1)
                spread.append(jnp.where(expert == codes[0][q], grads[0][q], jnp.where(expert == codes[1][q], grads[1][q], 0.0)).astype(BF16))
            total += dot(jnp.concatenate(spread, axis=1), x_all[z0:z0 + zs].reshape(zs * ny * 256, x_all.shape[-1]), 1, 0)
        gate_ref[...] = total.T
        saves[2].start()

    d_plans = []
    moves = {'t': tok_plans, 'g': grad_plans, 'm': row_plan, 'y': ys, 'x': dxs, 'd': d_plans}
    works = {'f': [functools.partial(forward, i) for i in range(steps)], 'b': [functools.partial(backward, i) for i in range(steps)],
             'B': [functools.partial(backward_rows, i) for i in range(steps)], 'w': [functools.partial(weight_grad, k) for k in range(8)],
             'h': [read_rows], 'c': [combine], 'k': [gate_grad], 'e': [finish]}
    for turn in SCHEDULE:
        if turn in moves:
            advance(moves[turn])
        elif works[turn]:
            works[turn].pop(0)()
    for link in all_links:
        link.finish(pad, pad_row)
    for cp in saves:
        cp.wait()


def block_call(dims, tokens, grad_out, ids, w_gate, w1, w2):
    nz, ny, nx, nc = dims
    d_model, d_hidden = w1.shape
    n_tok = tokens.shape[0]
    n_dev = nz * ny * nx * nc
    n_row = n_dev * CAP
    tile = (CAP, 128)
    hbm = pl.BlockSpec(memory_space=pltpu.HBM)
    out = jax.ShapeDtypeStruct
    work = [(4, 4, nz), (4, 2, 4, nz), (2, 2, 2, nz), (4, 4, nz), (2, 4, nz // 2), (4, 4, nz), (nz, 3), (nz, 3), (nz, 4)]
    n_group = 4 * 10 + 4 + 4 * 11 + 4
    sems = [pltpu.SemaphoreType.DMA((10,)), pltpu.SemaphoreType.DMA((n_group,))]
    results = [(tokens.shape, BF16), (tokens.shape, BF16), ((d_model, n_dev), F32), ((d_model, d_hidden), F32), ((d_hidden, d_model), F32)]
    row = (1, 128)
    kept = [(tokens.shape, BF16), (tokens.shape, BF16), (ids.shape, jnp.int32), (w_gate.shape, BF16), (w1.shape, BF16), (w2.shape, BF16), (row, F32), (dims + row, F32),
            (dims + tokens.shape, BF16), (dims + tokens.shape, BF16), ((n_row, d_model), BF16), ((n_row, d_model), BF16), ((n_row, d_hidden), BF16), ((n_row, d_hidden), BF16), ((n_row, d_hidden), F32), ((n_dev, 128), F32), (tile, F32),
            (dims + row, F32), ((n_dev, 128), F32), ((1024,) + tile, BF16), ((n_dev,) + row, F32)]
    return pl.pallas_call(
        functools.partial(block_kernel, dims, (6, len(results), len(results), len(kept), 4, 4 * len(work), 3, len(sems))),
        out_shape=[out(*r) for r in results],
        in_specs=[hbm] * 6,
        out_specs=[hbm] * len(results),
        scratch_shapes=[pltpu.VMEM(*r) for r in results + kept] + [pltpu.VMEM((nc, nx, ny, nz) + tile, BF16)] * 4 + [pltpu.VMEM(w + tile, BF16) for w in work] * 4
        + [pltpu.SemaphoreType.DMA((k,)) for k in (8, 1, len(results))] + sems,
        compiler_params=pltpu.CompilerParams(collective_id=0, has_side_effects=True, vmem_limit_bytes=VMEM_LIMIT),
        name='block',
    )(tokens, grad_out, ids, w_gate, w1, w2)


VMEM_LIMIT = 67043328
SCHEDULE = 'mttmttmgttttgttgmth' + 'fggfgyfgyfy' + 'gygy' + 'bybybyBBxbyxBBxy' + 'wwxxwxwwxyc' + 'xwwdxdxwddkxe'


def pass_kernel(n, *refs):
    refs = iter(refs)
    given, passed, held, (load_sem, save_sem) = [list(itertools.islice(refs, k)) for k in (n, n, n, 2)]
    loads = [pltpu.make_async_copy(given[k], held[k], load_sem.at[k]) for k in range(n)]
    saves = [pltpu.make_async_copy(held[k], passed[k], save_sem.at[k]) for k in range(n)]
    for cp in loads:
        cp.start()
    for load, save in zip(loads, saves):
        load.wait()
        save.start()
    for cp in saves:
        cp.wait()


def pass_on(*arrays):
    n = len(arrays)
    return pl.pallas_call(
        functools.partial(pass_kernel, n),
        out_shape=[jax.ShapeDtypeStruct(v.shape, v.dtype) for v in arrays],
        in_specs=[pl.BlockSpec(memory_space=pltpu.HBM)] * n,
        out_specs=[pl.BlockSpec(memory_space=pltpu.HBM)] * n,
        scratch_shapes=[pltpu.VMEM(v.shape, v.dtype) for v in arrays] + [pltpu.SemaphoreType.DMA((n,))] * 2,
        compiler_params=pltpu.CompilerParams(vmem_limit_bytes=VMEM_LIMIT),
        name='pass_on',
    )(*arrays)


def local_block(dims, tokens, grad_out, expert_ids, w_gate, w_in, w_out):
    y_out, grad_x, grad_w_gate, g1, g2 = pass_on(*block_call(dims, tokens, grad_out, expert_ids.T, w_gate, w_in[0], w_out[0]))
    return y_out, grad_x, g1[None], g2[None], grad_w_gate


def solution(mesh):
    dims = (8, 4, 4, 2)
    return jax.shard_map(functools.partial(local_block, dims), mesh=mesh, in_specs=(P('ep'), P('ep'), P('ep'), P(), P('ep'), P('ep')), out_specs=(P('ep'), P('ep'), P('ep'), P('ep'), P()), check_vma=False)
```

```python
import functools
import itertools
import math

import jax
import jax.numpy as jnp
from jax import lax
from jax.experimental import pallas as pl
from jax.experimental.pallas import tpu as pltpu
from jax.sharding import PartitionSpec as P

MESH = pl.DeviceIdType.MESH
F32 = jnp.float32
BF16 = jnp.bfloat16
CAP = 8


def coords(dims):
    nz, ny, nx, nc = dims
    me = lax.axis_index('ep')
    c = lax.rem(me, nc)
    x = lax.rem(me // nc, nx)
    y = lax.rem(me // (nc * nx), ny)
    z = me // (nc * nx * ny)

    def dev(z, y, x, c):
        return (((z * ny + y) * nx + x) * nc + c,)

    return z, y, x, c, dev


def dot(a, b, ca, cb):
    return lax.dot_general(a, b, (((ca,), (cb,)), ((), ())), preferred_element_type=F32)


def iota(shape, axis):
    return lax.broadcasted_iota(jnp.int32, shape, axis)


def as_row(col):
    n = col.shape[0]
    return jnp.sum(jnp.where(iota((n, n), 0) == iota((n, n), 1), col, 0.0), axis=0, keepdims=True)


def as_col(row):
    n = row.shape[1]
    return jnp.sum(jnp.where(iota((n, n), 0) == iota((n, n), 1), row, 0.0), axis=1, keepdims=True)


def gates(tok, i0, i1, w_gate):
    logits = dot(tok, w_gate, 1, 0)
    expert = iota(logits.shape, 1).astype(F32)
    l0, l1 = (jnp.sum(jnp.where(expert == i, logits, 0.0), axis=1, keepdims=True) for i in (i0, i1))
    top = jnp.maximum(l0, l1)
    p0, p1 = jnp.exp(l0 - top), jnp.exp(l1 - top)
    total = p0 + p1
    return p0 / total, p1 / total


def choice_row(tok, ids, w_gate):
    r0, r1 = ids[0:1].astype(F32), ids[1:2].astype(F32)
    i0, i1 = as_col(r0), as_col(r1)
    g0, g1 = gates(tok, i0, i1, w_gate)

    def code(i):
        n = jnp.sum((i == r0).astype(F32) + (i == r1).astype(F32), axis=1, keepdims=True)
        return as_row(jnp.where(n > 1.5, i + 256.0, i))

    return jnp.concatenate([code(i0), code(i1), as_row(g0), as_row(g1)], axis=1)


def gelu_tanh(a):
    k = 0.7978845608028654
    sq = a * a
    return jnp.tanh(a * (k + (k * 0.044715) * sq)), sq


def gelu(a):
    half = 0.5 * a
    return half + half * gelu_tanh(a)[0]


def gelu_slope(a):
    k = 0.7978845608028654
    t, sq = gelu_tanh(a)
    return (0.5 + 0.5 * t) + (0.5 * a) * (1.0 - t * t) * (k + (3 * k * 0.044715) * sq)


def token_lanes(ref, k, start, n):
    lane = iota((n, 128), 1) // 32
    out = jnp.zeros((n, 128), F32)
    for j in range(4):
        r = ref[pl.ds(start + j, n, stride=4), :]
        out = jnp.where(lane == j, r if j == k else pltpu.roll(r, 32 * (j - k) % 128, 1), out)
    return out


def pair_rows(v):
    return jnp.concatenate([jnp.concatenate([v[2 * i:2 * i + 1], v[2 * i + 1:2 * i + 2]], axis=1) for i in range(v.shape[0] // 2)], axis=0)


def plain_id(code):
    return jnp.where(code >= 256.0, code - 256.0, code)


class Links:
    def __init__(self, send, recv, pool):
        self.send, self.recv, self.pool, self.bytes = send, recv, pool, 0

    def group(self):
        return self.recv.at[next(self.pool)]

    def go(self, src, dst, to, group):
        pltpu.make_async_remote_copy(src_ref=src, dst_ref=dst, send_sem=self.send, recv_sem=group, device_id=to, device_id_type=MESH).start()
        self.bytes += math.prod(src.shape) * jnp.dtype(src.dtype).itemsize

    def wait(self, group, ref):
        pltpu.make_async_copy(ref, ref, group).wait()

    def finish(self, *pads):
        for pad in pads:
            unit = math.prod(pad.shape[1:]) * jnp.dtype(pad.dtype).itemsize
            if self.bytes % unit == 0:
                return self.wait(self.send, pad.at[pl.ds(0, self.bytes // unit)])
        raise ValueError(self.bytes)


def block_kernel(dims, sizes, *refs):
    nz, ny, nx, nc = dims
    refs = iter(refs)
    refs = [list(itertools.islice(refs, n)) for n in sizes]
    (tok_hbm, dout_hbm, ids_hbm, wg_hbm, w1_hbm, w2_hbm), outs, held, kept, rows, areas, (load_sem, keep_sem, save_sem), sems = refs
    out_ref, gx_ref, gate_ref, g1_ref, g2_ref = held
    tok, dout, ids, wg, w1, w2, row, m_land, x_all, g_all, xs_ref, dys_ref, h_ref, da_ref, a_ref, m_all, hot_ref, d_land, d_all, pad, pad_row = kept
    z, y, x, c, dev = coords(dims)
    saves = [pltpu.make_async_copy(held[k], outs[k], save_sem.at[k]) for k in range(len(held))]

    def save(k, part):
        pltpu.make_async_copy(held[k].at[part], outs[k].at[part], save_sem.at[k]).start()

    send_sem, recv_sem = sems
    pool = itertools.count()
    all_links = [Links(send_sem.at[k], recv_sem, pool) for k in range(send_sem.shape[0])]
    links = iter(all_links)

    loads = [pltpu.make_async_copy(s, d, load_sem.at[k]) for k, (s, d) in enumerate(
        [(tok_hbm, x_all.at[z, y, x, c]), (dout_hbm, g_all.at[z, y, x, c]), (tok_hbm, tok), (ids_hbm, ids), (wg_hbm, wg), (dout_hbm, dout), (w1_hbm, w1), (w2_hbm, w2)])]
    for ld in loads:
        ld.start()
    peers = [dev(lax.rem(z + d, nz), y, x, c) for d in range(1, nz)]
    for d in (1, 2, 3):
        peers.append(dev(z, lax.rem(y + d, ny), x, c))
        peers.append(dev(z, y, lax.rem(x + d, nx), c))
    mate = dev(z, y, x, 1 - c)
    peers.append(mate)
    barrier = pltpu.get_barrier_semaphore()
    for peer in peers:
        pl.semaphore_signal(barrier, inc=1, device_id=peer, device_id_type=MESH)
    for ld in loads[2:5]:
        ld.wait()
    row[...] = choice_row(tok[...], ids[...], wg[...])
    place = pltpu.make_async_copy(row, m_land.at[z, y, x, c], keep_sem.at[0])
    place.start()
    loads[0].wait()
    loads[1].wait()
    place.wait()
    pl.semaphore_wait(barrier, len(peers))

    full = slice(None)
    by_distance = sorted(range(1, nz), key=lambda d: abs(d - nz // 2))

    def step(v, d, m=4):
        return lax.rem(v + d, m)

    def by_lines(link, ref, rows, x_last, late):
        p0, q0 = (y, x) if x_last else (x, y)
        low, high = pl.ds(0, nz // 2), pl.ds(nz // 2, nz // 2)

        def at(zs, p, q):
            return ref.at[(zs, p, q, c, rows) if x_last else (zs, q, p, c, rows)]

        def go(part, p, q, group):
            link.go(part, part, dev(z, p, q, c) if x_last else dev(z, q, p, c), group)

        in_z, in_p, in_m, in_f, in_r, in_c = [link.group() for _ in range(6)]
        line = at(full, p0, q0)

        def over(q):
            part = at(full, full, q)
            link.go(part, part, mate, in_c)

        own = at(z, p0, q0)
        for d in by_distance:
            link.go(own, own, dev(step(z, d, nz), y, x, c), in_z)
        yield
        link.wait(in_z, at(pl.ds(0, nz - 1), p0, q0))
        pm, pp, po = step(p0, 3), step(p0, 1), step(p0, 2)
        qm, qp, qo = step(q0, 3), step(q0, 1), step(q0, 2)
        qs = []

        def spread(p):
            part = at(full, p, q0)
            qs.append((p, link.group()))
            go(part, p0, qp, qs[-1][1])
            go(part, p0, qm, qs[-1][1])

        def relay(i):
            p, group = qs[i]
            link.wait(group, at(full, pl.ds(0, 2), q0))
            go(at(low, p, qm), p0, qp, in_r)
            go(at(high, p, qp), p0, qm, in_r)

        def pass_one():
            link.wait(in_p, line)
            go(at(low, pm, q0), pp, q0, in_f)
            link.wait(in_m, line)
            go(at(high, pp, q0), pm, q0, in_f)

        go(line, pp, q0, in_p)
        go(line, pm, q0, in_m)
        if late:
            yield
            pass_one()
            yield
            link.wait(in_f, line)
            for p in (p0, pm, pp, po):
                spread(p)
            over(q0)
            yield
            relay(0)
        else:
            yield
            spread(p0)
            yield
            pass_one()
            yield
            spread(pm)
            spread(pp)
            yield
            relay(0)
            yield
            link.wait(in_f, line)
            spread(po)
            over(q0)
        for i in range(1, 4):
            yield
            relay(i)
        over(qm)
        over(qp)
        yield
        link.wait(in_r, at(full, full, q0))
        over(qo)
        yield
        link.wait(in_c, ref.at[full, full, full, c, rows])

    def gather_rows(link, held, order):
        have = [z, y, x, c]
        for axis in order:
            size = (nz, ny, nx, nc)[axis]
            part = held.at[tuple(have)]
            group = link.group()
            for d in sorted(range(1, size), key=lambda d: abs(d - size // 2)):
                there = [z, y, x, c]
                there[axis] = lax.rem(there[axis] + d, size)
                link.go(part, part, dev(*there), group)
            have[axis] = pl.ds(0, size - 1)
            yield
            link.wait(group, held.at[tuple(have)])
            have[axis] = full

    def advance(plans):
        for g in plans:
            next(g, None)

    halves = [slice(0, 16), slice(16, 32)]
    tok_plans, grad_plans = [[by_lines(next(links), ref, half, half.start == 0, ref is g_all) for half in halves] for ref in (x_all, g_all)]
    row_plan = [gather_rows(next(links), m_land, range(4))]
    advance(row_plan + tok_plans + grad_plans)
    def flatten(land, flat):
        def lines(zz, carry):
            for k in range(ny * nx * nc):
                flat[pl.ds(zz * (ny * nx * nc) + k, 1), :] = land[zz, k // (nx * nc), k // nc % nx, k % nc]
            return carry

        lax.fori_loop(0, nz, lines, 0)


    me = lax.axis_index('ep').astype(F32)
    def read_rows():
        flatten(m_land, m_all)
        for ld in loads[5:]:
            ld.wait()
        code = m_all[...]
        left = jnp.where((iota(code.shape, 1) < 64) & (code >= 256.0), code - 256.0, 999.0)
        found = []
        for _ in range(3):
            best = jnp.min(jnp.min(left, axis=0, keepdims=True), axis=1, keepdims=True)
            left = jnp.where(left == best, 999.0, left)
            found.append(jnp.broadcast_to(best, (1, 128)))
        hot_ref[...] = jnp.concatenate(found + [jnp.full((5, 128), 999.0, F32)], axis=0)

    steps = 4 if nz == 8 else 1
    per = nz // steps
    n_quad = per * ny * nx * nc // 4
    n_pair = n_quad // 2
    n_slot = n_pair * 8 * CAP

    places = [(cc, xx, yy, zz) for cc in range(nc) for xx in range(nx) for yy in range(ny) for zz in range(per)]

    def select(i, ref, with_gate):
        c0, c1, g0, g1 = (pair_rows(token_lanes(m_all, k, pl.multiple_of(4 * n_quad * i, 4 * n_quad), n_quad)) for k in range(4))
        hit0, hit1 = plain_id(c0) == me, plain_id(c1) == me
        hit = (hit0 | hit1).astype(F32)
        gate = jnp.where(hit0, g0, 0.0) + jnp.where(hit1, g1, 0.0)
        before, after = iota((256, 256), 0), iota((256, 256), 1)
        tri = ((before < after) & (before // 32 == after // 32)).astype(F32).astype(BF16)
        rank = dot(hit.astype(BF16), tri, 1, 0)
        src = (iota((n_pair, 256), 1) // 32).astype(F32)
        key = jnp.where(hit > 0.0, src * CAP + rank, -1.0)
        slot = iota((8 * CAP, 256), 0).astype(F32)
        short, key_short, one = slot.astype(BF16), key.astype(BF16), jnp.ones((), BF16)
        parts = []
        for p in range(n_pair):
            sel = (slot == key[p:p + 1]).astype(F32) if with_gate else jnp.where(short == key_short[p:p + 1], one, one - one)
            v = dot(sel.astype(BF16), ref[i * per + p // ny, p % ny].reshape(256, 256), 1, 0)
            parts.append(v * jnp.sum(sel * gate[p:p + 1], axis=1, keepdims=True) if with_gate else v)
        return jnp.concatenate([parts[zz * ny + yy][CAP * (xx * nc + cc):CAP * (xx * nc + cc + 1)] for cc, xx, yy, zz in places], axis=0).astype(BF16)

    def put(i, v, to):
        for k, (cc, xx, yy, zz) in enumerate(places):
            for half in range(2):
                to[half][cc, xx, yy, i * per + zz] = v[CAP * k:CAP * (k + 1), 128 * half:128 * (half + 1)].astype(BF16)

    def forward(i):
        here = pl.ds(i * n_slot, n_slot)
        xs = select(i, x_all, False)
        a = dot(xs, w1[...], 1, 0)
        h = gelu(a).astype(BF16)
        xs_ref[here], h_ref[here], a_ref[here] = xs, h, a
        put(i, dot(h, w2[...], 1, 0), rows[:2])

    def backward(i):
        here = pl.ds(i * n_slot, n_slot)
        dys = select(i, g_all, True)
        dys_ref[here] = dys
        da_ref[here] = (dot(dys, w2[...], 1, 1) * gelu_slope(a_ref[here])).astype(BF16)

    def backward_rows(i):
        put(i, dot(da_ref[pl.ds(i * n_slot, n_slot)], w1[...], 1, 1), rows[2:])

    def back(i):
        h = rows[i]
        other, near, via, out2, via2, in2, out3, hot_land, cold_land = areas[9 * i:9 * i + 9]
        link = next(links)
        go = link.go
        in_c, in_e, in_h = [[link.group(), link.group()] for _ in range(3)]
        in_n, in_v, in_2, in_l, in_s = [link.group() for _ in range(5)]
        x_first = i % 2 == 0
        a, b = (x, y) if x_first else (y, x)

        def to(a, b):
            return dev(z, b, a, c) if x_first else dev(z, a, b, c)

        def index(lead, a, bs):
            return lead + ((a, bs) if x_first else (bs, a))

        up, dn, far = step(a, 1), step(a, 3), step(a, 2)
        lo, hi = pl.ds(0, 2), pl.ds(2, 2)
        parts = [pl.ds(0, nz // 2), pl.ds(nz // 2, nz // 2)]

        def start(k):
            zs = parts[k]
            go(h.at[1 - c, :, :, zs], other.at[:, :, zs], mate, in_c[k])
            spread(h, (c,), c, zs, in_e[k])

        def follow(k):
            link.wait(in_c[k], other.at[:, :, parts[k]])
            spread(other, (), 1 - c, parts[k], in_h[k])

        def spread(ref, lead, e, zs, group):
            go(ref.at[index(lead, far, lo) + (zs,)], via.at[0, e, :, zs], to(up, b), group)
            go(ref.at[index(lead, far, hi) + (zs,)], via.at[1, e, :, zs], to(dn, b), group)
            go(ref.at[index(lead, up, full) + (zs,)], near.at[a, e, :, zs], to(up, b), in_n)
            go(ref.at[index(lead, dn, full) + (zs,)], near.at[a, e, :, zs], to(dn, b), in_n)

        def relay(e, zs, group):
            link.wait(group, via.at[:, e, :, zs])
            go(via.at[0, e, :, zs], near.at[dn, e, lo, zs], to(up, b), in_n)
            go(via.at[1, e, :, zs], near.at[up, e, hi, zs], to(dn, b), in_n)

        start(0)
        yield
        follow(0)
        yield
        start(1)
        yield
        follow(1)
        yield
        relay(c, parts[0], in_e[0])
        relay(1 - c, parts[0], in_h[0])
        yield
        relay(c, parts[1], in_e[1])
        yield
        relay(1 - c, parts[1], in_h[1])
        yield
        link.wait(in_n, near.at[pl.ds(0, 3)])

        def expert(s, e):
            return ((z * ny + y) * nx + s) * nc + e if x_first else ((z * ny + s) * nx + x) * nc + e

        places = [(step(a, d), e) for d in range(4) for e in (c, 1 - c)]
        is_hot = [[(hot_ref[j:j + 1, :] == expert(s, e).astype(F32)).astype(F32) for s, e in places] for j in range(3)]
        wide = lambda v: jnp.broadcast_to(v, (8, 128))
        weight = [[wide(v).astype(BF16) for v in r] for r in is_hot]
        line = iota((8, 128), 0)
        mine = [(wide(is_hot[0][k] + is_hot[1][k] + is_hot[2][k]) < 0.5) & (line == s * nc + e) for k, (s, e) in enumerate(places)]

        def squeeze(bb):
            given = [h[index((c,), a, bb)], other[index((), a, bb)]] + [near[s, e, bb] for s, e in places[2:]]
            for j in range(3):
                out2[bb, j] = sum(given[k] * weight[j][k] for k in range(8))
            singles = jnp.zeros((nz, 8, 128), F32)
            for k in range(8):
                singles = jnp.where(mine[k], jnp.sum(given[k].astype(F32), axis=1, keepdims=True), singles)
            out2[bb, 3] = singles.astype(BF16)

        up, dn, far = step(b, 1), step(b, 3), step(b, 2)
        lo, hi = pl.ds(0, nz // 2), pl.ds(nz // 2, nz // 2)
        squeeze(far)
        squeeze(up)
        go(out2.at[far, :, lo], via2.at[0], to(a, up), in_v)
        go(out2.at[far, :, hi], via2.at[1], to(a, dn), in_v)
        squeeze(dn)
        go(out2.at[up], in2.at[b], to(a, up), in_2)
        squeeze(b)
        go(out2.at[dn], in2.at[b], to(a, dn), in_2)
        in2[b] = out2[b]
        yield
        link.wait(in_v, via2)
        go(via2.at[0], in2.at[dn, :, lo], to(a, up), in_2)
        go(via2.at[1], in2.at[up, :, hi], to(a, dn), in_2)
        yield
        link.wait(in_2, in2.at[pl.ds(0, 3)])
        for d in by_distance:
            zz = lax.rem(z + d, nz)
            go(in2.at[:, 3, zz], cold_land.at[z], dev(zz, y, x, c), in_s)
        for j in range(3):
            out3[:, j] = (in2[0, j] + in2[1, j]) + (in2[2, j] + in2[3, j])
        for d in by_distance:
            zz = lax.rem(z + d, nz)
            go(out3.at[zz], hot_land.at[z], dev(zz, y, x, c), in_l)
        cold_land[z] = in2[:, 3, z]
        hot_land[z] = out3[z]
        yield
        link.wait(in_s, cold_land.at[pl.ds(0, nz - 1)])
        link.wait(in_l, hot_land.at[pl.ds(0, nz - 1)])

    def weight_grad(k):
        if k % 2 == 0:
            part = slice(w2.shape[0] // 4 * (k // 2), w2.shape[0] // 4 * (k // 2 + 1))
            g2_ref[part, :] = dot(h_ref[:, part], dys_ref[...], 0, 0)
            save(4, (part, full))
        else:
            part = slice(w1.shape[1] // 4 * (k // 2), w1.shape[1] // 4 * (k // 2 + 1))
            g1_ref[:, part] = dot(xs_ref[...], da_ref[:, part], 0, 0)
            save(3, (full, part))

    ys, dxs = [back(0), back(1)], [back(2), back(3)]
    n_tok = tok.shape[0]
    memo = {}
    earlier = iota((n_tok, n_tok), 1) < iota((n_tok, n_tok), 0)
    n_exp = wg.shape[1]

    def where_from(i, r0, r1):
        rank = jnp.sum(jnp.where(earlier & ((i == r0) | (i == r1)), 1.0, 0.0), axis=1, keepdims=True)
        slot = jnp.full((n_tok, 1), -1.0, F32)
        for j in range(3):
            slot = jnp.where(i == hot_ref[j:j + 1, 0:1], CAP * j + rank, slot)
        e = i.astype(jnp.int32)
        core, xx, yy, zz = e % nc, (e // nc) % nx, (e // (nc * nx)) % ny, e // (nc * nx * ny)
        lane, single = iota((n_tok, n_exp), 1), slot < 0.0
        pick = lambda m: m.astype(F32).astype(BF16)
        return pick(iota((n_tok, 32), 1).astype(F32) == slot), (pick((lane == e) & single), pick((lane == ((zz * nx + xx) * ny + yy) * nc + core) & single))

    def rows_of(kind, chosen):
        parts = []
        for half in range(2):
            hot_land, cold_land = areas[9 * (kind + half) + 7:9 * (kind + half) + 9]
            hot = jnp.sum(hot_land[...].astype(F32), axis=0).reshape(24, 128)
            hot = jnp.concatenate([hot, jnp.zeros((8, 128), F32)], axis=0).astype(BF16)
            cold = cold_land[...].astype(F32).reshape(n_exp, 128).astype(BF16)
            parts.append([dot(by_slot, hot, 1, 0) + dot(by_place[half], cold, 1, 0) for by_slot, by_place in chosen])
        return [jnp.concatenate([parts[0][k], parts[1][k]], axis=1) for k in range(2)]

    def combine():
        r0, r1 = ids[0:1].astype(F32), ids[1:2].astype(F32)
        i0, i1 = as_col(r0), as_col(r1)
        g0, g1 = gates(tok[...], i0, i1, wg[...])
        chosen = [where_from(i, r0, r1) for i in (i0, i1)]
        y0, y1 = rows_of(0, chosen)
        grad = dout[...].astype(F32)
        dg0, dg1 = (jnp.sum(grad * v, axis=1, keepdims=True) for v in (y0, y1))
        mean = g0 * dg0 + g1 * dg1
        d0, d1 = ((g * (dg - mean)).astype(BF16).astype(F32) for g, dg in ((g0, dg0), (g1, dg1)))
        d_land[z, y, x, c] = jnp.concatenate([as_row(d0), as_row(d1), jnp.zeros((1, 2 * n_tok), F32)], axis=1)
        out_ref[...] = (g0 * y0 + g1 * y1).astype(BF16)
        saves[0].start()
        d_plans.append(gather_rows(next(links), d_land, range(4)))
        advance(d_plans)
        expert = iota((n_tok, n_exp), 1).astype(F32)
        spread = jnp.where(expert == i0, d0, jnp.where(expert == i1, d1, 0.0)).astype(BF16)
        memo.update(chosen=chosen, through=dot(spread, wg[...], 1, 1))

    def finish():
        dx0, dx1 = rows_of(2, memo['chosen'])
        gx_ref[...] = (dx0 + dx1 + memo['through']).astype(BF16)
        saves[1].start()

    n_dev = nz * ny * nx * nc

    def gate_grad():
        flatten(d_land, d_all)
        expert = iota((n_exp, 256), 0).astype(F32).astype(BF16)
        codes = [plain_id(pair_rows(token_lanes(m_all, k, 0, n_dev // 4))).astype(BF16) for k in range(2)]
        grads = [pair_rows(token_lanes(d_all, k, 0, n_dev // 4)).astype(BF16) for k in range(2)]
        none = jnp.zeros((), BF16)
        total = jnp.zeros((n_exp, x_all.shape[-1]), F32)
        zs = nz // 4 or 1
        for z0 in range(0, nz, zs):
            spread = []
            for p in range(z0 * ny, (z0 + zs) * ny):
                q = slice(p, p + 1)
                spread.append(jnp.where(expert == codes[0][q], grads[0][q], jnp.where(expert == codes[1][q], grads[1][q], none)))
            total += dot(jnp.concatenate(spread, axis=1), x_all[z0:z0 + zs].reshape(zs * ny * 256, x_all.shape[-1]), 1, 0)
        gate_ref[...] = total.T
        saves[2].start()

    d_plans = []
    moves = {'t': tok_plans, 'g': grad_plans, 'm': row_plan, 'y': ys, 'x': dxs, 'd': d_plans}
    works = {'f': [functools.partial(forward, i) for i in range(steps)], 'b': [functools.partial(backward, i) for i in range(steps)],
             'B': [functools.partial(backward_rows, i) for i in range(steps)], 'w': [functools.partial(weight_grad, k) for k in range(8)],
             'h': [read_rows], 'c': [combine], 'k': [gate_grad], 'e': [finish]}
    for turn in SCHEDULE:
        if turn in moves:
            advance(moves[turn])
        elif works[turn]:
            works[turn].pop(0)()
    for link in all_links:
        link.finish(pad, pad_row)
    for cp in saves:
        cp.wait()


def block_call(dims, tokens, grad_out, ids, w_gate, w1, w2):
    nz, ny, nx, nc = dims
    d_model, d_hidden = w1.shape
    n_tok = tokens.shape[0]
    n_dev = nz * ny * nx * nc
    n_row = n_dev * CAP
    tile = (CAP, 128)
    hbm = pl.BlockSpec(memory_space=pltpu.HBM)
    out = jax.ShapeDtypeStruct
    work = [(4, 4, nz), (4, 2, 4, nz), (2, 2, 2, nz), (4, 4, nz), (2, 4, nz // 2), (4, 4, nz), (nz, 3), (nz, 3), (nz, 4)]
    n_group = 4 * 10 + 4 + 4 * 11 + 4
    sems = [pltpu.SemaphoreType.DMA((10,)), pltpu.SemaphoreType.DMA((n_group,))]
    results = [(tokens.shape, BF16), (tokens.shape, BF16), ((d_model, n_dev), F32), ((d_model, d_hidden), F32), ((d_hidden, d_model), F32)]
    row = (1, 128)
    kept = [(tokens.shape, BF16), (tokens.shape, BF16), (ids.shape, jnp.int32), (w_gate.shape, BF16), (w1.shape, BF16), (w2.shape, BF16), (row, F32), (dims + row, F32),
            (dims + tokens.shape, BF16), (dims + tokens.shape, BF16), ((n_row, d_model), BF16), ((n_row, d_model), BF16), ((n_row, d_hidden), BF16), ((n_row, d_hidden), BF16), ((n_row, d_hidden), F32), ((n_dev, 128), F32), (tile, F32),
            (dims + row, F32), ((n_dev, 128), F32), ((1024,) + tile, BF16), ((n_dev,) + row, F32)]
    return pl.pallas_call(
        functools.partial(block_kernel, dims, (6, len(results), len(results), len(kept), 4, 4 * len(work), 3, len(sems))),
        out_shape=[out(*r) for r in results],
        in_specs=[hbm] * 6,
        out_specs=[hbm] * len(results),
        scratch_shapes=[pltpu.VMEM(*r) for r in results + kept] + [pltpu.VMEM((nc, nx, ny, nz) + tile, BF16)] * 4 + [pltpu.VMEM(w + tile, BF16) for w in work] * 4
        + [pltpu.SemaphoreType.DMA((k,)) for k in (8, 1, len(results))] + sems,
        compiler_params=pltpu.CompilerParams(collective_id=0, has_side_effects=True, vmem_limit_bytes=VMEM_LIMIT),
        name='block',
    )(tokens, grad_out, ids, w_gate, w1, w2)


VMEM_LIMIT = 67043328
SCHEDULE = 'mttmttmgttttgttgmth' + 'fggfgyfgyfy' + 'gygy' + 'bybybyBBxbyxBBxy' + 'wwxxwxwwxyc' + 'xwwdxdxwddkxe'


def pass_kernel(n, *refs):
    refs = iter(refs)
    given, passed, held, (load_sem, save_sem) = [list(itertools.islice(refs, k)) for k in (n, n, n, 2)]
    loads = [pltpu.make_async_copy(given[k], held[k], load_sem.at[k]) for k in range(n)]
    saves = [pltpu.make_async_copy(held[k], passed[k], save_sem.at[k]) for k in range(n)]
    for cp in loads:
        cp.start()
    for load, save in zip(loads, saves):
        load.wait()
        save.start()
    for cp in saves:
        cp.wait()


def pass_on(*arrays):
    n = len(arrays)
    return pl.pallas_call(
        functools.partial(pass_kernel, n),
        out_shape=[jax.ShapeDtypeStruct(v.shape, v.dtype) for v in arrays],
        in_specs=[pl.BlockSpec(memory_space=pltpu.HBM)] * n,
        out_specs=[pl.BlockSpec(memory_space=pltpu.HBM)] * n,
        scratch_shapes=[pltpu.VMEM(v.shape, v.dtype) for v in arrays] + [pltpu.SemaphoreType.DMA((n,))] * 2,
        compiler_params=pltpu.CompilerParams(vmem_limit_bytes=VMEM_LIMIT),
        name='pass_on',
    )(*arrays)


def local_block(dims, tokens, grad_out, expert_ids, w_gate, w_in, w_out):
    y_out, grad_x, grad_w_gate, g1, g2 = pass_on(*block_call(dims, tokens, grad_out, expert_ids.T, w_gate, w_in[0], w_out[0]))
    return y_out, grad_x, g1[None], g2[None], grad_w_gate


def solution(mesh):
    dims = (8, 4, 4, 2)
    return jax.shard_map(functools.partial(local_block, dims), mesh=mesh, in_specs=(P('ep'), P('ep'), P('ep'), P(), P('ep'), P('ep')), out_specs=(P('ep'), P('ep'), P('ep'), P('ep'), P()), check_vma=False)
```

```python
import functools
import itertools
import math

import jax
import jax.numpy as jnp
from jax import lax
from jax.experimental import pallas as pl
from jax.experimental.pallas import tpu as pltpu
from jax.sharding import PartitionSpec as P

MESH = pl.DeviceIdType.MESH
F32 = jnp.float32
BF16 = jnp.bfloat16
CAP = 8


def coords(dims):
    nz, ny, nx, nc = dims
    me = lax.axis_index('ep')
    c = lax.rem(me, nc)
    x = lax.rem(me // nc, nx)
    y = lax.rem(me // (nc * nx), ny)
    z = me // (nc * nx * ny)

    def dev(z, y, x, c):
        return (((z * ny + y) * nx + x) * nc + c,)

    return z, y, x, c, dev


def dot(a, b, ca, cb):
    return lax.dot_general(a, b, (((ca,), (cb,)), ((), ())), preferred_element_type=F32)


def iota(shape, axis):
    return lax.broadcasted_iota(jnp.int32, shape, axis)


def as_row(col):
    n = col.shape[0]
    return jnp.sum(jnp.where(iota((n, n), 0) == iota((n, n), 1), col, 0.0), axis=0, keepdims=True)


def as_col(row):
    n = row.shape[1]
    return jnp.sum(jnp.where(iota((n, n), 0) == iota((n, n), 1), row, 0.0), axis=1, keepdims=True)


def gates(tok, i0, i1, w_gate):
    logits = dot(tok, w_gate, 1, 0)
    expert = iota(logits.shape, 1).astype(F32)
    l0, l1 = (jnp.sum(jnp.where(expert == i, logits, 0.0), axis=1, keepdims=True) for i in (i0, i1))
    top = jnp.maximum(l0, l1)
    p0, p1 = jnp.exp(l0 - top), jnp.exp(l1 - top)
    total = p0 + p1
    return p0 / total, p1 / total


def choice_row(tok, ids, w_gate):
    r0, r1 = ids[0:1].astype(F32), ids[1:2].astype(F32)
    i0, i1 = as_col(r0), as_col(r1)
    g0, g1 = gates(tok, i0, i1, w_gate)

    def code(i):
        n = jnp.sum((i == r0).astype(F32) + (i == r1).astype(F32), axis=1, keepdims=True)
        return as_row(jnp.where(n > 1.5, i + 256.0, i))

    return jnp.concatenate([code(i0), code(i1), as_row(g0), as_row(g1)], axis=1)


def gelu_tanh(a):
    k = 0.7978845608028654
    sq = a * a
    return jnp.tanh(a * (k + (k * 0.044715) * sq)), sq


def gelu(a):
    half = 0.5 * a
    return half + half * gelu_tanh(a)[0]


def gelu_slope(a):
    k = 0.7978845608028654
    t, sq = gelu_tanh(a)
    return (0.5 + 0.5 * t) + (0.5 * a) * (1.0 - t * t) * (k + (3 * k * 0.044715) * sq)


def token_lanes(ref, k, start, n):
    lane = iota((n, 128), 1) // 32
    out = jnp.zeros((n, 128), F32)
    for j in range(4):
        r = ref[pl.ds(start + j, n, stride=4), :]
        out = jnp.where(lane == j, r if j == k else pltpu.roll(r, 32 * (j - k) % 128, 1), out)
    return out


def pair_rows(v):
    return jnp.concatenate([jnp.concatenate([v[2 * i:2 * i + 1], v[2 * i + 1:2 * i + 2]], axis=1) for i in range(v.shape[0] // 2)], axis=0)


def plain_id(code):
    return jnp.where(code >= 256.0, code - 256.0, code)


class Links:
    def __init__(self, send, recv, pool):
        self.send, self.recv, self.pool, self.bytes = send, recv, pool, 0

    def group(self):
        return self.recv.at[next(self.pool)]

    def go(self, src, dst, to, group):
        pltpu.make_async_remote_copy(src_ref=src, dst_ref=dst, send_sem=self.send, recv_sem=group, device_id=to, device_id_type=MESH).start()
        self.bytes += math.prod(src.shape) * jnp.dtype(src.dtype).itemsize

    def wait(self, group, ref):
        pltpu.make_async_copy(ref, ref, group).wait()

    def finish(self, *pads):
        for pad in pads:
            unit = math.prod(pad.shape[1:]) * jnp.dtype(pad.dtype).itemsize
            if self.bytes % unit == 0:
                return self.wait(self.send, pad.at[pl.ds(0, self.bytes // unit)])
        raise ValueError(self.bytes)


def block_kernel(dims, sizes, *refs):
    nz, ny, nx, nc = dims
    refs = iter(refs)
    refs = [list(itertools.islice(refs, n)) for n in sizes]
    (tok_hbm, dout_hbm, ids_hbm, wg_hbm, w1_hbm, w2_hbm), outs, held, kept, rows, areas, (load_sem, keep_sem, save_sem), sems = refs
    out_ref, gx_ref, gate_ref, g1_ref, g2_ref = held
    tok, dout, ids, wg, w1, w2, row, m_land, x_all, g_all, xs_ref, dys_ref, h_ref, da_ref, a_ref, m_all, hot_ref, d_land, d_all, pad, pad_row = kept
    z, y, x, c, dev = coords(dims)
    saves = [pltpu.make_async_copy(held[k], outs[k], save_sem.at[k]) for k in range(len(held))]

    def save(k, part):
        pltpu.make_async_copy(held[k].at[part], outs[k].at[part], save_sem.at[k]).start()

    send_sem, recv_sem = sems
    pool = itertools.count()
    all_links = [Links(send_sem.at[k], recv_sem, pool) for k in range(send_sem.shape[0])]
    links = iter(all_links)

    loads = [pltpu.make_async_copy(s, d, load_sem.at[k]) for k, (s, d) in enumerate(
        [(tok_hbm, x_all.at[z, y, x, c]), (dout_hbm, g_all.at[z, y, x, c]), (tok_hbm, tok), (ids_hbm, ids), (wg_hbm, wg), (dout_hbm, dout), (w1_hbm, w1), (w2_hbm, w2)])]
    for ld in loads:
        ld.start()
    peers = [dev(lax.rem(z + d, nz), y, x, c) for d in range(1, nz)]
    for d in (1, 2, 3):
        peers.append(dev(z, lax.rem(y + d, ny), x, c))
        peers.append(dev(z, y, lax.rem(x + d, nx), c))
    mate = dev(z, y, x, 1 - c)
    peers.append(mate)
    barrier = pltpu.get_barrier_semaphore()
    for peer in peers:
        pl.semaphore_signal(barrier, inc=1, device_id=peer, device_id_type=MESH)
    for ld in loads[2:5]:
        ld.wait()
    row[...] = choice_row(tok[...], ids[...], wg[...])
    place = pltpu.make_async_copy(row, m_land.at[z, y, x, c], keep_sem.at[0])
    place.start()
    loads[0].wait()
    loads[1].wait()
    place.wait()
    pl.semaphore_wait(barrier, len(peers))

    full = slice(None)
    by_distance = sorted(range(1, nz), key=lambda d: abs(d - nz // 2))

    def step(v, d, m=4):
        return lax.rem(v + d, m)

    def by_lines(link, ref, rows, x_last, late):
        p0, q0 = (y, x) if x_last else (x, y)
        low, high = pl.ds(0, nz // 2), pl.ds(nz // 2, nz // 2)

        def at(zs, p, q):
            return ref.at[(zs, p, q, c, rows) if x_last else (zs, q, p, c, rows)]

        def go(part, p, q, group):
            link.go(part, part, dev(z, p, q, c) if x_last else dev(z, q, p, c), group)

        in_z, in_p, in_m, in_f, in_r, in_c = [link.group() for _ in range(6)]
        line = at(full, p0, q0)

        def over(q):
            part = at(full, full, q)
            link.go(part, part, mate, in_c)

        own = at(z, p0, q0)
        for d in by_distance:
            link.go(own, own, dev(step(z, d, nz), y, x, c), in_z)
        yield
        link.wait(in_z, at(pl.ds(0, nz - 1), p0, q0))
        pm, pp, po = step(p0, 3), step(p0, 1), step(p0, 2)
        qm, qp, qo = step(q0, 3), step(q0, 1), step(q0, 2)
        qs = []

        def spread(p):
            part = at(full, p, q0)
            qs.append((p, link.group()))
            go(part, p0, qp, qs[-1][1])
            go(part, p0, qm, qs[-1][1])

        def relay(i):
            p, group = qs[i]
            link.wait(group, at(full, pl.ds(0, 2), q0))
            go(at(low, p, qm), p0, qp, in_r)
            go(at(high, p, qp), p0, qm, in_r)

        def pass_one():
            link.wait(in_p, line)
            go(at(low, pm, q0), pp, q0, in_f)
            link.wait(in_m, line)
            go(at(high, pp, q0), pm, q0, in_f)

        go(line, pp, q0, in_p)
        go(line, pm, q0, in_m)
        if late:
            yield
            pass_one()
            yield
            link.wait(in_f, line)
            for p in (p0, pm, pp, po):
                spread(p)
            over(q0)
            yield
            relay(0)
        else:
            yield
            spread(p0)
            yield
            pass_one()
            yield
            spread(pm)
            spread(pp)
            yield
            relay(0)
            yield
            link.wait(in_f, line)
            spread(po)
            over(q0)
        for i in range(1, 4):
            yield
            relay(i)
        over(qm)
        over(qp)
        yield
        link.wait(in_r, at(full, full, q0))
        over(qo)
        yield
        link.wait(in_c, ref.at[full, full, full, c, rows])

    def gather_rows(link, held, order):
        have = [z, y, x, c]
        for axis in order:
            size = (nz, ny, nx, nc)[axis]
            part = held.at[tuple(have)]
            group = link.group()
            for d in sorted(range(1, size), key=lambda d: abs(d - size // 2)):
                there = [z, y, x, c]
                there[axis] = lax.rem(there[axis] + d, size)
                link.go(part, part, dev(*there), group)
            have[axis] = pl.ds(0, size - 1)
            yield
            link.wait(group, held.at[tuple(have)])
            have[axis] = full

    def advance(plans):
        for g in plans:
            next(g, None)

    halves = [slice(0, 16), slice(16, 32)]
    tok_plans, grad_plans = [[by_lines(next(links), ref, half, half.start == 0, ref is g_all) for half in halves] for ref in (x_all, g_all)]
    row_plan = [gather_rows(next(links), m_land, range(4))]
    advance(row_plan + tok_plans + grad_plans)
    def flatten(land, flat):
        def lines(zz, carry):
            for k in range(ny * nx * nc):
                flat[pl.ds(zz * (ny * nx * nc) + k, 1), :] = land[zz, k // (nx * nc), k // nc % nx, k % nc]
            return carry

        lax.fori_loop(0, nz, lines, 0)


    me = lax.axis_index('ep').astype(F32)
    def read_rows():
        flatten(m_land, m_all)
        for ld in loads[5:]:
            ld.wait()
        code = m_all[...]
        left = jnp.where((iota(code.shape, 1) < 64) & (code >= 256.0), code - 256.0, 999.0)
        found = []
        for _ in range(3):
            best = jnp.min(jnp.min(left, axis=0, keepdims=True), axis=1, keepdims=True)
            left = jnp.where(left == best, 999.0, left)
            found.append(jnp.broadcast_to(best, (1, 128)))
        hot_ref[...] = jnp.concatenate(found + [jnp.full((5, 128), 999.0, F32)], axis=0)

    steps = 4 if nz == 8 else 1
    per = nz // steps
    n_quad = per * ny * nx * nc // 4
    n_pair = n_quad // 2
    n_slot = n_pair * 8 * CAP

    places = [(cc, xx, yy, zz) for cc in range(nc) for xx in range(nx) for yy in range(ny) for zz in range(per)]

    def select(i, ref, with_gate):
        c0, c1, g0, g1 = (pair_rows(token_lanes(m_all, k, pl.multiple_of(4 * n_quad * i, 4 * n_quad), n_quad)) for k in range(4))
        hit0, hit1 = plain_id(c0) == me, plain_id(c1) == me
        hit = (hit0 | hit1).astype(F32)
        gate = jnp.where(hit0, g0, 0.0) + jnp.where(hit1, g1, 0.0)
        before, after = iota((256, 256), 0), iota((256, 256), 1)
        tri = ((before < after) & (before // 32 == after // 32)).astype(F32).astype(BF16)
        rank = dot(hit.astype(BF16), tri, 1, 0)
        src = (iota((n_pair, 256), 1) // 32).astype(F32)
        key = jnp.where(hit > 0.0, src * CAP + rank, -1.0)
        slot = iota((8 * CAP, 256), 0).astype(F32)
        short, key_short, one = slot.astype(BF16), key.astype(BF16), jnp.ones((), BF16)
        parts = []
        for p in range(n_pair):
            sel = (slot == key[p:p + 1]).astype(F32) if with_gate else jnp.where(short == key_short[p:p + 1], one, one - one)
            v = dot(sel.astype(BF16), ref[i * per + p // ny, p % ny].reshape(256, 256), 1, 0)
            parts.append(v * jnp.sum(sel * gate[p:p + 1], axis=1, keepdims=True) if with_gate else v)
        return jnp.concatenate([parts[zz * ny + yy][CAP * (xx * nc + cc):CAP * (xx * nc + cc + 1)] for cc, xx, yy, zz in places], axis=0).astype(BF16)

    def put(i, v, to):
        for k, (cc, xx, yy, zz) in enumerate(places):
            for half in range(2):
                to[half][cc, xx, yy, i * per + zz] = v[CAP * k:CAP * (k + 1), 128 * half:128 * (half + 1)].astype(BF16)

    def forward(i):
        here = pl.ds(i * n_slot, n_slot)
        xs = select(i, x_all, False)
        a = dot(xs, w1[...], 1, 0)
        h = gelu(a).astype(BF16)
        xs_ref[here], h_ref[here], a_ref[here] = xs, h, a
        put(i, dot(h, w2[...], 1, 0), rows[:2])

    def backward(i):
        here = pl.ds(i * n_slot, n_slot)
        dys = select(i, g_all, True)
        dys_ref[here] = dys
        da_ref[here] = (dot(dys, w2[...], 1, 1) * gelu_slope(a_ref[here])).astype(BF16)

    def backward_rows(i):
        put(i, dot(da_ref[pl.ds(i * n_slot, n_slot)], w1[...], 1, 1), rows[2:])

    def back(i):
        h = rows[i]
        other, near, via, out2, via2, in2, out3, hot_land, cold_land = areas[9 * i:9 * i + 9]
        link = next(links)
        go = link.go
        in_c, in_e, in_h = [[link.group(), link.group()] for _ in range(3)]
        in_n, in_v, in_2, in_l, in_s = [link.group() for _ in range(5)]
        x_first = i % 2 == 0
        a, b = (x, y) if x_first else (y, x)

        def to(a, b):
            return dev(z, b, a, c) if x_first else dev(z, a, b, c)

        def index(lead, a, bs):
            return lead + ((a, bs) if x_first else (bs, a))

        up, dn, far = step(a, 1), step(a, 3), step(a, 2)
        lo, hi = pl.ds(0, 2), pl.ds(2, 2)
        parts = [pl.ds(0, nz // 2), pl.ds(nz // 2, nz // 2)]

        def start(k):
            zs = parts[k]
            go(h.at[1 - c, :, :, zs], other.at[:, :, zs], mate, in_c[k])
            spread(h, (c,), c, zs, in_e[k])

        def follow(k):
            link.wait(in_c[k], other.at[:, :, parts[k]])
            spread(other, (), 1 - c, parts[k], in_h[k])

        def spread(ref, lead, e, zs, group):
            go(ref.at[index(lead, far, lo) + (zs,)], via.at[0, e, :, zs], to(up, b), group)
            go(ref.at[index(lead, far, hi) + (zs,)], via.at[1, e, :, zs], to(dn, b), group)
            go(ref.at[index(lead, up, full) + (zs,)], near.at[a, e, :, zs], to(up, b), in_n)
            go(ref.at[index(lead, dn, full) + (zs,)], near.at[a, e, :, zs], to(dn, b), in_n)

        def relay(e, zs, group):
            link.wait(group, via.at[:, e, :, zs])
            go(via.at[0, e, :, zs], near.at[dn, e, lo, zs], to(up, b), in_n)
            go(via.at[1, e, :, zs], near.at[up, e, hi, zs], to(dn, b), in_n)

        start(0)
        yield
        follow(0)
        yield
        start(1)
        yield
        follow(1)
        yield
        relay(c, parts[0], in_e[0])
        relay(1 - c, parts[0], in_h[0])
        yield
        relay(c, parts[1], in_e[1])
        yield
        relay(1 - c, parts[1], in_h[1])
        yield
        link.wait(in_n, near.at[pl.ds(0, 3)])

        def expert(s, e):
            return ((z * ny + y) * nx + s) * nc + e if x_first else ((z * ny + s) * nx + x) * nc + e

        places = [(step(a, d), e) for d in range(4) for e in (c, 1 - c)]
        is_hot = [[(hot_ref[j:j + 1, :] == expert(s, e).astype(F32)).astype(F32) for s, e in places] for j in range(3)]
        wide = lambda v: jnp.broadcast_to(v, (8, 128))
        weight = [[wide(v).astype(BF16) for v in r] for r in is_hot]
        line = iota((8, 128), 0)
        mine = [(wide(is_hot[0][k] + is_hot[1][k] + is_hot[2][k]) < 0.5) & (line == s * nc + e) for k, (s, e) in enumerate(places)]

        def squeeze(bb):
            given = [h[index((c,), a, bb)], other[index((), a, bb)]] + [near[s, e, bb] for s, e in places[2:]]
            for j in range(3):
                out2[bb, j] = sum(given[k] * weight[j][k] for k in range(8))
            singles = jnp.zeros((nz, 8, 128), F32)
            for k in range(8):
                singles = jnp.where(mine[k], jnp.sum(given[k].astype(F32), axis=1, keepdims=True), singles)
            out2[bb, 3] = singles.astype(BF16)

        up, dn, far = step(b, 1), step(b, 3), step(b, 2)
        lo, hi = pl.ds(0, nz // 2), pl.ds(nz // 2, nz // 2)
        squeeze(far)
        squeeze(up)
        go(out2.at[far, :, lo], via2.at[0], to(a, up), in_v)
        go(out2.at[far, :, hi], via2.at[1], to(a, dn), in_v)
        squeeze(dn)
        go(out2.at[up], in2.at[b], to(a, up), in_2)
        squeeze(b)
        go(out2.at[dn], in2.at[b], to(a, dn), in_2)
        in2[b] = out2[b]
        yield
        link.wait(in_v, via2)
        go(via2.at[0], in2.at[dn, :, lo], to(a, up), in_2)
        go(via2.at[1], in2.at[up, :, hi], to(a, dn), in_2)
        yield
        link.wait(in_2, in2.at[pl.ds(0, 3)])
        for d in by_distance:
            zz = lax.rem(z + d, nz)
            go(in2.at[:, 3, zz], cold_land.at[z], dev(zz, y, x, c), in_s)
        for j in range(3):
            out3[:, j] = (in2[0, j] + in2[1, j]) + (in2[2, j] + in2[3, j])
        for d in by_distance:
            zz = lax.rem(z + d, nz)
            go(out3.at[zz], hot_land.at[z], dev(zz, y, x, c), in_l)
        cold_land[z] = in2[:, 3, z]
        hot_land[z] = out3[z]
        yield
        link.wait(in_s, cold_land.at[pl.ds(0, nz - 1)])
        link.wait(in_l, hot_land.at[pl.ds(0, nz - 1)])

    def weight_grad(k):
        if k % 2 == 0:
            part = slice(w2.shape[0] // 4 * (k // 2), w2.shape[0] // 4 * (k // 2 + 1))
            g2_ref[part, :] = dot(h_ref[:, part], dys_ref[...], 0, 0)
            save(4, (part, full))
        else:
            part = slice(w1.shape[1] // 4 * (k // 2), w1.shape[1] // 4 * (k // 2 + 1))
            g1_ref[:, part] = dot(xs_ref[...], da_ref[:, part], 0, 0)
            save(3, (full, part))

    ys, dxs = [back(0), back(1)], [back(2), back(3)]
    n_tok = tok.shape[0]
    memo = {}
    earlier = iota((n_tok, n_tok), 1) < iota((n_tok, n_tok), 0)
    n_exp = wg.shape[1]

    def where_from(i, r0, r1):
        rank = jnp.sum(jnp.where(earlier & ((i == r0) | (i == r1)), 1.0, 0.0), axis=1, keepdims=True)
        slot = jnp.full((n_tok, 1), -1.0, F32)
        for j in range(3):
            slot = jnp.where(i == hot_ref[j:j + 1, 0:1], CAP * j + rank, slot)
        e = i.astype(jnp.int32)
        core, xx, yy, zz = e % nc, (e // nc) % nx, (e // (nc * nx)) % ny, e // (nc * nx * ny)
        lane, single = iota((n_tok, n_exp), 1), slot < 0.0
        pick = lambda m: m.astype(F32).astype(BF16)
        return pick(iota((n_tok, 32), 1).astype(F32) == slot), (pick((lane == e) & single), pick((lane == ((zz * nx + xx) * ny + yy) * nc + core) & single))

    def rows_of(kind, chosen):
        parts = []
        for half in range(2):
            hot_land, cold_land = areas[9 * (kind + half) + 7:9 * (kind + half) + 9]
            hot = jnp.sum(hot_land[...].astype(F32), axis=0).reshape(24, 128)
            hot = jnp.concatenate([hot, jnp.zeros((8, 128), F32)], axis=0).astype(BF16)
            cold = cold_land[...].astype(F32).reshape(n_exp, 128).astype(BF16)
            parts.append([dot(by_slot, hot, 1, 0) + dot(by_place[half], cold, 1, 0) for by_slot, by_place in chosen])
        return [jnp.concatenate([parts[0][k], parts[1][k]], axis=1) for k in range(2)]

    def combine():
        r0, r1 = ids[0:1].astype(F32), ids[1:2].astype(F32)
        i0, i1 = as_col(r0), as_col(r1)
        g0, g1 = gates(tok[...], i0, i1, wg[...])
        chosen = [where_from(i, r0, r1) for i in (i0, i1)]
        y0, y1 = rows_of(0, chosen)
        grad = dout[...].astype(F32)
        dg0, dg1 = (jnp.sum(grad * v, axis=1, keepdims=True) for v in (y0, y1))
        mean = g0 * dg0 + g1 * dg1
        d0, d1 = ((g * (dg - mean)).astype(BF16).astype(F32) for g, dg in ((g0, dg0), (g1, dg1)))
        d_land[z, y, x, c] = jnp.concatenate([as_row(d0), as_row(d1), jnp.zeros((1, 2 * n_tok), F32)], axis=1)
        out_ref[...] = (g0 * y0 + g1 * y1).astype(BF16)
        saves[0].start()
        d_plans.append(gather_rows(next(links), d_land, range(4)))
        advance(d_plans)
        expert = iota((n_tok, n_exp), 1).astype(F32)
        spread = jnp.where(expert == i0, d0, jnp.where(expert == i1, d1, 0.0)).astype(BF16)
        memo.update(chosen=chosen, through=dot(spread, wg[...], 1, 1))

    def finish():
        dx0, dx1 = rows_of(2, memo['chosen'])
        gx_ref[...] = (dx0 + dx1 + memo['through']).astype(BF16)
        saves[1].start()

    n_dev = nz * ny * nx * nc

    def gate_grad():
        flatten(d_land, d_all)
        expert = iota((n_exp, 256), 0).astype(F32).astype(BF16)
        codes = [plain_id(pair_rows(token_lanes(m_all, k, 0, n_dev // 4))).astype(BF16) for k in range(2)]
        grads = [pair_rows(token_lanes(d_all, k, 0, n_dev // 4)).astype(BF16) for k in range(2)]
        none = jnp.zeros((), BF16)
        total = jnp.zeros((n_exp, x_all.shape[-1]), F32)
        zs = nz // 4 or 1
        for z0 in range(0, nz, zs):
            spread = []
            for p in range(z0 * ny, (z0 + zs) * ny):
                q = slice(p, p + 1)
                spread.append(jnp.where(expert == codes[0][q], grads[0][q], jnp.where(expert == codes[1][q], grads[1][q], none)))
            total += dot(jnp.concatenate(spread, axis=1), x_all[z0:z0 + zs].reshape(zs * ny * 256, x_all.shape[-1]), 1, 0)
        gate_ref[...] = total.T
        saves[2].start()

    d_plans = []
    moves = {'t': tok_plans, 'g': grad_plans, 'm': row_plan, 'y': ys, 'x': dxs, 'd': d_plans}
    works = {'f': [functools.partial(forward, i) for i in range(steps)], 'b': [functools.partial(backward, i) for i in range(steps)],
             'B': [functools.partial(backward_rows, i) for i in range(steps)], 'w': [functools.partial(weight_grad, k) for k in range(8)],
             'h': [read_rows], 'c': [combine], 'k': [gate_grad], 'e': [finish]}
    for turn in SCHEDULE:
        if turn in moves:
            advance(moves[turn])
        elif works[turn]:
            works[turn].pop(0)()
    for link in all_links:
        link.finish(pad, pad_row)
    for cp in saves:
        cp.wait()


def block_call(dims, tokens, grad_out, ids, w_gate, w1, w2):
    nz, ny, nx, nc = dims
    d_model, d_hidden = w1.shape
    n_tok = tokens.shape[0]
    n_dev = nz * ny * nx * nc
    n_row = n_dev * CAP
    tile = (CAP, 128)
    hbm = pl.BlockSpec(memory_space=pltpu.HBM)
    out = jax.ShapeDtypeStruct
    work = [(4, 4, nz), (4, 2, 4, nz), (2, 2, 2, nz), (4, 4, nz), (2, 4, nz // 2), (4, 4, nz), (nz, 3), (nz, 3), (nz, 4)]
    n_group = 4 * 10 + 4 + 4 * 11 + 4
    sems = [pltpu.SemaphoreType.DMA((10,)), pltpu.SemaphoreType.DMA((n_group,))]
    results = [(tokens.shape, BF16), (tokens.shape, BF16), ((d_model, n_dev), F32), ((d_model, d_hidden), F32), ((d_hidden, d_model), F32)]
    row = (1, 128)
    kept = [(tokens.shape, BF16), (tokens.shape, BF16), (ids.shape, jnp.int32), (w_gate.shape, BF16), (w1.shape, BF16), (w2.shape, BF16), (row, F32), (dims + row, F32),
            (dims + tokens.shape, BF16), (dims + tokens.shape, BF16), ((n_row, d_model), BF16), ((n_row, d_model), BF16), ((n_row, d_hidden), BF16), ((n_row, d_hidden), BF16), ((n_row, d_hidden), F32), ((n_dev, 128), F32), (tile, F32),
            (dims + row, F32), ((n_dev, 128), F32), ((1024,) + tile, BF16), ((n_dev,) + row, F32)]
    return pl.pallas_call(
        functools.partial(block_kernel, dims, (6, len(results), len(results), len(kept), 4, 4 * len(work), 3, len(sems))),
        out_shape=[out(*r) for r in results],
        in_specs=[hbm] * 6,
        out_specs=[hbm] * len(results),
        scratch_shapes=[pltpu.VMEM(*r) for r in results + kept] + [pltpu.VMEM((nc, nx, ny, nz) + tile, BF16)] * 4 + [pltpu.VMEM(w + tile, BF16) for w in work] * 4
        + [pltpu.SemaphoreType.DMA((k,)) for k in (8, 1, len(results))] + sems,
        compiler_params=pltpu.CompilerParams(collective_id=0, has_side_effects=True, vmem_limit_bytes=VMEM_LIMIT),
        name='block',
    )(tokens, grad_out, ids, w_gate, w1, w2)


VMEM_LIMIT = 67043328
SCHEDULE = 'mttmttmgttttgttgmth' + 'ffggyfggyfy' + 'gygy' + 'bybybyBBxbyxBBxy' + 'wwxxwxwwxyc' + 'xwwdxdxwddkxe'


def pass_kernel(n, *refs):
    refs = iter(refs)
    given, passed, held, (load_sem, save_sem) = [list(itertools.islice(refs, k)) for k in (n, n, n, 2)]
    loads = [pltpu.make_async_copy(given[k], held[k], load_sem.at[k]) for k in range(n)]
    saves = [pltpu.make_async_copy(held[k], passed[k], save_sem.at[k]) for k in range(n)]
    for cp in loads:
        cp.start()
    for load, save in zip(loads, saves):
        load.wait()
        save.start()
    for cp in saves:
        cp.wait()


def pass_on(*arrays):
    n = len(arrays)
    return pl.pallas_call(
        functools.partial(pass_kernel, n),
        out_shape=[jax.ShapeDtypeStruct(v.shape, v.dtype) for v in arrays],
        in_specs=[pl.BlockSpec(memory_space=pltpu.HBM)] * n,
        out_specs=[pl.BlockSpec(memory_space=pltpu.HBM)] * n,
        scratch_shapes=[pltpu.VMEM(v.shape, v.dtype) for v in arrays] + [pltpu.SemaphoreType.DMA((n,))] * 2,
        compiler_params=pltpu.CompilerParams(vmem_limit_bytes=VMEM_LIMIT),
        name='pass_on',
    )(*arrays)


def local_block(dims, tokens, grad_out, expert_ids, w_gate, w_in, w_out):
    y_out, grad_x, grad_w_gate, g1, g2 = pass_on(*block_call(dims, tokens, grad_out, expert_ids.T, w_gate, w_in[0], w_out[0]))
    return y_out, grad_x, g1[None], g2[None], grad_w_gate


def solution(mesh):
    dims = (8, 4, 4, 2)
    return jax.shard_map(functools.partial(local_block, dims), mesh=mesh, in_specs=(P('ep'), P('ep'), P('ep'), P(), P('ep'), P('ep')), out_specs=(P('ep'), P('ep'), P('ep'), P('ep'), P()), check_vma=False)
```

```python
import functools
import itertools
import math

import jax
import jax.numpy as jnp
from jax import lax
from jax.experimental import pallas as pl
from jax.experimental.pallas import tpu as pltpu
from jax.sharding import PartitionSpec as P

MESH = pl.DeviceIdType.MESH
F32 = jnp.float32
BF16 = jnp.bfloat16
CAP = 8


def coords(dims):
    nz, ny, nx, nc = dims
    me = lax.axis_index('ep')
    c = lax.rem(me, nc)
    x = lax.rem(me // nc, nx)
    y = lax.rem(me // (nc * nx), ny)
    z = me // (nc * nx * ny)

    def dev(z, y, x, c):
        return (((z * ny + y) * nx + x) * nc + c,)

    return z, y, x, c, dev


def dot(a, b, ca, cb):
    return lax.dot_general(a, b, (((ca,), (cb,)), ((), ())), preferred_element_type=F32)


def iota(shape, axis):
    return lax.broadcasted_iota(jnp.int32, shape, axis)


def as_row(col):
    n = col.shape[0]
    return jnp.sum(jnp.where(iota((n, n), 0) == iota((n, n), 1), col, 0.0), axis=0, keepdims=True)


def as_col(row):
    n = row.shape[1]
    return jnp.sum(jnp.where(iota((n, n), 0) == iota((n, n), 1), row, 0.0), axis=1, keepdims=True)


def gates(tok, i0, i1, w_gate):
    logits = dot(tok, w_gate, 1, 0)
    expert = iota(logits.shape, 1).astype(F32)
    l0, l1 = (jnp.sum(jnp.where(expert == i, logits, 0.0), axis=1, keepdims=True) for i in (i0, i1))
    top = jnp.maximum(l0, l1)
    p0, p1 = jnp.exp(l0 - top), jnp.exp(l1 - top)
    total = p0 + p1
    return p0 / total, p1 / total


def choice_row(tok, ids, w_gate):
    r0, r1 = ids[0:1].astype(F32), ids[1:2].astype(F32)
    i0, i1 = as_col(r0), as_col(r1)
    g0, g1 = gates(tok, i0, i1, w_gate)

    def code(i):
        n = jnp.sum((i == r0).astype(F32) + (i == r1).astype(F32), axis=1, keepdims=True)
        return as_row(jnp.where(n > 1.5, i + 256.0, i))

    return jnp.concatenate([code(i0), code(i1), as_row(g0), as_row(g1)], axis=1)


def gelu_tanh(a):
    k = 0.7978845608028654
    sq = a * a
    return jnp.tanh(a * (k + (k * 0.044715) * sq)), sq


def gelu(a):
    half = 0.5 * a
    return half + half * gelu_tanh(a)[0]


def gelu_slope(a):
    k = 0.7978845608028654
    t, sq = gelu_tanh(a)
    return (0.5 + 0.5 * t) + (0.5 * a) * (1.0 - t * t) * (k + (3 * k * 0.044715) * sq)


def token_lanes(ref, k, start, n):
    lane = iota((n, 128), 1) // 32
    out = jnp.zeros((n, 128), F32)
    for j in range(4):
        r = ref[pl.ds(start + j, n, stride=4), :]
        out = jnp.where(lane == j, r if j == k else pltpu.roll(r, 32 * (j - k) % 128, 1), out)
    return out


def pair_rows(v):
    return jnp.concatenate([jnp.concatenate([v[2 * i:2 * i + 1], v[2 * i + 1:2 * i + 2]], axis=1) for i in range(v.shape[0] // 2)], axis=0)


def plain_id(code):
    return jnp.where(code >= 256.0, code - 256.0, code)


class Links:
    def __init__(self, send, recv, pool):
        self.send, self.recv, self.pool, self.bytes = send, recv, pool, 0

    def group(self):
        return self.recv.at[next(self.pool)]

    def go(self, src, dst, to, group):
        pltpu.make_async_remote_copy(src_ref=src, dst_ref=dst, send_sem=self.send, recv_sem=group, device_id=to, device_id_type=MESH).start()
        self.bytes += math.prod(src.shape) * jnp.dtype(src.dtype).itemsize

    def wait(self, group, ref):
        pltpu.make_async_copy(ref, ref, group).wait()

    def finish(self, *pads):
        for pad in pads:
            unit = math.prod(pad.shape[1:]) * jnp.dtype(pad.dtype).itemsize
            if self.bytes % unit == 0:
                return self.wait(self.send, pad.at[pl.ds(0, self.bytes // unit)])
        raise ValueError(self.bytes)


def block_kernel(dims, sizes, *refs):
    nz, ny, nx, nc = dims
    refs = iter(refs)
    refs = [list(itertools.islice(refs, n)) for n in sizes]
    (tok_hbm, dout_hbm, ids_hbm, wg_hbm, w1_hbm, w2_hbm), outs, held, kept, rows, areas, (load_sem, keep_sem, save_sem), sems = refs
    out_ref, gx_ref, gate_ref, g1_ref, g2_ref = held
    tok, dout, ids, wg, w1, w2, row, m_land, x_all, g_all, xs_ref, dys_ref, h_ref, da_ref, a_ref, m_all, hot_ref, d_land, d_all, pad, pad_row = kept
    z, y, x, c, dev = coords(dims)
    saves = [pltpu.make_async_copy(held[k], outs[k], save_sem.at[k]) for k in range(len(held))]

    def save(k, part):
        pltpu.make_async_copy(held[k].at[part], outs[k].at[part], save_sem.at[k]).start()

    send_sem, recv_sem = sems
    pool = itertools.count()
    all_links = [Links(send_sem.at[k], recv_sem, pool) for k in range(send_sem.shape[0])]
    links = iter(all_links)

    loads = [pltpu.make_async_copy(s, d, load_sem.at[k]) for k, (s, d) in enumerate(
        [(tok_hbm, x_all.at[z, y, x, c]), (dout_hbm, g_all.at[z, y, x, c]), (tok_hbm, tok), (ids_hbm, ids), (wg_hbm, wg), (dout_hbm, dout), (w1_hbm, w1), (w2_hbm, w2)])]
    for ld in loads:
        ld.start()
    peers = [dev(lax.rem(z + d, nz), y, x, c) for d in range(1, nz)]
    for d in (1, 2, 3):
        peers.append(dev(z, lax.rem(y + d, ny), x, c))
        peers.append(dev(z, y, lax.rem(x + d, nx), c))
    mate = dev(z, y, x, 1 - c)
    peers.append(mate)
    barrier = pltpu.get_barrier_semaphore()
    for peer in peers:
        pl.semaphore_signal(barrier, inc=1, device_id=peer, device_id_type=MESH)
    for ld in loads[2:5]:
        ld.wait()
    row[...] = choice_row(tok[...], ids[...], wg[...])
    place = pltpu.make_async_copy(row, m_land.at[z, y, x, c], keep_sem.at[0])
    place.start()
    loads[0].wait()
    loads[1].wait()
    place.wait()
    pl.semaphore_wait(barrier, len(peers))

    full = slice(None)
    by_distance = sorted(range(1, nz), key=lambda d: abs(d - nz // 2))

    def step(v, d, m=4):
        return lax.rem(v + d, m)

    def by_lines(link, ref, rows, x_last, late):
        p0, q0 = (y, x) if x_last else (x, y)
        low, high = pl.ds(0, nz // 2), pl.ds(nz // 2, nz // 2)

        def at(zs, p, q):
            return ref.at[(zs, p, q, c, rows) if x_last else (zs, q, p, c, rows)]

        def go(part, p, q, group):
            link.go(part, part, dev(z, p, q, c) if x_last else dev(z, q, p, c), group)

        in_z, in_p, in_m, in_f, in_r, in_c = [link.group() for _ in range(6)]
        line = at(full, p0, q0)

        def over(q):
            part = at(full, full, q)
            link.go(part, part, mate, in_c)

        own = at(z, p0, q0)
        for d in by_distance:
            link.go(own, own, dev(step(z, d, nz), y, x, c), in_z)
        yield
        link.wait(in_z, at(pl.ds(0, nz - 1), p0, q0))
        pm, pp, po = step(p0, 3), step(p0, 1), step(p0, 2)
        qm, qp, qo = step(q0, 3), step(q0, 1), step(q0, 2)
        qs = []

        def spread(p):
            part = at(full, p, q0)
            qs.append((p, link.group()))
            go(part, p0, qp, qs[-1][1])
            go(part, p0, qm, qs[-1][1])

        def relay(i):
            p, group = qs[i]
            link.wait(group, at(full, pl.ds(0, 2), q0))
            go(at(low, p, qm), p0, qp, in_r)
            go(at(high, p, qp), p0, qm, in_r)

        def pass_one():
            link.wait(in_p, line)
            go(at(low, pm, q0), pp, q0, in_f)
            link.wait(in_m, line)
            go(at(high, pp, q0), pm, q0, in_f)

        go(line, pp, q0, in_p)
        go(line, pm, q0, in_m)
        if late:
            yield
            pass_one()
            yield
            link.wait(in_f, line)
            for p in (p0, pm, pp, po):
                spread(p)
            over(q0)
            yield
            relay(0)
        else:
            yield
            spread(p0)
            yield
            pass_one()
            yield
            spread(pm)
            spread(pp)
            yield
            relay(0)
            yield
            link.wait(in_f, line)
            spread(po)
            over(q0)
        for i in range(1, 4):
            yield
            relay(i)
        over(qm)
        over(qp)
        yield
        link.wait(in_r, at(full, full, q0))
        over(qo)
        yield
        link.wait(in_c, ref.at[full, full, full, c, rows])

    def gather_rows(link, held, order):
        have = [z, y, x, c]
        for axis in order:
            size = (nz, ny, nx, nc)[axis]
            part = held.at[tuple(have)]
            group = link.group()
            for d in sorted(range(1, size), key=lambda d: abs(d - size // 2)):
                there = [z, y, x, c]
                there[axis] = lax.rem(there[axis] + d, size)
                link.go(part, part, dev(*there), group)
            have[axis] = pl.ds(0, size - 1)
            yield
            link.wait(group, held.at[tuple(have)])
            have[axis] = full

    def advance(plans):
        for g in plans:
            next(g, None)

    halves = [slice(0, 16), slice(16, 32)]
    tok_plans, grad_plans = [[by_lines(next(links), ref, half, half.start == 0, ref is g_all) for half in halves] for ref in (x_all, g_all)]
    row_plan = [gather_rows(next(links), m_land, range(4))]
    advance(row_plan + tok_plans)
    def flatten(land, flat):
        def lines(zz, carry):
            for k in range(ny * nx * nc):
                flat[pl.ds(zz * (ny * nx * nc) + k, 1), :] = land[zz, k // (nx * nc), k // nc % nx, k % nc]
            return carry

        lax.fori_loop(0, nz, lines, 0)


    me = lax.axis_index('ep').astype(F32)
    def read_rows():
        flatten(m_land, m_all)
        for ld in loads[5:]:
            ld.wait()
        code = m_all[...]
        left = jnp.where((iota(code.shape, 1) < 64) & (code >= 256.0), code - 256.0, 999.0)
        found = []
        for _ in range(3):
            best = jnp.min(jnp.min(left, axis=0, keepdims=True), axis=1, keepdims=True)
            left = jnp.where(left == best, 999.0, left)
            found.append(jnp.broadcast_to(best, (1, 128)))
        hot_ref[...] = jnp.concatenate(found + [jnp.full((5, 128), 999.0, F32)], axis=0)

    steps = 4 if nz == 8 else 1
    per = nz // steps
    n_quad = per * ny * nx * nc // 4
    n_pair = n_quad // 2
    n_slot = n_pair * 8 * CAP

    places = [(cc, xx, yy, zz) for cc in range(nc) for xx in range(nx) for yy in range(ny) for zz in range(per)]

    def select(i, ref, with_gate):
        c0, c1, g0, g1 = (pair_rows(token_lanes(m_all, k, pl.multiple_of(4 * n_quad * i, 4 * n_quad), n_quad)) for k in range(4))
        hit0, hit1 = plain_id(c0) == me, plain_id(c1) == me
        hit = (hit0 | hit1).astype(F32)
        gate = jnp.where(hit0, g0, 0.0) + jnp.where(hit1, g1, 0.0)
        before, after = iota((256, 256), 0), iota((256, 256), 1)
        tri = ((before < after) & (before // 32 == after // 32)).astype(F32).astype(BF16)
        rank = dot(hit.astype(BF16), tri, 1, 0)
        src = (iota((n_pair, 256), 1) // 32).astype(F32)
        key = jnp.where(hit > 0.0, src * CAP + rank, -1.0)
        slot = iota((8 * CAP, 256), 0).astype(F32)
        short, key_short, one = slot.astype(BF16), key.astype(BF16), jnp.ones((), BF16)
        parts = []
        for p in range(n_pair):
            sel = (slot == key[p:p + 1]).astype(F32) if with_gate else jnp.where(short == key_short[p:p + 1], one, one - one)
            v = dot(sel.astype(BF16), ref[i * per + p // ny, p % ny].reshape(256, 256), 1, 0)
            parts.append(v * jnp.sum(sel * gate[p:p + 1], axis=1, keepdims=True) if with_gate else v)
        return jnp.concatenate([parts[zz * ny + yy][CAP * (xx * nc + cc):CAP * (xx * nc + cc + 1)] for cc, xx, yy, zz in places], axis=0).astype(BF16)

    def put(i, v, to):
        for k, (cc, xx, yy, zz) in enumerate(places):
            for half in range(2):
                to[half][cc, xx, yy, i * per + zz] = v[CAP * k:CAP * (k + 1), 128 * half:128 * (half + 1)].astype(BF16)

    def forward(i):
        here = pl.ds(i * n_slot, n_slot)
        xs = select(i, x_all, False)
        a = dot(xs, w1[...], 1, 0)
        h = gelu(a).astype(BF16)
        xs_ref[here], h_ref[here], a_ref[here] = xs, h, a
        put(i, dot(h, w2[...], 1, 0), rows[:2])

    def backward(i):
        here = pl.ds(i * n_slot, n_slot)
        dys = select(i, g_all, True)
        dys_ref[here] = dys
        da_ref[here] = (dot(dys, w2[...], 1, 1) * gelu_slope(a_ref[here])).astype(BF16)

    def backward_rows(i):
        put(i, dot(da_ref[pl.ds(i * n_slot, n_slot)], w1[...], 1, 1), rows[2:])

    def back(i):
        h = rows[i]
        other, near, via, out2, via2, in2, out3, hot_land, cold_land = areas[9 * i:9 * i + 9]
        link = next(links)
        go = link.go
        in_c, in_e, in_h = [[link.group(), link.group()] for _ in range(3)]
        in_n, in_v, in_2, in_l, in_s = [link.group() for _ in range(5)]
        x_first = i % 2 == 0
        a, b = (x, y) if x_first else (y, x)

        def to(a, b):
            return dev(z, b, a, c) if x_first else dev(z, a, b, c)

        def index(lead, a, bs):
            return lead + ((a, bs) if x_first else (bs, a))

        up, dn, far = step(a, 1), step(a, 3), step(a, 2)
        lo, hi = pl.ds(0, 2), pl.ds(2, 2)
        parts = [pl.ds(0, nz // 2), pl.ds(nz // 2, nz // 2)]

        def start(k):
            zs = parts[k]
            go(h.at[1 - c, :, :, zs], other.at[:, :, zs], mate, in_c[k])
            spread(h, (c,), c, zs, in_e[k])

        def follow(k):
            link.wait(in_c[k], other.at[:, :, parts[k]])
            spread(other, (), 1 - c, parts[k], in_h[k])

        def spread(ref, lead, e, zs, group):
            go(ref.at[index(lead, far, lo) + (zs,)], via.at[0, e, :, zs], to(up, b), group)
            go(ref.at[index(lead, far, hi) + (zs,)], via.at[1, e, :, zs], to(dn, b), group)
            go(ref.at[index(lead, up, full) + (zs,)], near.at[a, e, :, zs], to(up, b), in_n)
            go(ref.at[index(lead, dn, full) + (zs,)], near.at[a, e, :, zs], to(dn, b), in_n)

        def relay(e, zs, group):
            link.wait(group, via.at[:, e, :, zs])
            go(via.at[0, e, :, zs], near.at[dn, e, lo, zs], to(up, b), in_n)
            go(via.at[1, e, :, zs], near.at[up, e, hi, zs], to(dn, b), in_n)

        start(0)
        yield
        follow(0)
        yield
        start(1)
        yield
        follow(1)
        yield
        relay(c, parts[0], in_e[0])
        relay(1 - c, parts[0], in_h[0])
        yield
        relay(c, parts[1], in_e[1])
        yield
        relay(1 - c, parts[1], in_h[1])
        yield
        link.wait(in_n, near.at[pl.ds(0, 3)])

        def expert(s, e):
            return ((z * ny + y) * nx + s) * nc + e if x_first else ((z * ny + s) * nx + x) * nc + e

        places = [(step(a, d), e) for d in range(4) for e in (c, 1 - c)]
        is_hot = [[(hot_ref[j:j + 1, :] == expert(s, e).astype(F32)).astype(F32) for s, e in places] for j in range(3)]
        wide = lambda v: jnp.broadcast_to(v, (8, 128))
        weight = [[wide(v).astype(BF16) for v in r] for r in is_hot]
        line = iota((8, 128), 0)
        mine = [(wide(is_hot[0][k] + is_hot[1][k] + is_hot[2][k]) < 0.5) & (line == s * nc + e) for k, (s, e) in enumerate(places)]

        def squeeze(bb):
            given = [h[index((c,), a, bb)], other[index((), a, bb)]] + [near[s, e, bb] for s, e in places[2:]]
            for j in range(3):
                out2[bb, j] = sum(given[k] * weight[j][k] for k in range(8))
            singles = jnp.zeros((nz, 8, 128), F32)
            for k in range(8):
                singles = jnp.where(mine[k], jnp.sum(given[k].astype(F32), axis=1, keepdims=True), singles)
            out2[bb, 3] = singles.astype(BF16)

        up, dn, far = step(b, 1), step(b, 3), step(b, 2)
        lo, hi = pl.ds(0, nz // 2), pl.ds(nz // 2, nz // 2)
        squeeze(far)
        squeeze(up)
        go(out2.at[far, :, lo], via2.at[0], to(a, up), in_v)
        go(out2.at[far, :, hi], via2.at[1], to(a, dn), in_v)
        squeeze(dn)
        go(out2.at[up], in2.at[b], to(a, up), in_2)
        squeeze(b)
        go(out2.at[dn], in2.at[b], to(a, dn), in_2)
        in2[b] = out2[b]
        yield
        link.wait(in_v, via2)
        go(via2.at[0], in2.at[dn, :, lo], to(a, up), in_2)
        go(via2.at[1], in2.at[up, :, hi], to(a, dn), in_2)
        yield
        link.wait(in_2, in2.at[pl.ds(0, 3)])
        for d in by_distance:
            zz = lax.rem(z + d, nz)
            go(in2.at[:, 3, zz], cold_land.at[z], dev(zz, y, x, c), in_s)
        for j in range(3):
            out3[:, j] = (in2[0, j] + in2[1, j]) + (in2[2, j] + in2[3, j])
        for d in by_distance:
            zz = lax.rem(z + d, nz)
            go(out3.at[zz], hot_land.at[z], dev(zz, y, x, c), in_l)
        cold_land[z] = in2[:, 3, z]
        hot_land[z] = out3[z]
        yield
        link.wait(in_s, cold_land.at[pl.ds(0, nz - 1)])
        link.wait(in_l, hot_land.at[pl.ds(0, nz - 1)])

    def weight_grad(k):
        if k % 2 == 0:
            part = slice(w2.shape[0] // 4 * (k // 2), w2.shape[0] // 4 * (k // 2 + 1))
            g2_ref[part, :] = dot(h_ref[:, part], dys_ref[...], 0, 0)
            save(4, (part, full))
        else:
            part = slice(w1.shape[1] // 4 * (k // 2), w1.shape[1] // 4 * (k // 2 + 1))
            g1_ref[:, part] = dot(xs_ref[...], da_ref[:, part], 0, 0)
            save(3, (full, part))

    ys, dxs = [back(0), back(1)], [back(2), back(3)]
    n_tok = tok.shape[0]
    memo = {}
    earlier = iota((n_tok, n_tok), 1) < iota((n_tok, n_tok), 0)
    n_exp = wg.shape[1]

    def where_from(i, r0, r1):
        rank = jnp.sum(jnp.where(earlier & ((i == r0) | (i == r1)), 1.0, 0.0), axis=1, keepdims=True)
        slot = jnp.full((n_tok, 1), -1.0, F32)
        for j in range(3):
            slot = jnp.where(i == hot_ref[j:j + 1, 0:1], CAP * j + rank, slot)
        e = i.astype(jnp.int32)
        core, xx, yy, zz = e % nc, (e // nc) % nx, (e // (nc * nx)) % ny, e // (nc * nx * ny)
        lane, single = iota((n_tok, n_exp), 1), slot < 0.0
        pick = lambda m: m.astype(F32).astype(BF16)
        return pick(iota((n_tok, 32), 1).astype(F32) == slot), (pick((lane == e) & single), pick((lane == ((zz * nx + xx) * ny + yy) * nc + core) & single))

    def rows_of(kind, chosen):
        parts = []
        for half in range(2):
            hot_land, cold_land = areas[9 * (kind + half) + 7:9 * (kind + half) + 9]
            hot = jnp.sum(hot_land[...].astype(F32), axis=0).reshape(24, 128)
            hot = jnp.concatenate([hot, jnp.zeros((8, 128), F32)], axis=0).astype(BF16)
            cold = cold_land[...].astype(F32).reshape(n_exp, 128).astype(BF16)
            parts.append([dot(by_slot, hot, 1, 0) + dot(by_place[half], cold, 1, 0) for by_slot, by_place in chosen])
        return [jnp.concatenate([parts[0][k], parts[1][k]], axis=1) for k in range(2)]

    def combine():
        r0, r1 = ids[0:1].astype(F32), ids[1:2].astype(F32)
        i0, i1 = as_col(r0), as_col(r1)
        g0, g1 = gates(tok[...], i0, i1, wg[...])
        chosen = [where_from(i, r0, r1) for i in (i0, i1)]
        y0, y1 = rows_of(0, chosen)
        grad = dout[...].astype(F32)
        dg0, dg1 = (jnp.sum(grad * v, axis=1, keepdims=True) for v in (y0, y1))
        mean = g0 * dg0 + g1 * dg1
        d0, d1 = ((g * (dg - mean)).astype(BF16).astype(F32) for g, dg in ((g0, dg0), (g1, dg1)))
        d_land[z, y, x, c] = jnp.concatenate([as_row(d0), as_row(d1), jnp.zeros((1, 2 * n_tok), F32)], axis=1)
        out_ref[...] = (g0 * y0 + g1 * y1).astype(BF16)
        saves[0].start()
        d_plans.append(gather_rows(next(links), d_land, range(4)))
        advance(d_plans)
        expert = iota((n_tok, n_exp), 1).astype(F32)
        spread = jnp.where(expert == i0, d0, jnp.where(expert == i1, d1, 0.0)).astype(BF16)
        memo.update(chosen=chosen, through=dot(spread, wg[...], 1, 1))

    def finish():
        dx0, dx1 = rows_of(2, memo['chosen'])
        gx_ref[...] = (dx0 + dx1 + memo['through']).astype(BF16)
        saves[1].start()

    n_dev = nz * ny * nx * nc

    def gate_grad():
        flatten(d_land, d_all)
        expert = iota((n_exp, 256), 0).astype(F32).astype(BF16)
        codes = [plain_id(pair_rows(token_lanes(m_all, k, 0, n_dev // 4))).astype(BF16) for k in range(2)]
        grads = [pair_rows(token_lanes(d_all, k, 0, n_dev // 4)).astype(BF16) for k in range(2)]
        none = jnp.zeros((), BF16)
        total = jnp.zeros((n_exp, x_all.shape[-1]), F32)
        zs = nz // 4 or 1
        for z0 in range(0, nz, zs):
            spread = []
            for p in range(z0 * ny, (z0 + zs) * ny):
                q = slice(p, p + 1)
                spread.append(jnp.where(expert == codes[0][q], grads[0][q], jnp.where(expert == codes[1][q], grads[1][q], none)))
            total += dot(jnp.concatenate(spread, axis=1), x_all[z0:z0 + zs].reshape(zs * ny * 256, x_all.shape[-1]), 1, 0)
        gate_ref[...] = total.T
        saves[2].start()

    d_plans = []
    moves = {'t': tok_plans, 'g': grad_plans, 'm': row_plan, 'y': ys, 'x': dxs, 'd': d_plans}
    works = {'f': [functools.partial(forward, i) for i in range(steps)], 'b': [functools.partial(backward, i) for i in range(steps)],
             'B': [functools.partial(backward_rows, i) for i in range(steps)], 'w': [functools.partial(weight_grad, k) for k in range(8)],
             'h': [read_rows], 'c': [combine], 'k': [gate_grad], 'e': [finish]}
    for turn in SCHEDULE:
        if turn in moves:
            advance(moves[turn])
        elif works[turn]:
            works[turn].pop(0)()
    for link in all_links:
        link.finish(pad, pad_row)
    for cp in saves:
        cp.wait()


def block_call(dims, tokens, grad_out, ids, w_gate, w1, w2):
    nz, ny, nx, nc = dims
    d_model, d_hidden = w1.shape
    n_tok = tokens.shape[0]
    n_dev = nz * ny * nx * nc
    n_row = n_dev * CAP
    tile = (CAP, 128)
    hbm = pl.BlockSpec(memory_space=pltpu.HBM)
    out = jax.ShapeDtypeStruct
    work = [(4, 4, nz), (4, 2, 4, nz), (2, 2, 2, nz), (4, 4, nz), (2, 4, nz // 2), (4, 4, nz), (nz, 3), (nz, 3), (nz, 4)]
    n_group = 4 * 10 + 4 + 4 * 11 + 4
    sems = [pltpu.SemaphoreType.DMA((10,)), pltpu.SemaphoreType.DMA((n_group,))]
    results = [(tokens.shape, BF16), (tokens.shape, BF16), ((d_model, n_dev), F32), ((d_model, d_hidden), F32), ((d_hidden, d_model), F32)]
    row = (1, 128)
    kept = [(tokens.shape, BF16), (tokens.shape, BF16), (ids.shape, jnp.int32), (w_gate.shape, BF16), (w1.shape, BF16), (w2.shape, BF16), (row, F32), (dims + row, F32),
            (dims + tokens.shape, BF16), (dims + tokens.shape, BF16), ((n_row, d_model), BF16), ((n_row, d_model), BF16), ((n_row, d_hidden), BF16), ((n_row, d_hidden), BF16), ((n_row, d_hidden), F32), ((n_dev, 128), F32), (tile, F32),
            (dims + row, F32), ((n_dev, 128), F32), ((1024,) + tile, BF16), ((n_dev,) + row, F32)]
    return pl.pallas_call(
        functools.partial(block_kernel, dims, (6, len(results), len(results), len(kept), 4, 4 * len(work), 3, len(sems))),
        out_shape=[out(*r) for r in results],
        in_specs=[hbm] * 6,
        out_specs=[hbm] * len(results),
        scratch_shapes=[pltpu.VMEM(*r) for r in results + kept] + [pltpu.VMEM((nc, nx, ny, nz) + tile, BF16)] * 4 + [pltpu.VMEM(w + tile, BF16) for w in work] * 4
        + [pltpu.SemaphoreType.DMA((k,)) for k in (8, 1, len(results))] + sems,
        compiler_params=pltpu.CompilerParams(collective_id=0, has_side_effects=True, vmem_limit_bytes=VMEM_LIMIT),
        name='block',
    )(tokens, grad_out, ids, w_gate, w1, w2)


VMEM_LIMIT = 67043328
SCHEDULE = 'mtgtmttmgttttgttgmth' + 'ffggyfggyfy' + 'gygy' + 'bybybyBBxbyxBBxy' + 'wwxxwxwwxyc' + 'xwwdxdxwddkxe'


def pass_kernel(n, *refs):
    refs = iter(refs)
    given, passed, held, (load_sem, save_sem) = [list(itertools.islice(refs, k)) for k in (n, n, n, 2)]
    loads = [pltpu.make_async_copy(given[k], held[k], load_sem.at[k]) for k in range(n)]
    saves = [pltpu.make_async_copy(held[k], passed[k], save_sem.at[k]) for k in range(n)]
    for cp in loads:
        cp.start()
    for load, save in zip(loads, saves):
        load.wait()
        save.start()
    for cp in saves:
        cp.wait()


def pass_on(*arrays):
    n = len(arrays)
    return pl.pallas_call(
        functools.partial(pass_kernel, n),
        out_shape=[jax.ShapeDtypeStruct(v.shape, v.dtype) for v in arrays],
        in_specs=[pl.BlockSpec(memory_space=pltpu.HBM)] * n,
        out_specs=[pl.BlockSpec(memory_space=pltpu.HBM)] * n,
        scratch_shapes=[pltpu.VMEM(v.shape, v.dtype) for v in arrays] + [pltpu.SemaphoreType.DMA((n,))] * 2,
        compiler_params=pltpu.CompilerParams(vmem_limit_bytes=VMEM_LIMIT),
        name='pass_on',
    )(*arrays)


def local_block(dims, tokens, grad_out, expert_ids, w_gate, w_in, w_out):
    y_out, grad_x, grad_w_gate, g1, g2 = pass_on(*block_call(dims, tokens, grad_out, expert_ids.T, w_gate, w_in[0], w_out[0]))
    return y_out, grad_x, g1[None], g2[None], grad_w_gate


def solution(mesh):
    dims = (8, 4, 4, 2)
    return jax.shard_map(functools.partial(local_block, dims), mesh=mesh, in_specs=(P('ep'), P('ep'), P('ep'), P(), P('ep'), P('ep')), out_specs=(P('ep'), P('ep'), P('ep'), P('ep'), P()), check_vma=False)
```

```python
import functools
import itertools
import math

import jax
import jax.numpy as jnp
from jax import lax
from jax.experimental import pallas as pl
from jax.experimental.pallas import tpu as pltpu
from jax.sharding import PartitionSpec as P

MESH = pl.DeviceIdType.MESH
F32 = jnp.float32
BF16 = jnp.bfloat16
CAP = 8


def coords(dims):
    nz, ny, nx, nc = dims
    me = lax.axis_index('ep')
    c = lax.rem(me, nc)
    x = lax.rem(me // nc, nx)
    y = lax.rem(me // (nc * nx), ny)
    z = me // (nc * nx * ny)

    def dev(z, y, x, c):
        return (((z * ny + y) * nx + x) * nc + c,)

    return z, y, x, c, dev


def dot(a, b, ca, cb):
    return lax.dot_general(a, b, (((ca,), (cb,)), ((), ())), preferred_element_type=F32)


def iota(shape, axis):
    return lax.broadcasted_iota(jnp.int32, shape, axis)


def as_row(col):
    n = col.shape[0]
    return jnp.sum(jnp.where(iota((n, n), 0) == iota((n, n), 1), col, 0.0), axis=0, keepdims=True)


def as_col(row):
    n = row.shape[1]
    return jnp.sum(jnp.where(iota((n, n), 0) == iota((n, n), 1), row, 0.0), axis=1, keepdims=True)


def gates(tok, i0, i1, w_gate):
    logits = dot(tok, w_gate, 1, 0)
    expert = iota(logits.shape, 1).astype(F32)
    l0, l1 = (jnp.sum(jnp.where(expert == i, logits, 0.0), axis=1, keepdims=True) for i in (i0, i1))
    top = jnp.maximum(l0, l1)
    p0, p1 = jnp.exp(l0 - top), jnp.exp(l1 - top)
    total = p0 + p1
    return p0 / total, p1 / total


def choice_row(tok, ids, w_gate):
    r0, r1 = ids[0:1].astype(F32), ids[1:2].astype(F32)
    i0, i1 = as_col(r0), as_col(r1)
    g0, g1 = gates(tok, i0, i1, w_gate)

    def code(i):
        n = jnp.sum((i == r0).astype(F32) + (i == r1).astype(F32), axis=1, keepdims=True)
        return as_row(jnp.where(n > 1.5, i + 256.0, i))

    return jnp.concatenate([code(i0), code(i1), as_row(g0), as_row(g1)], axis=1)


def gelu_tanh(a):
    k = 0.7978845608028654
    sq = a * a
    return jnp.tanh(a * (k + (k * 0.044715) * sq)), sq


def gelu(a):
    half = 0.5 * a
    return half + half * gelu_tanh(a)[0]


def gelu_slope(a):
    k = 0.7978845608028654
    t, sq = gelu_tanh(a)
    return (0.5 + 0.5 * t) + (0.5 * a) * (1.0 - t * t) * (k + (3 * k * 0.044715) * sq)


def token_lanes(ref, k, start, n):
    lane = iota((n, 128), 1) // 32
    out = jnp.zeros((n, 128), F32)
    for j in range(4):
        r = ref[pl.ds(start + j, n, stride=4), :]
        out = jnp.where(lane == j, r if j == k else pltpu.roll(r, 32 * (j - k) % 128, 1), out)
    return out


def pair_rows(v):
    return jnp.concatenate([jnp.concatenate([v[2 * i:2 * i + 1], v[2 * i + 1:2 * i + 2]], axis=1) for i in range(v.shape[0] // 2)], axis=0)


def plain_id(code):
    return jnp.where(code >= 256.0, code - 256.0, code)


class Links:
    def __init__(self, send, recv, pool):
        self.send, self.recv, self.pool, self.bytes = send, recv, pool, 0

    def group(self):
        return self.recv.at[next(self.pool)]

    def go(self, src, dst, to, group):
        pltpu.make_async_remote_copy(src_ref=src, dst_ref=dst, send_sem=self.send, recv_sem=group, device_id=to, device_id_type=MESH).start()
        self.bytes += math.prod(src.shape) * jnp.dtype(src.dtype).itemsize

    def wait(self, group, ref):
        pltpu.make_async_copy(ref, ref, group).wait()

    def finish(self, *pads):
        for pad in pads:
            unit = math.prod(pad.shape[1:]) * jnp.dtype(pad.dtype).itemsize
            if self.bytes % unit == 0:
                return self.wait(self.send, pad.at[pl.ds(0, self.bytes // unit)])
        raise ValueError(self.bytes)


def block_kernel(dims, sizes, *refs):
    nz, ny, nx, nc = dims
    refs = iter(refs)
    refs = [list(itertools.islice(refs, n)) for n in sizes]
    (tok_hbm, dout_hbm, ids_hbm, wg_hbm, w1_hbm, w2_hbm), outs, held, kept, rows, areas, (load_sem, keep_sem, save_sem), sems = refs
    out_ref, gx_ref, gate_ref, g1_ref, g2_ref = held
    tok, dout, ids, wg, w1, w2, row, m_land, x_all, g_all, xs_ref, dys_ref, h_ref, da_ref, a_ref, m_all, hot_ref, d_land, d_all, pad, pad_row = kept
    z, y, x, c, dev = coords(dims)
    saves = [pltpu.make_async_copy(held[k], outs[k], save_sem.at[k]) for k in range(len(held))]

    def save(k, part):
        pltpu.make_async_copy(held[k].at[part], outs[k].at[part], save_sem.at[k]).start()

    send_sem, recv_sem = sems
    pool = itertools.count()
    all_links = [Links(send_sem.at[k], recv_sem, pool) for k in range(send_sem.shape[0])]
    links = iter(all_links)

    loads = [pltpu.make_async_copy(s, d, load_sem.at[k]) for k, (s, d) in enumerate(
        [(tok_hbm, x_all.at[z, y, x, c]), (dout_hbm, g_all.at[z, y, x, c]), (tok_hbm, tok), (ids_hbm, ids), (wg_hbm, wg), (dout_hbm, dout), (w1_hbm, w1), (w2_hbm, w2)])]
    for ld in loads:
        ld.start()
    peers = [dev(lax.rem(z + d, nz), y, x, c) for d in range(1, nz)]
    for d in (1, 2, 3):
        peers.append(dev(z, lax.rem(y + d, ny), x, c))
        peers.append(dev(z, y, lax.rem(x + d, nx), c))
    mate = dev(z, y, x, 1 - c)
    peers.append(mate)
    barrier = pltpu.get_barrier_semaphore()
    for peer in peers:
        pl.semaphore_signal(barrier, inc=1, device_id=peer, device_id_type=MESH)
    for ld in loads[2:5]:
        ld.wait()
    row[...] = choice_row(tok[...], ids[...], wg[...])
    place = pltpu.make_async_copy(row, m_land.at[z, y, x, c], keep_sem.at[0])
    place.start()
    loads[0].wait()
    loads[1].wait()
    place.wait()
    pl.semaphore_wait(barrier, len(peers))

    full = slice(None)
    by_distance = sorted(range(1, nz), key=lambda d: abs(d - nz // 2))

    def step(v, d, m=4):
        return lax.rem(v + d, m)

    def by_lines(link, ref, rows, x_last, late):
        p0, q0 = (y, x) if x_last else (x, y)
        low, high = pl.ds(0, nz // 2), pl.ds(nz // 2, nz // 2)

        def at(zs, p, q):
            return ref.at[(zs, p, q, c, rows) if x_last else (zs, q, p, c, rows)]

        def go(part, p, q, group):
            link.go(part, part, dev(z, p, q, c) if x_last else dev(z, q, p, c), group)

        in_z, in_p, in_m, in_f, in_r, in_c = [link.group() for _ in range(6)]
        line = at(full, p0, q0)

        def over(q):
            part = at(full, full, q)
            link.go(part, part, mate, in_c)

        own = at(z, p0, q0)
        for d in by_distance:
            link.go(own, own, dev(step(z, d, nz), y, x, c), in_z)
        yield
        link.wait(in_z, at(pl.ds(0, nz - 1), p0, q0))
        pm, pp, po = step(p0, 3), step(p0, 1), step(p0, 2)
        qm, qp, qo = step(q0, 3), step(q0, 1), step(q0, 2)
        qs = []

        def spread(p):
            part = at(full, p, q0)
            qs.append((p, link.group()))
            go(part, p0, qp, qs[-1][1])
            go(part, p0, qm, qs[-1][1])

        def relay(i):
            p, group = qs[i]
            link.wait(group, at(full, pl.ds(0, 2), q0))
            go(at(low, p, qm), p0, qp, in_r)
            go(at(high, p, qp), p0, qm, in_r)

        def pass_one():
            link.wait(in_p, line)
            go(at(low, pm, q0), pp, q0, in_f)
            link.wait(in_m, line)
            go(at(high, pp, q0), pm, q0, in_f)

        go(line, pp, q0, in_p)
        go(line, pm, q0, in_m)
        if late:
            yield
            pass_one()
            yield
            link.wait(in_f, line)
            for p in (p0, pm, pp, po):
                spread(p)
            over(q0)
            yield
            relay(0)
        else:
            yield
            spread(p0)
            yield
            pass_one()
            yield
            spread(pm)
            spread(pp)
            yield
            relay(0)
            yield
            link.wait(in_f, line)
            spread(po)
            over(q0)
        for i in range(1, 4):
            yield
            relay(i)
        over(qm)
        over(qp)
        yield
        link.wait(in_r, at(full, full, q0))
        over(qo)
        yield
        link.wait(in_c, ref.at[full, full, full, c, rows])

    def gather_rows(link, held, order):
        have = [z, y, x, c]
        for axis in order:
            size = (nz, ny, nx, nc)[axis]
            part = held.at[tuple(have)]
            group = link.group()
            for d in sorted(range(1, size), key=lambda d: abs(d - size // 2)):
                there = [z, y, x, c]
                there[axis] = lax.rem(there[axis] + d, size)
                link.go(part, part, dev(*there), group)
            have[axis] = pl.ds(0, size - 1)
            yield
            link.wait(group, held.at[tuple(have)])
            have[axis] = full

    def advance(plans):
        for g in plans:
            next(g, None)

    halves = [slice(0, 16), slice(16, 32)]
    tok_plans, grad_plans = [[by_lines(next(links), ref, half, half.start == 0, ref is g_all) for half in halves] for ref in (x_all, g_all)]
    row_plan = [gather_rows(next(links), m_land, range(4))]
    advance(row_plan + tok_plans)
    def flatten(land, flat):
        def lines(zz, carry):
            for k in range(ny * nx * nc):
                flat[pl.ds(zz * (ny * nx * nc) + k, 1), :] = land[zz, k // (nx * nc), k // nc % nx, k % nc]
            return carry

        lax.fori_loop(0, nz, lines, 0)


    me = lax.axis_index('ep').astype(F32)
    def read_rows():
        flatten(m_land, m_all)
        for ld in loads[5:]:
            ld.wait()
        code = m_all[...]
        left = jnp.where((iota(code.shape, 1) < 64) & (code >= 256.0), code - 256.0, 999.0)
        found = []
        for _ in range(3):
            best = jnp.min(jnp.min(left, axis=0, keepdims=True), axis=1, keepdims=True)
            left = jnp.where(left == best, 999.0, left)
            found.append(jnp.broadcast_to(best, (1, 128)))
        hot_ref[...] = jnp.concatenate(found + [jnp.full((5, 128), 999.0, F32)], axis=0)

    steps = 4 if nz == 8 else 1
    per = nz // steps
    n_quad = per * ny * nx * nc // 4
    n_pair = n_quad // 2
    n_slot = n_pair * 8 * CAP

    places = [(cc, xx, yy, zz) for cc in range(nc) for xx in range(nx) for yy in range(ny) for zz in range(per)]

    def select(i, ref, with_gate):
        c0, c1, g0, g1 = (pair_rows(token_lanes(m_all, k, pl.multiple_of(4 * n_quad * i, 4 * n_quad), n_quad)) for k in range(4))
        hit0, hit1 = plain_id(c0) == me, plain_id(c1) == me
        hit = (hit0 | hit1).astype(F32)
        gate = jnp.where(hit0, g0, 0.0) + jnp.where(hit1, g1, 0.0)
        before, after = iota((256, 256), 0), iota((256, 256), 1)
        tri = ((before < after) & (before // 32 == after // 32)).astype(F32).astype(BF16)
        rank = dot(hit.astype(BF16), tri, 1, 0)
        src = (iota((n_pair, 256), 1) // 32).astype(F32)
        key = jnp.where(hit > 0.0, src * CAP + rank, -1.0)
        slot = iota((8 * CAP, 256), 0).astype(F32)
        short, key_short, one = slot.astype(BF16), key.astype(BF16), jnp.ones((), BF16)
        parts = []
        for p in range(n_pair):
            sel = (slot == key[p:p + 1]).astype(F32) if with_gate else jnp.where(short == key_short[p:p + 1], one, one - one)
            v = dot(sel.astype(BF16), ref[i * per + p // ny, p % ny].reshape(256, 256), 1, 0)
            parts.append(v * jnp.sum(sel * gate[p:p + 1], axis=1, keepdims=True) if with_gate else v)
        return jnp.concatenate([parts[zz * ny + yy][CAP * (xx * nc + cc):CAP * (xx * nc + cc + 1)] for cc, xx, yy, zz in places], axis=0).astype(BF16)

    def put(i, v, to):
        for k, (cc, xx, yy, zz) in enumerate(places):
            for half in range(2):
                to[half][cc, xx, yy, i * per + zz] = v[CAP * k:CAP * (k + 1), 128 * half:128 * (half + 1)].astype(BF16)

    def forward(i):
        here = pl.ds(i * n_slot, n_slot)
        xs = select(i, x_all, False)
        a = dot(xs, w1[...], 1, 0)
        h = gelu(a).astype(BF16)
        xs_ref[here], h_ref[here], a_ref[here] = xs, h, a
        put(i, dot(h, w2[...], 1, 0), rows[:2])

    def backward(i):
        here = pl.ds(i * n_slot, n_slot)
        dys = select(i, g_all, True)
        dys_ref[here] = dys
        da_ref[here] = (dot(dys, w2[...], 1, 1) * gelu_slope(a_ref[here])).astype(BF16)

    def backward_rows(i):
        put(i, dot(da_ref[pl.ds(i * n_slot, n_slot)], w1[...], 1, 1), rows[2:])

    def back(i):
        h = rows[i]
        other, near, via, out2, via2, in2, out3, hot_land, cold_land = areas[9 * i:9 * i + 9]
        link = next(links)
        go = link.go
        in_c, in_e, in_h = [[link.group(), link.group()] for _ in range(3)]
        in_n, in_v, in_2, in_l, in_s = [link.group() for _ in range(5)]
        x_first = i % 2 == 0
        a, b = (x, y) if x_first else (y, x)

        def to(a, b):
            return dev(z, b, a, c) if x_first else dev(z, a, b, c)

        def index(lead, a, bs):
            return lead + ((a, bs) if x_first else (bs, a))

        up, dn, far = step(a, 1), step(a, 3), step(a, 2)
        lo, hi = pl.ds(0, 2), pl.ds(2, 2)
        parts = [pl.ds(0, nz // 2), pl.ds(nz // 2, nz // 2)]

        def start(k):
            zs = parts[k]
            go(h.at[1 - c, :, :, zs], other.at[:, :, zs], mate, in_c[k])
            spread(h, (c,), c, zs, in_e[k])

        def follow(k):
            link.wait(in_c[k], other.at[:, :, parts[k]])
            spread(other, (), 1 - c, parts[k], in_h[k])

        def spread(ref, lead, e, zs, group):
            go(ref.at[index(lead, far, lo) + (zs,)], via.at[0, e, :, zs], to(up, b), group)
            go(ref.at[index(lead, far, hi) + (zs,)], via.at[1, e, :, zs], to(dn, b), group)
            go(ref.at[index(lead, up, full) + (zs,)], near.at[a, e, :, zs], to(up, b), in_n)
            go(ref.at[index(lead, dn, full) + (zs,)], near.at[a, e, :, zs], to(dn, b), in_n)

        def relay(e, zs, group):
            link.wait(group, via.at[:, e, :, zs])
            go(via.at[0, e, :, zs], near.at[dn, e, lo, zs], to(up, b), in_n)
            go(via.at[1, e, :, zs], near.at[up, e, hi, zs], to(dn, b), in_n)

        start(0)
        yield
        follow(0)
        yield
        start(1)
        yield
        follow(1)
        yield
        relay(c, parts[0], in_e[0])
        relay(1 - c, parts[0], in_h[0])
        yield
        relay(c, parts[1], in_e[1])
        yield
        relay(1 - c, parts[1], in_h[1])
        yield
        link.wait(in_n, near.at[pl.ds(0, 3)])

        def expert(s, e):
            return ((z * ny + y) * nx + s) * nc + e if x_first else ((z * ny + s) * nx + x) * nc + e

        places = [(step(a, d), e) for d in range(4) for e in (c, 1 - c)]
        is_hot = [[(hot_ref[j:j + 1, :] == expert(s, e).astype(F32)).astype(F32) for s, e in places] for j in range(3)]
        wide = lambda v: jnp.broadcast_to(v, (8, 128))
        weight = [[wide(v).astype(BF16) for v in r] for r in is_hot]
        line = iota((8, 128), 0)
        mine = [(wide(is_hot[0][k] + is_hot[1][k] + is_hot[2][k]) < 0.5) & (line == s * nc + e) for k, (s, e) in enumerate(places)]

        def squeeze(bb):
            given = [h[index((c,), a, bb)], other[index((), a, bb)]] + [near[s, e, bb] for s, e in places[2:]]
            for j in range(3):
                out2[bb, j] = sum(given[k] * weight[j][k] for k in range(8))
            singles = jnp.zeros((nz, 8, 128), F32)
            for k in range(8):
                singles = jnp.where(mine[k], jnp.sum(given[k].astype(F32), axis=1, keepdims=True), singles)
            out2[bb, 3] = singles.astype(BF16)

        up, dn, far = step(b, 1), step(b, 3), step(b, 2)
        lo, hi = pl.ds(0, nz // 2), pl.ds(nz // 2, nz // 2)
        squeeze(far)
        squeeze(up)
        go(out2.at[far, :, lo], via2.at[0], to(a, up), in_v)
        go(out2.at[far, :, hi], via2.at[1], to(a, dn), in_v)
        squeeze(dn)
        go(out2.at[up], in2.at[b], to(a, up), in_2)
        squeeze(b)
        go(out2.at[dn], in2.at[b], to(a, dn), in_2)
        in2[b] = out2[b]
        yield
        link.wait(in_v, via2)
        go(via2.at[0], in2.at[dn, :, lo], to(a, up), in_2)
        go(via2.at[1], in2.at[up, :, hi], to(a, dn), in_2)
        yield
        link.wait(in_2, in2.at[pl.ds(0, 3)])
        for d in by_distance:
            zz = lax.rem(z + d, nz)
            go(in2.at[:, 3, zz], cold_land.at[z], dev(zz, y, x, c), in_s)
        for j in range(3):
            out3[:, j] = (in2[0, j] + in2[1, j]) + (in2[2, j] + in2[3, j])
        for d in by_distance:
            zz = lax.rem(z + d, nz)
            go(out3.at[zz], hot_land.at[z], dev(zz, y, x, c), in_l)
        cold_land[z] = in2[:, 3, z]
        hot_land[z] = out3[z]
        yield
        link.wait(in_s, cold_land.at[pl.ds(0, nz - 1)])
        link.wait(in_l, hot_land.at[pl.ds(0, nz - 1)])

    def weight_grad(k):
        if k % 2 == 0:
            part = slice(w2.shape[0] // 4 * (k // 2), w2.shape[0] // 4 * (k // 2 + 1))
            g2_ref[part, :] = dot(h_ref[:, part], dys_ref[...], 0, 0)
            save(4, (part, full))
        else:
            part = slice(w1.shape[1] // 4 * (k // 2), w1.shape[1] // 4 * (k // 2 + 1))
            g1_ref[:, part] = dot(xs_ref[...], da_ref[:, part], 0, 0)
            save(3, (full, part))

    ys, dxs = [back(0), back(1)], [back(2), back(3)]
    n_tok = tok.shape[0]
    memo = {}
    earlier = iota((n_tok, n_tok), 1) < iota((n_tok, n_tok), 0)
    n_exp = wg.shape[1]

    def where_from(i, r0, r1):
        rank = jnp.sum(jnp.where(earlier & ((i == r0) | (i == r1)), 1.0, 0.0), axis=1, keepdims=True)
        slot = jnp.full((n_tok, 1), -1.0, F32)
        for j in range(3):
            slot = jnp.where(i == hot_ref[j:j + 1, 0:1], CAP * j + rank, slot)
        e = i.astype(jnp.int32)
        core, xx, yy, zz = e % nc, (e // nc) % nx, (e // (nc * nx)) % ny, e // (nc * nx * ny)
        lane, single = iota((n_tok, n_exp), 1), slot < 0.0
        pick = lambda m: m.astype(F32).astype(BF16)
        return pick(iota((n_tok, 32), 1).astype(F32) == slot), (pick((lane == e) & single), pick((lane == ((zz * nx + xx) * ny + yy) * nc + core) & single))

    def rows_of(kind, chosen):
        parts = []
        for half in range(2):
            hot_land, cold_land = areas[9 * (kind + half) + 7:9 * (kind + half) + 9]
            hot = jnp.sum(hot_land[...].astype(F32), axis=0).reshape(24, 128)
            hot = jnp.concatenate([hot, jnp.zeros((8, 128), F32)], axis=0).astype(BF16)
            cold = cold_land[...].astype(F32).reshape(n_exp, 128).astype(BF16)
            parts.append([dot(by_slot, hot, 1, 0) + dot(by_place[half], cold, 1, 0) for by_slot, by_place in chosen])
        return [jnp.concatenate([parts[0][k], parts[1][k]], axis=1) for k in range(2)]

    def combine():
        r0, r1 = ids[0:1].astype(F32), ids[1:2].astype(F32)
        i0, i1 = as_col(r0), as_col(r1)
        g0, g1 = gates(tok[...], i0, i1, wg[...])
        chosen = [where_from(i, r0, r1) for i in (i0, i1)]
        y0, y1 = rows_of(0, chosen)
        grad = dout[...].astype(F32)
        dg0, dg1 = (jnp.sum(grad * v, axis=1, keepdims=True) for v in (y0, y1))
        mean = g0 * dg0 + g1 * dg1
        d0, d1 = ((g * (dg - mean)).astype(BF16).astype(F32) for g, dg in ((g0, dg0), (g1, dg1)))
        d_land[z, y, x, c] = jnp.concatenate([as_row(d0), as_row(d1), jnp.zeros((1, 2 * n_tok), F32)], axis=1)
        out_ref[...] = (g0 * y0 + g1 * y1).astype(BF16)
        saves[0].start()
        d_plans.append(gather_rows(next(links), d_land, range(4)))
        advance(d_plans)
        expert = iota((n_tok, n_exp), 1).astype(F32)
        spread = jnp.where(expert == i0, d0, jnp.where(expert == i1, d1, 0.0)).astype(BF16)
        memo.update(chosen=chosen, through=dot(spread, wg[...], 1, 1))

    def finish():
        dx0, dx1 = rows_of(2, memo['chosen'])
        gx_ref[...] = (dx0 + dx1 + memo['through']).astype(BF16)
        saves[1].start()

    n_dev = nz * ny * nx * nc

    def gate_grad():
        flatten(d_land, d_all)
        expert = iota((n_exp, 256), 0).astype(F32).astype(BF16)
        codes = [plain_id(pair_rows(token_lanes(m_all, k, 0, n_dev // 4))).astype(BF16) for k in range(2)]
        grads = [pair_rows(token_lanes(d_all, k, 0, n_dev // 4)).astype(BF16) for k in range(2)]
        none = jnp.zeros((), BF16)
        total = jnp.zeros((n_exp, x_all.shape[-1]), F32)
        zs = nz // 4 or 1
        for z0 in range(0, nz, zs):
            spread = []
            for p in range(z0 * ny, (z0 + zs) * ny):
                q = slice(p, p + 1)
                spread.append(jnp.where(expert == codes[0][q], grads[0][q], jnp.where(expert == codes[1][q], grads[1][q], none)))
            total += dot(jnp.concatenate(spread, axis=1), x_all[z0:z0 + zs].reshape(zs * ny * 256, x_all.shape[-1]), 1, 0)
        gate_ref[...] = total.T
        saves[2].start()

    d_plans = []
    moves = {'t': tok_plans, 'g': grad_plans, 'm': row_plan, 'y': ys, 'x': dxs, 'd': d_plans}
    works = {'f': [functools.partial(forward, i) for i in range(steps)], 'b': [functools.partial(backward, i) for i in range(steps)],
             'B': [functools.partial(backward_rows, i) for i in range(steps)], 'w': [functools.partial(weight_grad, k) for k in range(8)],
             'h': [read_rows], 'c': [combine], 'k': [gate_grad], 'e': [finish]}
    for turn in SCHEDULE:
        if turn in moves:
            advance(moves[turn])
        elif works[turn]:
            works[turn].pop(0)()
    for link in all_links:
        link.finish(pad, pad_row)
    for cp in saves:
        cp.wait()


def block_call(dims, tokens, grad_out, ids, w_gate, w1, w2):
    nz, ny, nx, nc = dims
    d_model, d_hidden = w1.shape
    n_tok = tokens.shape[0]
    n_dev = nz * ny * nx * nc
    n_row = n_dev * CAP
    tile = (CAP, 128)
    hbm = pl.BlockSpec(memory_space=pltpu.HBM)
    out = jax.ShapeDtypeStruct
    work = [(4, 4, nz), (4, 2, 4, nz), (2, 2, 2, nz), (4, 4, nz), (2, 4, nz // 2), (4, 4, nz), (nz, 3), (nz, 3), (nz, 4)]
    n_group = 4 * 10 + 4 + 4 * 11 + 4
    sems = [pltpu.SemaphoreType.DMA((10,)), pltpu.SemaphoreType.DMA((n_group,))]
    results = [(tokens.shape, BF16), (tokens.shape, BF16), ((d_model, n_dev), F32), ((d_model, d_hidden), F32), ((d_hidden, d_model), F32)]
    row = (1, 128)
    kept = [(tokens.shape, BF16), (tokens.shape, BF16), (ids.shape, jnp.int32), (w_gate.shape, BF16), (w1.shape, BF16), (w2.shape, BF16), (row, F32), (dims + row, F32),
            (dims + tokens.shape, BF16), (dims + tokens.shape, BF16), ((n_row, d_model), BF16), ((n_row, d_model), BF16), ((n_row, d_hidden), BF16), ((n_row, d_hidden), BF16), ((n_row, d_hidden), F32), ((n_dev, 128), F32), (tile, F32),
            (dims + row, F32), ((n_dev, 128), F32), ((1024,) + tile, BF16), ((n_dev,) + row, F32)]
    return pl.pallas_call(
        functools.partial(block_kernel, dims, (6, len(results), len(results), len(kept), 4, 4 * len(work), 3, len(sems))),
        out_shape=[out(*r) for r in results],
        in_specs=[hbm] * 6,
        out_specs=[hbm] * len(results),
        scratch_shapes=[pltpu.VMEM(*r) for r in results + kept] + [pltpu.VMEM((nc, nx, ny, nz) + tile, BF16)] * 4 + [pltpu.VMEM(w + tile, BF16) for w in work] * 4
        + [pltpu.SemaphoreType.DMA((k,)) for k in (8, 1, len(results))] + sems,
        compiler_params=pltpu.CompilerParams(collective_id=0, has_side_effects=True, vmem_limit_bytes=VMEM_LIMIT),
        name='block',
    )(tokens, grad_out, ids, w_gate, w1, w2)


VMEM_LIMIT = 67043328
SCHEDULE = 'mtgtmttmtgtttgttgmth' + 'ffggyfggyfy' + 'gygy' + 'bybybyBBxbyxBBxy' + 'wwxxwxwwxyc' + 'xwwdxdxwddkxe'


def pass_kernel(n, *refs):
    refs = iter(refs)
    given, passed, held, (load_sem, save_sem) = [list(itertools.islice(refs, k)) for k in (n, n, n, 2)]
    loads = [pltpu.make_async_copy(given[k], held[k], load_sem.at[k]) for k in range(n)]
    saves = [pltpu.make_async_copy(held[k], passed[k], save_sem.at[k]) for k in range(n)]
    for cp in loads:
        cp.start()
    for load, save in zip(loads, saves):
        load.wait()
        save.start()
    for cp in saves:
        cp.wait()


def pass_on(*arrays):
    n = len(arrays)
    return pl.pallas_call(
        functools.partial(pass_kernel, n),
        out_shape=[jax.ShapeDtypeStruct(v.shape, v.dtype) for v in arrays],
        in_specs=[pl.BlockSpec(memory_space=pltpu.HBM)] * n,
        out_specs=[pl.BlockSpec(memory_space=pltpu.HBM)] * n,
        scratch_shapes=[pltpu.VMEM(v.shape, v.dtype) for v in arrays] + [pltpu.SemaphoreType.DMA((n,))] * 2,
        compiler_params=pltpu.CompilerParams(vmem_limit_bytes=VMEM_LIMIT),
        name='pass_on',
    )(*arrays)


def local_block(dims, tokens, grad_out, expert_ids, w_gate, w_in, w_out):
    y_out, grad_x, grad_w_gate, g1, g2 = pass_on(*block_call(dims, tokens, grad_out, expert_ids.T, w_gate, w_in[0], w_out[0]))
    return y_out, grad_x, g1[None], g2[None], grad_w_gate


def solution(mesh):
    dims = (8, 4, 4, 2)
    return jax.shard_map(functools.partial(local_block, dims), mesh=mesh, in_specs=(P('ep'), P('ep'), P('ep'), P(), P('ep'), P('ep')), out_specs=(P('ep'), P('ep'), P('ep'), P('ep'), P()), check_vma=False)
```

```python
import functools
import itertools
import math

import jax
import jax.numpy as jnp
from jax import lax
from jax.experimental import pallas as pl
from jax.experimental.pallas import tpu as pltpu
from jax.sharding import PartitionSpec as P

MESH = pl.DeviceIdType.MESH
F32 = jnp.float32
BF16 = jnp.bfloat16
CAP = 8


def coords(dims):
    nz, ny, nx, nc = dims
    me = lax.axis_index('ep')
    c = lax.rem(me, nc)
    x = lax.rem(me // nc, nx)
    y = lax.rem(me // (nc * nx), ny)
    z = me // (nc * nx * ny)

    def dev(z, y, x, c):
        return (((z * ny + y) * nx + x) * nc + c,)

    return z, y, x, c, dev


def dot(a, b, ca, cb):
    return lax.dot_general(a, b, (((ca,), (cb,)), ((), ())), preferred_element_type=F32)


def iota(shape, axis):
    return lax.broadcasted_iota(jnp.int32, shape, axis)


def as_row(col):
    n = col.shape[0]
    return jnp.sum(jnp.where(iota((n, n), 0) == iota((n, n), 1), col, 0.0), axis=0, keepdims=True)


def as_col(row):
    n = row.shape[1]
    return jnp.sum(jnp.where(iota((n, n), 0) == iota((n, n), 1), row, 0.0), axis=1, keepdims=True)


def gates(tok, i0, i1, w_gate):
    logits = dot(tok, w_gate, 1, 0)
    expert = iota(logits.shape, 1).astype(F32)
    l0, l1 = (jnp.sum(jnp.where(expert == i, logits, 0.0), axis=1, keepdims=True) for i in (i0, i1))
    top = jnp.maximum(l0, l1)
    p0, p1 = jnp.exp(l0 - top), jnp.exp(l1 - top)
    total = p0 + p1
    return p0 / total, p1 / total


def choice_row(tok, ids, w_gate):
    r0, r1 = ids[0:1].astype(F32), ids[1:2].astype(F32)
    i0, i1 = as_col(r0), as_col(r1)
    g0, g1 = gates(tok, i0, i1, w_gate)

    def code(i):
        n = jnp.sum((i == r0).astype(F32) + (i == r1).astype(F32), axis=1, keepdims=True)
        return as_row(jnp.where(n > 1.5, i + 256.0, i))

    return jnp.concatenate([code(i0), code(i1), as_row(g0), as_row(g1)], axis=1)


def gelu_tanh(a):
    k = 0.7978845608028654
    sq = a * a
    return jnp.tanh(a * (k + (k * 0.044715) * sq)), sq


def gelu(a):
    half = 0.5 * a
    return half + half * gelu_tanh(a)[0]


def gelu_slope(a):
    k = 0.7978845608028654
    t, sq = gelu_tanh(a)
    return (0.5 + 0.5 * t) + (0.5 * a) * (1.0 - t * t) * (k + (3 * k * 0.044715) * sq)


def token_lanes(ref, k, start, n):
    lane = iota((n, 128), 1) // 32
    out = jnp.zeros((n, 128), F32)
    for j in range(4):
        r = ref[pl.ds(start + j, n, stride=4), :]
        out = jnp.where(lane == j, r if j == k else pltpu.roll(r, 32 * (j - k) % 128, 1), out)
    return out


def pair_rows(v):
    return jnp.concatenate([jnp.concatenate([v[2 * i:2 * i + 1], v[2 * i + 1:2 * i + 2]], axis=1) for i in range(v.shape[0] // 2)], axis=0)


def plain_id(code):
    return jnp.where(code >= 256.0, code - 256.0, code)


class Links:
    def __init__(self, send, recv, pool):
        self.send, self.recv, self.pool, self.bytes = send, recv, pool, 0

    def group(self):
        return self.recv.at[next(self.pool)]

    def go(self, src, dst, to, group):
        pltpu.make_async_remote_copy(src_ref=src, dst_ref=dst, send_sem=self.send, recv_sem=group, device_id=to, device_id_type=MESH).start()
        self.bytes += math.prod(src.shape) * jnp.dtype(src.dtype).itemsize

    def wait(self, group, ref):
        pltpu.make_async_copy(ref, ref, group).wait()

    def finish(self, *pads):
        for pad in pads:
            unit = math.prod(pad.shape[1:]) * jnp.dtype(pad.dtype).itemsize
            if self.bytes % unit == 0:
                return self.wait(self.send, pad.at[pl.ds(0, self.bytes // unit)])
        raise ValueError(self.bytes)


def block_kernel(dims, sizes, *refs):
    nz, ny, nx, nc = dims
    refs = iter(refs)
    refs = [list(itertools.islice(refs, n)) for n in sizes]
    (tok_hbm, dout_hbm, ids_hbm, wg_hbm, w1_hbm, w2_hbm), outs, held, kept, rows, areas, (load_sem, keep_sem, save_sem), sems = refs
    out_ref, gx_ref, gate_ref, g1_ref, g2_ref = held
    tok, dout, ids, wg, w1, w2, row, m_land, x_all, g_all, xs_ref, dys_ref, h_ref, da_ref, a_ref, m_all, hot_ref, d_land, d_all, pad, pad_row = kept
    z, y, x, c, dev = coords(dims)
    saves = [pltpu.make_async_copy(held[k], outs[k], save_sem.at[k]) for k in range(len(held))]

    def save(k, part):
        pltpu.make_async_copy(held[k].at[part], outs[k].at[part], save_sem.at[k]).start()

    send_sem, recv_sem = sems
    pool = itertools.count()
    all_links = [Links(send_sem.at[k], recv_sem, pool) for k in range(send_sem.shape[0])]
    links = iter(all_links)

    loads = [pltpu.make_async_copy(s, d, load_sem.at[k]) for k, (s, d) in enumerate(
        [(tok_hbm, x_all.at[z, y, x, c]), (dout_hbm, g_all.at[z, y, x, c]), (tok_hbm, tok), (ids_hbm, ids), (wg_hbm, wg), (dout_hbm, dout), (w1_hbm, w1), (w2_hbm, w2)])]
    for ld in loads:
        ld.start()
    peers = [dev(lax.rem(z + d, nz), y, x, c) for d in range(1, nz)]
    for d in (1, 2, 3):
        peers.append(dev(z, lax.rem(y + d, ny), x, c))
        peers.append(dev(z, y, lax.rem(x + d, nx), c))
    mate = dev(z, y, x, 1 - c)
    peers.append(mate)
    barrier = pltpu.get_barrier_semaphore()
    for peer in peers:
        pl.semaphore_signal(barrier, inc=1, device_id=peer, device_id_type=MESH)
    for ld in loads[2:5]:
        ld.wait()
    row[...] = choice_row(tok[...], ids[...], wg[...])
    place = pltpu.make_async_copy(row, m_land.at[z, y, x, c], keep_sem.at[0])
    place.start()
    loads[0].wait()
    loads[1].wait()
    place.wait()
    pl.semaphore_wait(barrier, len(peers))

    full = slice(None)
    by_distance = sorted(range(1, nz), key=lambda d: abs(d - nz // 2))

    def step(v, d, m=4):
        return lax.rem(v + d, m)

    def by_lines(link, ref, rows, x_last, late):
        p0, q0 = (y, x) if x_last else (x, y)
        low, high = pl.ds(0, nz // 2), pl.ds(nz // 2, nz // 2)

        def at(zs, p, q):
            return ref.at[(zs, p, q, c, rows) if x_last else (zs, q, p, c, rows)]

        def go(part, p, q, group):
            link.go(part, part, dev(z, p, q, c) if x_last else dev(z, q, p, c), group)

        in_z, in_p, in_m, in_f, in_r, in_c = [link.group() for _ in range(6)]
        line = at(full, p0, q0)

        def over(q):
            part = at(full, full, q)
            link.go(part, part, mate, in_c)

        own = at(z, p0, q0)
        for d in by_distance:
            link.go(own, own, dev(step(z, d, nz), y, x, c), in_z)
        yield
        link.wait(in_z, at(pl.ds(0, nz - 1), p0, q0))
        pm, pp, po = step(p0, 3), step(p0, 1), step(p0, 2)
        qm, qp, qo = step(q0, 3), step(q0, 1), step(q0, 2)
        qs = []

        def spread(p):
            part = at(full, p, q0)
            qs.append((p, link.group()))
            go(part, p0, qp, qs[-1][1])
            go(part, p0, qm, qs[-1][1])

        def relay(i):
            p, group = qs[i]
            link.wait(group, at(full, pl.ds(0, 2), q0))
            go(at(low, p, qm), p0, qp, in_r)
            go(at(high, p, qp), p0, qm, in_r)

        def pass_one():
            link.wait(in_p, line)
            go(at(low, pm, q0), pp, q0, in_f)
            link.wait(in_m, line)
            go(at(high, pp, q0), pm, q0, in_f)

        go(line, pp, q0, in_p)
        go(line, pm, q0, in_m)
        if late:
            yield
            pass_one()
            yield
            link.wait(in_f, line)
            for p in (p0, pm, pp, po):
                spread(p)
            over(q0)
            yield
            relay(0)
        else:
            yield
            spread(p0)
            yield
            pass_one()
            yield
            spread(pm)
            spread(pp)
            yield
            relay(0)
            yield
            link.wait(in_f, line)
            spread(po)
            over(q0)
        for i in range(1, 4):
            yield
            relay(i)
        over(qm)
        over(qp)
        yield
        link.wait(in_r, at(full, full, q0))
        over(qo)
        yield
        link.wait(in_c, ref.at[full, full, full, c, rows])

    def gather_rows(link, held, order):
        have = [z, y, x, c]
        for axis in order:
            size = (nz, ny, nx, nc)[axis]
            part = held.at[tuple(have)]
            group = link.group()
            for d in sorted(range(1, size), key=lambda d: abs(d - size // 2)):
                there = [z, y, x, c]
                there[axis] = lax.rem(there[axis] + d, size)
                link.go(part, part, dev(*there), group)
            have[axis] = pl.ds(0, size - 1)
            yield
            link.wait(group, held.at[tuple(have)])
            have[axis] = full

    def advance(plans):
        for g in plans:
            next(g, None)

    halves = [slice(0, 16), slice(16, 32)]
    tok_plans, grad_plans = [[by_lines(next(links), ref, half, half.start == 0, ref is g_all) for half in halves] for ref in (x_all, g_all)]
    row_plan = [gather_rows(next(links), m_land, range(4))]
    advance(row_plan + tok_plans)
    def flatten(land, flat):
        def lines(zz, carry):
            for k in range(ny * nx * nc):
                flat[pl.ds(zz * (ny * nx * nc) + k, 1), :] = land[zz, k // (nx * nc), k // nc % nx, k % nc]
            return carry

        lax.fori_loop(0, nz, lines, 0)


    me = lax.axis_index('ep').astype(F32)
    def read_rows():
        flatten(m_land, m_all)
        for ld in loads[5:]:
            ld.wait()
        code = m_all[...]
        left = jnp.where((iota(code.shape, 1) < 64) & (code >= 256.0), code - 256.0, 999.0)
        found = []
        for _ in range(3):
            best = jnp.min(jnp.min(left, axis=0, keepdims=True), axis=1, keepdims=True)
            left = jnp.where(left == best, 999.0, left)
            found.append(jnp.broadcast_to(best, (1, 128)))
        hot_ref[...] = jnp.concatenate(found + [jnp.full((5, 128), 999.0, F32)], axis=0)

    steps = 4 if nz == 8 else 1
    per = nz // steps
    n_quad = per * ny * nx * nc // 4
    n_pair = n_quad // 2
    n_slot = n_pair * 8 * CAP

    places = [(cc, xx, yy, zz) for cc in range(nc) for xx in range(nx) for yy in range(ny) for zz in range(per)]

    def select(i, ref, with_gate):
        c0, c1, g0, g1 = (pair_rows(token_lanes(m_all, k, pl.multiple_of(4 * n_quad * i, 4 * n_quad), n_quad)) for k in range(4))
        hit0, hit1 = plain_id(c0) == me, plain_id(c1) == me
        hit = (hit0 | hit1).astype(F32)
        gate = jnp.where(hit0, g0, 0.0) + jnp.where(hit1, g1, 0.0)
        before, after = iota((256, 256), 0), iota((256, 256), 1)
        tri = ((before < after) & (before // 32 == after // 32)).astype(F32).astype(BF16)
        rank = dot(hit.astype(BF16), tri, 1, 0)
        src = (iota((n_pair, 256), 1) // 32).astype(F32)
        key = jnp.where(hit > 0.0, src * CAP + rank, -1.0)
        slot = iota((8 * CAP, 256), 0).astype(F32)
        short, key_short, one = slot.astype(BF16), key.astype(BF16), jnp.ones((), BF16)
        parts = []
        for p in range(n_pair):
            sel = (slot == key[p:p + 1]).astype(F32) if with_gate else jnp.where(short == key_short[p:p + 1], one, one - one)
            v = dot(sel.astype(BF16), ref[i * per + p // ny, p % ny].reshape(256, 256), 1, 0)
            parts.append(v * jnp.sum(sel * gate[p:p + 1], axis=1, keepdims=True) if with_gate else v)
        return jnp.concatenate([parts[zz * ny + yy][CAP * (xx * nc + cc):CAP * (xx * nc + cc + 1)] for cc, xx, yy, zz in places], axis=0).astype(BF16)

    def put(i, v, to):
        for k, (cc, xx, yy, zz) in enumerate(places):
            for half in range(2):
                to[half][cc, xx, yy, i * per + zz] = v[CAP * k:CAP * (k + 1), 128 * half:128 * (half + 1)].astype(BF16)

    def forward(i):
        here = pl.ds(i * n_slot, n_slot)
        xs = select(i, x_all, False)
        a = dot(xs, w1[...], 1, 0)
        h = gelu(a).astype(BF16)
        xs_ref[here], h_ref[here], a_ref[here] = xs, h, a
        put(i, dot(h, w2[...], 1, 0), rows[:2])

    def backward(i):
        here = pl.ds(i * n_slot, n_slot)
        dys = select(i, g_all, True)
        dys_ref[here] = dys
        da_ref[here] = (dot(dys, w2[...], 1, 1) * gelu_slope(a_ref[here])).astype(BF16)

    def backward_rows(i):
        put(i, dot(da_ref[pl.ds(i * n_slot, n_slot)], w1[...], 1, 1), rows[2:])

    def back(i):
        h = rows[i]
        other, near, via, out2, via2, in2, out3, hot_land, cold_land = areas[9 * i:9 * i + 9]
        link = next(links)
        go = link.go
        in_c, in_e, in_h = [[link.group(), link.group()] for _ in range(3)]
        in_n, in_v, in_2, in_l, in_s = [link.group() for _ in range(5)]
        x_first = i % 2 == 0
        a, b = (x, y) if x_first else (y, x)

        def to(a, b):
            return dev(z, b, a, c) if x_first else dev(z, a, b, c)

        def index(lead, a, bs):
            return lead + ((a, bs) if x_first else (bs, a))

        up, dn, far = step(a, 1), step(a, 3), step(a, 2)
        lo, hi = pl.ds(0, 2), pl.ds(2, 2)
        parts = [pl.ds(0, nz // 2), pl.ds(nz // 2, nz // 2)]

        def start(k):
            zs = parts[k]
            go(h.at[1 - c, :, :, zs], other.at[:, :, zs], mate, in_c[k])
            spread(h, (c,), c, zs, in_e[k])

        def follow(k):
            link.wait(in_c[k], other.at[:, :, parts[k]])
            spread(other, (), 1 - c, parts[k], in_h[k])

        def spread(ref, lead, e, zs, group):
            go(ref.at[index(lead, far, lo) + (zs,)], via.at[0, e, :, zs], to(up, b), group)
            go(ref.at[index(lead, far, hi) + (zs,)], via.at[1, e, :, zs], to(dn, b), group)
            go(ref.at[index(lead, up, full) + (zs,)], near.at[a, e, :, zs], to(up, b), in_n)
            go(ref.at[index(lead, dn, full) + (zs,)], near.at[a, e, :, zs], to(dn, b), in_n)

        def relay(e, zs, group):
            link.wait(group, via.at[:, e, :, zs])
            go(via.at[0, e, :, zs], near.at[dn, e, lo, zs], to(up, b), in_n)
            go(via.at[1, e, :, zs], near.at[up, e, hi, zs], to(dn, b), in_n)

        start(0)
        yield
        follow(0)
        yield
        start(1)
        yield
        follow(1)
        yield
        relay(c, parts[0], in_e[0])
        relay(1 - c, parts[0], in_h[0])
        yield
        relay(c, parts[1], in_e[1])
        yield
        relay(1 - c, parts[1], in_h[1])
        yield
        link.wait(in_n, near.at[pl.ds(0, 3)])

        def expert(s, e):
            return ((z * ny + y) * nx + s) * nc + e if x_first else ((z * ny + s) * nx + x) * nc + e

        places = [(step(a, d), e) for d in range(4) for e in (c, 1 - c)]
        is_hot = [[(hot_ref[j:j + 1, :] == expert(s, e).astype(F32)).astype(F32) for s, e in places] for j in range(3)]
        wide = lambda v: jnp.broadcast_to(v, (8, 128))
        weight = [[wide(v).astype(BF16) for v in r] for r in is_hot]
        line = iota((8, 128), 0)
        mine = [(wide(is_hot[0][k] + is_hot[1][k] + is_hot[2][k]) < 0.5) & (line == s * nc + e) for k, (s, e) in enumerate(places)]

        def squeeze(bb):
            given = [h[index((c,), a, bb)], other[index((), a, bb)]] + [near[s, e, bb] for s, e in places[2:]]
            for j in range(3):
                out2[bb, j] = sum(given[k] * weight[j][k] for k in range(8))
            singles = jnp.zeros((nz, 8, 128), F32)
            for k in range(8):
                singles = jnp.where(mine[k], jnp.sum(given[k].astype(F32), axis=1, keepdims=True), singles)
            out2[bb, 3] = singles.astype(BF16)

        up, dn, far = step(b, 1), step(b, 3), step(b, 2)
        lo, hi = pl.ds(0, nz // 2), pl.ds(nz // 2, nz // 2)
        squeeze(far)
        squeeze(up)
        go(out2.at[far, :, lo], via2.at[0], to(a, up), in_v)
        go(out2.at[far, :, hi], via2.at[1], to(a, dn), in_v)
        squeeze(dn)
        go(out2.at[up], in2.at[b], to(a, up), in_2)
        squeeze(b)
        go(out2.at[dn], in2.at[b], to(a, dn), in_2)
        in2[b] = out2[b]
        yield
        link.wait(in_v, via2)
        go(via2.at[0], in2.at[dn, :, lo], to(a, up), in_2)
        go(via2.at[1], in2.at[up, :, hi], to(a, dn), in_2)
        yield
        link.wait(in_2, in2.at[pl.ds(0, 3)])
        for d in by_distance:
            zz = lax.rem(z + d, nz)
            go(in2.at[:, 3, zz], cold_land.at[z], dev(zz, y, x, c), in_s)
        for j in range(3):
            out3[:, j] = (in2[0, j] + in2[1, j]) + (in2[2, j] + in2[3, j])
        for d in by_distance:
            zz = lax.rem(z + d, nz)
            go(out3.at[zz], hot_land.at[z], dev(zz, y, x, c), in_l)
        cold_land[z] = in2[:, 3, z]
        hot_land[z] = out3[z]
        yield
        link.wait(in_s, cold_land.at[pl.ds(0, nz - 1)])
        link.wait(in_l, hot_land.at[pl.ds(0, nz - 1)])

    def weight_grad(k):
        if k % 2 == 0:
            part = slice(w2.shape[0] // 4 * (k // 2), w2.shape[0] // 4 * (k // 2 + 1))
            g2_ref[part, :] = dot(h_ref[:, part], dys_ref[...], 0, 0)
            save(4, (part, full))
        else:
            part = slice(w1.shape[1] // 4 * (k // 2), w1.shape[1] // 4 * (k // 2 + 1))
            g1_ref[:, part] = dot(xs_ref[...], da_ref[:, part], 0, 0)
            save(3, (full, part))

    ys, dxs = [back(0), back(1)], [back(2), back(3)]
    n_tok = tok.shape[0]
    memo = {}
    earlier = iota((n_tok, n_tok), 1) < iota((n_tok, n_tok), 0)
    n_exp = wg.shape[1]

    def where_from(i, r0, r1):
        rank = jnp.sum(jnp.where(earlier & ((i == r0) | (i == r1)), 1.0, 0.0), axis=1, keepdims=True)
        slot = jnp.full((n_tok, 1), -1.0, F32)
        for j in range(3):
            slot = jnp.where(i == hot_ref[j:j + 1, 0:1], CAP * j + rank, slot)
        e = i.astype(jnp.int32)
        core, xx, yy, zz = e % nc, (e // nc) % nx, (e // (nc * nx)) % ny, e // (nc * nx * ny)
        lane, single = iota((n_tok, n_exp), 1), slot < 0.0
        pick = lambda m: m.astype(F32).astype(BF16)
        return pick(iota((n_tok, 32), 1).astype(F32) == slot), (pick((lane == e) & single), pick((lane == ((zz * nx + xx) * ny + yy) * nc + core) & single))

    def rows_of(kind, chosen):
        parts = []
        for half in range(2):
            hot_land, cold_land = areas[9 * (kind + half) + 7:9 * (kind + half) + 9]
            hot = jnp.sum(hot_land[...].astype(F32), axis=0).reshape(24, 128)
            hot = jnp.concatenate([hot, jnp.zeros((8, 128), F32)], axis=0).astype(BF16)
            cold = cold_land[...].astype(F32).reshape(n_exp, 128).astype(BF16)
            parts.append([dot(by_slot, hot, 1, 0) + dot(by_place[half], cold, 1, 0) for by_slot, by_place in chosen])
        return [jnp.concatenate([parts[0][k], parts[1][k]], axis=1) for k in range(2)]

    def combine():
        r0, r1 = ids[0:1].astype(F32), ids[1:2].astype(F32)
        i0, i1 = as_col(r0), as_col(r1)
        g0, g1 = gates(tok[...], i0, i1, wg[...])
        chosen = [where_from(i, r0, r1) for i in (i0, i1)]
        y0, y1 = rows_of(0, chosen)
        grad = dout[...].astype(F32)
        dg0, dg1 = (jnp.sum(grad * v, axis=1, keepdims=True) for v in (y0, y1))
        mean = g0 * dg0 + g1 * dg1
        d0, d1 = ((g * (dg - mean)).astype(BF16).astype(F32) for g, dg in ((g0, dg0), (g1, dg1)))
        d_land[z, y, x, c] = jnp.concatenate([as_row(d0), as_row(d1), jnp.zeros((1, 2 * n_tok), F32)], axis=1)
        out_ref[...] = (g0 * y0 + g1 * y1).astype(BF16)
        saves[0].start()
        d_plans.append(gather_rows(next(links), d_land, range(4)))
        advance(d_plans)
        expert = iota((n_tok, n_exp), 1).astype(F32)
        spread = jnp.where(expert == i0, d0, jnp.where(expert == i1, d1, 0.0)).astype(BF16)
        memo.update(chosen=chosen, through=dot(spread, wg[...], 1, 1))

    def finish():
        dx0, dx1 = rows_of(2, memo['chosen'])
        gx_ref[...] = (dx0 + dx1 + memo['through']).astype(BF16)
        saves[1].start()

    n_dev = nz * ny * nx * nc

    def gate_grad():
        flatten(d_land, d_all)
        expert = iota((n_exp, 256), 0).astype(F32).astype(BF16)
        codes = [plain_id(pair_rows(token_lanes(m_all, k, 0, n_dev // 4))).astype(BF16) for k in range(2)]
        grads = [pair_rows(token_lanes(d_all, k, 0, n_dev // 4)).astype(BF16) for k in range(2)]
        none = jnp.zeros((), BF16)
        total = jnp.zeros((n_exp, x_all.shape[-1]), F32)
        zs = nz // 4 or 1
        for z0 in range(0, nz, zs):
            spread = []
            for p in range(z0 * ny, (z0 + zs) * ny):
                q = slice(p, p + 1)
                spread.append(jnp.where(expert == codes[0][q], grads[0][q], jnp.where(expert == codes[1][q], grads[1][q], none)))
            total += dot(jnp.concatenate(spread, axis=1), x_all[z0:z0 + zs].reshape(zs * ny * 256, x_all.shape[-1]), 1, 0)
        gate_ref[...] = total.T
        saves[2].start()

    d_plans = []
    moves = {'t': tok_plans, 'g': grad_plans, 'm': row_plan, 'y': ys, 'x': dxs, 'd': d_plans}
    works = {'f': [functools.partial(forward, i) for i in range(steps)], 'b': [functools.partial(backward, i) for i in range(steps)],
             'B': [functools.partial(backward_rows, i) for i in range(steps)], 'w': [functools.partial(weight_grad, k) for k in range(8)],
             'h': [read_rows], 'c': [combine], 'k': [gate_grad], 'e': [finish]}
    for turn in SCHEDULE:
        if turn in moves:
            advance(moves[turn])
        elif works[turn]:
            works[turn].pop(0)()
    for link in all_links:
        link.finish(pad, pad_row)
    for cp in saves:
        cp.wait()


def block_call(dims, tokens, grad_out, ids, w_gate, w1, w2):
    nz, ny, nx, nc = dims
    d_model, d_hidden = w1.shape
    n_tok = tokens.shape[0]
    n_dev = nz * ny * nx * nc
    n_row = n_dev * CAP
    tile = (CAP, 128)
    hbm = pl.BlockSpec(memory_space=pltpu.HBM)
    out = jax.ShapeDtypeStruct
    work = [(4, 4, nz), (4, 2, 4, nz), (2, 2, 2, nz), (4, 4, nz), (2, 4, nz // 2), (4, 4, nz), (nz, 3), (nz, 3), (nz, 4)]
    n_group = 4 * 10 + 4 + 4 * 11 + 4
    sems = [pltpu.SemaphoreType.DMA((10,)), pltpu.SemaphoreType.DMA((n_group,))]
    results = [(tokens.shape, BF16), (tokens.shape, BF16), ((d_model, n_dev), F32), ((d_model, d_hidden), F32), ((d_hidden, d_model), F32)]
    row = (1, 128)
    kept = [(tokens.shape, BF16), (tokens.shape, BF16), (ids.shape, jnp.int32), (w_gate.shape, BF16), (w1.shape, BF16), (w2.shape, BF16), (row, F32), (dims + row, F32),
            (dims + tokens.shape, BF16), (dims + tokens.shape, BF16), ((n_row, d_model), BF16), ((n_row, d_model), BF16), ((n_row, d_hidden), BF16), ((n_row, d_hidden), BF16), ((n_row, d_hidden), F32), ((n_dev, 128), F32), (tile, F32),
            (dims + row, F32), ((n_dev, 128), F32), ((1024,) + tile, BF16), ((n_dev,) + row, F32)]
    return pl.pallas_call(
        functools.partial(block_kernel, dims, (6, len(results), len(results), len(kept), 4, 4 * len(work), 3, len(sems))),
        out_shape=[out(*r) for r in results],
        in_specs=[hbm] * 6,
        out_specs=[hbm] * len(results),
        scratch_shapes=[pltpu.VMEM(*r) for r in results + kept] + [pltpu.VMEM((nc, nx, ny, nz) + tile, BF16)] * 4 + [pltpu.VMEM(w + tile, BF16) for w in work] * 4
        + [pltpu.SemaphoreType.DMA((k,)) for k in (8, 1, len(results))] + sems,
        compiler_params=pltpu.CompilerParams(collective_id=0, has_side_effects=True, vmem_limit_bytes=VMEM_LIMIT),
        name='block',
    )(tokens, grad_out, ids, w_gate, w1, w2)


VMEM_LIMIT = 67043328
SCHEDULE = 'mtgtmtttmgtttgttgmth' + 'ffggyfggyfy' + 'gygy' + 'bybybyBBxbyxBBxy' + 'wwxxwxwwxyc' + 'xwwdxdxwddkxe'


def pass_kernel(n, *refs):
    refs = iter(refs)
    given, passed, held, (load_sem, save_sem) = [list(itertools.islice(refs, k)) for k in (n, n, n, 2)]
    loads = [pltpu.make_async_copy(given[k], held[k], load_sem.at[k]) for k in range(n)]
    saves = [pltpu.make_async_copy(held[k], passed[k], save_sem.at[k]) for k in range(n)]
    for cp in loads:
        cp.start()
    for load, save in zip(loads, saves):
        load.wait()
        save.start()
    for cp in saves:
        cp.wait()


def pass_on(*arrays):
    n = len(arrays)
    return pl.pallas_call(
        functools.partial(pass_kernel, n),
        out_shape=[jax.ShapeDtypeStruct(v.shape, v.dtype) for v in arrays],
        in_specs=[pl.BlockSpec(memory_space=pltpu.HBM)] * n,
        out_specs=[pl.BlockSpec(memory_space=pltpu.HBM)] * n,
        scratch_shapes=[pltpu.VMEM(v.shape, v.dtype) for v in arrays] + [pltpu.SemaphoreType.DMA((n,))] * 2,
        compiler_params=pltpu.CompilerParams(vmem_limit_bytes=VMEM_LIMIT),
        name='pass_on',
    )(*arrays)


def local_block(dims, tokens, grad_out, expert_ids, w_gate, w_in, w_out):
    y_out, grad_x, grad_w_gate, g1, g2 = pass_on(*block_call(dims, tokens, grad_out, expert_ids.T, w_gate, w_in[0], w_out[0]))
    return y_out, grad_x, g1[None], g2[None], grad_w_gate


def solution(mesh):
    dims = (8, 4, 4, 2)
    return jax.shard_map(functools.partial(local_block, dims), mesh=mesh, in_specs=(P('ep'), P('ep'), P('ep'), P(), P('ep'), P('ep')), out_specs=(P('ep'), P('ep'), P('ep'), P('ep'), P()), check_vma=False)
```
